32 devices in a mesh: dp: 4 (over x, core), fsdp: 8 (over z, y).
Axes of the slice: x: 2, y: 2, z: 4, core: 2. Of those that a mesh axis runs over, the one named last changes fastest.
Arguments:
- tokens: bfloat16 [25088, 1024], P(('dp', 'fsdp')), may hold values from -6 to 6
- scale_codes: int32 [128], P(('dp', 'fsdp')), may hold values from 0 to 15
- w_qkv: float32 [1024, 3072], P('fsdp'), may hold values from -0.1875 to 0.1875
- b_q: float32 [1024], P('fsdp'), may hold values from -3 to 3
- b_v: float32 [1024], P('fsdp'), may hold values from -3 to 3
- w_out: float32 [1024, 1024], P('fsdp'), may hold values from -1.5 to 1.5
- b_out: float32 [1024], P('fsdp'), may hold values from -3 to 3
- gain_one: float32 [1024], P('fsdp'), may hold values from 0.5 to 1.5
- shift_one: float32 [1024], P('fsdp'), may hold values from -2 to 2
- w_fc1: float32 [1024, 4096], P('fsdp'), may hold values from -0.1875 to 0.1875
- b_fc1: float32 [4096], P('fsdp'), may hold values from -3 to 3
- w_fc2: float32 [4096, 1024], P('fsdp'), may hold values from -0.09375 to 0.09375
- b_fc2: float32 [1024], P('fsdp'), may hold values from -3 to 3
- gain_two: float32 [1024], P('fsdp'), may hold values from 0.5 to 1.5
- shift_two: float32 [1024], P('fsdp'), may hold values from -2 to 2
- cotangent: bfloat16 [25088, 1024], P(('dp', 'fsdp')), may hold values from -6 to 6
Outputs:
- block_out: bfloat16 [25088, 1024], P(('dp', 'fsdp'))
- grad_tokens: float32 [25088, 1024], P(('dp', 'fsdp'))
- grad_w_qkv: float32 [1024, 3072], P('fsdp')
- grad_b_q: float32 [1024], P('fsdp')
- grad_b_v: float32 [1024], P('fsdp')
- grad_w_out: float32 [1024, 1024], P('fsdp')
- grad_b_out: float32 [1024], P('fsdp')
- grad_gain_one: float32 [1024], P('fsdp')
- grad_shift_one: float32 [1024], P('fsdp')
- grad_w_fc1: float32 [1024, 4096], P('fsdp')
- grad_b_fc1: float32 [4096], P('fsdp')
- grad_w_fc2: float32 [4096, 1024], P('fsdp')
- grad_b_fc2: float32 [1024], P('fsdp')
- grad_gain_two: float32 [1024], P('fsdp')
- grad_shift_two: float32 [1024], P('fsdp')
The draws below stay inside these ranges and needn't reach their ends.
All inputs are finite; a program needn't handle non-finite values.
Results may differ from the reference program's by a relative error of at most 0.015.
Values may be sent and summed in bfloat16 or wider, within the bound.
No kernel may reach another device: no remote copies, remote signals or barrier semaphores. Data moves between devices by JAX's collectives and lax.ppermute only.
A program may use at most 256 MiB of HBM per device.

```python
import math
import jax
import jax.numpy as jnp
from jax import lax

D = 1024
HEADS = 16
HEAD = 64
FF = 4096
GRID = 14
NSCALE = 16
IMG_DEV = 4
PATCHES = 196
IMAGES = 128
TOKENS = 25088
DEVICES = 32


def plant(values, rng, least, largest):
    spot = [jax.random.randint(jax.random.fold_in(rng, axis), (), 0, length) for axis, length in enumerate(values.shape)]
    widest = values.shape.index(max(values.shape))
    beside = spot[:widest] + [(spot[widest] + 1) % values.shape[widest]] + spot[widest + 1:]
    return values.at[tuple(spot)].set(least).at[tuple(beside)].set(largest)


def raised(values, stream_key, source, target, blocks, factor):
    owner, partner = [(jnp.arange(values.shape[dim]) // (values.shape[dim] // blocks)).reshape([-1 if axis == dim else 1 for axis in range(values.ndim)]) for dim in (source, target)]
    chosen = jax.random.permutation(stream_key, blocks)[partner]
    strong = (owner == chosen) | (owner == (partner + blocks // 2) % blocks)
    return jnp.where(strong, factor * values, values)


def block_scale(stream_key, extent, shards, smallest, top_value):
    factor_of, own = 1.0, jax.random.fold_in(stream_key, 6)
    for position, shards_of in shards:
        draws = jnp.exp(jax.random.uniform(jax.random.fold_in(own, position), (shards_of,), jnp.float32, smallest / len(shards), top_value / len(shards)))
        factor_of = factor_of * jnp.repeat(draws, extent[position] // shards_of).reshape([-1 if axis == position else 1 for axis in range(len(extent))])
    return factor_of


def gaussian(key, extent, scale, reach, shards=(), kind=jnp.bfloat16):
    level = block_scale(key, extent, shards, -0.22, 0.18) if shards else 1.0
    drawn = jax.random.normal(key, extent, jnp.float32) * scale * level
    return jnp.minimum(jnp.maximum(drawn, -reach), reach).astype(kind)


def noise_with(key, dims, scale, most, pieces, heavy, kind=jnp.bfloat16):
    array = scale * jax.random.normal(key, dims, jnp.float32)
    if pieces:
        array = array * block_scale(key, dims, pieces, -0.22, 0.18)
    return jnp.clip(raised(array, jax.random.fold_in(key, 3), *heavy), -most, most).astype(kind)


def setup_inputs(seed: int = 0) -> dict:
    splits = jax.random.split(jax.random.key(seed), 17)
    return {
        "tokens": gaussian(splits[0], (TOKENS, D), 1.0, 6.0, ((0, 32),)),
        "scale_codes": plant(jax.random.randint(splits[1], (IMAGES,), 0, NSCALE), jax.random.fold_in(splits[1], 1), 0, NSCALE - 1).astype(jnp.int32),
        "w_qkv": gaussian(splits[2], (D, 3 * D), D ** -0.5, 0.1875, ((0, 8),), jnp.float32),
        "b_q": gaussian(splits[3], (D,), 0.5, 3.0, ((0, 8),), jnp.float32),
        "b_v": gaussian(splits[4], (D,), 0.5, 3.0, ((0, 8),), jnp.float32),
        "w_out": gaussian(splits[5], (D, D), (max(D // 64, 1)) ** -0.5, 1.5, ((0, 8),), jnp.float32),
        "b_out": gaussian(splits[6], (D,), 0.5, 3.0, ((0, 8),), jnp.float32),
        "gain_one": jnp.clip(1.0 + 0.1 * jax.random.normal(splits[7], (D,), jnp.float32), 0.5, 1.5),
        "shift_one": gaussian(splits[8], (D,), 0.3, 2.0, ((0, 8),), jnp.float32),
        "w_fc1": gaussian(splits[9], (D, FF), D ** -0.5, 0.1875, ((0, 8),), jnp.float32),
        "b_fc1": gaussian(splits[10], (FF,), 0.5, 3.0, ((0, 8),), jnp.float32),
        "w_fc2": gaussian(splits[11], (FF, D), FF ** -0.5, 0.09375, ((0, 8),), jnp.float32),
        "b_fc2": gaussian(splits[12], (D,), 0.5, 3.0, ((0, 8),), jnp.float32),
        "gain_two": jnp.clip(1.0 + 0.1 * jax.random.normal(splits[13], (D,), jnp.float32), 0.5, 1.5),
        "shift_two": gaussian(splits[14], (D,), 0.3, 2.0, ((0, 8),), jnp.float32),
        "cotangent": noise_with(splits[15], (TOKENS, D), 1.0, 6.0, ((0, 32),), (0, 1, 32, 2.75)),
    }


norm_eps = 1e-06

@jax.custom_vjp
def low(v):
    return lax.optimization_barrier(v.astype(jnp.bfloat16)).astype(jnp.float32)

@jax.custom_vjp
def low_back(v):
    return v

def low_keep(v):
    return (low(v), None)

def low_pass(kept, grad):
    return (grad,)

def back_keep(v):
    return (v, None)

def back_low(kept, grad):
    return (low(grad),)
low.defvjp(low_keep, low_pass)
low_back.defvjp(back_keep, back_low)

def positions(codes, grid_side, width):
    ratio = 0.3 * jnp.exp(codes.astype(jnp.float32) * (math.log(10.0 / 0.3) / (NSCALE - 1)))
    quarter = width // 4
    omega = jnp.exp(jnp.arange(quarter).astype(jnp.float32) * (-math.log(10000.0) / quarter))
    cells = jnp.arange(grid_side * grid_side, dtype=jnp.int32)
    row_place = (cells // grid_side).astype(jnp.float32)
    col_place = (cells % grid_side).astype(jnp.float32)
    row_angle = ratio[:, None, None] * row_place[None, :, None] * omega[None, None, :]
    col_angle = ratio[:, None, None] * col_place[None, :, None] * omega[None, None, :]
    return jnp.concatenate([jnp.sin(row_angle), jnp.cos(row_angle), jnp.sin(col_angle), jnp.cos(col_angle)], axis=-1)

def norm_affine(hidden, gain, shift):
    center = lax.optimization_barrier(jnp.mean(hidden, axis=-1, keepdims=True))
    offset = hidden - center
    spread = lax.optimization_barrier(jnp.mean(offset * offset, axis=-1, keepdims=True))
    return offset * lax.rsqrt(spread + norm_eps) * gain + shift

def highest(left, right):
    return jnp.dot(left, right, precision=lax.Precision.HIGHEST)

def block_rows(x_group, params):
    w_qkv, b_q, b_v, w_out, b_out, gain_one, shift_one, w_fc1, b_fc1, w_fc2, b_fc2, gain_two, shift_two = params
    n_img = x_group.shape[0]
    rows = x_group.reshape(n_img * PATCHES, D)
    normed_one = low(norm_affine(rows, gain_one, shift_one))
    qkv_bias = jnp.concatenate([b_q, jnp.zeros_like(b_q), b_v])
    projected = low_back(low(highest(normed_one, w_qkv) + qkv_bias)).reshape(n_img, PATCHES, 3, HEADS, HEAD)
    queries = projected[:, :, 0]
    keys_all = projected[:, :, 1]
    values_all = projected[:, :, 2]
    factor = 1.0 / math.sqrt(HEAD)
    scores = low_back(jnp.einsum('iqhd,ikhd->ihqk', queries, keys_all, precision=lax.Precision.HIGHEST) * factor)
    probs = jax.nn.softmax(scores, axis=-1)
    mixed = jnp.einsum('ihqk,ikhd->iqhd', low(probs), values_all, precision=lax.Precision.HIGHEST)
    mixed = low_back(low(mixed.reshape(n_img * PATCHES, D)))
    after_attn = rows + low_back(highest(mixed, w_out) + b_out)
    normed_two = low(norm_affine(after_attn, gain_two, shift_two))
    hidden_pre = low_back(highest(normed_two, w_fc1) + b_fc1)
    hidden_act = low(jax.nn.gelu(hidden_pre, approximate=False))
    result = after_attn + low_back(highest(hidden_act, w_fc2) + b_fc2)
    return result.reshape(x_group.shape)

def reference(tokens, scale_codes, w_qkv, b_q, b_v, w_out, b_out, gain_one, shift_one, w_fc1, b_fc1, w_fc2, b_fc2, gain_two, shift_two, cotangent):
    place = positions(scale_codes, GRID, D).reshape(TOKENS, D)

    def whole(x_rows, *weights):
        params = tuple((low(weight) for weight in weights))
        x_zero = (x_rows + place).reshape(DEVICES, IMG_DEV, PATCHES, D)
        apply_group = jax.checkpoint(lambda group: block_rows(group, params))
        return lax.map(apply_group, x_zero).reshape(TOKENS, D)
    block_out, pull = jax.vjp(whole, tokens.astype(jnp.float32), w_qkv, b_q, b_v, w_out, b_out, gain_one, shift_one, w_fc1, b_fc1, w_fc2, b_fc2, gain_two, shift_two)
    grads = pull(cotangent.astype(jnp.float32))
    return (block_out.astype(jnp.bfloat16), grads[0], grads[1], grads[2], grads[3], grads[4], grads[5], grads[6], grads[7], grads[8], grads[9], grads[10], grads[11], grads[12], grads[13])
```

```python
import math

import jax
import jax.numpy as jnp
from jax import lax
from jax.experimental import pallas as pl
from jax.experimental.pallas import tpu as pltpu
from jax.sharding import PartitionSpec as P

HEADS = 16
GRID = 14
NSCALE = 16
norm_eps = 1e-06
half = jnp.bfloat16
full = jnp.float32


def swap(value, axis, size, bit):
    return lax.ppermute(value, axis, [(i, i ^ (1 << bit)) for i in range(size)])


def core_swap(value):
    return swap(value, "dp", 4, 0)


def x_swap(value):
    return swap(value, "dp", 4, 1)


def masks(n):
    found = [0]
    for bit in reversed(range(n.bit_length() - 1)):
        found = found + [m | (1 << bit) for m in found]
    return found


def gather_shards(piece, n, last=0):
    held = piece[None]
    for bit in reversed(range(last, n.bit_length() - 1)):
        held = jnp.concatenate([held, swap(held, "fsdp", n, bit)])
    return held


def gather_quarters(piece, n):
    own = gather_shards(piece, n)
    beside = core_swap(own)
    across = x_swap(own)
    return own, beside, across, core_swap(across)


def add_half(a, b):
    return (a.astype(full) + b.astype(full)).astype(half)


def scatter_shards(low, high, n):
    for bit in range(n.bit_length() - 1):
        got = swap(high, "fsdp", n, bit)
        size = low.shape[0] // 2
        if size:
            low, high = add_half(low[:size], got[:size]), add_half(low[size:], got[size:])
        else:
            low = add_half(low, got)
    return low[0]


def reduce_quarters(parts, n):
    middle = n // 2
    beside = core_swap(parts[1])
    across = add_half(parts[2], core_swap(parts[3]))
    got = x_swap(across)
    total = [
        (parts[0][s].astype(full) + beside[s].astype(full) + got[s].astype(full)).astype(half)
        for s in (slice(0, middle), slice(middle, None))
    ]
    return scatter_shards(total[0], total[1], n)


def spread_quarters(piece, q):
    pair = [piece, core_swap(piece)]
    there = x_swap(jnp.stack(pair))
    pieces = pair + [there[0], there[1]]
    odd = (q & 1) == 1
    upper = q >= 2
    once = [jnp.where(odd, pieces[i ^ 1], pieces[i]) for i in range(4)]
    return [jnp.where(upper, once[i ^ 2], once[i]) for i in range(4)]


def moved(sources, shape, n, plan, order):
    def kernel(order_ref, *refs):
        ins, outs, sem = refs[: len(sources)], refs[len(sources) : -1], refs[-1]

        def step(r, carry):
            for src, dst in plan(r, order_ref, ins, outs):
                pltpu.make_async_copy(src, dst, sem.at[0]).start()
            return carry

        lax.fori_loop(0, n, step, 0)
        for out in outs:
            pltpu.make_async_copy(out, out, sem.at[0]).wait()

    anywhere = pl.BlockSpec(memory_space=pl.ANY)
    shapes = [jax.ShapeDtypeStruct(s, half) for s in shape]
    return pl.pallas_call(
        kernel,
        out_shape=shapes,
        grid_spec=pltpu.PrefetchScalarGridSpec(
            num_scalar_prefetch=1,
            grid=(1,),
            in_specs=[anywhere] * len(sources),
            out_specs=[anywhere] * len(shapes),
            scratch_shapes=[pltpu.SemaphoreType.DMA((1,))],
        ),
        name="moved",
    )(order, *sources)


def table(codes, width):
    ratio = 0.3 * jnp.exp(codes.astype(full) * (math.log(10.0 / 0.3) / (NSCALE - 1)))
    quarter = width // 4
    omega = jnp.exp(jnp.arange(quarter).astype(full) * (-math.log(10000.0) / quarter))
    steps = jnp.arange(GRID, dtype=jnp.int32).astype(full)
    angle = ratio[:, None, None] * steps[None, :, None] * omega[None, None, :]
    return jnp.concatenate([jnp.sin(angle), jnp.cos(angle)], axis=-1)


def norm_affine(hidden, gain, shift):
    center = jnp.mean(hidden, axis=-1, keepdims=True)
    offset = hidden - center
    spread = jnp.mean(offset * offset, axis=-1, keepdims=True)
    return offset * lax.rsqrt(spread + norm_eps) * gain + shift


def matmul(left, right):
    return jnp.dot(left, right, preferred_element_type=full)


def inner_rows(left, right):
    return lax.dot_general(left, right, (((0,), (0,)), ((), ())), preferred_element_type=full)


def times_transposed(left, right):
    return lax.dot_general(left, right, (((1,), (1,)), ((), ())), preferred_element_type=full)


def column_total(values):
    return jnp.sum(values.astype(full), axis=0)


def local(
    tokens,
    scale_codes,
    w_qkv,
    b_q,
    b_v,
    w_out,
    b_out,
    gain_one,
    shift_one,
    w_fc1,
    b_fc1,
    w_fc2,
    b_fc2,
    gain_two,
    shift_two,
    cotangent,
):
    n = lax.axis_size("fsdp")
    q = lax.axis_index("dp")
    f = lax.axis_index("fsdp")
    row_count, width = tokens.shape
    rows = width // n
    ff = b_fc1.shape[0] * n
    ffq = ff // n // 4
    quarter = width // 4
    n_img = scale_codes.shape[0]
    patches = row_count // n_img
    head_size = width // HEADS
    factor = 1.0 / math.sqrt(head_size)
    shard_order = jnp.asarray(masks(n), jnp.int32) ^ f
    group_order = jnp.arange(4, dtype=jnp.int32) ^ q
    order = jnp.concatenate([shard_order, group_order])

    def pick(value, axis):
        return lax.dynamic_index_in_dim(value, q, axis, keepdims=False)

    small = jnp.concatenate(
        [b_q, b_v, b_out, gain_one, shift_one, b_fc2, gain_two, shift_two, b_fc1]
    ).astype(half)
    pad = -small.shape[0] % 2048
    small_held = gather_shards(jnp.pad(small, (0, pad)).reshape(-1, 128), n).reshape(n, -1)
    inverse = jnp.zeros((n,), jnp.int32).at[shard_order].set(jnp.arange(n, dtype=jnp.int32))
    small_all = jnp.take(small_held, inverse, axis=0).astype(full)
    vectors = [small_all[:, i * rows : (i + 1) * rows].reshape(width) for i in range(8)]
    full_bq, full_bv, full_bout, gain_one_f, shift_one_f, full_bfc2, gain_two_f, shift_two_f = vectors
    bias_units = small_all[:, 8 * rows : 8 * rows + 4 * ffq].reshape(n, 4, ffq)
    bias_fc1 = jnp.take(bias_units, group_order, axis=1).transpose(1, 0, 2).reshape(ff)

    qkv_own = pick(w_qkv.reshape(rows, 3, 4, quarter), 2).reshape(rows, 3 * quarter).astype(half)
    qkv_parts = gather_quarters(qkv_own, n)
    out_own = pick(w_out.reshape(rows, 4, quarter), 1).astype(half)
    fc1_own = pick(w_fc1.reshape(rows, n, 4, ffq), 2).reshape(rows, n * ffq).astype(half)
    up_parts = gather_quarters(jnp.concatenate([fc1_own, out_own], axis=1), n)
    fc2_own = pick(w_fc2.reshape(4, ffq, width), 0).astype(half)
    column = gather_shards(fc2_own, n, 1)
    both = jnp.stack([column, x_swap(column)])
    far = swap(both, "fsdp", n, 0)
    down_own = jnp.concatenate([both[0], far[0]])
    down_across = jnp.concatenate([both[1], far[1]])
    down_parts = (down_own, core_swap(down_own), down_across, core_swap(down_across))

    hidden = n * ffq

    def plan_qkv(r, order_ref, ins, outs):
        s = order_ref[r]
        for j in range(4):
            for t in range(3):
                yield (
                    ins[j].at[r, :, pl.ds(t * quarter, quarter)],
                    outs[0].at[pl.ds(s * rows, rows), pl.ds(t * width + order_ref[n + j] * quarter, quarter)],
                )

    def plan_up(r, order_ref, ins, outs):
        s = order_ref[r]
        for j in range(4):
            yield ins[j].at[r, :, pl.ds(0, hidden)], outs[0].at[pl.ds(s * rows, rows), pl.ds(j * hidden, hidden)]
            yield (
                ins[j].at[r, :, pl.ds(hidden, quarter)],
                outs[1].at[pl.ds(s * rows, rows), pl.ds(order_ref[n + j] * quarter, quarter)],
            )

    def plan_down(r, order_ref, ins, outs):
        s = order_ref[r]
        for j in range(4):
            yield ins[j].at[r], outs[0].at[pl.ds(j * hidden + s * ffq, ffq)]

    (full_qkv,) = moved(qkv_parts, [(width, 3 * width)], n, plan_qkv, order)
    full_fc1, full_out = moved(up_parts, [(width, ff), (width, width)], n, plan_up, order)
    (full_fc2,) = moved(down_parts, [(ff, width)], n, plan_down, order)

    places = table(scale_codes, width)
    row_place = jnp.broadcast_to(places[:, :, None], (n_img, GRID, GRID, width // 2))
    col_place = jnp.broadcast_to(places[:, None], (n_img, GRID, GRID, width // 2))
    place = jnp.concatenate([row_place, col_place], axis=-1).reshape(row_count, width)
    x_zero = tokens.astype(full) + place
    normed_one = norm_affine(x_zero, gain_one_f, shift_one_f).astype(half)
    qkv_bias = jnp.concatenate([full_bq, jnp.zeros_like(full_bq), full_bv])
    projected = (
        (matmul(normed_one, full_qkv) + qkv_bias)
        .astype(half)
        .reshape(n_img, patches, 3, HEADS, head_size)
    )
    queries = projected[:, :, 0]
    keys_all = projected[:, :, 1]
    values_all = projected[:, :, 2]
    scores = (
        jnp.einsum("iqhd,ikhd->ihqk", queries, keys_all, preferred_element_type=full)
        * factor
    )
    top_score = jnp.max(scores, axis=-1, keepdims=True)
    raised = jnp.exp(scores - top_score)
    totals = jnp.sum(raised, axis=-1, keepdims=True)
    probs = raised / totals
    log_total = top_score + jnp.log(totals)
    mixed = jnp.einsum(
        "ihqk,ikhd->iqhd", probs.astype(half), values_all, preferred_element_type=full
    )
    mixed = mixed.reshape(row_count, width).astype(half)
    after_attn = x_zero + (matmul(mixed, full_out) + full_bout)
    normed_two = norm_affine(after_attn, gain_two_f, shift_two_f).astype(half)
    hidden_pre = matmul(normed_two, full_fc1) + bias_fc1
    hidden_act = jax.nn.gelu(hidden_pre, approximate=False).astype(half)
    block_out = (after_attn + (matmul(hidden_act, full_fc2) + full_bfc2)).astype(half)

    grad_w_fc2 = inner_rows(hidden_act, cotangent).astype(half)
    grad_b_fc2 = column_total(cotangent)
    grad_act = times_transposed(cotangent, full_fc2)
    unused_act, gelu_pull = jax.vjp(lambda pre: jax.nn.gelu(pre, approximate=False), hidden_pre)
    grad_pre = gelu_pull(grad_act)[0].astype(half)
    grad_w_fc1 = inner_rows(normed_two, grad_pre).astype(half)
    grad_b_fc1 = column_total(grad_pre)

    def plan_down_back(r, order_ref, ins, outs):
        s = order_ref[r]
        for j in range(4):
            yield ins[0].at[pl.ds(j * hidden + s * ffq, ffq)], outs[j].at[r]

    def plan_up_back(r, order_ref, ins, outs):
        s = order_ref[r]
        for j in range(4):
            yield ins[0].at[pl.ds(s * rows, rows), pl.ds(j * hidden, hidden)], outs[j].at[r]

    down_grads = moved([grad_w_fc2], [(n, ffq, width)] * 4, n, plan_down_back, order)
    up_grads = moved([grad_w_fc1], [(n, rows, hidden)] * 4, n, plan_up_back, order)

    middle = n // 2
    pair_low, pair_high = [], []
    for a, b in ((0, 1), (2, 3)):
        got = core_swap(down_grads[b])
        pair_low.append(add_half(down_grads[a][:middle], got[:middle]))
        pair_high.append(add_half(down_grads[a][middle:], got[middle:]))
    far = swap(jnp.stack(pair_high), "fsdp", n, 0)
    across = x_swap(add_half(pair_low[1], far[1]))
    down_low = (pair_low[0].astype(full) + far[0].astype(full) + across.astype(full)).astype(half)
    for bit in range(1, n.bit_length() - 1):
        size = down_low.shape[0] // 2
        got = swap(down_low[size:], "fsdp", n, bit)
        down_low = add_half(down_low[:size], got)
    down_pieces = spread_quarters(down_low[0], q)
    out_fc2 = jnp.concatenate(down_pieces).astype(full)
    up_pieces = spread_quarters(reduce_quarters(up_grads, n), q)
    out_fc1 = (
        jnp.stack([p.reshape(rows, n, ffq) for p in up_pieces], axis=2).reshape(rows, ff).astype(full)
    )

    grad_two_in = times_transposed(grad_pre, full_fc1)
    unused_two, norm_two_pull = jax.vjp(norm_affine, after_attn, gain_two_f, shift_two_f)
    part_two, grad_gain_two, grad_shift_two = norm_two_pull(grad_two_in)
    grad_after = cotangent.astype(full) + part_two
    branch_grad = grad_after.astype(half)
    grad_w_out = inner_rows(mixed, branch_grad).astype(half)
    grad_b_out = column_total(branch_grad)
    grad_mixed = (
        times_transposed(branch_grad, full_out)
        .astype(half)
        .reshape(n_img, patches, HEADS, head_size)
    )
    again_scores = (
        jnp.einsum("iqhd,ikhd->ihqk", queries, keys_all, preferred_element_type=full)
        * factor
    )
    again_probs = jnp.exp(again_scores - log_total)
    grad_values = jnp.einsum(
        "ihqk,iqhd->ikhd", again_probs.astype(half), grad_mixed, preferred_element_type=full
    )
    grad_probs = jnp.einsum(
        "iqhd,ikhd->ihqk", grad_mixed, values_all, preferred_element_type=full
    )
    weighted = jnp.sum(again_probs * grad_probs, axis=-1, keepdims=True)
    grad_scores = (again_probs * (grad_probs - weighted)).astype(half)
    grad_queries = (
        jnp.einsum("ihqk,ikhd->iqhd", grad_scores, keys_all, preferred_element_type=full)
        * factor
    )
    grad_keys = (
        jnp.einsum("ihqk,iqhd->ikhd", grad_scores, queries, preferred_element_type=full)
        * factor
    )
    grad_proj = (
        jnp.stack([grad_queries, grad_keys, grad_values], axis=2)
        .reshape(row_count, 3 * width)
        .astype(half)
    )
    grad_w_qkv = inner_rows(normed_one, grad_proj).astype(half)
    grad_b_q = column_total(grad_proj[:, :width])
    grad_b_v = column_total(grad_proj[:, 2 * width :])

    def plan_attn_back(r, order_ref, ins, outs):
        s = order_ref[r]
        for j in range(4):
            for t in range(3):
                yield (
                    ins[0].at[pl.ds(s * rows, rows), pl.ds(t * width + order_ref[n + j] * quarter, quarter)],
                    outs[j].at[r, :, pl.ds(t * quarter, quarter)],
                )
            yield (
                ins[1].at[pl.ds(s * rows, rows), pl.ds(order_ref[n + j] * quarter, quarter)],
                outs[j].at[r, :, pl.ds(3 * quarter, quarter)],
            )

    attn_grads = moved([grad_w_qkv, grad_w_out], [(n, rows, width)] * 4, n, plan_attn_back, order)
    attn_pieces = spread_quarters(reduce_quarters(attn_grads, n), q)
    out_qkv = (
        jnp.stack([p[:, : 3 * quarter].reshape(rows, 3, quarter) for p in attn_pieces], axis=2)
        .reshape(rows, 3 * width)
        .astype(full)
    )
    out_out = jnp.stack([p[:, 3 * quarter :] for p in attn_pieces], axis=1).reshape(rows, width).astype(full)

    grad_one_in = times_transposed(grad_proj, full_qkv)
    unused_one, norm_one_pull = jax.vjp(norm_affine, x_zero, gain_one_f, shift_one_f)
    part_one, grad_gain_one, grad_shift_one = norm_one_pull(grad_one_in)
    grad_tokens = grad_after + part_one

    sums = [
        grad_b_q, grad_b_v, grad_b_out, grad_gain_one, grad_shift_one, grad_b_fc2, grad_gain_two, grad_shift_two
    ]
    back_group = jnp.take(grad_b_fc1.reshape(4, n, ffq), group_order, axis=0).transpose(1, 0, 2)
    packed = jnp.concatenate([s.reshape(n, rows) for s in sums] + [back_group.reshape(n, 4 * ffq)], axis=1)
    packed = jnp.take(packed, shard_order, axis=0)
    pad = -packed.shape[1] % 1024
    packed = jnp.pad(packed, ((0, 0), (0, pad))).reshape(n, -1, 128)
    packed = packed + core_swap(packed)
    packed = packed + x_swap(packed)
    for bit in range(n.bit_length() - 1):
        size = packed.shape[0] // 2
        packed = packed[:size] + swap(packed[size:], "fsdp", n, bit)
    vector = packed.reshape(-1)
    small_out = [vector[i * rows : (i + 1) * rows] for i in range(8)]
    out_bfc1 = vector[8 * rows : 8 * rows + 4 * ffq]
    o_bq, o_bv, o_bout, o_gone, o_sone, o_bfc2, o_gtwo, o_stwo = small_out
    return (
        block_out,
        grad_tokens,
        out_qkv,
        o_bq,
        o_bv,
        out_out,
        o_bout,
        o_gone,
        o_sone,
        out_fc1,
        out_bfc1,
        out_fc2,
        o_bfc2,
        o_gtwo,
        o_stwo,
    )


def solution(mesh):
    rows_split = P(("dp", "fsdp"), None)
    matrix = P("fsdp", None)
    vector = P("fsdp")
    return jax.shard_map(
        local,
        mesh=mesh,
        in_specs=(
            rows_split, P(("dp", "fsdp")), matrix, vector, vector, matrix, vector, vector, vector,
            matrix, vector, matrix, vector, vector, vector, rows_split,
        ),
        out_specs=(
            rows_split, rows_split, matrix, vector, vector, matrix, vector, vector, vector,
            matrix, vector, matrix, vector, vector, vector,
        ),
        check_vma=False,
    )
```

```python
import math

import jax
import jax.numpy as jnp
from jax import lax
from jax.experimental import pallas as pl
from jax.experimental.pallas import tpu as pltpu
from jax.sharding import PartitionSpec as P

HEADS = 16
GRID = 14
NSCALE = 16
norm_eps = 1e-06
half = jnp.bfloat16
full = jnp.float32


def swap(value, axis, size, bit):
    return lax.ppermute(value, axis, [(i, i ^ (1 << bit)) for i in range(size)])


def core_swap(value):
    return swap(value, "dp", 4, 0)


def x_swap(value):
    return swap(value, "dp", 4, 1)


def masks(n):
    found = [0]
    for bit in reversed(range(n.bit_length() - 1)):
        found = found + [m | (1 << bit) for m in found]
    return found


def gather_shards(piece, n, last=0):
    held = piece[None]
    for bit in reversed(range(last, n.bit_length() - 1)):
        held = jnp.concatenate([held, swap(held, "fsdp", n, bit)])
    return held


def gather_quarters(piece, n):
    own = gather_shards(piece, n)
    beside = core_swap(own)
    across = x_swap(own)
    return own, beside, across, core_swap(across)


def add_half(a, b):
    return (a.astype(full) + b.astype(full)).astype(half)


def scatter_shards(low, high, n):
    for bit in range(n.bit_length() - 1):
        got = swap(high, "fsdp", n, bit)
        size = low.shape[0] // 2
        if size:
            low, high = add_half(low[:size], got[:size]), add_half(low[size:], got[size:])
        else:
            low = add_half(low, got)
    return low[0]


def reduce_quarters(parts, n):
    middle = n // 2
    beside = core_swap(parts[1])
    across = add_half(parts[2], core_swap(parts[3]))
    got = x_swap(across)
    total = [
        (parts[0][s].astype(full) + beside[s].astype(full) + got[s].astype(full)).astype(half)
        for s in (slice(0, middle), slice(middle, None))
    ]
    return scatter_shards(total[0], total[1], n)


def spread_quarters(piece, q):
    pair = [piece, core_swap(piece)]
    there = x_swap(jnp.stack(pair))
    pieces = pair + [there[0], there[1]]
    odd = (q & 1) == 1
    upper = q >= 2
    once = [jnp.where(odd, pieces[i ^ 1], pieces[i]) for i in range(4)]
    return [jnp.where(upper, once[i ^ 2], once[i]) for i in range(4)]


ANYWHERE = pl.BlockSpec(memory_space=pl.ANY)
ON_CHIP = pl.BlockSpec(memory_space=pltpu.VMEM)
SCALARS = pl.BlockSpec(memory_space=pltpu.SMEM)


def dot(left, right, dim_left, dim_right):
    return lax.dot_general(
        left, right, (((dim_left,), (dim_right,)), ((), ())), preferred_element_type=full
    )


def call(kernel, name, operands, in_specs, outs, out_specs, scratch, flops, moved, transcendentals=0):
    return pl.pallas_call(
        kernel,
        out_shape=[jax.ShapeDtypeStruct(shape, kind) for shape, kind in outs],
        in_specs=in_specs,
        out_specs=out_specs,
        scratch_shapes=scratch,
        compiler_params=pltpu.CompilerParams(vmem_limit_bytes=58 * 2**20),
        cost_estimate=pl.CostEstimate(
            flops=flops, bytes_accessed=moved, transcendentals=transcendentals
        ),
        name=name,
    )(*operands)


def loop(count, body):
    def step(i, carry):
        body(i)
        return carry

    lax.fori_loop(0, count, step, 0)


def tile(i, size):
    return pl.ds(pl.multiple_of(i * size, size), size)


def head_rows(s, q, n, rows, quarter):
    per = n // 4
    return pl.multiple_of(((s // per) ^ q) * quarter + (s % per) * rows, rows)


def softmax_pair(q2, k2, patches):
    lane = lax.broadcasted_iota(jnp.int32, q2.shape, 1)
    first = lane < q2.shape[1] // 2
    zero = jnp.zeros_like(q2)
    both = jnp.concatenate([jnp.where(first, q2, zero), jnp.where(first, zero, q2)])
    scores = dot(both, k2, 1, 1)
    key = lax.broadcasted_iota(jnp.int32, scores.shape, 1)
    scores = jnp.where(key < patches, scores, -1e30)
    raised = jnp.exp(scores - jnp.max(scores, axis=-1, keepdims=True))
    probs = raised * (1.0 / jnp.sum(raised, axis=-1, keepdims=True))
    return both, probs, first


def attention_forward(order, normed, bias, weights, n_img, patches, factor):
    groups = len(weights)
    n, rows, wide = weights[0].shape
    count, width = normed.shape
    padded = count // n_img
    quarter = wide // 3

    def kernel(order_ref, normed_ref, bias_ref, *refs):
        w_refs, refs = refs[:groups], refs[groups:]
        qkv_refs, mixed_refs, (w_held, sems) = refs[:groups], refs[groups : 2 * groups], refs[2 * groups :]
        for g in range(groups):

            def start(r, g=g):
                at = pl.multiple_of(order_ref[r] * rows, rows)
                pltpu.make_async_copy(w_refs[g].at[r], w_held.at[g, pl.ds(at, rows)], sems.at[g]).start()

            loop(n, start)
        for g in range(groups):
            pltpu.make_async_copy(w_held.at[g], w_held.at[g], sems.at[g]).wait()

            def project(t, g=g):
                at = tile(t, quarter)
                product = dot(normed_ref[...], w_held[g, :, at], 1, 0)
                qkv_refs[g][:, at] = (product + bias_ref[g, :, at]).astype(half)

            loop(3, project)

            def attend(i, g=g):
                at = tile(i // 2, padded)
                lanes = [pl.ds(pl.multiple_of(t * quarter + (i % 2) * 128, 128), 128) for t in range(3)]
                q2 = qkv_refs[g][at, lanes[0]] * factor
                k2 = qkv_refs[g][at, lanes[1]]
                v2 = qkv_refs[g][at, lanes[2]]
                _, probs, first = softmax_pair(q2, k2, patches)
                out = dot(probs.astype(half), v2, 1, 0)
                mixed_refs[g][at, lanes[0]] = jnp.where(first, out[:padded], out[padded:]).astype(half)

            loop(2 * n_img, attend)

    return call(
        kernel,
        "attention_forward",
        (order, normed, bias, *weights),
        [SCALARS, ON_CHIP, ON_CHIP] + [ANYWHERE] * groups,
        [((count, wide), half)] * groups + [((count, quarter), half)] * groups,
        [ON_CHIP] * (2 * groups),
        [pltpu.VMEM((groups, width, wide), half), pltpu.SemaphoreType.DMA((groups,))],
        groups * 2 * count * width * wide,
        2 * (count * width + groups * (width * wide + count * (wide + quarter))),
    )


def layer_norm(value, gain, shift):
    center = jnp.mean(value, axis=-1, keepdims=True)
    offset = value - center
    spread = jnp.mean(offset * offset, axis=-1, keepdims=True)
    return offset * lax.rsqrt(spread + norm_eps) * gain + shift


def layer_norm_back(value, grad, gain):
    center = jnp.mean(value, axis=-1, keepdims=True)
    offset = value - center
    scale = lax.rsqrt(jnp.mean(offset * offset, axis=-1, keepdims=True) + norm_eps)
    unit = offset * scale
    scaled = grad * gain
    inner = jnp.mean(scaled * unit, axis=-1, keepdims=True)
    return scale * (scaled - jnp.mean(scaled, axis=-1, keepdims=True) - unit * inner), grad * unit


def load_out(order_ref, up_refs, held, sem, n, rows, hidden, quarter):
    q = order_ref[n]

    def start(r):
        at = head_rows(order_ref[r], q, n, rows, quarter)
        for j in range(4):
            column = pl.multiple_of((q ^ j) * quarter, quarter)
            pltpu.make_async_copy(
                up_refs[j].at[r, :, pl.ds(hidden, quarter)],
                held.at[pl.ds(at, rows), pl.ds(column, quarter)],
                sem,
            ).start()

    loop(n, start)


CHUNK = 16


def attention_out(order, x_zero, mixed, ups, bias, gain, shift):
    count, width = x_zero.shape
    n, rows, _ = ups[0].shape
    quarter = mixed[0].shape[1]
    hidden = ups[0].shape[2] - quarter

    def kernel(order_ref, x_ref, bias_ref, gain_ref, shift_ref, *refs):
        mixed_refs, up_refs = refs[:4], refs[4:8]
        after_ref, normed_ref, held, sems = refs[8:]
        load_out(order_ref, up_refs, held, sems.at[0], n, rows, hidden, quarter)
        together = jnp.concatenate([m[...] for m in mixed_refs], axis=1)
        pltpu.make_async_copy(held, held, sems.at[0]).wait()
        after_ref[...] = dot(together, held[...], 1, 0)

        def finish(i):
            at = tile(i, CHUNK)
            after = x_ref[at] + (after_ref[at] + bias_ref[...])
            after_ref[at] = after
            normed_ref[at] = layer_norm(after, gain_ref[...], shift_ref[...]).astype(half)

        loop(count // CHUNK, finish)

    return call(
        kernel,
        "attention_out",
        (order, x_zero, bias, gain, shift, *mixed, *ups),
        [SCALARS] + [ON_CHIP] * 8 + [ANYWHERE] * 4,
        [((count, width), full), ((count, width), half)],
        [ON_CHIP] * 2,
        [pltpu.VMEM((width, width), half), pltpu.SemaphoreType.DMA((1,))],
        2 * count * width * width,
        14 * count * width + 2 * width * width,
    )


def mlp(order, normed, cot, bias, ups, downs, carried=None, ending=None):
    groups = len(ups)
    count, width = normed.shape
    n, rows, _ = ups[0].shape
    share = downs[0].shape[1]
    hidden = n * share
    step = min(512, hidden)
    steps = hidden // step
    more = [] if carried is None else [*carried, *ending]

    def kernel(order_ref, normed_ref, cot_ref, bias_ref, *refs):
        more_refs, refs = refs[: len(more)], refs[len(more) :]
        up_refs, down_refs, refs = refs[:groups], refs[groups : 2 * groups], refs[2 * groups :]
        g_up_refs, g_down_refs, refs = refs[:groups], refs[groups : 2 * groups], refs[2 * groups :]
        g_bias_ref, out_ref, back_ref, refs = refs[0], refs[1], refs[2], refs[3:]
        up, down, pre, act, act_half, pre_half, g_up, g_down, sems, out_sems = refs[-10:]
        for g in range(groups):

            def start(r, g=g):
                s = order_ref[r]
                pltpu.make_async_copy(
                    up_refs[g].at[r, :, pl.ds(0, hidden)],
                    up.at[g, pl.ds(pl.multiple_of(s * rows, rows), rows)],
                    sems.at[g],
                ).start()
                pltpu.make_async_copy(
                    down_refs[g].at[r],
                    down.at[g, pl.ds(pl.multiple_of(s * share, share), share)],
                    sems.at[groups + g],
                ).start()

            loop(n, start)
        if more:
            out_ref[...] = more_refs[0][...]
            back_ref[...] = more_refs[1][...]
        else:
            out_ref[...] = jnp.zeros_like(out_ref)
            back_ref[...] = jnp.zeros_like(back_ref)
        for g in range(groups):
            pltpu.make_async_copy(up.at[g], up.at[g], sems.at[g]).wait()
            pltpu.make_async_copy(down.at[g], down.at[g], sems.at[groups + g]).wait()

            def part(t, g=g):
                at = tile(t, step)
                pre[...] = dot(normed_ref[...], up[g, :, at], 1, 0)
                act[...] = dot(cot_ref[...], down[g, at, :], 1, 1)

                def gelu(i):
                    some = tile(i, CHUNK)
                    x = pre[some] + bias_ref[g, :, at]
                    below = 0.5 * (1.0 + lax.erf(x * math.sqrt(0.5)))
                    density = jnp.exp(-0.5 * x * x) * (1.0 / math.sqrt(2.0 * math.pi))
                    act_half[some] = (x * below).astype(half)
                    pre_half[some] = (act[some] * (below + x * density)).astype(half)

                loop(count // CHUNK, gelu)
                h = act_half[...]
                p = pre_half[...]
                out_ref[...] += dot(h, down[g, at, :], 1, 0)
                back_ref[...] += dot(p, up[g, :, at], 1, 1)
                g_down[g, at, :] = dot(h, cot_ref[...], 0, 0).astype(half)
                g_up[g, :, at] = dot(normed_ref[...], p, 0, 0).astype(half)
                g_bias_ref[g, :, at] = jnp.sum(p.astype(full), axis=0, keepdims=True)

            loop(steps, part)

            def send(r, g=g):
                s = order_ref[r]
                pltpu.make_async_copy(
                    g_up.at[g, pl.ds(pl.multiple_of(s * rows, rows), rows)],
                    g_up_refs[g].at[r],
                    out_sems.at[g],
                ).start()
                pltpu.make_async_copy(
                    g_down.at[g, pl.ds(pl.multiple_of(s * share, share), share)],
                    g_down_refs[g].at[r],
                    out_sems.at[groups + g],
                ).start()

            loop(n, send)
        if more:
            after_ref, end_ref, block_ref = more_refs[2], more_refs[3], refs[0]

            def finish(i):
                at = tile(i, CHUNK)
                block_ref[at] = (after_ref[at] + (out_ref[at] + end_ref[...])).astype(half)

            loop(count // CHUNK, finish)
        for g in range(groups):
            pltpu.make_async_copy(g_up_refs[g], g_up_refs[g], out_sems.at[g]).wait()
            pltpu.make_async_copy(g_down_refs[g], g_down_refs[g], out_sems.at[groups + g]).wait()

    outs = (
        [((n, rows, hidden), half)] * groups
        + [((n, share, width), half)] * groups
        + [((groups, 1, hidden), full), ((count, width), full), ((count, width), full)]
        + ([((count, width), half)] if more else [])
    )
    return call(
        kernel,
        "mlp",
        (order, normed, cot, bias, *more, *ups, *downs),
        [SCALARS] + [ON_CHIP] * (3 + len(more)) + [ANYWHERE] * (2 * groups),
        outs,
        [ANYWHERE] * (2 * groups) + [ON_CHIP] * (len(outs) - 2 * groups),
        [
            pltpu.VMEM((groups, width, hidden), half),
            pltpu.VMEM((groups, hidden, width), half),
            pltpu.VMEM((count, step), full),
            pltpu.VMEM((count, step), full),
            pltpu.VMEM((count, step), half),
            pltpu.VMEM((count, step), half),
            pltpu.VMEM((groups, width, hidden), half),
            pltpu.VMEM((groups, hidden, width), half),
            pltpu.SemaphoreType.DMA((2 * groups,)),
            pltpu.SemaphoreType.DMA((2 * groups,)),
        ],
        groups * 12 * count * width * hidden,
        groups * 8 * width * hidden + 20 * count * width,
        groups * 2 * count * hidden,
    )


def attention_out_back(order, grad, after, cot, gain, mixed, ups):
    count, width = after.shape
    n, rows, _ = ups[0].shape
    quarter = mixed[0].shape[1]
    hidden = ups[0].shape[2] - quarter

    def kernel(order_ref, grad_ref, after_ref, cot_ref, gain_ref, *refs):
        mixed_refs, up_refs, refs = refs[:4], refs[4:8], refs[8:]
        after_grad_ref, mixed_grad_refs, g_out_ref, sums_ref = refs[0], refs[1:5], refs[5], refs[6]
        held, branch, terms, sems = refs[7:]
        load_out(order_ref, up_refs, held, sems.at[0], n, rows, hidden, quarter)
        terms[...] = jnp.zeros_like(terms)

        def fold(value):
            return jnp.sum(value.reshape(CHUNK // 8, 8, width), axis=0)

        def back(i):
            at = tile(i, CHUNK)
            incoming = grad_ref[at]
            part, gain_terms = layer_norm_back(after_ref[at], incoming, gain_ref[...])
            own = cot_ref[at].astype(full)
            total = own + part
            after_grad_ref[at] = total
            rounded = total.astype(half)
            branch[at] = rounded
            terms[0] += fold(rounded.astype(full))
            terms[1] += fold(gain_terms)
            terms[2] += fold(incoming)
            terms[3] += fold(own)

        loop(count // CHUNK, back)
        for k in range(4):
            sums_ref[k] = jnp.sum(terms[k], axis=0, keepdims=True)
        pltpu.make_async_copy(held, held, sems.at[0]).wait()
        for j in range(4):
            mixed_grad_refs[j][...] = dot(branch[...], held[j * quarter : (j + 1) * quarter], 1, 1).astype(half)
            g_out_ref[j * quarter : (j + 1) * quarter] = dot(mixed_refs[j][...], branch[...], 0, 0).astype(half)

    return call(
        kernel,
        "attention_out_back",
        (order, grad, after, cot, gain, *mixed, *ups),
        [SCALARS] + [ON_CHIP] * 8 + [ANYWHERE] * 4,
        [((count, width), full)]
        + [((count, quarter), half)] * 4
        + [((width, width), half), ((4, 1, width), full)],
        [ON_CHIP] * 7,
        [
            pltpu.VMEM((width, width), half),
            pltpu.VMEM((count, width), half),
            pltpu.VMEM((4, 8, width), full),
            pltpu.SemaphoreType.DMA((1,)),
        ],
        4 * count * width * width,
        18 * count * width + 4 * width * width,
    )


def attention_back(order, normed, qkvs, mixed_grads, g_out, which, n_img, patches, factor, n):
    groups = len(qkvs)
    count, width = normed.shape
    wide = qkvs[0].shape[1]
    quarter = wide // 3
    padded = count // n_img
    rows = width // n

    def kernel(order_ref, normed_ref, g_out_ref, *refs):
        qkv_refs, mg_refs, refs = refs[:groups], refs[groups : 2 * groups], refs[2 * groups :]
        g_w_refs, proj_refs, sums_ref = refs[:groups], refs[groups : 2 * groups], refs[2 * groups]
        g_w, sems = refs[2 * groups + 1 :]
        q = order_ref[n]
        for g in range(groups):

            def send_out(r, g=g):
                at = head_rows(order_ref[r], q, n, rows, quarter)
                column = pl.multiple_of((q ^ which[g]) * quarter, quarter)
                pltpu.make_async_copy(
                    g_out_ref.at[pl.ds(at, rows), pl.ds(column, quarter)],
                    g_w_refs[g].at[r, :, pl.ds(wide, quarter)],
                    sems.at[g],
                ).start()

            loop(n, send_out)

            def attend(i, g=g):
                at = tile(i // 2, padded)
                lanes = [pl.ds(pl.multiple_of(t * quarter + (i % 2) * 128, 128), 128) for t in range(3)]
                q2 = qkv_refs[g][at, lanes[0]] * factor
                k2 = qkv_refs[g][at, lanes[1]]
                v2 = qkv_refs[g][at, lanes[2]]
                both, probs, first = softmax_pair(q2, k2, patches)
                o2 = mg_refs[g][at, lanes[0]]
                zero = jnp.zeros_like(o2)
                o_both = jnp.concatenate([jnp.where(first, o2, zero), jnp.where(first, zero, o2)])
                g_probs = dot(o_both, v2, 1, 1)
                weighted = jnp.sum(probs * g_probs, axis=-1, keepdims=True)
                g_scores = (probs * (g_probs - weighted)).astype(half)
                g_query = dot(g_scores, k2, 1, 0)
                g_query = jnp.where(first, g_query[:padded], g_query[padded:]) * factor
                proj_refs[g][at, lanes[0]] = g_query.astype(half)
                proj_refs[g][at, lanes[1]] = dot(g_scores, both, 0, 0).astype(half)
                proj_refs[g][at, lanes[2]] = dot(probs.astype(half), o_both, 0, 0).astype(half)

            loop(2 * n_img, attend)

            def weigh(t, g=g):
                at = tile(t, quarter)
                some = proj_refs[g][:, at]
                g_w[g, :, at] = dot(normed_ref[...], some, 0, 0).astype(half)
                sums_ref[g, :, at] = jnp.sum(some.astype(full), axis=0, keepdims=True)

            loop(3, weigh)

            def send(r, g=g):
                at = pl.multiple_of(order_ref[r] * rows, rows)
                pltpu.make_async_copy(
                    g_w.at[g, pl.ds(at, rows)], g_w_refs[g].at[r, :, pl.ds(0, wide)], sems.at[g]
                ).start()

            loop(n, send)
        for g in range(groups):
            pltpu.make_async_copy(g_w_refs[g], g_w_refs[g], sems.at[g]).wait()

    return call(
        kernel,
        "attention_back",
        (order, normed, g_out, *qkvs, *mixed_grads),
        [SCALARS] + [ON_CHIP] * (2 + 2 * groups),
        [((n, rows, wide + quarter), half)] * groups
        + [((count, wide), half)] * groups
        + [((groups, 1, wide), full)],
        [ANYWHERE] * groups + [ON_CHIP] * (groups + 1),
        [pltpu.VMEM((groups, width, wide), half), pltpu.SemaphoreType.DMA((groups,))],
        groups * 2 * count * width * wide * 2,
        2 * (count * width + width * width + groups * (width * wide + count * (2 * wide + quarter))),
    )


def input_back(order, x_zero, after_grad, gain, projs, weights):
    count, width = x_zero.shape
    n, rows, wide = weights[0].shape

    def kernel(order_ref, x_ref, after_ref, gain_ref, *refs):
        proj_refs, w_refs = refs[:4], refs[4:8]
        token_ref, sums_ref, held, terms, sems = refs[8:]
        for j in range(4):

            def start(r, j=j):
                at = pl.multiple_of(order_ref[r] * rows, rows)
                pltpu.make_async_copy(w_refs[j].at[r], held.at[j, pl.ds(at, rows)], sems.at[j]).start()

            loop(n, start)
        for j in range(4):
            pltpu.make_async_copy(held.at[j], held.at[j], sems.at[j]).wait()
            product = dot(proj_refs[j][...], held[j], 1, 1)
            if j == 0:
                token_ref[...] = product
            else:
                token_ref[...] += product
        terms[...] = jnp.zeros_like(terms)

        def fold(value):
            return jnp.sum(value.reshape(CHUNK // 8, 8, width), axis=0)

        def back(i):
            at = tile(i, CHUNK)
            incoming = token_ref[at]
            part, gain_terms = layer_norm_back(x_ref[at], incoming, gain_ref[...])
            token_ref[at] = after_ref[at] + part
            terms[0] += fold(gain_terms)
            terms[1] += fold(incoming)

        loop(count // CHUNK, back)
        for k in range(2):
            sums_ref[k] = jnp.sum(terms[k], axis=0, keepdims=True)

    return call(
        kernel,
        "input_back",
        (order, x_zero, after_grad, gain, *projs, *weights),
        [SCALARS] + [ON_CHIP] * 7 + [ANYWHERE] * 4,
        [((count, width), full), ((2, 1, width), full)],
        [ON_CHIP] * 2,
        [
            pltpu.VMEM((4, width, wide), half),
            pltpu.VMEM((2, 8, width), full),
            pltpu.SemaphoreType.DMA((4,)),
        ],
        8 * count * width * wide,
        12 * count * width + 8 * (width + count) * wide,
    )


def table(codes, width):
    ratio = 0.3 * jnp.exp(codes.astype(full) * (math.log(10.0 / 0.3) / (NSCALE - 1)))
    quarter = width // 4
    omega = jnp.exp(jnp.arange(quarter).astype(full) * (-math.log(10000.0) / quarter))
    steps = jnp.arange(GRID, dtype=jnp.int32).astype(full)
    angle = ratio[:, None, None] * steps[None, :, None] * omega[None, None, :]
    return jnp.concatenate([jnp.sin(angle), jnp.cos(angle)], axis=-1)


def local(
    tokens,
    scale_codes,
    w_qkv,
    b_q,
    b_v,
    w_out,
    b_out,
    gain_one,
    shift_one,
    w_fc1,
    b_fc1,
    w_fc2,
    b_fc2,
    gain_two,
    shift_two,
    cotangent,
):
    n = lax.axis_size("fsdp")
    q = lax.axis_index("dp")
    f = lax.axis_index("fsdp")
    row_count, width = tokens.shape
    rows = width // n
    ff = b_fc1.shape[0] * n
    ffq = ff // n // 4
    hidden = n * ffq
    quarter = width // 4
    n_img = scale_codes.shape[0]
    patches = row_count // n_img
    padded = -(-patches // 16) * 16
    factor = 1.0 / math.sqrt(width // HEADS)
    shard_order = jnp.asarray(masks(n), jnp.int32) ^ f
    group_order = jnp.arange(4, dtype=jnp.int32) ^ q
    order = jnp.concatenate([shard_order, q[None]])

    def pick(value, axis):
        return lax.dynamic_index_in_dim(value, q, axis, keepdims=False)

    small = jnp.concatenate(
        [b_q, b_v, b_out, gain_one, shift_one, b_fc2, gain_two, shift_two, b_fc1]
    ).astype(half)
    pad = -small.shape[0] % 2048
    small_held = gather_shards(jnp.pad(small, (0, pad)).reshape(-1, 128), n).reshape(n, -1)
    inverse = jnp.zeros((n,), jnp.int32).at[shard_order].set(jnp.arange(n, dtype=jnp.int32))
    small_all = jnp.take(small_held, inverse, axis=0).astype(full)
    vectors = [small_all[:, i * rows : (i + 1) * rows].reshape(1, width) for i in range(8)]
    full_bq, full_bv, full_bout, gain_one_f, shift_one_f, full_bfc2, gain_two_f, shift_two_f = vectors
    bias_units = small_all[:, 8 * rows : 8 * rows + 4 * ffq].reshape(n, 4, ffq)
    bias_fc1 = jnp.take(bias_units, group_order, axis=1).transpose(1, 0, 2).reshape(4, 1, hidden)
    bias_q = jnp.take(full_bq.reshape(4, quarter), group_order, axis=0)
    bias_v = jnp.take(full_bv.reshape(4, quarter), group_order, axis=0)
    bias_qkv = jnp.concatenate([bias_q, jnp.zeros_like(bias_q), bias_v], axis=1)[:, None]

    qkv_own = pick(w_qkv.reshape(rows, 3, 4, quarter), 2).reshape(rows, 3 * quarter).astype(half)
    qkv_parts = gather_quarters(qkv_own, n)
    out_own = pick(w_out.reshape(rows, 4, quarter), 1).astype(half)
    fc1_own = pick(w_fc1.reshape(rows, n, 4, ffq), 2).reshape(rows, n * ffq).astype(half)
    up_parts = gather_quarters(jnp.concatenate([fc1_own, out_own], axis=1), n)
    fc2_own = pick(w_fc2.reshape(4, ffq, width), 0).astype(half)
    column = gather_shards(fc2_own, n, 1)
    both = jnp.stack([column, x_swap(column)])
    far = swap(both, "fsdp", n, 0)
    down_own = jnp.concatenate([both[0], far[0]])
    down_across = jnp.concatenate([both[1], far[1]])
    down_parts = (down_own, core_swap(down_own), down_across, core_swap(down_across))

    def spread_rows(value):
        split = value.reshape(n_img, patches, width)
        return jnp.pad(split, ((0, 0), (0, padded - patches), (0, 0)))

    def compact(value):
        return value.reshape(n_img, padded, width)[:, :patches].reshape(row_count, width)

    places = table(scale_codes, width)
    row_place = jnp.broadcast_to(places[:, :, None], (n_img, GRID, GRID, width // 2))
    col_place = jnp.broadcast_to(places[:, None], (n_img, GRID, GRID, width // 2))
    place = jnp.concatenate([row_place, col_place], axis=-1).reshape(n_img, patches, width)
    place = jnp.pad(place, ((0, 0), (0, padded - patches), (0, 0)))
    x_zero = (spread_rows(tokens).astype(full) + place).reshape(-1, width)
    normed_one = layer_norm(x_zero, gain_one_f, shift_one_f).astype(half)
    cot = spread_rows(cotangent).reshape(-1, width)

    first = attention_forward(order, normed_one, bias_qkv[:2], qkv_parts[:2], n_img, patches, factor)
    second = attention_forward(order, normed_one, bias_qkv[2:], qkv_parts[2:], n_img, patches, factor)
    qkvs = (*first[:2], *second[:2])
    mixed = (*first[2:], *second[2:])
    after_attn, normed_two = attention_out(
        order, x_zero, mixed, up_parts, full_bout, gain_two_f, shift_two_f
    )

    g_up0, g_up1, g_down0, g_down1, g_bias_a, out_a, back_a = mlp(
        order, normed_two, cot, bias_fc1[:2], up_parts[:2], down_parts[:2]
    )
    g_up2, g_up3, g_down2, g_down3, g_bias_b, _, grad_two_in, block = mlp(
        order, normed_two, cot, bias_fc1[2:], up_parts[2:], down_parts[2:], (out_a, back_a), (after_attn, full_bfc2)
    )
    block_out = compact(block)
    up_grads = (g_up0, g_up1, g_up2, g_up3)
    down_grads = (g_down0, g_down1, g_down2, g_down3)

    middle = n // 2
    pair_low, pair_high = [], []
    for a, b in ((0, 1), (2, 3)):
        got = core_swap(down_grads[b])
        pair_low.append(add_half(down_grads[a][:middle], got[:middle]))
        pair_high.append(add_half(down_grads[a][middle:], got[middle:]))
    far = swap(jnp.stack(pair_high), "fsdp", n, 0)
    across = x_swap(add_half(pair_low[1], far[1]))
    down_low = (pair_low[0].astype(full) + far[0].astype(full) + across.astype(full)).astype(half)
    for bit in range(1, n.bit_length() - 1):
        size = down_low.shape[0] // 2
        got = swap(down_low[size:], "fsdp", n, bit)
        down_low = add_half(down_low[:size], got)
    down_pieces = spread_quarters(down_low[0], q)
    out_fc2 = jnp.concatenate(down_pieces).astype(full)
    up_pieces = spread_quarters(reduce_quarters(up_grads, n), q)
    out_fc1 = (
        jnp.stack([p.reshape(rows, n, ffq) for p in up_pieces], axis=2).reshape(rows, ff).astype(full)
    )

    after_grad, mg0, mg1, mg2, mg3, g_out, sums_two = attention_out_back(
        order, grad_two_in, after_attn, cot, gain_two_f, mixed, up_parts
    )
    g_w2, g_w3, proj2, proj3, sums_b = attention_back(
        order, normed_one, qkvs[2:], (mg2, mg3), g_out, (2, 3), n_img, patches, factor, n
    )
    g_w0, g_w1, proj0, proj1, sums_a = attention_back(
        order, normed_one, qkvs[:2], (mg0, mg1), g_out, (0, 1), n_img, patches, factor, n
    )
    attn_pieces = spread_quarters(reduce_quarters((g_w0, g_w1, g_w2, g_w3), n), q)
    out_qkv = (
        jnp.stack([p[:, : 3 * quarter].reshape(rows, 3, quarter) for p in attn_pieces], axis=2)
        .reshape(rows, 3 * width)
        .astype(full)
    )
    out_out = jnp.stack([p[:, 3 * quarter :] for p in attn_pieces], axis=1).reshape(rows, width).astype(full)
    tokens_grad, sums_one = input_back(
        order, x_zero, after_grad, gain_one_f, (proj0, proj1, proj2, proj3), qkv_parts
    )
    grad_tokens = compact(tokens_grad)

    sums_proj = jnp.take(jnp.concatenate([sums_a, sums_b])[:, 0], group_order, axis=0)
    sums = [
        sums_proj[:, :quarter],
        sums_proj[:, 2 * quarter :],
        sums_two[0],
        sums_one[0],
        sums_one[1],
        sums_two[3],
        sums_two[1],
        sums_two[2],
    ]
    units = jnp.concatenate([g_bias_a, g_bias_b]).reshape(4, n, ffq)
    units = jnp.take(units, group_order, axis=0).transpose(1, 0, 2)
    packed = jnp.concatenate([s.reshape(n, rows) for s in sums] + [units.reshape(n, 4 * ffq)], axis=1)
    packed = jnp.take(packed, shard_order, axis=0)
    pad = -packed.shape[1] % 1024
    packed = jnp.pad(packed, ((0, 0), (0, pad))).reshape(n, -1, 128)
    packed = packed + core_swap(packed)
    packed = packed + x_swap(packed)
    for bit in range(n.bit_length() - 1):
        size = packed.shape[0] // 2
        packed = packed[:size] + swap(packed[size:], "fsdp", n, bit)
    vector = packed.reshape(-1)
    small_out = [vector[i * rows : (i + 1) * rows] for i in range(8)]
    out_bfc1 = vector[8 * rows : 8 * rows + 4 * ffq]
    o_bq, o_bv, o_bout, o_gone, o_sone, o_bfc2, o_gtwo, o_stwo = small_out
    return (
        block_out,
        grad_tokens,
        out_qkv,
        o_bq,
        o_bv,
        out_out,
        o_bout,
        o_gone,
        o_sone,
        out_fc1,
        out_bfc1,
        out_fc2,
        o_bfc2,
        o_gtwo,
        o_stwo,
    )


def solution(mesh):
    rows_split = P(("dp", "fsdp"), None)
    matrix = P("fsdp", None)
    vector = P("fsdp")
    return jax.shard_map(
        local,
        mesh=mesh,
        in_specs=(
            rows_split, P(("dp", "fsdp")), matrix, vector, vector, matrix, vector, vector, vector,
            matrix, vector, matrix, vector, vector, vector, rows_split,
        ),
        out_specs=(
            rows_split, rows_split, matrix, vector, vector, matrix, vector, vector, vector,
            matrix, vector, matrix, vector, vector, vector,
        ),
        check_vma=False,
    )
```

```python
import math

import jax
import jax.numpy as jnp
from jax import lax
from jax.experimental import pallas as pl
from jax.experimental.pallas import tpu as pltpu
from jax.sharding import PartitionSpec as P

HEADS = 16
GRID = 14
NSCALE = 16
norm_eps = 1e-06
half = jnp.bfloat16
full = jnp.float32


def swap(value, axis, size, bit):
    return lax.ppermute(value, axis, [(i, i ^ (1 << bit)) for i in range(size)])


def core_swap(value):
    return swap(value, "dp", 4, 0)


def x_swap(value):
    return swap(value, "dp", 4, 1)


def masks(n):
    found = [0]
    for bit in reversed(range(n.bit_length() - 1)):
        found = found + [m | (1 << bit) for m in found]
    return found


def add_half(a, b):
    return (a.astype(full) + b.astype(full)).astype(half)


def spread_quarters(piece, q):
    pair = [piece, core_swap(piece)]
    there = x_swap(jnp.stack(pair))
    pieces = pair + [there[0], there[1]]
    odd = (q & 1) == 1
    upper = q >= 2
    once = [jnp.where(odd, pieces[i ^ 1], pieces[i]) for i in range(4)]
    return [jnp.where(upper, once[i ^ 2], once[i]) for i in range(4)]


class Order:
    def __init__(self, value):
        self.value = value

    def at(self, value):
        value, self.value = lax.optimization_barrier((value, self.value))
        return value


class Gather:
    def __init__(self, seq, piece, n):
        self.seq, self.held, self.n = seq, piece[None], n
        self.bits = list(reversed(range(n.bit_length() - 1)))
        while len(self.bits) > 3:
            self.launch()
            self.land()

    def launch(self):
        self.held = self.seq.at(self.held)
        self.flight = swap(self.held, "fsdp", self.n, self.bits.pop(0))

    def land(self):
        self.held = jnp.concatenate([self.held, self.seq.at(self.flight)])
        return self.held


class Reduce:
    def __init__(self, seq, terms, n):
        self.seq, self.n, self.bits = seq, n, list(range(n.bit_length() - 1))
        middle = n // 2
        self.low, self.high = [
            sum(t[part].astype(full) for t in terms).astype(half)
            for part in (slice(0, middle), slice(middle, None))
        ]

    def launch(self):
        self.high = self.seq.at(self.high)
        self.flight = swap(self.high, "fsdp", self.n, self.bits.pop(0))

    def land(self):
        got = self.seq.at(self.flight)
        size = self.low.shape[0] // 2
        if size:
            self.low, self.high = add_half(self.low[:size], got[:size]), add_half(self.low[size:], got[size:])
        else:
            self.low = add_half(self.low, got)

    def rest(self):
        while self.bits:
            self.launch()
            self.land()
        return self.low[0]


ANYWHERE = pl.BlockSpec(memory_space=pl.ANY)
ON_CHIP = pl.BlockSpec(memory_space=pltpu.VMEM)
SCALARS = pl.BlockSpec(memory_space=pltpu.SMEM)


def dot(left, right, dim_left, dim_right):
    return lax.dot_general(
        left, right, (((dim_left,), (dim_right,)), ((), ())), preferred_element_type=full
    )


def call(kernel, name, operands, in_specs, outs, out_specs, scratch):
    return pl.pallas_call(
        kernel,
        out_shape=[jax.ShapeDtypeStruct(shape, kind) for shape, kind in outs],
        in_specs=in_specs,
        out_specs=out_specs,
        scratch_shapes=scratch,
        compiler_params=pltpu.CompilerParams(vmem_limit_bytes=58 * 2**20),
        name=name,
    )(*operands)


def loop(count, body):
    def step(i, carry):
        body(i)
        return carry

    lax.fori_loop(0, count, step, 0)


def tile(i, size):
    return pl.ds(pl.multiple_of(i * size, size), size)


def head_rows(s, q, n, rows, quarter):
    per = n // 4
    return pl.multiple_of(((s // per) ^ q) * quarter + (s % per) * rows, rows)


def softmax_pair(q2, k2, patches):
    lane = lax.broadcasted_iota(jnp.int32, q2.shape, 1)
    first = lane < q2.shape[1] // 2
    zero = jnp.zeros_like(q2)
    both = jnp.concatenate([jnp.where(first, q2, zero), jnp.where(first, zero, q2)])
    scores = dot(both, k2, 1, 1)
    key = lax.broadcasted_iota(jnp.int32, scores.shape, 1)
    scores = jnp.where(key < patches, scores, -1e30)
    raised = jnp.exp(scores - jnp.max(scores, axis=-1, keepdims=True))
    probs = raised * (1.0 / jnp.sum(raised, axis=-1, keepdims=True))
    return both, probs, first


def attention_forward(order, normed, bias, weights, n_img, patches, factor):
    groups = len(weights)
    n, rows, wide = weights[0].shape
    count, width = normed.shape
    padded = count // n_img
    quarter = wide // 3

    def kernel(order_ref, normed_ref, bias_ref, *refs):
        w_refs, refs = refs[:groups], refs[groups:]
        qkv_refs, mixed_refs, (w_held, sems) = refs[:groups], refs[groups : 2 * groups], refs[2 * groups :]
        for g in range(groups):

            def start(r, g=g):
                at = pl.multiple_of(order_ref[r] * rows, rows)
                pltpu.make_async_copy(w_refs[g].at[r], w_held.at[g, pl.ds(at, rows)], sems.at[g]).start()

            loop(n, start)
        for g in range(groups):
            pltpu.make_async_copy(w_held.at[g], w_held.at[g], sems.at[g]).wait()

            def project(t, g=g):
                at = tile(t, quarter)
                product = dot(normed_ref[...], w_held[g, :, at], 1, 0)
                qkv_refs[g][:, at] = (product + bias_ref[g, :, at]).astype(half)

            loop(3, project)

            def attend(i, g=g):
                at = tile(i // 2, padded)
                lanes = [pl.ds(pl.multiple_of(t * quarter + (i % 2) * 128, 128), 128) for t in range(3)]
                q2 = qkv_refs[g][at, lanes[0]] * factor
                k2 = qkv_refs[g][at, lanes[1]]
                v2 = qkv_refs[g][at, lanes[2]]
                _, probs, first = softmax_pair(q2, k2, patches)
                out = dot(probs.astype(half), v2, 1, 0)
                mixed_refs[g][at, lanes[0]] = jnp.where(first, out[:padded], out[padded:]).astype(half)

            loop(2 * n_img, attend)

    return call(
        kernel,
        "attention_forward",
        (order, normed, bias, *weights),
        [SCALARS, ON_CHIP, ON_CHIP] + [ANYWHERE] * groups,
        [((count, wide), half)] * groups + [((count, quarter), half)] * groups,
        [ON_CHIP] * (2 * groups),
        [pltpu.VMEM((groups, width, wide), half), pltpu.SemaphoreType.DMA((groups,))],
    )


def layer_norm(value, gain, shift):
    center = jnp.mean(value, axis=-1, keepdims=True)
    offset = value - center
    spread = jnp.mean(offset * offset, axis=-1, keepdims=True)
    return offset * lax.rsqrt(spread + norm_eps) * gain + shift


def layer_norm_back(value, grad, gain):
    center = jnp.mean(value, axis=-1, keepdims=True)
    offset = value - center
    scale = lax.rsqrt(jnp.mean(offset * offset, axis=-1, keepdims=True) + norm_eps)
    unit = offset * scale
    scaled = grad * gain
    inner = jnp.mean(scaled * unit, axis=-1, keepdims=True)
    return scale * (scaled - jnp.mean(scaled, axis=-1, keepdims=True) - unit * inner), grad * unit


def load_out(order_ref, up_refs, held, sem, n, rows, hidden, quarter):
    q = order_ref[n]

    def start(r):
        at = head_rows(order_ref[r], q, n, rows, quarter)
        for j in range(4):
            column = pl.multiple_of((q ^ j) * quarter, quarter)
            pltpu.make_async_copy(
                up_refs[j % 2].at[r, :, pl.ds(hidden + j // 2 * quarter, quarter)],
                held.at[pl.ds(at, rows), pl.ds(column, quarter)],
                sem,
            ).start()

    loop(n, start)


CHUNK = 16


def attention_out(order, x_zero, mixed, ups, bias, gain, shift):
    count, width = x_zero.shape
    n, rows, _ = ups[0].shape
    quarter = mixed[0].shape[1]
    hidden = ups[0].shape[2] - 2 * quarter

    def kernel(order_ref, x_ref, bias_ref, gain_ref, shift_ref, *refs):
        mixed_refs, up_refs = refs[:4], refs[4:6]
        after_ref, normed_ref, held, sems = refs[6:]
        load_out(order_ref, up_refs, held, sems.at[0], n, rows, hidden, quarter)
        together = jnp.concatenate([m[...] for m in mixed_refs], axis=1)
        pltpu.make_async_copy(held, held, sems.at[0]).wait()
        after_ref[...] = dot(together, held[...], 1, 0)

        def finish(i):
            at = tile(i, CHUNK)
            after = x_ref[at] + (after_ref[at] + bias_ref[...])
            after_ref[at] = after
            normed_ref[at] = layer_norm(after, gain_ref[...], shift_ref[...]).astype(half)

        loop(count // CHUNK, finish)

    return call(
        kernel,
        "attention_out",
        (order, x_zero, bias, gain, shift, *mixed, *ups),
        [SCALARS] + [ON_CHIP] * 8 + [ANYWHERE] * 2,
        [((count, width), full), ((count, width), half)],
        [ON_CHIP] * 2,
        [pltpu.VMEM((width, width), half), pltpu.SemaphoreType.DMA((1,))],
    )


def mlp(order, normed, cot, bias, ups, downs, carried=None, ending=None):
    groups = len(ups)
    count, width = normed.shape
    n, rows, _ = ups[0].shape
    share = downs[0].shape[1]
    hidden = n * share
    step = min(512, hidden)
    steps = hidden // step
    more = [] if carried is None else [*carried, *ending]

    def kernel(order_ref, normed_ref, cot_ref, bias_ref, *refs):
        more_refs, refs = refs[: len(more)], refs[len(more) :]
        up_refs, down_refs, refs = refs[:groups], refs[groups : 2 * groups], refs[2 * groups :]
        g_up_refs, g_down_refs, refs = refs[:groups], refs[groups : 2 * groups], refs[2 * groups :]
        g_bias_ref, out_ref, back_ref, refs = refs[0], refs[1], refs[2], refs[3:]
        up, down, pre, act, act_half, pre_half, g_up, g_down, sems, out_sems = refs[-10:]
        for g in range(groups):

            def start(r, g=g):
                s = order_ref[r]
                pltpu.make_async_copy(
                    up_refs[g].at[r, :, pl.ds(0, hidden)],
                    up.at[g, pl.ds(pl.multiple_of(s * rows, rows), rows)],
                    sems.at[g],
                ).start()
                pltpu.make_async_copy(
                    down_refs[g].at[r],
                    down.at[g, pl.ds(pl.multiple_of(s * share, share), share)],
                    sems.at[groups + g],
                ).start()

            loop(n, start)
        if more:
            out_ref[...] = more_refs[0][...]
            back_ref[...] = more_refs[1][...]
        else:
            out_ref[...] = jnp.zeros_like(out_ref)
            back_ref[...] = jnp.zeros_like(back_ref)
        for g in range(groups):
            pltpu.make_async_copy(up.at[g], up.at[g], sems.at[g]).wait()
            pltpu.make_async_copy(down.at[g], down.at[g], sems.at[groups + g]).wait()

            def part(t, g=g):
                at = tile(t, step)
                pre[...] = dot(normed_ref[...], up[g, :, at], 1, 0)
                act[...] = dot(cot_ref[...], down[g, at, :], 1, 1)

                def gelu(i):
                    some = tile(i, CHUNK)
                    x = pre[some] + bias_ref[g, :, at]
                    below = 0.5 * (1.0 + lax.erf(x * math.sqrt(0.5)))
                    density = jnp.exp(-0.5 * x * x) * (1.0 / math.sqrt(2.0 * math.pi))
                    act_half[some] = (x * below).astype(half)
                    pre_half[some] = (act[some] * (below + x * density)).astype(half)

                loop(count // CHUNK, gelu)
                h = act_half[...]
                p = pre_half[...]
                out_ref[...] += dot(h, down[g, at, :], 1, 0)
                back_ref[...] += dot(p, up[g, :, at], 1, 1)
                g_down[g, at, :] = dot(h, cot_ref[...], 0, 0).astype(half)
                g_up[g, :, at] = dot(normed_ref[...], p, 0, 0).astype(half)
                g_bias_ref[g, :, at] = jnp.sum(p.astype(full), axis=0, keepdims=True)

            loop(steps, part)

            def send(r, g=g):
                s = order_ref[r]
                pltpu.make_async_copy(
                    g_up.at[g, pl.ds(pl.multiple_of(s * rows, rows), rows)],
                    g_up_refs[g].at[r],
                    out_sems.at[g],
                ).start()
                pltpu.make_async_copy(
                    g_down.at[g, pl.ds(pl.multiple_of(s * share, share), share)],
                    g_down_refs[g].at[r],
                    out_sems.at[groups + g],
                ).start()

            loop(n, send)
        if more:
            after_ref, end_ref, block_ref = more_refs[2], more_refs[3], refs[0]

            def finish(i):
                at = tile(i, CHUNK)
                block_ref[at] = (after_ref[at] + (out_ref[at] + end_ref[...])).astype(half)

            loop(count // CHUNK, finish)
        for g in range(groups):
            pltpu.make_async_copy(g_up_refs[g], g_up_refs[g], out_sems.at[g]).wait()
            pltpu.make_async_copy(g_down_refs[g], g_down_refs[g], out_sems.at[groups + g]).wait()

    outs = (
        [((n, rows, hidden), half)] * groups
        + [((n, share, width), half)] * groups
        + [((groups, 1, hidden), full), ((count, width), full), ((count, width), full)]
        + ([((count, width), half)] if more else [])
    )
    return call(
        kernel,
        "mlp",
        (order, normed, cot, bias, *more, *ups, *downs),
        [SCALARS] + [ON_CHIP] * (3 + len(more)) + [ANYWHERE] * (2 * groups),
        outs,
        [ANYWHERE] * (2 * groups) + [ON_CHIP] * (len(outs) - 2 * groups),
        [
            pltpu.VMEM((groups, width, hidden), half),
            pltpu.VMEM((groups, hidden, width), half),
            pltpu.VMEM((count, step), full),
            pltpu.VMEM((count, step), full),
            pltpu.VMEM((count, step), half),
            pltpu.VMEM((count, step), half),
            pltpu.VMEM((groups, width, hidden), half),
            pltpu.VMEM((groups, hidden, width), half),
            pltpu.SemaphoreType.DMA((2 * groups,)),
            pltpu.SemaphoreType.DMA((2 * groups,)),
        ],
    )


def attention_out_back(order, grad, after, cot, gain, mixed, ups):
    count, width = after.shape
    n, rows, _ = ups[0].shape
    quarter = mixed[0].shape[1]
    hidden = ups[0].shape[2] - 2 * quarter

    def kernel(order_ref, grad_ref, after_ref, cot_ref, gain_ref, *refs):
        mixed_refs, up_refs, refs = refs[:4], refs[4:6], refs[6:]
        after_grad_ref, mixed_grad_refs, g_out_ref, sums_ref = refs[0], refs[1:5], refs[5], refs[6]
        held, branch, terms, sems = refs[7:]
        load_out(order_ref, up_refs, held, sems.at[0], n, rows, hidden, quarter)
        terms[...] = jnp.zeros_like(terms)

        def fold(value):
            return jnp.sum(value.reshape(CHUNK // 8, 8, width), axis=0)

        def back(i):
            at = tile(i, CHUNK)
            incoming = grad_ref[at]
            part, gain_terms = layer_norm_back(after_ref[at], incoming, gain_ref[...])
            own = cot_ref[at].astype(full)
            total = own + part
            after_grad_ref[at] = total
            rounded = total.astype(half)
            branch[at] = rounded
            terms[0] += fold(rounded.astype(full))
            terms[1] += fold(gain_terms)
            terms[2] += fold(incoming)
            terms[3] += fold(own)

        loop(count // CHUNK, back)
        for k in range(4):
            sums_ref[k] = jnp.sum(terms[k], axis=0, keepdims=True)
        pltpu.make_async_copy(held, held, sems.at[0]).wait()
        for j in range(4):
            mixed_grad_refs[j][...] = dot(branch[...], held[j * quarter : (j + 1) * quarter], 1, 1).astype(half)
            g_out_ref[j * quarter : (j + 1) * quarter] = dot(mixed_refs[j][...], branch[...], 0, 0).astype(half)

    return call(
        kernel,
        "attention_out_back",
        (order, grad, after, cot, gain, *mixed, *ups),
        [SCALARS] + [ON_CHIP] * 8 + [ANYWHERE] * 2,
        [((count, width), full)]
        + [((count, quarter), half)] * 4
        + [((width, width), half), ((4, 1, width), full)],
        [ON_CHIP] * 7,
        [
            pltpu.VMEM((width, width), half),
            pltpu.VMEM((count, width), half),
            pltpu.VMEM((4, 8, width), full),
            pltpu.SemaphoreType.DMA((1,)),
        ],
    )


def attention_back(order, normed, qkvs, mixed_grads, g_out, which, n_img, patches, factor, n):
    groups = len(qkvs)
    count, width = normed.shape
    wide = qkvs[0].shape[1]
    quarter = wide // 3
    padded = count // n_img
    rows = width // n

    def kernel(order_ref, normed_ref, g_out_ref, *refs):
        qkv_refs, mg_refs, refs = refs[:groups], refs[groups : 2 * groups], refs[2 * groups :]
        g_w_refs, proj_refs, sums_ref = refs[:groups], refs[groups : 2 * groups], refs[2 * groups]
        g_w, sems = refs[2 * groups + 1 :]
        q = order_ref[n]
        for g in range(groups):

            def send_out(r, g=g):
                at = head_rows(order_ref[r], q, n, rows, quarter)
                column = pl.multiple_of((q ^ which[g]) * quarter, quarter)
                pltpu.make_async_copy(
                    g_out_ref.at[pl.ds(at, rows), pl.ds(column, quarter)],
                    g_w_refs[g].at[r, :, pl.ds(wide, quarter)],
                    sems.at[g],
                ).start()

            loop(n, send_out)

            def attend(i, g=g):
                at = tile(i // 2, padded)
                lanes = [pl.ds(pl.multiple_of(t * quarter + (i % 2) * 128, 128), 128) for t in range(3)]
                q2 = qkv_refs[g][at, lanes[0]] * factor
                k2 = qkv_refs[g][at, lanes[1]]
                v2 = qkv_refs[g][at, lanes[2]]
                both, probs, first = softmax_pair(q2, k2, patches)
                o2 = mg_refs[g][at, lanes[0]]
                zero = jnp.zeros_like(o2)
                o_both = jnp.concatenate([jnp.where(first, o2, zero), jnp.where(first, zero, o2)])
                g_probs = dot(o_both, v2, 1, 1)
                weighted = jnp.sum(probs * g_probs, axis=-1, keepdims=True)
                g_scores = (probs * (g_probs - weighted)).astype(half)
                g_query = dot(g_scores, k2, 1, 0)
                g_query = jnp.where(first, g_query[:padded], g_query[padded:]) * factor
                proj_refs[g][at, lanes[0]] = g_query.astype(half)
                proj_refs[g][at, lanes[1]] = dot(g_scores, both, 0, 0).astype(half)
                proj_refs[g][at, lanes[2]] = dot(probs.astype(half), o_both, 0, 0).astype(half)

            loop(2 * n_img, attend)

            def weigh(t, g=g):
                at = tile(t, quarter)
                some = proj_refs[g][:, at]
                g_w[g, :, at] = dot(normed_ref[...], some, 0, 0).astype(half)
                sums_ref[g, :, at] = jnp.sum(some.astype(full), axis=0, keepdims=True)

            loop(3, weigh)

            def send(r, g=g):
                at = pl.multiple_of(order_ref[r] * rows, rows)
                pltpu.make_async_copy(
                    g_w.at[g, pl.ds(at, rows)], g_w_refs[g].at[r, :, pl.ds(0, wide)], sems.at[g]
                ).start()

            loop(n, send)
        for g in range(groups):
            pltpu.make_async_copy(g_w_refs[g], g_w_refs[g], sems.at[g]).wait()

    return call(
        kernel,
        "attention_back",
        (order, normed, g_out, *qkvs, *mixed_grads),
        [SCALARS] + [ON_CHIP] * (2 + 2 * groups),
        [((n, rows, wide + quarter), half)] * groups
        + [((count, wide), half)] * groups
        + [((groups, 1, wide), full)],
        [ANYWHERE] * groups + [ON_CHIP] * (groups + 1),
        [pltpu.VMEM((groups, width, wide), half), pltpu.SemaphoreType.DMA((groups,))],
    )


def input_back(order, x_zero, after_grad, gain, projs, weights):
    count, width = x_zero.shape
    n, rows, wide = weights[0].shape

    def kernel(order_ref, x_ref, after_ref, gain_ref, *refs):
        proj_refs, w_refs = refs[:4], refs[4:8]
        token_ref, sums_ref, held, terms, sems = refs[8:]
        for j in range(4):

            def start(r, j=j):
                at = pl.multiple_of(order_ref[r] * rows, rows)
                pltpu.make_async_copy(w_refs[j].at[r], held.at[j, pl.ds(at, rows)], sems.at[j]).start()

            loop(n, start)
        for j in range(4):
            pltpu.make_async_copy(held.at[j], held.at[j], sems.at[j]).wait()
            product = dot(proj_refs[j][...], held[j], 1, 1)
            if j == 0:
                token_ref[...] = product
            else:
                token_ref[...] += product
        terms[...] = jnp.zeros_like(terms)

        def fold(value):
            return jnp.sum(value.reshape(CHUNK // 8, 8, width), axis=0)

        def back(i):
            at = tile(i, CHUNK)
            incoming = token_ref[at]
            part, gain_terms = layer_norm_back(x_ref[at], incoming, gain_ref[...])
            token_ref[at] = after_ref[at] + part
            terms[0] += fold(gain_terms)
            terms[1] += fold(incoming)

        loop(count // CHUNK, back)
        for k in range(2):
            sums_ref[k] = jnp.sum(terms[k], axis=0, keepdims=True)

    return call(
        kernel,
        "input_back",
        (order, x_zero, after_grad, gain, *projs, *weights),
        [SCALARS] + [ON_CHIP] * 7 + [ANYWHERE] * 4,
        [((count, width), full), ((2, 1, width), full)],
        [ON_CHIP] * 2,
        [
            pltpu.VMEM((4, width, wide), half),
            pltpu.VMEM((2, 8, width), full),
            pltpu.SemaphoreType.DMA((4,)),
        ],
    )


def table(codes, width):
    ratio = 0.3 * jnp.exp(codes.astype(full) * (math.log(10.0 / 0.3) / (NSCALE - 1)))
    quarter = width // 4
    omega = jnp.exp(jnp.arange(quarter).astype(full) * (-math.log(10000.0) / quarter))
    steps = jnp.arange(GRID, dtype=jnp.int32).astype(full)
    angle = ratio[:, None, None] * steps[None, :, None] * omega[None, None, :]
    return jnp.concatenate([jnp.sin(angle), jnp.cos(angle)], axis=-1)


def local(
    tokens,
    scale_codes,
    w_qkv,
    b_q,
    b_v,
    w_out,
    b_out,
    gain_one,
    shift_one,
    w_fc1,
    b_fc1,
    w_fc2,
    b_fc2,
    gain_two,
    shift_two,
    cotangent,
):
    n = lax.axis_size("fsdp")
    q = lax.axis_index("dp")
    f = lax.axis_index("fsdp")
    row_count, width = tokens.shape
    rows = width // n
    ff = b_fc1.shape[0] * n
    ffq = ff // n // 4
    hidden = n * ffq
    quarter = width // 4
    n_img = scale_codes.shape[0]
    patches = row_count // n_img
    padded = -(-patches // 16) * 16
    factor = 1.0 / math.sqrt(width // HEADS)
    shard_order = jnp.asarray(masks(n), jnp.int32) ^ f
    group_order = jnp.arange(4, dtype=jnp.int32) ^ q
    order = jnp.concatenate([shard_order, q[None]])

    def pick(value, axis):
        return lax.dynamic_index_in_dim(value, q, axis, keepdims=False)

    seq = Order(q)

    qkv_own = pick(w_qkv.reshape(rows, 3, 4, quarter), 2).reshape(rows, 3 * quarter).astype(half)
    qkv = Gather(seq, qkv_own, n)
    qkv.launch()
    small = jnp.concatenate(
        [b_q, b_v, b_out, gain_one, shift_one, b_fc2, gain_two, shift_two, b_fc1]
    ).astype(half)
    pad = -small.shape[0] % 2048
    vec = Gather(seq, jnp.pad(small, (0, pad)).reshape(-1, 128), n)
    vec.launch()
    out_own = [
        lax.dynamic_index_in_dim(w_out.reshape(rows, 4, quarter), g, 1, keepdims=False) for g in (q, q ^ 2)
    ]
    fc1_own = pick(w_fc1.reshape(rows, n, 4, ffq), 2).reshape(rows, n * ffq)
    up = Gather(seq, jnp.concatenate([fc1_own, *out_own], axis=1).astype(half), n)
    fc2_own, fc2_across = [
        lax.dynamic_index_in_dim(w_fc2.reshape(4, ffq, width), g, 0, keepdims=False).astype(half)
        for g in (q, q ^ 2)
    ]
    down = Gather(seq, fc2_own, n)
    down_two = Gather(seq, fc2_across, n)

    def spread_rows(value):
        split = value.reshape(n_img, patches, width)
        return jnp.pad(split, ((0, 0), (0, padded - patches), (0, 0)))

    def compact(value):
        return value.reshape(n_img, padded, width)[:, :patches].reshape(row_count, width)

    places = table(scale_codes, width)
    row_place = jnp.broadcast_to(places[:, :, None], (n_img, GRID, GRID, width // 2))
    col_place = jnp.broadcast_to(places[:, None], (n_img, GRID, GRID, width // 2))
    place = jnp.concatenate([row_place, col_place], axis=-1).reshape(n_img, patches, width)
    place = jnp.pad(place, ((0, 0), (0, padded - patches), (0, 0)))
    x_zero = (spread_rows(tokens).astype(full) + place).reshape(-1, width)
    cot = spread_rows(cotangent).reshape(-1, width)

    qkv.land()
    qkv.launch()
    vec.land()
    vec.launch()
    x_zero = seq.at(x_zero)
    qkv.land()
    qkv.launch()
    up.launch()
    vec.land()
    vec.launch()
    cot = seq.at(cot)
    up.land()
    up.launch()
    down.launch()
    small_held = vec.land().reshape(n, -1)
    inverse = jnp.zeros((n,), jnp.int32).at[shard_order].set(jnp.arange(n, dtype=jnp.int32))
    small_all = jnp.take(small_held, inverse, axis=0).astype(full)
    vectors = [small_all[:, i * rows : (i + 1) * rows].reshape(1, width) for i in range(8)]
    full_bq, full_bv, full_bout, gain_one_f, shift_one_f, full_bfc2, gain_two_f, shift_two_f = vectors
    bias_units = small_all[:, 8 * rows : 8 * rows + 4 * ffq].reshape(n, 4, ffq)
    bias_fc1 = jnp.take(bias_units, group_order, axis=1).transpose(1, 0, 2).reshape(4, 1, hidden)
    bias_q = jnp.take(full_bq.reshape(4, quarter), group_order, axis=0)
    bias_v = jnp.take(full_bv.reshape(4, quarter), group_order, axis=0)
    bias_qkv = jnp.concatenate([bias_q, jnp.zeros_like(bias_q), bias_v], axis=1)[:, None]
    normed_one = seq.at(layer_norm(x_zero, gain_one_f, shift_one_f).astype(half))
    qkv_a = seq.at(qkv.land())
    qkv_b, qkv_c = core_swap(qkv_a), x_swap(qkv_a)
    qkv_b = seq.at(qkv_b)

    first = attention_forward(seq.at(order), normed_one, bias_qkv[:2], (qkv_a, qkv_b), n_img, patches, factor)
    first = (seq.at(first[0]), *first[1:])
    up.land()
    up.launch()
    down.land()
    down.launch()
    down_two.launch()
    qkv_c = seq.at(qkv_c)
    qkv_d = core_swap(qkv_c)
    qkv_d = seq.at(qkv_d)
    down.land()
    down.launch()
    down_two.land()
    down_two.launch()
    second = attention_forward(seq.at(order), normed_one, bias_qkv[2:], (qkv_c, qkv_d), n_img, patches, factor)
    second = (seq.at(second[0]), *second[1:])
    qkv_parts = (qkv_a, qkv_b, qkv_c, qkv_d)
    qkvs = (*first[:2], *second[:2])
    mixed = (*first[2:], *second[2:])
    up_a = seq.at(up.land())
    up_b = core_swap(up_a)
    up_c = x_swap(seq.at(up_a[:, :, :hidden]))
    up_b = seq.at(up_b)
    ups = (up_a, up_b)
    after_attn, normed_two = attention_out(
        seq.at(order), x_zero, mixed, ups, full_bout, gain_two_f, shift_two_f
    )
    normed_two = seq.at(normed_two)
    down_a = seq.at(down.land())
    down_b = core_swap(down_a)
    down_two.land()
    down_two.launch()
    down_b = seq.at(down_b)

    g_up0, g_up1, g_down0, g_down1, g_bias_a, out_a, back_a = mlp(
        seq.at(order), normed_two, cot, bias_fc1[:2], ups, (down_a, down_b)
    )
    g_up1, g_down1 = seq.at((g_up1, g_down1))
    got_up1, got_down1 = core_swap(g_up1), core_swap(g_down1)
    up_c = seq.at(up_c)
    up_d = core_swap(up_c)
    down_c = seq.at(down_two.land())
    down_d = core_swap(down_c)
    up_d, down_d = seq.at((up_d, down_d))
    g_up2, g_up3, g_down2, g_down3, g_bias_b, _, grad_two_in, block = mlp(
        seq.at(order), normed_two, cot, bias_fc1[2:], (up_c, up_d), (down_c, down_d),
        (out_a, back_a), (after_attn, full_bfc2),
    )
    block_out = compact(block)
    got_up1, got_down1 = seq.at((got_up1, got_down1))
    g_up3, g_down3 = seq.at((g_up3, g_down3))
    got_up3, got_down3 = core_swap(g_up3), core_swap(g_down3)
    red_down = Reduce(seq, (g_down0, got_down1), n)
    red_down.launch()
    got_up3 = seq.at(got_up3)
    up_across = x_swap(seq.at(add_half(g_up2, got_up3)))
    got_down3 = seq.at(got_down3)
    red_down_two = Reduce(seq, (g_down2, got_down3), n)
    red_down_two.launch()

    after_grad, mg0, mg1, mg2, mg3, g_out, sums_two = attention_out_back(
        seq.at(order), grad_two_in, after_attn, cot, gain_two_f, mixed, ups
    )
    mg2 = seq.at(mg2)
    red_down.land()
    red_down.launch()
    g_w2, g_w3, proj2, proj3, sums_b = attention_back(
        seq.at(order), normed_one, qkvs[2:], (mg2, mg3), g_out, (2, 3), n_img, patches, factor, n
    )
    g_w3 = seq.at(g_w3)
    red_down.land()
    red_down_two.land()
    up_across = seq.at(up_across)
    got_w3 = core_swap(seq.at(g_w3))
    red_up = Reduce(seq, (g_up0, got_up1, up_across), n)
    red_up.launch()
    red_down.launch()
    red_down_two.launch()
    got_w3 = seq.at(got_w3)
    red_w_two = Reduce(seq, (g_w2, got_w3), n)
    red_w_two.launch()
    g_w0, g_w1, proj0, proj1, sums_a = attention_back(
        seq.at(order), normed_one, qkvs[:2], (mg0, mg1), g_out, (0, 1), n_img, patches, factor, n
    )
    g_w1 = seq.at(g_w1)
    red_down.land()
    red_down_two.land()
    red_up.land()
    red_w_two.land()
    got_w1 = core_swap(seq.at(g_w1))
    red_down_two.launch()
    red_up.launch()
    red_w_two.launch()
    got_w1 = seq.at(got_w1)
    red_w = Reduce(seq, (g_w0, got_w1), n)
    red_w.launch()
    tokens_grad, sums_one = input_back(
        seq.at(order), x_zero, after_grad, gain_one_f, (proj0, proj1, proj2, proj3), qkv_parts
    )
    tokens_grad = seq.at(tokens_grad)
    grad_tokens = compact(tokens_grad)
    red_w.land()
    red_w.launch()
    red_down_two.land()
    red_up.land()
    red_w_two.land()
    red_up.launch()
    red_w_two.launch()

    sums_proj = jnp.take(jnp.concatenate([sums_a, sums_b])[:, 0], group_order, axis=0)
    sums = [
        sums_proj[:, :quarter],
        sums_proj[:, 2 * quarter :],
        sums_two[0],
        sums_one[0],
        sums_one[1],
        sums_two[3],
        sums_two[1],
        sums_two[2],
    ]
    units = jnp.concatenate([g_bias_a, g_bias_b]).reshape(4, n, ffq)
    units = jnp.take(units, group_order, axis=0).transpose(1, 0, 2)
    packed = jnp.concatenate([s.reshape(n, rows) for s in sums] + [units.reshape(n, 4 * ffq)], axis=1)
    packed = jnp.take(packed, shard_order, axis=0)
    pad = -packed.shape[1] % 1024
    packed = jnp.pad(packed, ((0, 0), (0, pad))).reshape(n, -1, 128)
    packed = packed + seq.at(core_swap(seq.at(packed)))
    packed = packed + seq.at(x_swap(packed))
    for bit in range(n.bit_length() - 1):
        size = packed.shape[0] // 2
        packed = packed[:size] + swap(packed[size:], "fsdp", n, bit)
    vector = packed.reshape(-1)

    down_shard = add_half(red_down.rest(), x_swap(red_down_two.rest()))
    down_pieces = spread_quarters(down_shard, q)
    out_fc2 = jnp.concatenate(down_pieces).astype(full)
    red_up.land()
    up_pieces = spread_quarters(red_up.rest(), q)
    out_fc1 = (
        jnp.stack([p.reshape(rows, n, ffq) for p in up_pieces], axis=2).reshape(rows, ff).astype(full)
    )
    red_w.land()
    red_w.launch()
    red_w_two.land()
    two_shard = x_swap(seq.at(red_w_two.rest()))
    red_w.land()
    attn_pieces = spread_quarters(add_half(red_w.rest(), two_shard), seq.value)
    out_qkv = (
        jnp.stack([p[:, : 3 * quarter].reshape(rows, 3, quarter) for p in attn_pieces], axis=2)
        .reshape(rows, 3 * width)
        .astype(full)
    )
    out_out = jnp.stack([p[:, 3 * quarter :] for p in attn_pieces], axis=1).reshape(rows, width).astype(full)
    small_out = [vector[i * rows : (i + 1) * rows] for i in range(8)]
    out_bfc1 = vector[8 * rows : 8 * rows + 4 * ffq]
    o_bq, o_bv, o_bout, o_gone, o_sone, o_bfc2, o_gtwo, o_stwo = small_out
    return (
        block_out,
        grad_tokens,
        out_qkv,
        o_bq,
        o_bv,
        out_out,
        o_bout,
        o_gone,
        o_sone,
        out_fc1,
        out_bfc1,
        out_fc2,
        o_bfc2,
        o_gtwo,
        o_stwo,
    )


def solution(mesh):
    rows_split = P(("dp", "fsdp"), None)
    matrix = P("fsdp", None)
    vector = P("fsdp")
    return jax.shard_map(
        local,
        mesh=mesh,
        in_specs=(
            rows_split, P(("dp", "fsdp")), matrix, vector, vector, matrix, vector, vector, vector,
            matrix, vector, matrix, vector, vector, vector, rows_split,
        ),
        out_specs=(
            rows_split, rows_split, matrix, vector, vector, matrix, vector, vector, vector,
            matrix, vector, matrix, vector, vector, vector,
        ),
        check_vma=False,
    )
```

```python
import math

import jax
import jax.numpy as jnp
from jax import lax
from jax.experimental import pallas as pl
from jax.experimental.pallas import tpu as pltpu
from jax.sharding import PartitionSpec as P

HEADS = 16
GRID = 14
NSCALE = 16
norm_eps = 1e-06
half = jnp.bfloat16
full = jnp.float32


def xor_swap(value, axis, size, mask):
    return lax.ppermute(value, axis, [(i, i ^ mask) for i in range(size)])


def core_swap(value):
    return xor_swap(value, "dp", 4, 1)


def x_swap(value):
    return xor_swap(value, "dp", 4, 2)


def masks(bits):
    found = [0]
    for bit in bits:
        found = found + [m | (1 << bit) for m in found]
    return found


class Order:
    def __init__(self, value):
        self.value = value

    def at(self, value):
        value, self.value = lax.optimization_barrier((value, self.value))
        return value

    def land(self, value, *sent):
        value, flights = self.at((value, [s.flight for s in sent]))
        for s, flight in zip(sent, flights, strict=True):
            s.accept(flight)
        return value


class Sent:
    def __init__(self, flight):
        self.flight = flight

    def accept(self, value):
        self.value = value


class Gather:
    def __init__(self, seq, piece, n, bits):
        self.seq, self.held, self.n, self.bits = seq, piece[None], n, list(bits)

    def launch(self):
        self.held = self.seq.at(self.held)
        self.flight = xor_swap(self.held, "fsdp", self.n, 1 << self.bits.pop(0))

    def accept(self, value):
        self.got = value

    def join(self):
        self.held = jnp.concatenate([self.held, self.got])
        return self.held


def rounded_sum(terms, kind=half):
    return sum(t.astype(full) for t in terms).astype(kind)


class Reduce:
    def __init__(self, seq, terms, n, kind=half):
        self.kind = kind
        self.seq, self.n, self.axes = seq, n, list(range(n.bit_length() - 1))
        self.terms = [t.reshape((2,) * len(self.axes) + t.shape[1:]) for t in terms]

    def launch(self, bit=None, more=()):
        bit = self.axes[0] if bit is None else bit
        axis = self.axes.index(bit)
        self.axes.pop(axis)
        low, high = [
            [lax.index_in_dim(t, side, axis, keepdims=False) for t in self.terms] for side in (0, 1)
        ]
        self.terms = low
        self.flight = xor_swap(self.seq.at(rounded_sum([*high, *more], self.kind)), "fsdp", self.n, 1 << bit)

    def accept(self, value):
        self.terms = [*self.terms, value]

    def rest(self):
        while self.axes:
            self.launch()
            self.seq.land((), self)
        return self

    def piece(self):
        return rounded_sum(self.terms, self.kind)


class Spread:
    def __init__(self, seq, piece):
        self.seq, self.own = seq, seq.at(piece)
        self.flight = core_swap(self.own)

    def cross(self):
        self.pair = jnp.stack([self.own, self.got])
        self.flight = x_swap(self.seq.at(self.pair))

    def accept(self, value):
        self.got = value


ANYWHERE = pl.BlockSpec(memory_space=pl.ANY)
ON_CHIP = pl.BlockSpec(memory_space=pltpu.VMEM)
SCALARS = pl.BlockSpec(memory_space=pltpu.SMEM)


def dot(left, right, dim_left, dim_right):
    return lax.dot_general(
        left, right, (((dim_left,), (dim_right,)), ((), ())), preferred_element_type=full
    )


def call(kernel, name, operands, in_specs, outs, out_specs, scratch):
    return pl.pallas_call(
        kernel,
        out_shape=[jax.ShapeDtypeStruct(shape, kind) for shape, kind in outs],
        in_specs=in_specs,
        out_specs=out_specs,
        scratch_shapes=scratch,
        compiler_params=pltpu.CompilerParams(vmem_limit_bytes=58 * 2**20),
        name=name,
    )(*operands)


def loop(count, body, unroll=1):
    def step(i, carry):
        body(i)
        return carry

    lax.fori_loop(0, count, step, 0, unroll=unroll)


def tile(i, size):
    return pl.ds(pl.multiple_of(i * size, size), size)


def fetch(parts, order_ref, place, sem):
    base = 0
    for part in parts:

        def start(r, part=part, base=base):
            shard = r if order_ref is None else order_ref[base + r]
            pltpu.make_async_copy(part.at[r], place(shard), sem).start()

        loop(part.shape[0], start)
        base += part.shape[0]


def head_rows(s, q, n, rows, quarter):
    per = n // 4
    return pl.multiple_of(((s // per) ^ q) * quarter + (s % per) * rows, rows)


def pair_scores(q2, k2):
    first = lax.broadcasted_iota(jnp.int32, q2.shape, 1) < q2.shape[1] // 2
    both = apart(q2, first)
    return both, dot(k2, both, 1, 1), first


def apart(value, first):
    zero = jnp.zeros_like(value)
    return jnp.concatenate([jnp.where(first, value, zero), jnp.where(first, zero, value)])


def attention_forward(order, normed, bias, weights, n_img, patches, factor):
    groups, n_parts = len(weights), len(weights[0])
    wide = weights[0][0].shape[2]
    count, width = normed.shape
    rows = width // sum(part.shape[0] for part in weights[0])
    padded = count // n_img
    quarter = wide // 3

    def kernel(order_ref, normed_ref, bias_ref, *refs):
        w_refs, refs = refs[: groups * n_parts], refs[groups * n_parts :]
        qkv_refs, mixed_refs, refs = refs[:groups], refs[groups : 2 * groups], refs[2 * groups :]
        lse_refs, (w_held, sems) = refs[:groups], refs[groups:]
        for g in range(groups):
            fetch(
                [w.at[:, pl.ds(0, rows)] for w in w_refs[g * n_parts : (g + 1) * n_parts]],
                order_ref,
                lambda s, g=g: w_held.at[g, pl.ds(pl.multiple_of(s * rows, rows), rows)],
                sems.at[g],
            )
        for g in range(groups):
            pltpu.make_async_copy(w_held.at[g], w_held.at[g], sems.at[g]).wait()

            def project(t, g=g):
                at = tile(t, quarter)
                product = dot(normed_ref[...], w_held[g, :, at], 1, 0)
                qkv_refs[g][:, at] = (product + bias_ref[g, :, at]).astype(half)

            loop(3, project)

            def attend(i, g=g):
                at = tile(i // 2, padded)
                lanes = [pl.ds(pl.multiple_of(t * quarter + (i % 2) * 128, 128), 128) for t in range(3)]
                q2 = qkv_refs[g][at, lanes[0]] * factor
                k2 = qkv_refs[g][at, lanes[1]]
                v2 = qkv_refs[g][at, lanes[2]]
                _, scores, first = pair_scores(q2, k2)
                key = lax.broadcasted_iota(jnp.int32, scores.shape, 0)
                scores = jnp.where(key < patches, scores, -1e30)
                top = jnp.max(scores, axis=0, keepdims=True)
                raised = jnp.exp(scores - top)
                total = jnp.sum(raised, axis=0, keepdims=True)
                lse_refs[g][i] = top + jnp.log(total)
                out = dot((raised * (1.0 / total)).astype(half), v2, 0, 0)
                mixed_refs[g][at, lanes[0]] = jnp.where(first, out[:padded], out[padded:]).astype(half)

            loop(2 * n_img, attend, 2 * n_img)

    return call(
        kernel,
        "attention_forward",
        (order, normed, bias, *(part for w in weights for part in w)),
        [SCALARS, ON_CHIP, ON_CHIP] + [ANYWHERE] * (groups * n_parts),
        [((count, wide), half)] * groups
        + [((count, quarter), half)] * groups
        + [((2 * n_img, 1, 2 * padded), full)] * groups,
        [ON_CHIP] * (3 * groups),
        [pltpu.VMEM((groups, width, wide), half), pltpu.SemaphoreType.DMA((groups,))],
    )


def layer_norm(value, gain, shift):
    center = jnp.mean(value, axis=-1, keepdims=True)
    offset = value - center
    spread = jnp.mean(offset * offset, axis=-1, keepdims=True)
    return offset * lax.rsqrt(spread + norm_eps) * gain + shift


def layer_norm_back(value, grad, gain):
    center = jnp.mean(value, axis=-1, keepdims=True)
    offset = value - center
    scale = lax.rsqrt(jnp.mean(offset * offset, axis=-1, keepdims=True) + norm_eps)
    unit = offset * scale
    scaled = grad * gain
    inner = jnp.mean(scaled * unit, axis=-1, keepdims=True)
    return scale * (scaled - jnp.mean(scaled, axis=-1, keepdims=True) - unit * inner), grad * unit


def load_out(order_ref, out_refs, held, sem, n, rows, quarter):
    q = order_ref[n]
    for j in range(4):
        column = pl.multiple_of((q ^ j) * quarter, quarter)
        fetch(
            [out_refs[j % 2].at[:, :, pl.ds(j // 2 * quarter, quarter)]],
            order_ref,
            lambda s, column=column: held.at[
                pl.ds(head_rows(s, q, n, rows, quarter), rows), pl.ds(column, quarter)
            ],
            sem,
        )


CHUNK = 16
ROWS = 64


def attention_out(order, x_zero, mixed, outs, bias, gain, shift):
    count, width = x_zero.shape
    n, rows, _ = outs[0].shape
    quarter = mixed[0].shape[1]

    def kernel(order_ref, x_ref, bias_ref, gain_ref, shift_ref, *refs):
        mixed_refs, out_refs = refs[:4], refs[4:6]
        after_ref, normed_ref, held, sems = refs[6:]
        load_out(order_ref, out_refs, held, sems.at[0], n, rows, quarter)
        together = jnp.concatenate([m[...] for m in mixed_refs], axis=1)
        pltpu.make_async_copy(held, held, sems.at[0]).wait()
        after_ref[...] = dot(together, held[...], 1, 0)

        def finish(i):
            at = tile(i, CHUNK)
            after = x_ref[at] + (after_ref[at] + bias_ref[...])
            after_ref[at] = after
            normed_ref[at] = layer_norm(after, gain_ref[...], shift_ref[...]).astype(half)

        loop(count // CHUNK, finish, 13)

    return call(
        kernel,
        "attention_out",
        (order, x_zero, bias, gain, shift, *mixed, *outs),
        [SCALARS] + [ON_CHIP] * 8 + [ANYWHERE] * 2,
        [((count, width), full), ((count, width), half)],
        [ON_CHIP] * 2,
        [pltpu.VMEM((width, width), half), pltpu.SemaphoreType.DMA((1,))],
    )


def mlp(order, normed, cot, bias, ups, downs, down_start, carried=None, ending=None):
    groups = len(ups)
    count, width = normed.shape
    n, rows, _ = ups[0].shape
    hidden = bias.shape[2]
    share = hidden // n
    step = min(512, hidden)
    steps = hidden // step
    more = [] if carried is None else [*carried, *ending]

    def kernel(order_ref, normed_ref, cot_ref, bias_ref, *refs):
        more_refs, refs = refs[: len(more)], refs[len(more) :]
        up_refs, down_refs, refs = refs[:groups], refs[groups : 2 * groups], refs[2 * groups :]
        g_up_refs, g_down_refs, refs = refs[:groups], refs[groups : 2 * groups], refs[2 * groups :]
        g_bias_ref, out_ref, back_ref, refs = refs[0], refs[1], refs[2], refs[3:]
        up, down, pre, act, act_half, pre_half, g_up, g_down, sems, out_sems = refs[-10:]
        for g in range(groups):
            fetch(
                [up_refs[g].at[:, :, pl.ds(0, hidden)]],
                None,
                lambda s, g=g: up.at[g, pl.ds(pl.multiple_of(s * rows, rows), rows)],
                sems.at[g],
            )
            fetch(
                [down_refs[g].at[:, :, pl.ds(down_start, width)]],
                None,
                lambda s, g=g: down.at[g, pl.ds(pl.multiple_of(s * share, share), share)],
                sems.at[groups + g],
            )
        if more:
            out_ref[...] = more_refs[0][...]
            back_ref[...] = more_refs[1][...]
        else:
            out_ref[...] = jnp.zeros_like(out_ref)
            back_ref[...] = jnp.zeros_like(back_ref)
        for g in range(groups):
            pltpu.make_async_copy(up.at[g], up.at[g], sems.at[g]).wait()
            pltpu.make_async_copy(down.at[g], down.at[g], sems.at[groups + g]).wait()

            def part(t, g=g):
                at = tile(t, step)
                pre[...] = dot(normed_ref[...], up[g, :, at], 1, 0)
                act[...] = dot(cot_ref[...], down[g, at, :], 1, 1)

                def gelu(i):
                    some = tile(i, 2 * CHUNK)
                    x = pre[some] + bias_ref[g, :, at]
                    below = 0.5 * (1.0 + lax.erf(x * math.sqrt(0.5)))
                    density = jnp.exp(-0.5 * x * x) * (1.0 / math.sqrt(2.0 * math.pi))
                    act_half[some] = (x * below).astype(half)
                    pre_half[some] = (act[some] * (below + x * density)).astype(half)

                loop(count // CHUNK // 2, gelu)
                h = act_half[...]
                p = pre_half[...]
                out_ref[...] += dot(h, down[g, at, :], 1, 0)
                back_ref[...] += dot(p, up[g, :, at], 1, 1)
                g_down[g, at, :] = dot(h, cot_ref[...], 0, 0).astype(half)
                g_up[g, :, at] = dot(normed_ref[...], p, 0, 0).astype(half)
                g_bias_ref[g, :, at] = jnp.sum(p.astype(full), axis=0, keepdims=True)

            loop(steps, part)

            def send(r, g=g):
                s = order_ref[r]
                pltpu.make_async_copy(
                    g_up.at[g, pl.ds(pl.multiple_of(s * rows, rows), rows)],
                    g_up_refs[g].at[r],
                    out_sems.at[g],
                ).start()
                pltpu.make_async_copy(
                    g_down.at[g, pl.ds(pl.multiple_of(s * share, share), share)],
                    g_down_refs[g].at[r],
                    out_sems.at[groups + g],
                ).start()

            loop(n, send)
        if more:
            after_ref, end_ref, block_ref = more_refs[2], more_refs[3], refs[0]

            def finish(i):
                at = tile(i, CHUNK)
                block_ref[at] = (after_ref[at] + (out_ref[at] + end_ref[...])).astype(half)

            loop(count // CHUNK, finish)
        for g in range(groups):
            pltpu.make_async_copy(g_up_refs[g], g_up_refs[g], out_sems.at[g]).wait()
            pltpu.make_async_copy(g_down_refs[g], g_down_refs[g], out_sems.at[groups + g]).wait()

    outs = (
        [((n, rows, hidden), half)] * groups
        + [((n, share, width), half)] * groups
        + [((groups, 1, hidden), full), ((count, width), full), ((count, width), full)]
        + ([((count, width), half)] if more else [])
    )
    return call(
        kernel,
        "mlp",
        (order, normed, cot, bias, *more, *ups, *downs),
        [SCALARS] + [ON_CHIP] * (3 + len(more)) + [ANYWHERE] * (2 * groups),
        outs,
        [ANYWHERE] * (2 * groups) + [ON_CHIP] * (len(outs) - 2 * groups),
        [
            pltpu.VMEM((groups, width, hidden), half),
            pltpu.VMEM((groups, hidden, width), half),
            pltpu.VMEM((count, step), full),
            pltpu.VMEM((count, step), full),
            pltpu.VMEM((count, step), half),
            pltpu.VMEM((count, step), half),
            pltpu.VMEM((groups, width, hidden), half),
            pltpu.VMEM((groups, hidden, width), half),
            pltpu.SemaphoreType.DMA((2 * groups,)),
            pltpu.SemaphoreType.DMA((2 * groups,)),
        ],
    )


def attention_out_back(order, grad, after, cot, gain, mixed, outs):
    count, width = after.shape
    n, rows, _ = outs[0].shape
    quarter = mixed[0].shape[1]

    def kernel(order_ref, grad_ref, after_ref, cot_ref, gain_ref, *refs):
        mixed_refs, out_refs, refs = refs[:4], refs[4:6], refs[6:]
        after_grad_ref, mixed_grad_refs, g_out_ref, sums_ref = refs[0], refs[1:5], refs[5], refs[6]
        held, branch, terms, sems = refs[7:]
        load_out(order_ref, out_refs, held, sems.at[0], n, rows, quarter)
        terms[...] = jnp.zeros_like(terms)

        def fold(value):
            return jnp.sum(value.reshape(CHUNK // 8, 8, width), axis=0)

        def back(i):
            at = tile(i, CHUNK)
            incoming = grad_ref[at]
            part, gain_terms = layer_norm_back(after_ref[at], incoming, gain_ref[...])
            own = cot_ref[at].astype(full)
            total = own + part
            after_grad_ref[at] = total
            rounded = total.astype(half)
            branch[at] = rounded
            terms[0] += fold(rounded.astype(full))
            terms[1] += fold(gain_terms)
            terms[2] += fold(incoming)
            terms[3] += fold(own)

        loop(count // CHUNK, back, 13)
        for k in range(4):
            sums_ref[k] = jnp.sum(terms[k], axis=0, keepdims=True)
        pltpu.make_async_copy(held, held, sems.at[0]).wait()
        for j in range(4):
            mixed_grad_refs[j][...] = dot(branch[...], held[j * quarter : (j + 1) * quarter], 1, 1).astype(half)
            g_out_ref[j * quarter : (j + 1) * quarter] = dot(mixed_refs[j][...], branch[...], 0, 0).astype(half)

    return call(
        kernel,
        "attention_out_back",
        (order, grad, after, cot, gain, *mixed, *outs),
        [SCALARS] + [ON_CHIP] * 8 + [ANYWHERE] * 2,
        [((count, width), full)]
        + [((count, quarter), half)] * 4
        + [((width, width), half), ((4, 1, width), full)],
        [ON_CHIP] * 7,
        [
            pltpu.VMEM((width, width), half),
            pltpu.VMEM((count, width), half),
            pltpu.VMEM((4, 8, width), full),
            pltpu.SemaphoreType.DMA((1,)),
        ],
    )


def attention_back(order, normed, qkvs, lses, mixed_grads, g_out, which, n_img, patches, factor, n):
    groups = len(qkvs)
    count, width = normed.shape
    wide = qkvs[0].shape[1]
    quarter = wide // 3
    padded = count // n_img
    rows = width // n

    def kernel(order_ref, normed_ref, g_out_ref, *refs):
        qkv_refs, mg_refs, refs = refs[:groups], refs[groups : 2 * groups], refs[2 * groups :]
        lse_refs, refs = refs[:groups], refs[groups:]
        g_w_refs, proj_refs, sums_ref = refs[:groups], refs[groups : 2 * groups], refs[2 * groups]
        g_w, sems = refs[2 * groups + 1 :]
        q = order_ref[n]
        for g in range(groups):

            def send_out(r, g=g):
                at = head_rows(order_ref[r], q, n, rows, quarter)
                column = pl.multiple_of((q ^ which[g]) * quarter, quarter)
                pltpu.make_async_copy(
                    g_out_ref.at[pl.ds(at, rows), pl.ds(column, quarter)],
                    g_w_refs[g].at[r, :, pl.ds(wide, quarter)],
                    sems.at[g],
                ).start()

            loop(n, send_out)

            def attend(i, g=g):
                at = tile(i // 2, padded)
                lanes = [pl.ds(pl.multiple_of(t * quarter + (i % 2) * 128, 128), 128) for t in range(3)]
                q2 = qkv_refs[g][at, lanes[0]] * factor
                k2 = qkv_refs[g][at, lanes[1]]
                v2 = qkv_refs[g][at, lanes[2]]
                both, scores, first = pair_scores(q2, k2)
                key = lax.broadcasted_iota(jnp.int32, scores.shape, 0)
                probs = jnp.where(key < patches, jnp.exp(scores - lse_refs[g][i]), 0.0)
                o_both = apart(mg_refs[g][at, lanes[0]], first)
                g_probs = dot(v2, o_both, 1, 1)
                weighted = jnp.sum(probs * g_probs, axis=0, keepdims=True)
                g_scores = (probs * (g_probs - weighted)).astype(half)
                g_query = dot(g_scores, k2, 0, 0)
                g_query = jnp.where(first, g_query[:padded], g_query[padded:]) * factor
                proj_refs[g][at, lanes[0]] = g_query.astype(half)
                proj_refs[g][at, lanes[1]] = dot(g_scores, both, 1, 0).astype(half)
                proj_refs[g][at, lanes[2]] = dot(probs.astype(half), o_both, 1, 0).astype(half)

            loop(2 * n_img, attend, 4)

            def weigh(t, g=g):
                at = tile(t, quarter)
                some = proj_refs[g][:, at]
                g_w[g, :, at] = dot(normed_ref[...], some, 0, 0).astype(half)
                sums_ref[g, :, at] = jnp.sum(some.astype(full), axis=0, keepdims=True)

            loop(3, weigh)

            def send(r, g=g):
                at = pl.multiple_of(order_ref[r] * rows, rows)
                pltpu.make_async_copy(
                    g_w.at[g, pl.ds(at, rows)], g_w_refs[g].at[r, :, pl.ds(0, wide)], sems.at[g]
                ).start()

            loop(n, send)
        for g in range(groups):
            pltpu.make_async_copy(g_w_refs[g], g_w_refs[g], sems.at[g]).wait()

    return call(
        kernel,
        "attention_back",
        (order, normed, g_out, *qkvs, *mixed_grads, *lses),
        [SCALARS] + [ON_CHIP] * (2 + 3 * groups),
        [((n, rows, wide + quarter), half)] * groups
        + [((count, wide), half)] * groups
        + [((groups, 1, wide), full)],
        [ANYWHERE] * groups + [ON_CHIP] * (groups + 1),
        [pltpu.VMEM((groups, width, wide), half), pltpu.SemaphoreType.DMA((groups,))],
    )


def input_back(order, x_zero, after_grad, gain, projs, weights):
    count, width = x_zero.shape
    wide = weights[0][0].shape[2]
    rows = width // sum(part.shape[0] for part in weights[0])
    parts = [part for w in weights for part in w]
    n_parts = len(weights[0])

    def kernel(order_ref, x_ref, after_ref, gain_ref, *refs):
        proj_refs, w_refs = refs[:4], refs[4 : 4 + len(parts)]
        token_ref, sums_ref, held, terms, sems = refs[4 + len(parts) :]
        for j in range(4):
            fetch(
                [w.at[:, pl.ds(0, rows)] for w in w_refs[j * n_parts : (j + 1) * n_parts]],
                order_ref,
                lambda s, j=j: held.at[j, pl.ds(pl.multiple_of(s * rows, rows), rows)],
                sems.at[j],
            )
        for j in range(4):
            pltpu.make_async_copy(held.at[j], held.at[j], sems.at[j]).wait()
            product = dot(proj_refs[j][...], held[j], 1, 1)
            if j == 0:
                token_ref[...] = product
            else:
                token_ref[...] += product
        terms[...] = jnp.zeros_like(terms)

        def fold(value):
            return jnp.sum(value.reshape(ROWS // 8, 8, width), axis=0)

        def back(i):
            at = tile(i, ROWS)
            incoming = token_ref[at]
            part, gain_terms = layer_norm_back(x_ref[at], incoming, gain_ref[...])
            token_ref[at] = after_ref[at] + part
            terms[0] += fold(gain_terms)
            terms[1] += fold(incoming)

        loop(count // ROWS, back)
        for k in range(2):
            sums_ref[k] = jnp.sum(terms[k], axis=0, keepdims=True)

    return call(
        kernel,
        "input_back",
        (order, x_zero, after_grad, gain, *projs, *parts),
        [SCALARS] + [ON_CHIP] * 7 + [ANYWHERE] * len(parts),
        [((count, width), full), ((2, 1, width), full)],
        [ON_CHIP] * 2,
        [
            pltpu.VMEM((4, width, wide), half),
            pltpu.VMEM((2, 8, width), full),
            pltpu.SemaphoreType.DMA((4,)),
        ],
    )


def payloads(which, w_fc1, w_fc2):
    rows, ff = w_fc1.shape
    full_share, width = w_fc2.shape
    share = full_share // 4
    n = ff // full_share
    hidden = n * share
    own, across = which
    if share % 128:
        fc1 = [lax.dynamic_slice(w_fc1, (0, (4 * s + own) * share), (rows, share)) for s in range(n)]
        fc2 = [lax.dynamic_slice(w_fc2, (g * share, 0), (share, width)).astype(half) for g in which]
        rest = jnp.concatenate([*fc1, fc2[0].reshape(rows, -1).astype(full)], axis=1)
        return rest.astype(half), fc2[1]

    def kernel(which_ref, fc1_ref, fc2_ref, rest_ref, two_ref):
        for s in range(n):
            at = pl.ds(pl.multiple_of((4 * s + which_ref[0]) * share, share), share)
            rest_ref[:, s * share : (s + 1) * share] = fc1_ref[:, at].astype(half)
        rest_ref[:, hidden : hidden + width] = fc2_ref[tile(which_ref[0], share), :].astype(half)
        two_ref[...] = fc2_ref[tile(which_ref[1], share), :].astype(half)

    return call(
        kernel,
        "payloads",
        (jnp.stack(which), w_fc1, w_fc2),
        [SCALARS] + [ON_CHIP] * 2,
        [((rows, hidden + width), half), ((share, width), half)],
        [ON_CHIP] * 2,
        [],
    )


def finish_mlp(q, pair, there, n):
    _, _, rows, width = pair.shape
    hidden = width
    share = hidden // n
    if share % 128:
        pieces = natural_quarters(q, pair, there)
        fc1 = jnp.stack([p[0].reshape(rows, n, share) for p in pieces], axis=2).reshape(rows, 4 * hidden)
        return fc1.astype(full), jnp.concatenate([p[1] for p in pieces]).astype(full)

    def kernel(q_ref, pair_ref, there_ref, fc1_ref, fc2_ref):
        for j in range(4):
            g = q_ref[0] ^ j
            held = pair_ref if j < 2 else there_ref
            for s in range(n):
                at = pl.ds(pl.multiple_of((4 * s + g) * share, share), share)
                fc1_ref[:, at] = held[j % 2, 0, :, s * share : (s + 1) * share].astype(full)
            fc2_ref[tile(g, rows), :] = held[j % 2, 1].astype(full)

    return call(
        kernel,
        "finish_mlp",
        (q[None], pair, there),
        [SCALARS, ON_CHIP, ON_CHIP],
        [((rows, 4 * hidden), full), ((4 * rows, width), full)],
        [ON_CHIP] * 2,
        [],
    )


def natural_quarters(q, pair, there):
    pieces = [pair[0], pair[1], there[0], there[1]]
    once = [jnp.where((q & 1) == 1, pieces[i ^ 1], pieces[i]) for i in range(4)]
    return [jnp.where(q >= 2, once[i ^ 2], once[i]) for i in range(4)]


def finish_attention(q, pair, there):
    _, rows, width = pair.shape
    quarter = width // 4

    def kernel(q_ref, pair_ref, there_ref, qkv_ref, out_ref):
        for j in range(4):
            g = q_ref[0] ^ j
            held = pair_ref if j < 2 else there_ref
            for t in range(3):
                at = pl.ds(pl.multiple_of(t * width + g * quarter, quarter), quarter)
                qkv_ref[:, at] = held[j % 2, :, t * quarter : (t + 1) * quarter].astype(full)
            out_ref[:, tile(g, quarter)] = held[j % 2, :, 3 * quarter :].astype(full)

    return call(
        kernel,
        "finish_attention",
        (q[None], pair, there),
        [SCALARS, ON_CHIP, ON_CHIP],
        [((rows, 3 * width), full), ((rows, width), full)],
        [ON_CHIP] * 2,
        [],
    )


def table(codes, width):
    ratio = 0.3 * jnp.exp(codes.astype(full) * (math.log(10.0 / 0.3) / (NSCALE - 1)))
    quarter = width // 4
    omega = jnp.exp(jnp.arange(quarter).astype(full) * (-math.log(10000.0) / quarter))
    steps = jnp.arange(GRID, dtype=jnp.int32).astype(full)
    angle = ratio[:, None, None] * steps[None, :, None] * omega[None, None, :]
    return jnp.concatenate([jnp.sin(angle), jnp.cos(angle)], axis=-1)


def local(
    tokens,
    scale_codes,
    w_qkv,
    b_q,
    b_v,
    w_out,
    b_out,
    gain_one,
    shift_one,
    w_fc1,
    b_fc1,
    w_fc2,
    b_fc2,
    gain_two,
    shift_two,
    cotangent,
):
    n = lax.axis_size("fsdp")
    q = lax.axis_index("dp")
    f = lax.axis_index("fsdp")
    row_count, width = tokens.shape
    rows = width // n
    ff = b_fc1.shape[0] * n
    ffq = ff // n // 4
    hidden = n * ffq
    quarter = width // 4
    n_img = scale_codes.shape[0]
    patches = row_count // n_img
    padded = -(-patches // 16) * 16
    factor = 1.0 / math.sqrt(width // HEADS)
    seq = Order(q)
    bits = list(reversed(range(n.bit_length() - 1)))
    near = min(1, len(bits) - 1)
    shard_order = jnp.asarray(masks(bits), jnp.int32) ^ f
    group_order = jnp.arange(4, dtype=jnp.int32) ^ q
    order = jnp.concatenate([shard_order, q[None]])

    def last_three(chain):
        while len(chain.bits) > 3:
            chain.launch()
            seq.land((), chain)
            chain.join()
        return chain

    small = jnp.concatenate(
        [b_q, b_v, b_out, gain_one, shift_one, b_fc2, gain_two, shift_two, b_fc1]
    )
    below = -(-small.shape[0] // (3 * quarter * 16)) * 16
    small = jnp.pad(small, (0, below * 3 * quarter - small.shape[0])).reshape(below, 3 * quarter)
    qkv_own = jnp.concatenate(
        [lax.dynamic_slice(w_qkv, (0, t * width + q * quarter), (rows, quarter)) for t in range(3)], axis=1
    )
    qkv = last_three(Gather(seq, jnp.concatenate([qkv_own, small]).astype(half), n, bits))
    qkv.launch()
    rest_own, two_own = payloads([seq.at(q), q ^ 2], w_fc1, w_fc2)
    rest_own, two_own = seq.land((rest_own, two_own), qkv)
    rest = Sent(lax.all_gather(rest_own, "fsdp", axis=0, tiled=False))
    two = Sent(lax.all_gather(two_own, "fsdp", axis=0, tiled=False))
    out_own = [lax.dynamic_slice(w_out, (0, g * quarter), (rows, quarter)) for g in (q, q ^ 2)]
    out = last_three(Gather(seq, jnp.concatenate(out_own, axis=1).astype(half), n, bits))

    def spread_rows(value):
        split = value.reshape(n_img, patches, width)
        return jnp.pad(split, ((0, 0), (0, padded - patches), (0, 0)))

    def compact(value):
        return value.reshape(n_img, padded, width)[:, :patches].reshape(row_count, width)

    qkv.join()
    qkv.launch()
    out.launch()
    spread_tokens = seq.land(spread_rows(seq.at(tokens)), qkv)
    qkv_near = qkv.join()
    qkv.launch()
    near_b, near_c = Sent(core_swap(qkv.held)), Sent(x_swap(qkv.held))
    seq.land((), out)
    out.join()
    out.launch()
    places = table(scale_codes, width)
    row_place = jnp.broadcast_to(places[:, :, None], (n_img, GRID, GRID, width // 2))
    col_place = jnp.broadcast_to(places[:, None], (n_img, GRID, GRID, width // 2))
    place = jnp.concatenate([row_place, col_place], axis=-1).reshape(n_img, patches, width)
    place = jnp.pad(place, ((0, 0), (0, padded - patches), (0, 0)))
    x_zero = (seq.at(spread_tokens).astype(full) + place).reshape(-1, width)
    x_zero = seq.land(x_zero, qkv, near_b)
    qkv_far = seq.at(qkv.got)
    far_b, far_c = Sent(core_swap(qkv_far)), Sent(x_swap(qkv_far))
    small_held = jnp.concatenate([qkv_near[:, rows:], qkv_far[:, rows:]]).reshape(n, -1)
    inverse = jnp.zeros((n,), jnp.int32).at[shard_order].set(jnp.arange(n, dtype=jnp.int32))
    small_all = jnp.take(small_held, inverse, axis=0).astype(full)
    vectors = [small_all[:, i * rows : (i + 1) * rows].reshape(1, width) for i in range(8)]
    full_bq, full_bv, full_bout, gain_one_f, shift_one_f, full_bfc2, gain_two_f, shift_two_f = vectors
    bias_units = small_all[:, 8 * rows : 8 * rows + 4 * ffq].reshape(n, 4, ffq)
    bias_fc1 = jnp.take(bias_units, group_order, axis=1).transpose(1, 0, 2).reshape(4, 1, hidden)
    bias_q = jnp.take(full_bq.reshape(4, quarter), group_order, axis=0)
    bias_v = jnp.take(full_bv.reshape(4, quarter), group_order, axis=0)
    bias_qkv = jnp.concatenate([bias_q, jnp.zeros_like(bias_q), bias_v], axis=1)[:, None]
    normed_one = layer_norm(x_zero, gain_one_f, shift_one_f).astype(half)
    normed_one = seq.land(normed_one, far_b, out)
    out.join()
    out.launch()

    first = attention_forward(
        seq.at(order), normed_one, bias_qkv[:2], ((qkv_near, qkv_far), (near_b.value, far_b.value)),
        n_img, patches, factor,
    )
    first = (seq.land(first[0], near_c, far_c), *first[1:])
    near_c, far_c = seq.at((near_c.value, far_c.value))
    near_d, far_d = Sent(core_swap(near_c)), Sent(core_swap(far_c))
    cot = seq.land(spread_rows(cotangent).reshape(-1, width), near_d, far_d, out)
    out_a = seq.at(out.join())
    out_b = Sent(core_swap(out_a))
    second = attention_forward(
        seq.at(order), normed_one, bias_qkv[2:], ((near_c, far_c), (near_d.value, far_d.value)),
        n_img, patches, factor,
    )
    second = (seq.land(second[0], out_b), *second[1:])
    outs = (out_a, out_b.value)
    qkv_parts = (
        (qkv_near, qkv_far), (near_b.value, far_b.value), (near_c, far_c), (near_d.value, far_d.value)
    )
    qkvs = (*first[:2], *second[:2])
    mixed = (*first[2:4], *second[2:4])
    lses = (*first[4:], *second[4:])
    after_attn, normed_two = attention_out(
        seq.at(order), x_zero, mixed, outs, full_bout, gain_two_f, shift_two_f
    )
    normed_two = seq.land(normed_two, rest)
    rest_a = seq.at(rest.value)
    rest_b = Sent(core_swap(rest_a))
    up_c = Sent(x_swap(seq.at(rest_a[:, :, :hidden])))
    seq.land((), rest_b)
    rests = (rest_a, rest_b.value)

    g_up0, g_up1, g_down0, g_down1, g_bias_a, out_sum, back_sum = mlp(
        seq.at(order), normed_two, cot, bias_fc1[:2], rests, rests, hidden
    )
    g_up1, g_down1 = seq.land((g_up1, g_down1), up_c, two)
    up_c, two = seq.at((up_c.value, two.value))
    up_d, two_d = Sent(core_swap(up_c)), Sent(core_swap(two))
    up_1, down_1 = Sent(core_swap(g_up1)), Sent(core_swap(g_down1))
    seq.land((), up_d, two_d, up_1, down_1)
    red_up = Reduce(seq, (g_up0, up_1.value), n)
    red_up.launch()
    red_down = Reduce(seq, (g_down0, down_1.value), n)
    red_down.launch(near)
    g_up2, g_up3, g_down2, g_down3, g_bias_b, _, grad_two_in, block = mlp(
        seq.at(order), normed_two, cot, bias_fc1[2:], (up_c, up_d.value), (two, two_d.value), 0,
        (out_sum, back_sum), (after_attn, full_bfc2),
    )
    block_out = compact(block)
    g_up3, g_down3 = seq.land((g_up3, g_down3), red_up, red_down)
    up_3, down_3 = Sent(core_swap(g_up3)), Sent(core_swap(g_down3))
    red_up.launch()
    red_down.launch()
    seq.land((), up_3, down_3)
    red_up_two = Reduce(seq, (g_up2, up_3.value), n)
    red_up_two.launch()
    red_down_two = Reduce(seq, (g_down2, down_3.value), n)
    red_down_two.launch(near)

    after_grad, mg0, mg1, mg2, mg3, g_out, sums_two = attention_out_back(
        seq.at(order), grad_two_in, after_attn, cot, gain_two_f, mixed, outs
    )
    mg2 = seq.land(mg2, red_up, red_down)
    red_up.launch()
    red_down.launch()
    g_w2, g_w3, proj2, proj3, sums_b = attention_back(
        seq.at(order), normed_one, qkvs[2:], lses[2:], (mg2, mg3), g_out, (2, 3), n_img, patches, factor, n
    )
    g_w3 = seq.land(g_w3, red_up, red_down, red_up_two, red_down_two)
    w_3 = Sent(core_swap(g_w3))
    red_up_two.launch()
    red_down_two.launch()
    seq.land((), w_3)
    middle = n // 2
    half_shape = (2,) * (len(bits) - 1)
    w_high = Sent(x_swap(seq.at(rounded_sum([g_w2[middle:], w_3.value[middle:]]))))
    g_w0, g_w1, proj0, proj1, sums_a = attention_back(
        seq.at(order), normed_one, qkvs[:2], lses[:2], (mg0, mg1), g_out, (0, 1), n_img, patches, factor, n
    )
    g_w1 = seq.land(g_w1, red_up_two, red_down_two, w_high)
    w_1 = Sent(core_swap(g_w1))
    red_up_two.launch()
    red_down_two.launch()
    seq.land((), w_1)
    red_w = Reduce(seq, (g_w0, w_1.value), n)
    red_w.launch(0, [w_high.value.reshape(half_shape + w_high.value.shape[1:])])
    w_low = Sent(x_swap(seq.at(rounded_sum([g_w2[:middle], w_3.value[:middle]]))))
    tokens_grad, sums_one = input_back(
        seq.at(order), x_zero, after_grad, gain_one_f, (proj0, proj1, proj2, proj3), qkv_parts
    )
    sums_one = seq.land(sums_one, red_up_two, red_down_two, red_w, w_low)
    red_w.terms = [*red_w.terms, w_low.value.reshape(half_shape + w_low.value.shape[1:])]
    while len(red_w.axes) > 2:
        red_w.launch()
        seq.land((), red_w)
    red_w.launch()
    for chain in (red_up, red_up_two, red_down, red_down_two):
        chain.rest()
    cross = Sent(x_swap(seq.at(jnp.stack([red_up_two.piece(), red_down_two.piece()]))))

    sums_proj = jnp.take(jnp.concatenate([sums_a, sums_b])[:, 0], group_order, axis=0)
    sums = [
        sums_proj[:, :quarter],
        sums_proj[:, 2 * quarter :],
        sums_two[0],
        sums_one[0],
        sums_one[1],
        sums_two[3],
        sums_two[1],
        sums_two[2],
    ]
    units = jnp.concatenate([g_bias_a, g_bias_b]).reshape(4, n, ffq)
    units = jnp.take(units, group_order, axis=0).transpose(1, 0, 2)
    packed = jnp.concatenate([s.reshape(n, rows) for s in sums] + [units.reshape(n, 4 * ffq)], axis=1)
    packed = jnp.take(packed, shard_order, axis=0)
    pad = -packed.shape[1] % 1024
    packed = jnp.pad(packed, ((0, 0), (0, pad))).reshape(n, -1, 128)
    small_sum = Reduce(seq, (packed,), n, full)
    stage = 0
    while small_sum.axes:
        small_sum.launch()
        if small_sum.axes:
            seq.land((), small_sum)
            if stage == 1:
                seq.land((), red_w)
                red_w.launch()
        else:
            seq.land((), small_sum, cross)
        stage += 1
    packed = seq.at(small_sum.piece())
    peers = Sent([xor_swap(packed, "dp", 4, m) for m in (1, 2, 3)])
    mlp_spread = Spread(
        seq,
        jnp.stack([rounded_sum([*red_up.terms, cross.value[0]]), rounded_sum([*red_down.terms, cross.value[1]])]),
    )
    seq.land((), mlp_spread, peers)
    vector = (packed + sum(peers.value)).reshape(-1)
    mlp_spread.cross()
    block_out, tokens_grad = seq.at((block_out, tokens_grad))
    grad_tokens = compact(tokens_grad)
    if len(bits) < 3:
        red_w.rest()
    else:
        seq.land((), red_w)
    w_spread = Spread(seq, red_w.piece())
    seq.land((), w_spread)
    w_spread.cross()
    seq.land((), mlp_spread)
    out_fc1, out_fc2 = finish_mlp(q, mlp_spread.pair, mlp_spread.got, n)
    out_fc2 = seq.land(out_fc2, w_spread)
    out_qkv, out_out = finish_attention(seq.value, w_spread.pair, w_spread.got)
    small_out = [vector[i * rows : (i + 1) * rows] for i in range(8)]
    out_bfc1 = vector[8 * rows : 8 * rows + 4 * ffq]
    o_bq, o_bv, o_bout, o_gone, o_sone, o_bfc2, o_gtwo, o_stwo = small_out
    return (
        block_out,
        grad_tokens,
        out_qkv,
        o_bq,
        o_bv,
        out_out,
        o_bout,
        o_gone,
        o_sone,
        out_fc1,
        out_bfc1,
        out_fc2,
        o_bfc2,
        o_gtwo,
        o_stwo,
    )


def solution(mesh):
    rows_split = P(("dp", "fsdp"), None)
    matrix = P("fsdp", None)
    vector = P("fsdp")
    return jax.shard_map(
        local,
        mesh=mesh,
        in_specs=(
            rows_split, P(("dp", "fsdp")), matrix, vector, vector, matrix, vector, vector, vector,
            matrix, vector, matrix, vector, vector, vector, rows_split,
        ),
        out_specs=(
            rows_split, rows_split, matrix, vector, vector, matrix, vector, vector, vector,
            matrix, vector, matrix, vector, vector, vector,
        ),
        check_vma=False,
    )
```

```python
import math

import jax
import jax.numpy as jnp
from jax import lax
from jax.experimental import pallas as pl
from jax.experimental.pallas import tpu as pltpu
from jax.sharding import PartitionSpec as P

HEADS = 16
GRID = 14
NSCALE = 16
norm_eps = 1e-06
half = jnp.bfloat16
full = jnp.float32


def xor_swap(value, axis, size, mask):
    return lax.ppermute(value, axis, [(i, i ^ mask) for i in range(size)])


def core_swap(value):
    return xor_swap(value, "dp", 4, 1)


def x_swap(value):
    return xor_swap(value, "dp", 4, 2)


def masks(bits):
    found = [0]
    for bit in bits:
        found = found + [m | (1 << bit) for m in found]
    return found


class Order:
    def __init__(self, value):
        self.value = value

    def at(self, value):
        value, self.value = lax.optimization_barrier((value, self.value))
        return value

    def land(self, value, *sent):
        value, flights = self.at((value, [s.flight for s in sent]))
        for s, flight in zip(sent, flights, strict=True):
            s.accept(flight)
        return value


class Sent:
    def __init__(self, flight):
        self.flight = flight

    def accept(self, value):
        self.value = value


class Gather:
    def __init__(self, seq, piece, n, bits):
        self.seq, self.held, self.n, self.bits = seq, piece[None], n, list(bits)

    def launch(self):
        self.held = self.seq.at(self.held)
        self.flight = xor_swap(self.held, "fsdp", self.n, 1 << self.bits.pop(0))

    def accept(self, value):
        self.got = value

    def join(self):
        self.held = jnp.concatenate([self.held, self.got])
        return self.held


def rounded_sum(terms, kind=half):
    return sum(t.astype(full) for t in terms).astype(kind)


class Reduce:
    def __init__(self, seq, terms, n, kind=half):
        self.kind = kind
        self.seq, self.n, self.axes = seq, n, list(range(n.bit_length() - 1))
        self.terms = [t.reshape((2,) * len(self.axes) + t.shape[1:]) for t in terms]

    def launch(self, bit=None, more=()):
        bit = self.axes[0] if bit is None else bit
        axis = self.axes.index(bit)
        self.axes.pop(axis)
        low, high = [
            [lax.index_in_dim(t, side, axis, keepdims=False) for t in self.terms] for side in (0, 1)
        ]
        self.terms = low
        self.flight = xor_swap(self.seq.at(rounded_sum([*high, *more], self.kind)), "fsdp", self.n, 1 << bit)

    def accept(self, value):
        self.terms = [*self.terms, value]

    def rest(self):
        while self.axes:
            self.launch()
            self.seq.land((), self)
        return self

    def piece(self):
        return rounded_sum(self.terms, self.kind)


class Spread:
    def __init__(self, seq, piece):
        self.seq, self.pieces = seq, [seq.at(piece)]
        self.flight = [core_swap(self.pieces[0]), x_swap(self.pieces[0])]

    def cross(self):
        self.flight = [core_swap(self.seq.at(self.pieces[2]))]

    def accept(self, value):
        self.pieces += value


ANYWHERE = pl.BlockSpec(memory_space=pl.ANY)
ON_CHIP = pl.BlockSpec(memory_space=pltpu.VMEM)
SCALARS = pl.BlockSpec(memory_space=pltpu.SMEM)


def dot(left, right, dim_left, dim_right):
    return lax.dot_general(
        left, right, (((dim_left,), (dim_right,)), ((), ())), preferred_element_type=full
    )


def call(kernel, name, operands, in_specs, outs, out_specs, scratch):
    return pl.pallas_call(
        kernel,
        out_shape=[jax.ShapeDtypeStruct(shape, kind) for shape, kind in outs],
        in_specs=in_specs,
        out_specs=out_specs,
        scratch_shapes=scratch,
        compiler_params=pltpu.CompilerParams(vmem_limit_bytes=58 * 2**20),
        name=name,
    )(*operands)


def loop(count, body, unroll=1):
    def step(i, carry):
        body(i)
        return carry

    lax.fori_loop(0, count, step, 0, unroll=unroll)


def tile(i, size):
    return pl.ds(pl.multiple_of(i * size, size), size)


def fetch(parts, order_ref, place, sem):
    base = 0
    for part in parts:

        def start(r, part=part, base=base):
            shard = r if order_ref is None else order_ref[base + r]
            pltpu.make_async_copy(part.at[r], place(shard), sem).start()

        loop(part.shape[0], start)
        base += part.shape[0]


def head_rows(s, q, n, rows, quarter):
    per = n // 4
    return pl.multiple_of(((s // per) ^ q) * quarter + (s % per) * rows, rows)


def pair_scores(q2, k2):
    first = lax.broadcasted_iota(jnp.int32, q2.shape, 1) < q2.shape[1] // 2
    both = apart(q2, first)
    return both, dot(k2, both, 1, 1), first


def apart(value, first):
    zero = jnp.zeros_like(value)
    return jnp.concatenate([jnp.where(first, value, zero), jnp.where(first, zero, value)])


def attention_forward(order, normed, bias, weights, n_img, patches, factor):
    groups, n_parts = len(weights), len(weights[0])
    wide = weights[0][0].shape[2]
    count, width = normed.shape
    rows = width // sum(part.shape[0] for part in weights[0])
    padded = count // n_img
    quarter = wide // 3

    def kernel(order_ref, normed_ref, bias_ref, *refs):
        w_refs, refs = refs[: groups * n_parts], refs[groups * n_parts :]
        qkv_refs, mixed_refs, refs = refs[:groups], refs[groups : 2 * groups], refs[2 * groups :]
        lse_refs, (w_held, sems) = refs[:groups], refs[groups:]
        for g in range(groups):
            fetch(
                [w.at[:, pl.ds(0, rows)] for w in w_refs[g * n_parts : (g + 1) * n_parts]],
                order_ref,
                lambda s, g=g: w_held.at[g, pl.ds(pl.multiple_of(s * rows, rows), rows)],
                sems.at[g],
            )
        for g in range(groups):
            pltpu.make_async_copy(w_held.at[g], w_held.at[g], sems.at[g]).wait()

            def project(t, g=g):
                at = tile(t, quarter)
                product = dot(normed_ref[...], w_held[g, :, at], 1, 0)
                qkv_refs[g][:, at] = (product + bias_ref[g, :, at]).astype(half)

            loop(3, project)

            def attend(i, g=g):
                at = tile(i // 2, padded)
                lanes = [pl.ds(pl.multiple_of(t * quarter + (i % 2) * 128, 128), 128) for t in range(3)]
                q2 = qkv_refs[g][at, lanes[0]] * factor
                k2 = qkv_refs[g][at, lanes[1]]
                v2 = qkv_refs[g][at, lanes[2]]
                _, scores, first = pair_scores(q2, k2)
                key = lax.broadcasted_iota(jnp.int32, scores.shape, 0)
                scores = jnp.where(key < patches, scores, -1e30)
                top = jnp.max(scores, axis=0, keepdims=True)
                raised = jnp.exp(scores - top)
                total = jnp.sum(raised, axis=0, keepdims=True)
                lse_refs[g][i] = top + jnp.log(total)
                out = dot((raised * (1.0 / total)).astype(half), v2, 0, 0)
                mixed_refs[g][at, lanes[0]] = jnp.where(first, out[:padded], out[padded:]).astype(half)

            loop(2 * n_img, attend, 2 * n_img)

    return call(
        kernel,
        "attention_forward",
        (order, normed, bias, *(part for w in weights for part in w)),
        [SCALARS, ON_CHIP, ON_CHIP] + [ANYWHERE] * (groups * n_parts),
        [((count, wide), half)] * groups
        + [((count, quarter), half)] * groups
        + [((2 * n_img, 1, 2 * padded), full)] * groups,
        [ON_CHIP] * (3 * groups),
        [pltpu.VMEM((groups, width, wide), half), pltpu.SemaphoreType.DMA((groups,))],
    )


def layer_norm(value, gain, shift):
    center = jnp.mean(value, axis=-1, keepdims=True)
    offset = value - center
    spread = jnp.mean(offset * offset, axis=-1, keepdims=True)
    return offset * lax.rsqrt(spread + norm_eps) * gain + shift


def layer_norm_back(value, grad, gain):
    center = jnp.mean(value, axis=-1, keepdims=True)
    offset = value - center
    scale = lax.rsqrt(jnp.mean(offset * offset, axis=-1, keepdims=True) + norm_eps)
    unit = offset * scale
    scaled = grad * gain
    inner = jnp.mean(scaled * unit, axis=-1, keepdims=True)
    return scale * (scaled - jnp.mean(scaled, axis=-1, keepdims=True) - unit * inner), grad * unit


def load_out(order_ref, out_refs, held, sem, n, rows, quarter):
    q = order_ref[n]
    for j in range(4):
        column = pl.multiple_of((q ^ j) * quarter, quarter)
        fetch(
            [out_refs[j % 2].at[:, :, pl.ds(j // 2 * quarter, quarter)]],
            order_ref,
            lambda s, column=column: held.at[
                pl.ds(head_rows(s, q, n, rows, quarter), rows), pl.ds(column, quarter)
            ],
            sem,
        )


CHUNK = 16
ROWS = 64


def attention_out(order, x_zero, mixed, outs, bias, gain, shift):
    count, width = x_zero.shape
    n, rows, _ = outs[0].shape
    quarter = mixed[0].shape[1]

    def kernel(order_ref, x_ref, bias_ref, gain_ref, shift_ref, *refs):
        mixed_refs, out_refs = refs[:4], refs[4:6]
        after_ref, normed_ref, held, sems = refs[6:]
        load_out(order_ref, out_refs, held, sems.at[0], n, rows, quarter)
        together = jnp.concatenate([m[...] for m in mixed_refs], axis=1)
        pltpu.make_async_copy(held, held, sems.at[0]).wait()
        after_ref[...] = dot(together, held[...], 1, 0)

        def finish(i):
            at = tile(i, CHUNK)
            after = x_ref[at] + (after_ref[at] + bias_ref[...])
            after_ref[at] = after
            normed_ref[at] = layer_norm(after, gain_ref[...], shift_ref[...]).astype(half)

        loop(count // CHUNK, finish, 13)

    return call(
        kernel,
        "attention_out",
        (order, x_zero, bias, gain, shift, *mixed, *outs),
        [SCALARS] + [ON_CHIP] * 8 + [ANYWHERE] * 2,
        [((count, width), full), ((count, width), half)],
        [ON_CHIP] * 2,
        [pltpu.VMEM((width, width), half), pltpu.SemaphoreType.DMA((1,))],
    )


def mlp(order, normed, cot, bias, ups, downs, down_start, carried=None, ending=None):
    groups = len(ups)
    count, width = normed.shape
    n, rows, _ = ups[0].shape
    hidden = bias.shape[2]
    share = hidden // n
    step = min(512, hidden)
    steps = hidden // step
    more = [] if carried is None else [*carried, *ending]

    def kernel(order_ref, normed_ref, cot_ref, bias_ref, *refs):
        more_refs, refs = refs[: len(more)], refs[len(more) :]
        up_refs, down_refs, refs = refs[:groups], refs[groups : 2 * groups], refs[2 * groups :]
        grad_refs, refs = refs[:groups], refs[groups:]
        g_bias_ref, out_ref, back_ref, refs = refs[0], refs[1], refs[2], refs[3:]
        up, down, pre, act, act_half, pre_half, g_up, g_down, sems, out_sems = refs[-10:]
        for g in range(groups):
            fetch(
                [up_refs[g].at[:, :, pl.ds(0, hidden)]],
                None,
                lambda s, g=g: up.at[g, pl.ds(pl.multiple_of(s * rows, rows), rows)],
                sems.at[g],
            )
            fetch(
                [down_refs[g].at[:, :, pl.ds(down_start, width)]],
                None,
                lambda s, g=g: down.at[g, pl.ds(pl.multiple_of(s * share, share), share)],
                sems.at[groups + g],
            )
        if more:
            out_ref[...] = more_refs[0][...]
            back_ref[...] = more_refs[1][...]
        else:
            out_ref[...] = jnp.zeros_like(out_ref)
            back_ref[...] = jnp.zeros_like(back_ref)
        for g in range(groups):
            pltpu.make_async_copy(up.at[g], up.at[g], sems.at[g]).wait()
            pltpu.make_async_copy(down.at[g], down.at[g], sems.at[groups + g]).wait()

            def part(t, g=g):
                at = tile(t, step)
                pre[...] = dot(normed_ref[...], up[g, :, at], 1, 0)
                act[...] = dot(cot_ref[...], down[g, at, :], 1, 1)

                def gelu(i):
                    some = tile(i, 2 * CHUNK)
                    x = pre[some] + bias_ref[g, :, at]
                    below = 0.5 * (1.0 + lax.erf(x * math.sqrt(0.5)))
                    density = jnp.exp(-0.5 * x * x) * (1.0 / math.sqrt(2.0 * math.pi))
                    act_half[some] = (x * below).astype(half)
                    pre_half[some] = (act[some] * (below + x * density)).astype(half)

                loop(count // CHUNK // 2, gelu)
                h = act_half[...]
                p = pre_half[...]
                out_ref[...] += dot(h, down[g, at, :], 1, 0)
                back_ref[...] += dot(p, up[g, :, at], 1, 1)
                g_down[g, at, :] = dot(h, cot_ref[...], 0, 0).astype(half)
                g_up[g, :, at] = dot(normed_ref[...], p, 0, 0).astype(half)
                g_bias_ref[g, :, at] = jnp.sum(p.astype(full), axis=0, keepdims=True)

            loop(steps, part)

            def send(r, g=g):
                s = order_ref[r]
                pltpu.make_async_copy(
                    g_up.at[g, pl.ds(pl.multiple_of(s * rows, rows), rows)],
                    grad_refs[g].at[r, 0],
                    out_sems.at[g],
                ).start()
                pltpu.make_async_copy(
                    g_down.at[g, pl.ds(pl.multiple_of(s * share, share), share)],
                    grad_refs[g].at[r, 1],
                    out_sems.at[g],
                ).start()

            loop(n, send)
        if more:
            after_ref, end_ref, block_ref = more_refs[2], more_refs[3], refs[0]

            def finish(i):
                at = tile(i, CHUNK)
                block_ref[at] = (after_ref[at] + (out_ref[at] + end_ref[...])).astype(half)

            loop(count // CHUNK, finish)
        for g in range(groups):
            pltpu.make_async_copy(grad_refs[g], grad_refs[g], out_sems.at[g]).wait()

    outs = (
        [((n, 2, rows, width), half)] * groups
        + [((groups, 1, hidden), full), ((count, width), full), ((count, width), full)]
        + ([((count, width), half)] if more else [])
    )
    return call(
        kernel,
        "mlp",
        (order, normed, cot, bias, *more, *ups, *downs),
        [SCALARS] + [ON_CHIP] * (3 + len(more)) + [ANYWHERE] * (2 * groups),
        outs,
        [ANYWHERE] * groups + [ON_CHIP] * (len(outs) - groups),
        [
            pltpu.VMEM((groups, width, hidden), half),
            pltpu.VMEM((groups, hidden, width), half),
            pltpu.VMEM((count, step), full),
            pltpu.VMEM((count, step), full),
            pltpu.VMEM((count, step), half),
            pltpu.VMEM((count, step), half),
            pltpu.VMEM((groups, width, hidden), half),
            pltpu.VMEM((groups, hidden, width), half),
            pltpu.SemaphoreType.DMA((2 * groups,)),
            pltpu.SemaphoreType.DMA((groups,)),
        ],
    )


def attention_out_back(order, grad, after, cot, gain, mixed, outs):
    count, width = after.shape
    n, rows, _ = outs[0].shape
    quarter = mixed[0].shape[1]

    def kernel(order_ref, grad_ref, after_ref, cot_ref, gain_ref, *refs):
        mixed_refs, out_refs, refs = refs[:4], refs[4:6], refs[6:]
        after_grad_ref, mixed_grad_refs, g_out_ref, sums_ref = refs[0], refs[1:5], refs[5], refs[6]
        held, branch, terms, sems = refs[7:]
        load_out(order_ref, out_refs, held, sems.at[0], n, rows, quarter)
        terms[...] = jnp.zeros_like(terms)

        def fold(value):
            return jnp.sum(value.reshape(CHUNK // 8, 8, width), axis=0)

        def back(i):
            at = tile(i, CHUNK)
            incoming = grad_ref[at]
            part, gain_terms = layer_norm_back(after_ref[at], incoming, gain_ref[...])
            own = cot_ref[at].astype(full)
            total = own + part
            after_grad_ref[at] = total
            rounded = total.astype(half)
            branch[at] = rounded
            terms[0] += fold(rounded.astype(full))
            terms[1] += fold(gain_terms)
            terms[2] += fold(incoming)
            terms[3] += fold(own)

        loop(count // CHUNK, back, 13)
        for k in range(4):
            sums_ref[k] = jnp.sum(terms[k], axis=0, keepdims=True)
        pltpu.make_async_copy(held, held, sems.at[0]).wait()
        for j in range(4):
            mixed_grad_refs[j][...] = dot(branch[...], held[j * quarter : (j + 1) * quarter], 1, 1).astype(half)
            g_out_ref[j * quarter : (j + 1) * quarter] = dot(mixed_refs[j][...], branch[...], 0, 0).astype(half)

    return call(
        kernel,
        "attention_out_back",
        (order, grad, after, cot, gain, *mixed, *outs),
        [SCALARS] + [ON_CHIP] * 8 + [ANYWHERE] * 2,
        [((count, width), full)]
        + [((count, quarter), half)] * 4
        + [((width, width), half), ((4, 1, width), full)],
        [ON_CHIP] * 7,
        [
            pltpu.VMEM((width, width), half),
            pltpu.VMEM((count, width), half),
            pltpu.VMEM((4, 8, width), full),
            pltpu.SemaphoreType.DMA((1,)),
        ],
    )


def attention_back(order, normed, qkvs, lses, mixed_grads, g_out, which, n_img, patches, factor, n):
    groups = len(qkvs)
    count, width = normed.shape
    wide = qkvs[0].shape[1]
    quarter = wide // 3
    padded = count // n_img
    rows = width // n

    def kernel(order_ref, normed_ref, g_out_ref, *refs):
        qkv_refs, mg_refs, refs = refs[:groups], refs[groups : 2 * groups], refs[2 * groups :]
        lse_refs, refs = refs[:groups], refs[groups:]
        g_w_refs, proj_refs, sums_ref = refs[:groups], refs[groups : 2 * groups], refs[2 * groups]
        g_w, sems = refs[2 * groups + 1 :]
        q = order_ref[n]
        for g in range(groups):

            def send_out(r, g=g):
                at = head_rows(order_ref[r], q, n, rows, quarter)
                column = pl.multiple_of((q ^ which[g]) * quarter, quarter)
                pltpu.make_async_copy(
                    g_out_ref.at[pl.ds(at, rows), pl.ds(column, quarter)],
                    g_w_refs[g].at[r, :, pl.ds(wide, quarter)],
                    sems.at[g],
                ).start()

            loop(n, send_out)

            def attend(i, g=g):
                at = tile(i // 2, padded)
                lanes = [pl.ds(pl.multiple_of(t * quarter + (i % 2) * 128, 128), 128) for t in range(3)]
                q2 = qkv_refs[g][at, lanes[0]] * factor
                k2 = qkv_refs[g][at, lanes[1]]
                v2 = qkv_refs[g][at, lanes[2]]
                both, scores, first = pair_scores(q2, k2)
                key = lax.broadcasted_iota(jnp.int32, scores.shape, 0)
                probs = jnp.where(key < patches, jnp.exp(scores - lse_refs[g][i]), 0.0)
                o_both = apart(mg_refs[g][at, lanes[0]], first)
                g_probs = dot(v2, o_both, 1, 1)
                weighted = jnp.sum(probs * g_probs, axis=0, keepdims=True)
                g_scores = (probs * (g_probs - weighted)).astype(half)
                g_query = dot(g_scores, k2, 0, 0)
                g_query = jnp.where(first, g_query[:padded], g_query[padded:]) * factor
                proj_refs[g][at, lanes[0]] = g_query.astype(half)
                proj_refs[g][at, lanes[1]] = dot(g_scores, both, 1, 0).astype(half)
                proj_refs[g][at, lanes[2]] = dot(probs.astype(half), o_both, 1, 0).astype(half)

            loop(2 * n_img, attend, 4)

            def weigh(t, g=g):
                at = tile(t, quarter)
                some = proj_refs[g][:, at]
                g_w[g, :, at] = dot(normed_ref[...], some, 0, 0).astype(half)
                sums_ref[g, :, at] = jnp.sum(some.astype(full), axis=0, keepdims=True)

            loop(3, weigh)

            def send(r, g=g):
                at = pl.multiple_of(order_ref[r] * rows, rows)
                pltpu.make_async_copy(
                    g_w.at[g, pl.ds(at, rows)], g_w_refs[g].at[r, :, pl.ds(0, wide)], sems.at[g]
                ).start()

            loop(n, send)
        for g in range(groups):
            pltpu.make_async_copy(g_w_refs[g], g_w_refs[g], sems.at[g]).wait()

    return call(
        kernel,
        "attention_back",
        (order, normed, g_out, *qkvs, *mixed_grads, *lses),
        [SCALARS] + [ON_CHIP] * (2 + 3 * groups),
        [((n, rows, wide + quarter), half)] * groups
        + [((count, wide), half)] * groups
        + [((groups, 1, wide), full)],
        [ANYWHERE] * groups + [ON_CHIP] * (groups + 1),
        [pltpu.VMEM((groups, width, wide), half), pltpu.SemaphoreType.DMA((groups,))],
    )


def input_back(order, x_zero, after_grad, gain, projs, weights):
    count, width = x_zero.shape
    wide = weights[0][0].shape[2]
    rows = width // sum(part.shape[0] for part in weights[0])
    parts = [part for w in weights for part in w]
    n_parts = len(weights[0])

    def kernel(order_ref, x_ref, after_ref, gain_ref, *refs):
        proj_refs, w_refs = refs[:4], refs[4 : 4 + len(parts)]
        token_ref, sums_ref, held, terms, sems = refs[4 + len(parts) :]
        for j in range(4):
            fetch(
                [w.at[:, pl.ds(0, rows)] for w in w_refs[j * n_parts : (j + 1) * n_parts]],
                order_ref,
                lambda s, j=j: held.at[j, pl.ds(pl.multiple_of(s * rows, rows), rows)],
                sems.at[j],
            )
        for j in range(4):
            pltpu.make_async_copy(held.at[j], held.at[j], sems.at[j]).wait()
            product = dot(proj_refs[j][...], held[j], 1, 1)
            if j == 0:
                token_ref[...] = product
            else:
                token_ref[...] += product
        terms[...] = jnp.zeros_like(terms)

        def fold(value):
            return jnp.sum(value.reshape(ROWS // 8, 8, width), axis=0)

        def back(i):
            at = tile(i, ROWS)
            incoming = token_ref[at]
            part, gain_terms = layer_norm_back(x_ref[at], incoming, gain_ref[...])
            token_ref[at] = after_ref[at] + part
            terms[0] += fold(gain_terms)
            terms[1] += fold(incoming)

        loop(count // ROWS, back)
        for k in range(2):
            sums_ref[k] = jnp.sum(terms[k], axis=0, keepdims=True)

    return call(
        kernel,
        "input_back",
        (order, x_zero, after_grad, gain, *projs, *parts),
        [SCALARS] + [ON_CHIP] * 7 + [ANYWHERE] * len(parts),
        [((count, width), full), ((2, 1, width), full)],
        [ON_CHIP] * 2,
        [
            pltpu.VMEM((4, width, wide), half),
            pltpu.VMEM((2, 8, width), full),
            pltpu.SemaphoreType.DMA((4,)),
        ],
    )


def payloads(which, w_fc1, w_fc2):
    rows, ff = w_fc1.shape
    full_share, width = w_fc2.shape
    share = full_share // 4
    n = ff // full_share
    hidden = n * share
    own, across = which
    if share % 128:
        fc1 = [lax.dynamic_slice(w_fc1, (0, (4 * s + own) * share), (rows, share)) for s in range(n)]
        fc2 = [lax.dynamic_slice(w_fc2, (g * share, 0), (share, width)).astype(half) for g in which]
        rest = jnp.concatenate([*fc1, fc2[0].reshape(rows, -1).astype(full)], axis=1)
        return rest.astype(half), fc2[1]

    def kernel(which_ref, fc1_ref, fc2_ref, rest_ref, two_ref):
        for s in range(n):
            at = pl.ds(pl.multiple_of((4 * s + which_ref[0]) * share, share), share)
            rest_ref[:, s * share : (s + 1) * share] = fc1_ref[:, at].astype(half)
        rest_ref[:, hidden : hidden + width] = fc2_ref[tile(which_ref[0], share), :].astype(half)
        two_ref[...] = fc2_ref[tile(which_ref[1], share), :].astype(half)

    return call(
        kernel,
        "payloads",
        (jnp.stack(which), w_fc1, w_fc2),
        [SCALARS] + [ON_CHIP] * 2,
        [((rows, hidden + width), half), ((share, width), half)],
        [ON_CHIP] * 2,
        [],
    )


def natural_quarters(q, pieces):
    once = [jnp.where((q & 1) == 1, pieces[i ^ 1], pieces[i]) for i in range(4)]
    return [jnp.where(q >= 2, once[i ^ 2], once[i]) for i in range(4)]


def finish_mlp(q, pieces, n):
    _, rows, width = pieces[0].shape
    share = width // n
    if share % 128:
        pieces = natural_quarters(q, pieces)
        fc1 = jnp.stack([p[0].reshape(rows, n, share) for p in pieces], axis=2).reshape(rows, 4 * width)
        return fc1.astype(full), jnp.concatenate([p[1] for p in pieces]).astype(full)

    def kernel(q_ref, *refs):
        fc1_ref, fc2_ref = refs[4:]
        for j in range(4):
            g = q_ref[0] ^ j
            for s in range(n):
                at = pl.ds(pl.multiple_of((4 * s + g) * share, share), share)
                fc1_ref[:, at] = refs[j][0, :, s * share : (s + 1) * share].astype(full)
            fc2_ref[tile(g, rows), :] = refs[j][1].astype(full)

    return call(
        kernel,
        "finish_mlp",
        (q[None], *pieces),
        [SCALARS] + [ON_CHIP] * 4,
        [((rows, 4 * width), full), ((4 * rows, width), full)],
        [ON_CHIP] * 2,
        [],
    )


def finish_attention(q, pieces):
    rows, width = pieces[0].shape
    quarter = width // 4

    def kernel(q_ref, *refs):
        qkv_ref, out_ref = refs[4:]
        for j in range(4):
            g = q_ref[0] ^ j
            for t in range(3):
                at = pl.ds(pl.multiple_of(t * width + g * quarter, quarter), quarter)
                qkv_ref[:, at] = refs[j][:, t * quarter : (t + 1) * quarter].astype(full)
            out_ref[:, tile(g, quarter)] = refs[j][:, 3 * quarter :].astype(full)

    return call(
        kernel,
        "finish_attention",
        (q[None], *pieces),
        [SCALARS] + [ON_CHIP] * 4,
        [((rows, 3 * width), full), ((rows, width), full)],
        [ON_CHIP] * 2,
        [],
    )


BELOW = 16


def first_payload(q, w_qkv, vectors):
    rows, columns = w_qkv.shape
    width = columns // 3
    quarter = width // 4
    wide = 3 * quarter

    def kernel(q_ref, w_ref, *refs):
        out_ref, held, low, sem = refs[len(vectors) :]
        for t in range(3):
            at = pl.multiple_of(t * width + q_ref[0] * quarter, quarter)
            pltpu.make_async_copy(
                w_ref.at[:, pl.ds(at, quarter)], held.at[:, pl.ds(t * quarter, quarter)], sem.at[0]
            ).start()
        low[...] = jnp.zeros_like(low)
        for k, vector in enumerate(refs[: len(vectors)]):
            low[k : k + 1, : vector.shape[1]] = vector[...]
        out_ref[rows:] = low[...].astype(half)
        pltpu.make_async_copy(held, held, sem.at[0]).wait()
        out_ref[:rows] = held[...].astype(half)

    return call(
        kernel,
        "first_payload",
        (q[None], w_qkv, *(v[None] for v in vectors)),
        [SCALARS, ANYWHERE] + [ON_CHIP] * len(vectors),
        [((rows + BELOW, wide), half)],
        [ON_CHIP],
        [pltpu.VMEM((rows, wide), full), pltpu.VMEM((BELOW, wide), full), pltpu.SemaphoreType.DMA((1,))],
    )[0]


def unpack_vectors(order, parts, n, rows, share):
    width = n * rows
    quarter = width // 4
    if rows % 128 or share % 128:
        q = order[n]
        held = jnp.concatenate([p[:, rows:] for p in parts]).astype(full)
        held = held[jnp.zeros((n,), jnp.int32).at[order[:n]].set(jnp.arange(n, dtype=jnp.int32))]
        groups = jnp.arange(4, dtype=jnp.int32) ^ q
        vectors = jnp.stack([held[:, k, :rows].reshape(1, width) for k in range(8)])
        units = held[:, 8, : 4 * share].reshape(n, 4, share).transpose(1, 0, 2)[groups]
        ends = [vectors[k].reshape(4, 1, quarter)[groups] for k in range(2)]
        return vectors, units.reshape(4, 1, width), jnp.concatenate([ends[0], 0 * ends[0], ends[1]], axis=2)

    def kernel(order_ref, *refs):
        part_refs, (vector_ref, fc1_ref, qkv_ref, held, wider, sem) = refs[: len(parts)], refs[len(parts) :]
        base = 0
        for part in part_refs:
            size = part.shape[0]
            pltpu.make_async_copy(part.at[:, pl.ds(rows, BELOW)], held.at[pl.ds(base, size)], sem.at[0]).start()
            base += size
        pltpu.make_async_copy(held, held, sem.at[0]).wait()
        wider[...] = held[...].astype(full)
        q = order_ref[n]
        for r in range(n):
            at = tile(order_ref[r], rows)
            for k in range(8):
                vector_ref[k, :, at] = wider[r, k : k + 1, :rows]
            for j in range(4):
                fc1_ref[j, :, tile(order_ref[r], share)] = wider[r, 8:9, tile(q ^ j, share)]
        for j in range(4):
            at = tile(q ^ j, quarter)
            qkv_ref[j, :, :quarter] = vector_ref[0, :, at]
            qkv_ref[j, :, quarter : 2 * quarter] = jnp.zeros((1, quarter), full)
            qkv_ref[j, :, 2 * quarter :] = vector_ref[1, :, at]

    return call(
        kernel,
        "unpack_vectors",
        (order, *parts),
        [SCALARS] + [ANYWHERE] * len(parts),
        [((8, 1, width), full), ((4, 1, width), full), ((4, 1, 3 * quarter), full)],
        [ON_CHIP] * 3,
        [
            pltpu.VMEM((n, BELOW, 3 * quarter), half),
            pltpu.VMEM((n, BELOW, 3 * quarter), full),
            pltpu.SemaphoreType.DMA((1,)),
        ],
    )


def pack_sums(order, n, rows, share, proj_sums, unit_sums, wide_sums):
    width = n * rows
    quarter = width // 4
    if rows % 128 or share % 128:
        groups = jnp.arange(4, dtype=jnp.int32) ^ order[n]
        proj = jnp.concatenate(proj_sums)[groups]
        units = jnp.concatenate(unit_sums)[groups].reshape(4, n, share)
        flat = [proj[:, :, :quarter].reshape(width), proj[:, :, 2 * quarter :].reshape(width)]
        two, one = wide_sums
        flat += [two[0], one[0], one[1], two[3], two[1], two[2]]
        flat = [v.reshape(n, 1, rows) for v in flat]
        stacked = [jnp.pad(v, ((0, 0), (0, 0), (0, 128 - rows))) for v in flat]
        stacked.append(jnp.pad(units.transpose(1, 0, 2), ((0, 0), (0, 4), (0, 128 - share))))
        return jnp.concatenate(stacked, axis=1)[order[:n]]

    def kernel(order_ref, proj_a, proj_b, unit_a, unit_b, two_ref, one_ref, out_ref, proj, units):
        proj[:2], proj[2:] = proj_a[...], proj_b[...]
        units[:2], units[2:] = unit_a[...], unit_b[...]
        q = order_ref[n]
        per = n // 4
        for r in range(n):
            s = order_ref[r]
            j = (s // per) ^ q
            at = tile(s, rows)
            inside = pl.multiple_of((s % per) * rows, rows)
            out_ref[r, 0:1] = proj[j, :, pl.ds(inside, rows)]
            out_ref[r, 1:2] = proj[j, :, pl.ds(2 * quarter + inside, rows)]
            for k, (ref, row) in enumerate(
                ((two_ref, 0), (one_ref, 0), (one_ref, 1), (two_ref, 3), (two_ref, 1), (two_ref, 2))
            ):
                out_ref[r, 2 + k : 3 + k] = ref[row, :, at]
            for g in range(4):
                out_ref[r, 8 + g : 9 + g] = units[q ^ g, :, tile(s, share)]
            out_ref[r, 12:] = jnp.zeros((4, rows), full)

    sums_two, sums_one = wide_sums
    return call(
        kernel,
        "pack_sums",
        (order, *proj_sums, *unit_sums, sums_two, sums_one),
        [SCALARS] + [ON_CHIP] * 6,
        [((n, 16, rows), full)],
        [ON_CHIP],
        [pltpu.VMEM((4, 1, 3 * quarter), full), pltpu.VMEM((4, 1, width), full)],
    )[0]


def table(codes, width):
    ratio = 0.3 * jnp.exp(codes.astype(full) * (math.log(10.0 / 0.3) / (NSCALE - 1)))
    quarter = width // 4
    omega = jnp.exp(jnp.arange(quarter).astype(full) * (-math.log(10000.0) / quarter))
    steps = jnp.arange(GRID, dtype=jnp.int32).astype(full)
    angle = ratio[:, None, None] * steps[None, :, None] * omega[None, None, :]
    return jnp.concatenate([jnp.sin(angle), jnp.cos(angle)], axis=-1)


def local(
    tokens,
    scale_codes,
    w_qkv,
    b_q,
    b_v,
    w_out,
    b_out,
    gain_one,
    shift_one,
    w_fc1,
    b_fc1,
    w_fc2,
    b_fc2,
    gain_two,
    shift_two,
    cotangent,
):
    n = lax.axis_size("fsdp")
    q = lax.axis_index("dp")
    f = lax.axis_index("fsdp")
    row_count, width = tokens.shape
    rows = width // n
    ff = b_fc1.shape[0] * n
    ffq = ff // n // 4
    hidden = n * ffq
    quarter = width // 4
    n_img = scale_codes.shape[0]
    patches = row_count // n_img
    padded = -(-patches // 16) * 16
    factor = 1.0 / math.sqrt(width // HEADS)
    seq = Order(q)
    bits = list(reversed(range(n.bit_length() - 1)))
    near = min(1, len(bits) - 1)
    shard_order = jnp.asarray(masks(bits), jnp.int32) ^ f
    group_order = jnp.arange(4, dtype=jnp.int32) ^ q
    order = jnp.concatenate([shard_order, q[None]])

    def last_three(chain):
        while len(chain.bits) > 3:
            chain.launch()
            seq.land((), chain)
            chain.join()
        return chain

    small = [b_q, b_v, b_out, gain_one, shift_one, b_fc2, gain_two, shift_two, b_fc1]
    qkv = last_three(Gather(seq, first_payload(q, w_qkv, small), n, bits))
    qkv.launch()
    rest_own, two_own = payloads([seq.at(q), q ^ 2], w_fc1, w_fc2)
    rest_own, two_own = seq.land((rest_own, two_own), qkv)
    rest = Sent(lax.all_gather(rest_own, "fsdp", axis=0, tiled=False))
    two = Sent(lax.all_gather(two_own, "fsdp", axis=0, tiled=False))
    out_own = [lax.dynamic_slice(w_out, (0, g * quarter), (rows, quarter)) for g in (q, q ^ 2)]
    out = last_three(Gather(seq, jnp.concatenate(out_own, axis=1).astype(half), n, bits))

    def spread_rows(value):
        split = value.reshape(n_img, patches, width)
        return jnp.pad(split, ((0, 0), (0, padded - patches), (0, 0)))

    def compact(value):
        return value.reshape(n_img, padded, width)[:, :patches].reshape(row_count, width)

    qkv.join()
    qkv.launch()
    out.launch()
    spread_tokens = seq.land(spread_rows(seq.at(tokens)), qkv)
    qkv_near = qkv.join()
    qkv.launch()
    near_b, near_c = Sent(core_swap(qkv.held)), Sent(x_swap(qkv.held))
    seq.land((), out)
    out.join()
    out.launch()
    places = table(scale_codes, width)
    row_place = jnp.broadcast_to(places[:, :, None], (n_img, GRID, GRID, width // 2))
    col_place = jnp.broadcast_to(places[:, None], (n_img, GRID, GRID, width // 2))
    place = jnp.concatenate([row_place, col_place], axis=-1).reshape(n_img, patches, width)
    place = jnp.pad(place, ((0, 0), (0, padded - patches), (0, 0)))
    x_zero = (seq.at(spread_tokens).astype(full) + place).reshape(-1, width)
    x_zero = seq.land(x_zero, qkv, near_b)
    qkv_far = seq.at(qkv.got)
    far_b, far_c = Sent(core_swap(qkv_far)), Sent(x_swap(qkv_far))
    vectors, bias_fc1, bias_qkv = unpack_vectors(seq.at(order), (qkv_near, qkv_far), n, rows, ffq)
    _, _, full_bout, gain_one_f, shift_one_f, full_bfc2, gain_two_f, shift_two_f = vectors
    normed_one = layer_norm(x_zero, gain_one_f, shift_one_f).astype(half)
    normed_one = seq.land(normed_one, far_b, out)
    out.join()
    out.launch()

    first = attention_forward(
        seq.at(order), normed_one, bias_qkv[:2], ((qkv_near, qkv_far), (near_b.value, far_b.value)),
        n_img, patches, factor,
    )
    first = (seq.land(first[0], near_c, far_c, out), *first[1:])
    near_c, far_c = seq.at((near_c.value, far_c.value))
    near_d, far_d = Sent(core_swap(near_c)), Sent(core_swap(far_c))
    out_a = seq.at(out.join())
    out_b = Sent(core_swap(out_a))
    cot = seq.land(spread_rows(cotangent).reshape(-1, width), near_d, far_d)
    second = attention_forward(
        seq.at(order), normed_one, bias_qkv[2:], ((near_c, far_c), (near_d.value, far_d.value)),
        n_img, patches, factor,
    )
    second = (seq.land(second[0], out_b), *second[1:])
    outs = (out_a, out_b.value)
    qkv_parts = (
        (qkv_near, qkv_far), (near_b.value, far_b.value), (near_c, far_c), (near_d.value, far_d.value)
    )
    qkvs = (*first[:2], *second[:2])
    mixed = (*first[2:4], *second[2:4])
    lses = (*first[4:], *second[4:])
    after_attn, normed_two = attention_out(
        seq.at(order), x_zero, mixed, outs, full_bout, gain_two_f, shift_two_f
    )
    normed_two = seq.land(normed_two, rest)
    rest_a = seq.at(rest.value)
    rest_b = Sent(core_swap(rest_a))
    up_c = Sent(x_swap(seq.at(rest_a[:, :, :hidden])))
    seq.land((), rest_b)
    rests = (rest_a, rest_b.value)

    g_0, g_1, g_bias_a, out_sum, back_sum = mlp(
        seq.at(order), normed_two, cot, bias_fc1[:2], rests, rests, hidden
    )
    g_1 = seq.land(g_1, up_c, two)
    up_c, two = seq.at((up_c.value, two.value))
    up_d, two_d = Sent(core_swap(up_c)), Sent(core_swap(two))
    got_1 = Sent(core_swap(g_1))
    seq.land((), up_d, two_d, got_1)
    red = Reduce(seq, (g_0, got_1.value), n)
    red.launch()
    g_2, g_3, g_bias_b, _, grad_two_in, block = mlp(
        seq.at(order), normed_two, cot, bias_fc1[2:], (up_c, up_d.value), (two, two_d.value), 0,
        (out_sum, back_sum), (after_attn, full_bfc2),
    )
    g_3 = seq.land(g_3, red)
    got_3 = Sent(core_swap(g_3))
    red.launch()
    seq.land((), got_3)
    red_two = Reduce(seq, (g_2, got_3.value), n)
    red_two.launch()

    after_grad, mg0, mg1, mg2, mg3, g_out, sums_two = attention_out_back(
        seq.at(order), grad_two_in, after_attn, cot, gain_two_f, mixed, outs
    )
    mg2 = seq.land(mg2, red)
    red.launch()
    g_w2, g_w3, proj2, proj3, sums_b = attention_back(
        seq.at(order), normed_one, qkvs[2:], lses[2:], (mg2, mg3), g_out, (2, 3), n_img, patches, factor, n
    )
    g_w3 = seq.land(g_w3, red, red_two)
    w_3 = Sent(core_swap(g_w3))
    red_two.launch()
    seq.land((), w_3)
    middle = n // 2
    half_shape = (2,) * (len(bits) - 1)
    w_high = Sent(x_swap(seq.at(rounded_sum([g_w2[middle:], w_3.value[middle:]]))))
    g_w0, g_w1, proj0, proj1, sums_a = attention_back(
        seq.at(order), normed_one, qkvs[:2], lses[:2], (mg0, mg1), g_out, (0, 1), n_img, patches, factor, n
    )
    g_w1 = seq.land(g_w1, red_two, w_high)
    w_1 = Sent(core_swap(g_w1))
    red_two.launch()
    seq.land((), w_1)
    red_w = Reduce(seq, (g_w0, w_1.value), n)
    red_w.launch(0, [w_high.value.reshape(half_shape + w_high.value.shape[1:])])
    w_low = Sent(x_swap(seq.at(rounded_sum([g_w2[:middle], w_3.value[:middle]]))))
    tokens_grad, sums_one = input_back(
        seq.at(order), x_zero, after_grad, gain_one_f, (proj0, proj1, proj2, proj3), qkv_parts
    )
    sums_one = seq.land(sums_one, red_two, red_w, w_low)
    red_w.terms = [*red_w.terms, w_low.value.reshape(half_shape + w_low.value.shape[1:])]
    while len(red_w.axes) > 2:
        red_w.launch()
        seq.land((), red_w)
    red_w.launch()
    cross = Sent(x_swap(seq.at(red_two.rest().piece())))
    packed = pack_sums(
        seq.at(order), n, rows, ffq, (sums_a, sums_b), (g_bias_a, g_bias_b), (sums_two, sums_one)
    )
    sums = Reduce(seq, (packed,), n, full)
    while len(sums.axes) > 1:
        sums.launch()
        if len(sums.axes) > 1:
            seq.land((), sums)
    seq.land((), sums, red_w, cross)
    if red_w.axes:
        red_w.launch()
    mlp_spread = Spread(seq, rounded_sum([*red.rest().terms, cross.value]))
    sums.launch()
    block, tokens_grad = seq.at((block, tokens_grad))
    block_out, grad_tokens = compact(block), compact(tokens_grad)
    seq.land((), sums, mlp_spread)
    packed = seq.at(sums.piece())
    peers = Sent([xor_swap(packed, "dp", 4, m) for m in (1, 2, 3)])
    mlp_spread.cross()
    seq.land((), peers, mlp_spread, *([red_w] if len(bits) > 1 else []))
    small_sums = packed + peers.value[0] + peers.value[1] + peers.value[2]
    w_spread = Spread(seq, red_w.piece())
    mlp_pieces = seq.at(mlp_spread.pieces)
    out_fc1, out_fc2 = finish_mlp(q, mlp_pieces, n)
    out_fc2, small_sums = seq.land((out_fc2, small_sums), w_spread)
    w_spread.cross()
    seq.land((), w_spread)
    out_qkv, out_out = finish_attention(seq.value, w_spread.pieces)
    small_out = [small_sums[k, :rows] for k in range(8)]
    out_bfc1 = small_sums[8:12, :ffq].reshape(-1)
    o_bq, o_bv, o_bout, o_gone, o_sone, o_bfc2, o_gtwo, o_stwo = small_out
    return (
        block_out,
        grad_tokens,
        out_qkv,
        o_bq,
        o_bv,
        out_out,
        o_bout,
        o_gone,
        o_sone,
        out_fc1,
        out_bfc1,
        out_fc2,
        o_bfc2,
        o_gtwo,
        o_stwo,
    )


def solution(mesh):
    rows_split = P(("dp", "fsdp"), None)
    matrix = P("fsdp", None)
    vector = P("fsdp")
    return jax.shard_map(
        local,
        mesh=mesh,
        in_specs=(
            rows_split, P(("dp", "fsdp")), matrix, vector, vector, matrix, vector, vector, vector,
            matrix, vector, matrix, vector, vector, vector, rows_split,
        ),
        out_specs=(
            rows_split, rows_split, matrix, vector, vector, matrix, vector, vector, vector,
            matrix, vector, matrix, vector, vector, vector,
        ),
        check_vma=False,
    )
```

```python
import math

import jax
import jax.numpy as jnp
from jax import lax
from jax.experimental import pallas as pl
from jax.experimental.pallas import tpu as pltpu
from jax.sharding import PartitionSpec as P

HEADS = 16
GRID = 14
NSCALE = 16
norm_eps = 1e-06
half = jnp.bfloat16
full = jnp.float32


def xor_swap(value, axis, size, mask):
    return lax.ppermute(value, axis, [(i, i ^ mask) for i in range(size)])


def core_swap(value):
    return xor_swap(value, "dp", 4, 1)


def x_swap(value):
    return xor_swap(value, "dp", 4, 2)


def masks(bits):
    found = [0]
    for bit in bits:
        found = found + [m | (1 << bit) for m in found]
    return found


class Order:
    def __init__(self, value):
        self.value = value

    def at(self, value):
        value, self.value = lax.optimization_barrier((value, self.value))
        return value

    def land(self, value, *sent):
        value, flights = self.at((value, [s.flight for s in sent]))
        for s, flight in zip(sent, flights, strict=True):
            s.accept(flight)
        return value


class Sent:
    def __init__(self, flight):
        self.flight = flight

    def accept(self, value):
        self.value = value


class Gather:
    def __init__(self, seq, piece, n, bits):
        self.seq, self.held, self.n, self.bits = seq, piece[None], n, list(bits)

    def launch(self):
        self.held = self.seq.at(self.held)
        self.flight = xor_swap(self.held, "fsdp", self.n, 1 << self.bits.pop(0))

    def accept(self, value):
        self.got = value

    def join(self):
        self.held = jnp.concatenate([self.held, self.got])
        return self.held


def rounded_sum(terms, kind=half):
    return sum(t.astype(full) for t in terms).astype(kind)


class Reduce:
    def __init__(self, seq, terms, n, kind=half):
        self.kind = kind
        self.seq, self.n, self.axes = seq, n, list(range(n.bit_length() - 1))
        self.terms = [t.reshape((2,) * len(self.axes) + t.shape[1:]) for t in terms]

    def launch(self, bit=None, more=()):
        bit = self.axes[0] if bit is None else bit
        axis = self.axes.index(bit)
        self.axes.pop(axis)
        low, high = [
            [lax.index_in_dim(t, side, axis, keepdims=False) for t in self.terms] for side in (0, 1)
        ]
        self.terms = low
        self.flight = xor_swap(self.seq.at(rounded_sum([*high, *more], self.kind)), "fsdp", self.n, 1 << bit)

    def accept(self, value):
        self.terms = [*self.terms, value]

    def rest(self):
        while self.axes:
            self.launch()
            self.seq.land((), self)
        return self

    def piece(self):
        return rounded_sum(self.terms, self.kind)


class Spread:
    def __init__(self, seq, piece):
        self.seq, self.pieces = seq, [seq.at(piece)]
        self.flight = [core_swap(self.pieces[0]), x_swap(self.pieces[0])]

    def cross(self):
        self.flight = [core_swap(self.seq.at(self.pieces[2]))]

    def accept(self, value):
        self.pieces += value


ANYWHERE = pl.BlockSpec(memory_space=pl.ANY)
ON_CHIP = pl.BlockSpec(memory_space=pltpu.VMEM)
SCALARS = pl.BlockSpec(memory_space=pltpu.SMEM)


def dot(left, right, dim_left, dim_right):
    return lax.dot_general(
        left, right, (((dim_left,), (dim_right,)), ((), ())), preferred_element_type=full
    )


def call(kernel, name, operands, in_specs, outs, out_specs, scratch):
    return pl.pallas_call(
        kernel,
        out_shape=[jax.ShapeDtypeStruct(shape, kind) for shape, kind in outs],
        in_specs=in_specs,
        out_specs=out_specs,
        scratch_shapes=scratch,
        compiler_params=pltpu.CompilerParams(vmem_limit_bytes=58 * 2**20),
        name=name,
    )(*operands)


def loop(count, body, unroll=1):
    def step(i, carry):
        body(i)
        return carry

    lax.fori_loop(0, count, step, 0, unroll=unroll)


def tile(i, size):
    return pl.ds(pl.multiple_of(i * size, size), size)


def fetch(parts, order_ref, place, sem):
    base = 0
    for part in parts:

        def start(r, part=part, base=base):
            shard = r if order_ref is None else order_ref[base + r]
            pltpu.make_async_copy(part.at[r], place(shard), sem).start()

        loop(part.shape[0], start)
        base += part.shape[0]


def head_rows(s, q, n, rows, quarter):
    per = n // 4
    return pl.multiple_of(((s // per) ^ q) * quarter + (s % per) * rows, rows)


def pair_scores(q2, k2):
    first = lax.broadcasted_iota(jnp.int32, q2.shape, 1) < q2.shape[1] // 2
    both = apart(q2, first)
    return both, dot(k2, both, 1, 1), first


def apart(value, first):
    zero = jnp.zeros_like(value)
    return jnp.concatenate([jnp.where(first, value, zero), jnp.where(first, zero, value)])


def attention_forward(order, normed, bias, weights, n_img, patches, factor):
    groups, n_parts = len(weights), len(weights[0])
    wide = weights[0][0].shape[2]
    count, width = normed.shape
    rows = width // sum(part.shape[0] for part in weights[0])
    padded = count // n_img
    quarter = wide // 3

    def kernel(order_ref, normed_ref, bias_ref, *refs):
        w_refs, refs = refs[: groups * n_parts], refs[groups * n_parts :]
        qkv_refs, mixed_refs, refs = refs[:groups], refs[groups : 2 * groups], refs[2 * groups :]
        lse_refs, (w_held, sems) = refs[:groups], refs[groups:]
        for g in range(groups):
            fetch(
                [w.at[:, pl.ds(0, rows)] for w in w_refs[g * n_parts : (g + 1) * n_parts]],
                order_ref,
                lambda s, g=g: w_held.at[g, pl.ds(pl.multiple_of(s * rows, rows), rows)],
                sems.at[g],
            )
        for g in range(groups):
            pltpu.make_async_copy(w_held.at[g], w_held.at[g], sems.at[g]).wait()

            def project(t, g=g):
                at = tile(t, quarter)
                product = dot(normed_ref[...], w_held[g, :, at], 1, 0)
                qkv_refs[g][:, at] = (product + bias_ref[g, :, at]).astype(half)

            loop(3, project)

            def attend(i, g=g):
                at = tile(i // 2, padded)
                lanes = [pl.ds(pl.multiple_of(t * quarter + (i % 2) * 128, 128), 128) for t in range(3)]
                q2 = qkv_refs[g][at, lanes[0]] * factor
                k2 = qkv_refs[g][at, lanes[1]]
                v2 = qkv_refs[g][at, lanes[2]]
                _, scores, first = pair_scores(q2, k2)
                key = lax.broadcasted_iota(jnp.int32, scores.shape, 0)
                scores = jnp.where(key < patches, scores, -1e30)
                top = jnp.max(scores, axis=0, keepdims=True)
                raised = jnp.exp(scores - top)
                total = jnp.sum(raised, axis=0, keepdims=True)
                lse_refs[g][i] = top + jnp.log(total)
                out = dot((raised * (1.0 / total)).astype(half), v2, 0, 0)
                mixed_refs[g][at, lanes[0]] = jnp.where(first, out[:padded], out[padded:]).astype(half)

            loop(2 * n_img, attend, 2 * n_img)

    return call(
        kernel,
        "attention_forward",
        (order, normed, bias, *(part for w in weights for part in w)),
        [SCALARS, ON_CHIP, ON_CHIP] + [ANYWHERE] * (groups * n_parts),
        [((count, wide), half)] * groups
        + [((count, quarter), half)] * groups
        + [((2 * n_img, 1, 2 * padded), full)] * groups,
        [ON_CHIP] * (3 * groups),
        [pltpu.VMEM((groups, width, wide), half), pltpu.SemaphoreType.DMA((groups,))],
    )


def layer_norm(value, gain, shift):
    center = jnp.mean(value, axis=-1, keepdims=True)
    offset = value - center
    spread = jnp.mean(offset * offset, axis=-1, keepdims=True)
    return offset * lax.rsqrt(spread + norm_eps) * gain + shift


def layer_norm_back(value, grad, gain):
    center = jnp.mean(value, axis=-1, keepdims=True)
    offset = value - center
    scale = lax.rsqrt(jnp.mean(offset * offset, axis=-1, keepdims=True) + norm_eps)
    unit = offset * scale
    scaled = grad * gain
    inner = jnp.mean(scaled * unit, axis=-1, keepdims=True)
    return scale * (scaled - jnp.mean(scaled, axis=-1, keepdims=True) - unit * inner), grad * unit


def load_out(order_ref, out_refs, held, sem, n, rows, quarter):
    q = order_ref[n]
    for j in range(4):
        column = pl.multiple_of((q ^ j) * quarter, quarter)
        fetch(
            [out_refs[j % 2].at[:, :, pl.ds(j // 2 * quarter, quarter)]],
            order_ref,
            lambda s, column=column: held.at[
                pl.ds(head_rows(s, q, n, rows, quarter), rows), pl.ds(column, quarter)
            ],
            sem,
        )


CHUNK = 16
ROWS = 64


def attention_out(order, x_zero, mixed, outs, bias, gain, shift):
    count, width = x_zero.shape
    n, rows, _ = outs[0].shape
    quarter = mixed[0].shape[1]

    def kernel(order_ref, x_ref, bias_ref, gain_ref, shift_ref, *refs):
        mixed_refs, out_refs = refs[:4], refs[4:6]
        after_ref, normed_ref, held, sems = refs[6:]
        load_out(order_ref, out_refs, held, sems.at[0], n, rows, quarter)
        together = jnp.concatenate([m[...] for m in mixed_refs], axis=1)
        pltpu.make_async_copy(held, held, sems.at[0]).wait()
        after_ref[...] = dot(together, held[...], 1, 0)

        def finish(i):
            at = tile(i, CHUNK)
            after = x_ref[at] + (after_ref[at] + bias_ref[...])
            after_ref[at] = after
            normed_ref[at] = layer_norm(after, gain_ref[...], shift_ref[...]).astype(half)

        loop(count // CHUNK, finish, 13)

    return call(
        kernel,
        "attention_out",
        (order, x_zero, bias, gain, shift, *mixed, *outs),
        [SCALARS] + [ON_CHIP] * 8 + [ANYWHERE] * 2,
        [((count, width), full), ((count, width), half)],
        [ON_CHIP] * 2,
        [pltpu.VMEM((width, width), half), pltpu.SemaphoreType.DMA((1,))],
    )


def mlp(order, normed, cot, bias, ups, downs, down_start, carried=None, ending=None):
    groups = len(ups)
    count, width = normed.shape
    n, rows, _ = ups[0].shape
    hidden = bias.shape[2]
    share = hidden // n
    step = min(512, hidden)
    steps = hidden // step
    more = [] if carried is None else [*carried, *ending]

    def kernel(order_ref, normed_ref, cot_ref, bias_ref, *refs):
        more_refs, refs = refs[: len(more)], refs[len(more) :]
        up_refs, down_refs, refs = refs[:groups], refs[groups : 2 * groups], refs[2 * groups :]
        grad_refs, refs = refs[:groups], refs[groups:]
        g_bias_ref, out_ref, back_ref, refs = refs[0], refs[1], refs[2], refs[3:]
        up, down, pre, act, act_half, pre_half, g_up, g_down, sems, out_sems = refs[-10:]
        for g in range(groups):
            fetch(
                [up_refs[g].at[:, :, pl.ds(0, hidden)]],
                None,
                lambda s, g=g: up.at[g, pl.ds(pl.multiple_of(s * rows, rows), rows)],
                sems.at[g],
            )
            fetch(
                [down_refs[g].at[:, :, pl.ds(down_start, width)]],
                None,
                lambda s, g=g: down.at[g, pl.ds(pl.multiple_of(s * share, share), share)],
                sems.at[groups + g],
            )
        if more:
            out_ref[...] = more_refs[0][...]
            back_ref[...] = more_refs[1][...]
        else:
            out_ref[...] = jnp.zeros_like(out_ref)
            back_ref[...] = jnp.zeros_like(back_ref)
        for g in range(groups):
            pltpu.make_async_copy(up.at[g], up.at[g], sems.at[g]).wait()
            pltpu.make_async_copy(down.at[g], down.at[g], sems.at[groups + g]).wait()

            def part(t, g=g):
                at = tile(t, step)
                pre[...] = dot(normed_ref[...], up[g, :, at], 1, 0)
                act[...] = dot(cot_ref[...], down[g, at, :], 1, 1)

                def gelu(i):
                    some = tile(i, 2 * CHUNK)
                    x = pre[some] + bias_ref[g, :, at]
                    below = 0.5 * (1.0 + lax.erf(x * math.sqrt(0.5)))
                    density = jnp.exp(-0.5 * x * x) * (1.0 / math.sqrt(2.0 * math.pi))
                    act_half[some] = (x * below).astype(half)
                    pre_half[some] = (act[some] * (below + x * density)).astype(half)

                loop(count // CHUNK // 2, gelu)
                h = act_half[...]
                p = pre_half[...]
                out_ref[...] += dot(h, down[g, at, :], 1, 0)
                back_ref[...] += dot(p, up[g, :, at], 1, 1)
                g_down[g, at, :] = dot(h, cot_ref[...], 0, 0).astype(half)
                g_up[g, :, at] = dot(normed_ref[...], p, 0, 0).astype(half)
                g_bias_ref[g, :, at] = jnp.sum(p.astype(full), axis=0, keepdims=True)

            loop(steps, part)

            def send(r, g=g):
                s = order_ref[r]
                pltpu.make_async_copy(
                    g_up.at[g, pl.ds(pl.multiple_of(s * rows, rows), rows)],
                    grad_refs[g].at[r, 0],
                    out_sems.at[g],
                ).start()
                pltpu.make_async_copy(
                    g_down.at[g, pl.ds(pl.multiple_of(s * share, share), share)],
                    grad_refs[g].at[r, 1],
                    out_sems.at[g],
                ).start()

            loop(n, send)
        if more:
            after_ref, end_ref, block_ref = more_refs[2], more_refs[3], refs[0]

            def finish(i):
                at = tile(i, CHUNK)
                block_ref[at] = (after_ref[at] + (out_ref[at] + end_ref[...])).astype(half)

            loop(count // CHUNK, finish)
        for g in range(groups):
            pltpu.make_async_copy(grad_refs[g], grad_refs[g], out_sems.at[g]).wait()

    outs = (
        [((n, 2, rows, width), half)] * groups
        + [((groups, 1, hidden), full), ((count, width), full), ((count, width), full)]
        + ([((count, width), half)] if more else [])
    )
    return call(
        kernel,
        "mlp",
        (order, normed, cot, bias, *more, *ups, *downs),
        [SCALARS] + [ON_CHIP] * (3 + len(more)) + [ANYWHERE] * (2 * groups),
        outs,
        [ANYWHERE] * groups + [ON_CHIP] * (len(outs) - groups),
        [
            pltpu.VMEM((groups, width, hidden), half),
            pltpu.VMEM((groups, hidden, width), half),
            pltpu.VMEM((count, step), full),
            pltpu.VMEM((count, step), full),
            pltpu.VMEM((count, step), half),
            pltpu.VMEM((count, step), half),
            pltpu.VMEM((groups, width, hidden), half),
            pltpu.VMEM((groups, hidden, width), half),
            pltpu.SemaphoreType.DMA((2 * groups,)),
            pltpu.SemaphoreType.DMA((groups,)),
        ],
    )


def attention_out_back(order, grad, after, cot, gain, mixed, outs):
    count, width = after.shape
    n, rows, _ = outs[0].shape
    quarter = mixed[0].shape[1]

    def kernel(order_ref, grad_ref, after_ref, cot_ref, gain_ref, *refs):
        mixed_refs, out_refs, refs = refs[:4], refs[4:6], refs[6:]
        after_grad_ref, mixed_grad_refs, g_out_ref, sums_ref = refs[0], refs[1:5], refs[5], refs[6]
        held, branch, terms, sems = refs[7:]
        load_out(order_ref, out_refs, held, sems.at[0], n, rows, quarter)
        terms[...] = jnp.zeros_like(terms)

        def fold(value):
            return jnp.sum(value.reshape(CHUNK // 8, 8, width), axis=0)

        def back(i):
            at = tile(i, CHUNK)
            incoming = grad_ref[at]
            part, gain_terms = layer_norm_back(after_ref[at], incoming, gain_ref[...])
            own = cot_ref[at].astype(full)
            total = own + part
            after_grad_ref[at] = total
            rounded = total.astype(half)
            branch[at] = rounded
            terms[0] += fold(rounded.astype(full))
            terms[1] += fold(gain_terms)
            terms[2] += fold(incoming)
            terms[3] += fold(own)

        loop(count // CHUNK, back, 13)
        for k in range(4):
            sums_ref[k] = jnp.sum(terms[k], axis=0, keepdims=True)
        pltpu.make_async_copy(held, held, sems.at[0]).wait()
        for j in range(4):
            mixed_grad_refs[j][...] = dot(branch[...], held[j * quarter : (j + 1) * quarter], 1, 1).astype(half)
            g_out_ref[j * quarter : (j + 1) * quarter] = dot(mixed_refs[j][...], branch[...], 0, 0).astype(half)

    return call(
        kernel,
        "attention_out_back",
        (order, grad, after, cot, gain, *mixed, *outs),
        [SCALARS] + [ON_CHIP] * 8 + [ANYWHERE] * 2,
        [((count, width), full)]
        + [((count, quarter), half)] * 4
        + [((width, width), half), ((4, 1, width), full)],
        [ON_CHIP] * 7,
        [
            pltpu.VMEM((width, width), half),
            pltpu.VMEM((count, width), half),
            pltpu.VMEM((4, 8, width), full),
            pltpu.SemaphoreType.DMA((1,)),
        ],
    )


def attention_back(order, normed, qkvs, lses, mixed_grads, g_out, which, n_img, patches, factor, n):
    groups = len(qkvs)
    count, width = normed.shape
    wide = qkvs[0].shape[1]
    quarter = wide // 3
    padded = count // n_img
    rows = width // n

    def kernel(order_ref, normed_ref, g_out_ref, *refs):
        qkv_refs, mg_refs, refs = refs[:groups], refs[groups : 2 * groups], refs[2 * groups :]
        lse_refs, refs = refs[:groups], refs[groups:]
        g_w_refs, proj_refs, sums_ref = refs[:groups], refs[groups : 2 * groups], refs[2 * groups]
        g_w, sems = refs[2 * groups + 1 :]
        q = order_ref[n]
        for g in range(groups):

            def send_out(r, g=g):
                at = head_rows(order_ref[r], q, n, rows, quarter)
                column = pl.multiple_of((q ^ which[g]) * quarter, quarter)
                pltpu.make_async_copy(
                    g_out_ref.at[pl.ds(at, rows), pl.ds(column, quarter)],
                    g_w_refs[g].at[r, :, pl.ds(wide, quarter)],
                    sems.at[g],
                ).start()

            loop(n, send_out)

            def attend(i, g=g):
                at = tile(i // 2, padded)
                lanes = [pl.ds(pl.multiple_of(t * quarter + (i % 2) * 128, 128), 128) for t in range(3)]
                q2 = qkv_refs[g][at, lanes[0]] * factor
                k2 = qkv_refs[g][at, lanes[1]]
                v2 = qkv_refs[g][at, lanes[2]]
                both, scores, first = pair_scores(q2, k2)
                key = lax.broadcasted_iota(jnp.int32, scores.shape, 0)
                probs = jnp.where(key < patches, jnp.exp(scores - lse_refs[g][i]), 0.0)
                o_both = apart(mg_refs[g][at, lanes[0]], first)
                g_probs = dot(v2, o_both, 1, 1)
                weighted = jnp.sum(probs * g_probs, axis=0, keepdims=True)
                g_scores = (probs * (g_probs - weighted)).astype(half)
                g_query = dot(g_scores, k2, 0, 0)
                g_query = jnp.where(first, g_query[:padded], g_query[padded:]) * factor
                proj_refs[g][at, lanes[0]] = g_query.astype(half)
                proj_refs[g][at, lanes[1]] = dot(g_scores, both, 1, 0).astype(half)
                proj_refs[g][at, lanes[2]] = dot(probs.astype(half), o_both, 1, 0).astype(half)

            loop(2 * n_img, attend, 4)

            def weigh(t, g=g):
                at = tile(t, quarter)
                some = proj_refs[g][:, at]
                g_w[g, :, at] = dot(normed_ref[...], some, 0, 0).astype(half)
                sums_ref[g, :, at] = jnp.sum(some.astype(full), axis=0, keepdims=True)

            loop(3, weigh)

            def send(r, g=g):
                at = pl.multiple_of(order_ref[r] * rows, rows)
                pltpu.make_async_copy(
                    g_w.at[g, pl.ds(at, rows)], g_w_refs[g].at[r, :, pl.ds(0, wide)], sems.at[g]
                ).start()

            loop(n, send)
        for g in range(groups):
            pltpu.make_async_copy(g_w_refs[g], g_w_refs[g], sems.at[g]).wait()

    return call(
        kernel,
        "attention_back",
        (order, normed, g_out, *qkvs, *mixed_grads, *lses),
        [SCALARS] + [ON_CHIP] * (2 + 3 * groups),
        [((n, rows, wide + quarter), half)] * groups
        + [((count, wide), half)] * groups
        + [((groups, 1, wide), full)],
        [ANYWHERE] * groups + [ON_CHIP] * (groups + 1),
        [pltpu.VMEM((groups, width, wide), half), pltpu.SemaphoreType.DMA((groups,))],
    )


def input_back(order, x_zero, after_grad, gain, projs, weights):
    count, width = x_zero.shape
    wide = weights[0][0].shape[2]
    rows = width // sum(part.shape[0] for part in weights[0])
    parts = [part for w in weights for part in w]
    n_parts = len(weights[0])

    def kernel(order_ref, x_ref, after_ref, gain_ref, *refs):
        proj_refs, w_refs = refs[:4], refs[4 : 4 + len(parts)]
        token_ref, sums_ref, held, terms, sems = refs[4 + len(parts) :]
        for j in range(4):
            fetch(
                [w.at[:, pl.ds(0, rows)] for w in w_refs[j * n_parts : (j + 1) * n_parts]],
                order_ref,
                lambda s, j=j: held.at[j, pl.ds(pl.multiple_of(s * rows, rows), rows)],
                sems.at[j],
            )
        for j in range(4):
            pltpu.make_async_copy(held.at[j], held.at[j], sems.at[j]).wait()
            product = dot(proj_refs[j][...], held[j], 1, 1)
            if j == 0:
                token_ref[...] = product
            else:
                token_ref[...] += product
        terms[...] = jnp.zeros_like(terms)

        def fold(value):
            return jnp.sum(value.reshape(ROWS // 8, 8, width), axis=0)

        def back(i):
            at = tile(i, ROWS)
            incoming = token_ref[at]
            part, gain_terms = layer_norm_back(x_ref[at], incoming, gain_ref[...])
            token_ref[at] = after_ref[at] + part
            terms[0] += fold(gain_terms)
            terms[1] += fold(incoming)

        loop(count // ROWS, back)
        for k in range(2):
            sums_ref[k] = jnp.sum(terms[k], axis=0, keepdims=True)

    return call(
        kernel,
        "input_back",
        (order, x_zero, after_grad, gain, *projs, *parts),
        [SCALARS] + [ON_CHIP] * 7 + [ANYWHERE] * len(parts),
        [((count, width), full), ((2, 1, width), full)],
        [ON_CHIP] * 2,
        [
            pltpu.VMEM((4, width, wide), half),
            pltpu.VMEM((2, 8, width), full),
            pltpu.SemaphoreType.DMA((4,)),
        ],
    )


def payloads(which, w_fc1, w_fc2):
    rows, ff = w_fc1.shape
    full_share, width = w_fc2.shape
    share = full_share // 4
    n = ff // full_share
    hidden = n * share
    own, across = which
    if share % 128:
        fc1 = [lax.dynamic_slice(w_fc1, (0, (4 * s + own) * share), (rows, share)) for s in range(n)]
        fc2 = [lax.dynamic_slice(w_fc2, (g * share, 0), (share, width)).astype(half) for g in which]
        rest = jnp.concatenate([*fc1, fc2[0].reshape(rows, -1).astype(full)], axis=1)
        return rest.astype(half), fc2[1]

    def kernel(which_ref, fc1_ref, fc2_ref, rest_ref, two_ref):
        for s in range(n):
            at = pl.ds(pl.multiple_of((4 * s + which_ref[0]) * share, share), share)
            rest_ref[:, s * share : (s + 1) * share] = fc1_ref[:, at].astype(half)
        rest_ref[:, hidden : hidden + width] = fc2_ref[tile(which_ref[0], share), :].astype(half)
        two_ref[...] = fc2_ref[tile(which_ref[1], share), :].astype(half)

    return call(
        kernel,
        "payloads",
        (jnp.stack(which), w_fc1, w_fc2),
        [SCALARS] + [ON_CHIP] * 2,
        [((rows, hidden + width), half), ((share, width), half)],
        [ON_CHIP] * 2,
        [],
    )


def natural_quarters(q, pieces):
    once = [jnp.where((q & 1) == 1, pieces[i ^ 1], pieces[i]) for i in range(4)]
    return [jnp.where(q >= 2, once[i ^ 2], once[i]) for i in range(4)]


def finish_mlp(q, pieces, n):
    _, rows, width = pieces[0].shape
    share = width // n
    if share % 128:
        pieces = natural_quarters(q, pieces)
        fc1 = jnp.stack([p[0].reshape(rows, n, share) for p in pieces], axis=2).reshape(rows, 4 * width)
        return fc1.astype(full), jnp.concatenate([p[1] for p in pieces]).astype(full)

    def kernel(q_ref, *refs):
        fc1_ref, fc2_ref = refs[4:]
        for j in range(4):
            g = q_ref[0] ^ j
            for s in range(n):
                at = pl.ds(pl.multiple_of((4 * s + g) * share, share), share)
                fc1_ref[:, at] = refs[j][0, :, s * share : (s + 1) * share].astype(full)
            fc2_ref[tile(g, rows), :] = refs[j][1].astype(full)

    return call(
        kernel,
        "finish_mlp",
        (q[None], *pieces),
        [SCALARS] + [ON_CHIP] * 4,
        [((rows, 4 * width), full), ((4 * rows, width), full)],
        [ON_CHIP] * 2,
        [],
    )


def finish_attention(q, pieces):
    rows, width = pieces[0].shape
    quarter = width // 4

    def kernel(q_ref, *refs):
        qkv_ref, out_ref = refs[4:]
        for j in range(4):
            g = q_ref[0] ^ j
            for t in range(3):
                at = pl.ds(pl.multiple_of(t * width + g * quarter, quarter), quarter)
                qkv_ref[:, at] = refs[j][:, t * quarter : (t + 1) * quarter].astype(full)
            out_ref[:, tile(g, quarter)] = refs[j][:, 3 * quarter :].astype(full)

    return call(
        kernel,
        "finish_attention",
        (q[None], *pieces),
        [SCALARS] + [ON_CHIP] * 4,
        [((rows, 3 * width), full), ((rows, width), full)],
        [ON_CHIP] * 2,
        [],
    )


BELOW = 16


def first_payload(q, w_qkv, vectors):
    rows, columns = w_qkv.shape
    width = columns // 3
    quarter = width // 4
    wide = 3 * quarter

    def kernel(q_ref, w_ref, *refs):
        out_ref, held, low, sem = refs[len(vectors) :]
        for t in range(3):
            at = pl.multiple_of(t * width + q_ref[0] * quarter, quarter)
            pltpu.make_async_copy(
                w_ref.at[:, pl.ds(at, quarter)], held.at[:, pl.ds(t * quarter, quarter)], sem.at[0]
            ).start()
        low[...] = jnp.zeros_like(low)
        for k, vector in enumerate(refs[: len(vectors)]):
            low[k : k + 1, : vector.shape[1]] = vector[...]
        out_ref[rows:] = low[...].astype(half)
        pltpu.make_async_copy(held, held, sem.at[0]).wait()
        out_ref[:rows] = held[...].astype(half)

    return call(
        kernel,
        "first_payload",
        (q[None], w_qkv, *(v[None] for v in vectors)),
        [SCALARS, ANYWHERE] + [ON_CHIP] * len(vectors),
        [((rows + BELOW, wide), half)],
        [ON_CHIP],
        [pltpu.VMEM((rows, wide), full), pltpu.VMEM((BELOW, wide), full), pltpu.SemaphoreType.DMA((1,))],
    )[0]


def unpack_vectors(order, parts, n, rows, share):
    width = n * rows
    quarter = width // 4
    if rows % 128 or share % 128:
        q = order[n]
        held = jnp.concatenate([p[:, rows:] for p in parts]).astype(full)
        held = held[jnp.zeros((n,), jnp.int32).at[order[:n]].set(jnp.arange(n, dtype=jnp.int32))]
        groups = jnp.arange(4, dtype=jnp.int32) ^ q
        vectors = jnp.stack([held[:, k, :rows].reshape(1, width) for k in range(8)])
        units = held[:, 8, : 4 * share].reshape(n, 4, share).transpose(1, 0, 2)[groups]
        ends = [vectors[k].reshape(4, 1, quarter)[groups] for k in range(2)]
        return vectors, units.reshape(4, 1, width), jnp.concatenate([ends[0], 0 * ends[0], ends[1]], axis=2)

    def kernel(order_ref, *refs):
        part_refs, (vector_ref, fc1_ref, qkv_ref, held, wider, sem) = refs[: len(parts)], refs[len(parts) :]
        base = 0
        for part in part_refs:
            size = part.shape[0]
            pltpu.make_async_copy(part.at[:, pl.ds(rows, BELOW)], held.at[pl.ds(base, size)], sem.at[0]).start()
            base += size
        pltpu.make_async_copy(held, held, sem.at[0]).wait()
        wider[...] = held[...].astype(full)
        q = order_ref[n]
        for r in range(n):
            at = tile(order_ref[r], rows)
            for k in range(8):
                vector_ref[k, :, at] = wider[r, k : k + 1, :rows]
            for j in range(4):
                fc1_ref[j, :, tile(order_ref[r], share)] = wider[r, 8:9, tile(q ^ j, share)]
        for j in range(4):
            at = tile(q ^ j, quarter)
            qkv_ref[j, :, :quarter] = vector_ref[0, :, at]
            qkv_ref[j, :, quarter : 2 * quarter] = jnp.zeros((1, quarter), full)
            qkv_ref[j, :, 2 * quarter :] = vector_ref[1, :, at]

    return call(
        kernel,
        "unpack_vectors",
        (order, *parts),
        [SCALARS] + [ANYWHERE] * len(parts),
        [((8, 1, width), full), ((4, 1, width), full), ((4, 1, 3 * quarter), full)],
        [ON_CHIP] * 3,
        [
            pltpu.VMEM((n, BELOW, 3 * quarter), half),
            pltpu.VMEM((n, BELOW, 3 * quarter), full),
            pltpu.SemaphoreType.DMA((1,)),
        ],
    )


def pack_sums(order, n, rows, share, proj_sums, unit_sums, wide_sums):
    width = n * rows
    quarter = width // 4
    if rows % 128 or share % 128:
        groups = jnp.arange(4, dtype=jnp.int32) ^ order[n]
        proj = jnp.concatenate(proj_sums)[groups]
        units = jnp.concatenate(unit_sums)[groups].reshape(4, n, share)
        flat = [proj[:, :, :quarter].reshape(width), proj[:, :, 2 * quarter :].reshape(width)]
        two, one = wide_sums
        flat += [two[0], one[0], one[1], two[3], two[1], two[2]]
        flat = [v.reshape(n, 1, rows) for v in flat]
        stacked = [jnp.pad(v, ((0, 0), (0, 0), (0, 128 - rows))) for v in flat]
        stacked.append(jnp.pad(units.transpose(1, 0, 2), ((0, 0), (0, 4), (0, 128 - share))))
        return jnp.concatenate(stacked, axis=1)[order[:n]]

    def kernel(order_ref, proj_a, proj_b, unit_a, unit_b, two_ref, one_ref, out_ref, proj, units):
        proj[:2], proj[2:] = proj_a[...], proj_b[...]
        units[:2], units[2:] = unit_a[...], unit_b[...]
        q = order_ref[n]
        per = n // 4
        for r in range(n):
            s = order_ref[r]
            j = (s // per) ^ q
            at = tile(s, rows)
            inside = pl.multiple_of((s % per) * rows, rows)
            out_ref[r, 0:1] = proj[j, :, pl.ds(inside, rows)]
            out_ref[r, 1:2] = proj[j, :, pl.ds(2 * quarter + inside, rows)]
            for k, (ref, row) in enumerate(
                ((two_ref, 0), (one_ref, 0), (one_ref, 1), (two_ref, 3), (two_ref, 1), (two_ref, 2))
            ):
                out_ref[r, 2 + k : 3 + k] = ref[row, :, at]
            for g in range(4):
                out_ref[r, 8 + g : 9 + g] = units[q ^ g, :, tile(s, share)]
            out_ref[r, 12:] = jnp.zeros((4, rows), full)

    sums_two, sums_one = wide_sums
    return call(
        kernel,
        "pack_sums",
        (order, *proj_sums, *unit_sums, sums_two, sums_one),
        [SCALARS] + [ON_CHIP] * 6,
        [((n, 16, rows), full)],
        [ON_CHIP],
        [pltpu.VMEM((4, 1, 3 * quarter), full), pltpu.VMEM((4, 1, width), full)],
    )[0]


def table(codes, width):
    ratio = 0.3 * jnp.exp(codes.astype(full) * (math.log(10.0 / 0.3) / (NSCALE - 1)))
    quarter = width // 4
    omega = jnp.exp(jnp.arange(quarter).astype(full) * (-math.log(10000.0) / quarter))
    steps = jnp.arange(GRID, dtype=jnp.int32).astype(full)
    angle = ratio[:, None, None] * steps[None, :, None] * omega[None, None, :]
    return jnp.concatenate([jnp.sin(angle), jnp.cos(angle)], axis=-1)


def local(
    tokens,
    scale_codes,
    w_qkv,
    b_q,
    b_v,
    w_out,
    b_out,
    gain_one,
    shift_one,
    w_fc1,
    b_fc1,
    w_fc2,
    b_fc2,
    gain_two,
    shift_two,
    cotangent,
):
    n = lax.axis_size("fsdp")
    q = lax.axis_index("dp")
    f = lax.axis_index("fsdp")
    row_count, width = tokens.shape
    rows = width // n
    ff = b_fc1.shape[0] * n
    ffq = ff // n // 4
    hidden = n * ffq
    quarter = width // 4
    n_img = scale_codes.shape[0]
    patches = row_count // n_img
    padded = -(-patches // 16) * 16
    factor = 1.0 / math.sqrt(width // HEADS)
    seq = Order(q)
    bits = list(reversed(range(n.bit_length() - 1)))
    near = min(1, len(bits) - 1)
    shard_order = jnp.asarray(masks(bits), jnp.int32) ^ f
    group_order = jnp.arange(4, dtype=jnp.int32) ^ q
    order = jnp.concatenate([shard_order, q[None]])

    def last_three(chain):
        while len(chain.bits) > 3:
            chain.launch()
            seq.land((), chain)
            chain.join()
        return chain

    small = [b_q, b_v, b_out, gain_one, shift_one, b_fc2, gain_two, shift_two, b_fc1]
    qkv = last_three(Gather(seq, first_payload(q, w_qkv, small), n, bits))
    qkv.launch()
    rest_own, two_own = payloads([seq.at(q), q ^ 2], w_fc1, w_fc2)
    rest_own, two_own = seq.land((rest_own, two_own), qkv)
    rest = Sent(lax.all_gather(rest_own, "fsdp", axis=0, tiled=False))
    two = Sent(lax.all_gather(two_own, "fsdp", axis=0, tiled=False))
    out_own = [lax.dynamic_slice(w_out, (0, g * quarter), (rows, quarter)) for g in (q, q ^ 2)]
    out = last_three(Gather(seq, jnp.concatenate(out_own, axis=1).astype(half), n, bits))

    def spread_rows(value):
        split = value.reshape(n_img, patches, width)
        return jnp.pad(split, ((0, 0), (0, padded - patches), (0, 0)))

    def compact(value):
        return value.reshape(n_img, padded, width)[:, :patches].reshape(row_count, width)

    qkv.join()
    qkv.launch()
    out.launch()
    spread_tokens = seq.land(spread_rows(seq.at(tokens)), qkv)
    qkv_near = qkv.join()
    qkv.launch()
    near_b, near_c = Sent(core_swap(qkv.held)), Sent(x_swap(qkv.held))
    seq.land((), out)
    out.join()
    out.launch()
    places = table(scale_codes, width)
    row_place = jnp.broadcast_to(places[:, :, None], (n_img, GRID, GRID, width // 2))
    col_place = jnp.broadcast_to(places[:, None], (n_img, GRID, GRID, width // 2))
    place = jnp.concatenate([row_place, col_place], axis=-1).reshape(n_img, patches, width)
    place = jnp.pad(place, ((0, 0), (0, padded - patches), (0, 0)))
    x_zero = (seq.at(spread_tokens).astype(full) + place).reshape(-1, width)
    x_zero = seq.land(x_zero, qkv, near_b)
    qkv_far = seq.at(qkv.got)
    far_b, far_c = Sent(core_swap(qkv_far)), Sent(x_swap(qkv_far))
    vectors, bias_fc1, bias_qkv = unpack_vectors(seq.at(order), (qkv_near, qkv_far), n, rows, ffq)
    _, _, full_bout, gain_one_f, shift_one_f, full_bfc2, gain_two_f, shift_two_f = vectors
    normed_one = layer_norm(x_zero, gain_one_f, shift_one_f).astype(half)
    normed_one = seq.land(normed_one, far_b)

    first = attention_forward(
        seq.at(order), normed_one, bias_qkv[:2], ((qkv_near, qkv_far), (near_b.value, far_b.value)),
        n_img, patches, factor,
    )
    first = (seq.land(first[0], near_c, far_c, out), *first[1:])
    near_c, far_c = seq.at((near_c.value, far_c.value))
    near_d, far_d = Sent(core_swap(near_c)), Sent(core_swap(far_c))
    out.join()
    out.launch()
    cot = seq.land(spread_rows(cotangent).reshape(-1, width), near_d, far_d)
    second = attention_forward(
        seq.at(order), normed_one, bias_qkv[2:], ((near_c, far_c), (near_d.value, far_d.value)),
        n_img, patches, factor,
    )
    second = (seq.land(second[0], out), *second[1:])
    out_a = seq.at(out.join())
    out_b = Sent(core_swap(out_a))
    seq.land((), out_b)
    outs = (out_a, out_b.value)
    qkv_parts = (
        (qkv_near, qkv_far), (near_b.value, far_b.value), (near_c, far_c), (near_d.value, far_d.value)
    )
    qkvs = (*first[:2], *second[:2])
    mixed = (*first[2:4], *second[2:4])
    lses = (*first[4:], *second[4:])
    after_attn, normed_two = attention_out(
        seq.at(order), x_zero, mixed, outs, full_bout, gain_two_f, shift_two_f
    )
    normed_two = seq.land(normed_two, rest)
    rest_a = seq.at(rest.value)
    rest_b = Sent(core_swap(rest_a))
    up_c = Sent(x_swap(seq.at(rest_a[:, :, :hidden])))
    seq.land((), rest_b)
    rests = (rest_a, rest_b.value)

    g_0, g_1, g_bias_a, out_sum, back_sum = mlp(
        seq.at(order), normed_two, cot, bias_fc1[:2], rests, rests, hidden
    )
    g_1 = seq.land(g_1, up_c, two)
    up_c, two = seq.at((up_c.value, two.value))
    up_d, two_d = Sent(core_swap(up_c)), Sent(core_swap(two))
    got_1 = Sent(core_swap(g_1))
    seq.land((), up_d, two_d, got_1)
    red = Reduce(seq, (g_0, got_1.value), n)
    red.launch()
    g_2, g_3, g_bias_b, _, grad_two_in, block = mlp(
        seq.at(order), normed_two, cot, bias_fc1[2:], (up_c, up_d.value), (two, two_d.value), 0,
        (out_sum, back_sum), (after_attn, full_bfc2),
    )
    g_3 = seq.land(g_3, red)
    got_3 = Sent(core_swap(g_3))
    red.launch()
    seq.land((), got_3)
    red_two = Reduce(seq, (g_2, got_3.value), n)
    red_two.launch()

    after_grad, mg0, mg1, mg2, mg3, g_out, sums_two = attention_out_back(
        seq.at(order), grad_two_in, after_attn, cot, gain_two_f, mixed, outs
    )
    mg2 = seq.land(mg2, red)
    red.launch()
    g_w2, g_w3, proj2, proj3, sums_b = attention_back(
        seq.at(order), normed_one, qkvs[2:], lses[2:], (mg2, mg3), g_out, (2, 3), n_img, patches, factor, n
    )
    g_w3 = seq.land(g_w3, red, red_two)
    w_3 = Sent(core_swap(g_w3))
    red_two.launch()
    seq.land((), w_3)
    middle = n // 2
    half_shape = (2,) * (len(bits) - 1)
    w_high = Sent(x_swap(seq.at(rounded_sum([g_w2[middle:], w_3.value[middle:]]))))
    g_w0, g_w1, proj0, proj1, sums_a = attention_back(
        seq.at(order), normed_one, qkvs[:2], lses[:2], (mg0, mg1), g_out, (0, 1), n_img, patches, factor, n
    )
    g_w1 = seq.land(g_w1, red_two, w_high)
    w_1 = Sent(core_swap(g_w1))
    red_two.launch()
    seq.land((), w_1)
    red_w = Reduce(seq, (g_w0, w_1.value), n)
    red_w.launch(0, [w_high.value.reshape(half_shape + w_high.value.shape[1:])])
    w_low = Sent(x_swap(seq.at(rounded_sum([g_w2[:middle], w_3.value[:middle]]))))
    tokens_grad, sums_one = input_back(
        seq.at(order), x_zero, after_grad, gain_one_f, (proj0, proj1, proj2, proj3), qkv_parts
    )
    sums_one = seq.land(sums_one, red_two, red_w, w_low)
    red_w.terms = [*red_w.terms, w_low.value.reshape(half_shape + w_low.value.shape[1:])]
    while len(red_w.axes) > 2:
        red_w.launch()
        seq.land((), red_w)
    red_w.launch()
    cross = Sent(x_swap(seq.at(red_two.rest().piece())))
    packed = pack_sums(
        seq.at(order), n, rows, ffq, (sums_a, sums_b), (g_bias_a, g_bias_b), (sums_two, sums_one)
    )
    packed = seq.at(packed)
    peers = Sent([xor_swap(packed, "dp", 4, m) for m in (1, 2, 3)])
    seq.land((), peers)
    sums = Reduce(seq, (packed, *peers.value), n, full)
    while len(sums.axes) > 1:
        sums.launch()
        if len(sums.axes) > 1:
            seq.land((), sums)
    seq.land((), sums, red_w, cross)
    if red_w.axes:
        red_w.launch()
    mlp_spread = Spread(seq, rounded_sum([*red.rest().terms, cross.value]))
    sums.launch()
    block, tokens_grad = seq.at((block, tokens_grad))
    block_out, grad_tokens = seq.land(
        (compact(block), compact(tokens_grad)), sums, mlp_spread, *([red_w] if len(bits) > 1 else [])
    )
    small_sums = sums.piece()
    w_spread = Spread(seq, red_w.piece())
    mlp_spread.cross()
    small_sums = seq.land(small_sums, mlp_spread)
    mlp_pieces = seq.at(mlp_spread.pieces)
    out_fc1, out_fc2 = finish_mlp(q, mlp_pieces, n)
    out_fc2, small_sums = seq.land((out_fc2, small_sums), w_spread)
    w_spread.cross()
    seq.land((), w_spread)
    out_qkv, out_out = finish_attention(seq.value, w_spread.pieces)
    small_out = [small_sums[k, :rows] for k in range(8)]
    out_bfc1 = small_sums[8:12, :ffq].reshape(-1)
    o_bq, o_bv, o_bout, o_gone, o_sone, o_bfc2, o_gtwo, o_stwo = small_out
    return (
        block_out,
        grad_tokens,
        out_qkv,
        o_bq,
        o_bv,
        out_out,
        o_bout,
        o_gone,
        o_sone,
        out_fc1,
        out_bfc1,
        out_fc2,
        o_bfc2,
        o_gtwo,
        o_stwo,
    )


def solution(mesh):
    rows_split = P(("dp", "fsdp"), None)
    matrix = P("fsdp", None)
    vector = P("fsdp")
    return jax.shard_map(
        local,
        mesh=mesh,
        in_specs=(
            rows_split, P(("dp", "fsdp")), matrix, vector, vector, matrix, vector, vector, vector,
            matrix, vector, matrix, vector, vector, vector, rows_split,
        ),
        out_specs=(
            rows_split, rows_split, matrix, vector, vector, matrix, vector, vector, vector,
            matrix, vector, matrix, vector, vector, vector,
        ),
        check_vma=False,
    )
```

```python
import math

import jax
import jax.numpy as jnp
from jax import lax
from jax.experimental import pallas as pl
from jax.experimental.pallas import tpu as pltpu
from jax.sharding import PartitionSpec as P

HEADS = 16
GRID = 14
NSCALE = 16
norm_eps = 1e-06
half = jnp.bfloat16
full = jnp.float32


def xor_swap(value, axis, size, mask):
    return lax.ppermute(value, axis, [(i, i ^ mask) for i in range(size)])


def core_swap(value):
    return xor_swap(value, "dp", 4, 1)


def x_swap(value):
    return xor_swap(value, "dp", 4, 2)


def masks(bits):
    found = [0]
    for bit in bits:
        found = found + [m | (1 << bit) for m in found]
    return found


class Order:
    def __init__(self, value):
        self.value = value

    def at(self, value):
        value, self.value = lax.optimization_barrier((value, self.value))
        return value

    def land(self, value, *sent):
        value, flights = self.at((value, [s.flight for s in sent]))
        for s, flight in zip(sent, flights, strict=True):
            s.accept(flight)
        return value


class Sent:
    def __init__(self, flight):
        self.flight = flight

    def accept(self, value):
        self.value = value


class Gather:
    def __init__(self, seq, piece, n, bits):
        self.seq, self.held, self.n, self.bits = seq, piece[None], n, list(bits)

    def launch(self):
        self.held = self.seq.at(self.held)
        self.flight = xor_swap(self.held, "fsdp", self.n, 1 << self.bits.pop(0))

    def accept(self, value):
        self.got = value

    def join(self):
        self.held = jnp.concatenate([self.held, self.got])
        return self.held


def rounded_sum(terms, kind=half):
    return sum(t.astype(full) for t in terms).astype(kind)


class Reduce:
    def __init__(self, seq, terms, n, kind=half):
        self.kind = kind
        self.seq, self.n, self.axes = seq, n, list(range(n.bit_length() - 1))
        self.terms = [t.reshape((2,) * len(self.axes) + t.shape[1:]) for t in terms]

    def launch(self, bit=None, more=()):
        bit = self.axes[0] if bit is None else bit
        axis = self.axes.index(bit)
        self.axes.pop(axis)
        low, high = [
            [lax.index_in_dim(t, side, axis, keepdims=False) for t in self.terms] for side in (0, 1)
        ]
        self.terms = low
        self.flight = xor_swap(self.seq.at(rounded_sum([*high, *more], self.kind)), "fsdp", self.n, 1 << bit)

    def accept(self, value):
        self.terms = [*self.terms, value]

    def rest(self):
        while self.axes:
            self.launch()
            self.seq.land((), self)
        return self

    def piece(self):
        return rounded_sum(self.terms, self.kind)


class Spread:
    def __init__(self, seq, piece):
        self.seq, self.pieces = seq, [seq.at(piece)]
        self.flight = [core_swap(self.pieces[0]), x_swap(self.pieces[0])]

    def cross(self):
        self.flight = [core_swap(self.seq.at(self.pieces[2]))]

    def accept(self, value):
        self.pieces += value


ANYWHERE = pl.BlockSpec(memory_space=pl.ANY)
ON_CHIP = pl.BlockSpec(memory_space=pltpu.VMEM)
SCALARS = pl.BlockSpec(memory_space=pltpu.SMEM)


def dot(left, right, dim_left, dim_right):
    return lax.dot_general(
        left, right, (((dim_left,), (dim_right,)), ((), ())), preferred_element_type=full
    )


def call(kernel, name, operands, in_specs, outs, out_specs, scratch):
    return pl.pallas_call(
        kernel,
        out_shape=[jax.ShapeDtypeStruct(shape, kind) for shape, kind in outs],
        in_specs=in_specs,
        out_specs=out_specs,
        scratch_shapes=scratch,
        compiler_params=pltpu.CompilerParams(vmem_limit_bytes=58 * 2**20),
        name=name,
    )(*operands)


def loop(count, body, unroll=1):
    def step(i, carry):
        body(i)
        return carry

    lax.fori_loop(0, count, step, 0, unroll=unroll)


def tile(i, size):
    return pl.ds(pl.multiple_of(i * size, size), size)


def bring(src, dst, sem):
    pltpu.make_async_copy(src, dst, sem).start()


def arrived(dst, sem):
    pltpu.make_async_copy(dst, dst, sem).wait()


def fetch(parts, order_ref, place, sem):
    base = 0
    for part in parts:

        def start(r, part=part, base=base):
            shard = r if order_ref is None else order_ref[base + r]
            pltpu.make_async_copy(part.at[r], place(shard), sem).start()

        loop(part.shape[0], start)
        base += part.shape[0]


def head_rows(s, q, n, rows, quarter):
    per = n // 4
    return pl.multiple_of(((s // per) ^ q) * quarter + (s % per) * rows, rows)


def pair_scores(q2, k2):
    first = lax.broadcasted_iota(jnp.int32, q2.shape, 1) < q2.shape[1] // 2
    both = apart(q2, first)
    return both, dot(k2, both, 1, 1), first


def apart(value, first):
    zero = jnp.zeros_like(value)
    return jnp.concatenate([jnp.where(first, value, zero), jnp.where(first, zero, value)])


def attention_forward(order, normed, bias, weights, n_img, patches, factor):
    groups, n_parts = len(weights), len(weights[0])
    wide = weights[0][0].shape[2]
    count, width = normed.shape
    rows = width // sum(part.shape[0] for part in weights[0])
    padded = count // n_img
    quarter = wide // 3

    def kernel(order_ref, normed_ref, bias_ref, *refs):
        w_refs, refs = refs[: groups * n_parts], refs[groups * n_parts :]
        qkv_refs, mixed_refs, refs = refs[:groups], refs[groups : 2 * groups], refs[2 * groups :]
        lse_refs, (w_held, sems) = refs[:groups], refs[groups:]
        for g in range(groups):
            fetch(
                [w.at[:, pl.ds(0, rows)] for w in w_refs[g * n_parts : (g + 1) * n_parts]],
                order_ref,
                lambda s, g=g: w_held.at[g, pl.ds(pl.multiple_of(s * rows, rows), rows)],
                sems.at[g],
            )
        for g in range(groups):
            pltpu.make_async_copy(w_held.at[g], w_held.at[g], sems.at[g]).wait()

            def project(t, g=g):
                at = tile(t, quarter)
                product = dot(normed_ref[...], w_held[g, :, at], 1, 0)
                qkv_refs[g][:, at] = (product + bias_ref[g, :, at]).astype(half)

            loop(3, project)

            def attend(i, g=g):
                at = tile(i // 2, padded)
                lanes = [pl.ds(pl.multiple_of(t * quarter + (i % 2) * 128, 128), 128) for t in range(3)]
                q2 = qkv_refs[g][at, lanes[0]] * factor
                k2 = qkv_refs[g][at, lanes[1]]
                v2 = qkv_refs[g][at, lanes[2]]
                _, scores, first = pair_scores(q2, k2)
                key = lax.broadcasted_iota(jnp.int32, scores.shape, 0)
                scores = jnp.where(key < patches, scores, -1e30)
                top = jnp.max(scores, axis=0, keepdims=True)
                raised = jnp.exp(scores - top)
                total = jnp.sum(raised, axis=0, keepdims=True)
                lse_refs[g][i] = top + jnp.log(total)
                out = dot((raised * (1.0 / total)).astype(half), v2, 0, 0)
                mixed_refs[g][at, lanes[0]] = jnp.where(first, out[:padded], out[padded:]).astype(half)

            loop(2 * n_img, attend, 2 * n_img)

    return call(
        kernel,
        "attention_forward",
        (order, normed, bias, *(part for w in weights for part in w)),
        [SCALARS, ON_CHIP, ON_CHIP] + [ANYWHERE] * (groups * n_parts),
        [((count, wide), half)] * groups
        + [((count, quarter), half)] * groups
        + [((2 * n_img, 1, 2 * padded), full)] * groups,
        [ON_CHIP] * (3 * groups),
        [pltpu.VMEM((groups, width, wide), half), pltpu.SemaphoreType.DMA((groups,))],
    )


def layer_norm(value, gain, shift):
    center = jnp.mean(value, axis=-1, keepdims=True)
    offset = value - center
    spread = jnp.mean(offset * offset, axis=-1, keepdims=True)
    return offset * lax.rsqrt(spread + norm_eps) * gain + shift


def layer_norm_back(value, grad, gain):
    center = jnp.mean(value, axis=-1, keepdims=True)
    offset = value - center
    scale = lax.rsqrt(jnp.mean(offset * offset, axis=-1, keepdims=True) + norm_eps)
    unit = offset * scale
    scaled = grad * gain
    inner = jnp.mean(scaled * unit, axis=-1, keepdims=True)
    return scale * (scaled - jnp.mean(scaled, axis=-1, keepdims=True) - unit * inner), grad * unit


def load_out(order_ref, out_refs, held, sem, n, rows, quarter):
    q = order_ref[n]
    for j in range(4):
        column = pl.multiple_of((q ^ j) * quarter, quarter)
        fetch(
            [out_refs[j % 2].at[:, :, pl.ds(j // 2 * quarter, quarter)]],
            order_ref,
            lambda s, column=column: held.at[
                pl.ds(head_rows(s, q, n, rows, quarter), rows), pl.ds(column, quarter)
            ],
            sem,
        )


CHUNK = 16
ROWS = 64


def attention_out(order, x_zero, mixed, outs, bias, gain, shift):
    count, width = x_zero.shape
    n, rows, _ = outs[0].shape
    quarter = mixed[0].shape[1]

    def kernel(order_ref, x_ref, bias_ref, gain_ref, shift_ref, *refs):
        mixed_refs, out_refs = refs[:4], refs[4:6]
        after_ref, normed_ref, held, x_held, sems = refs[6:]
        bring(x_ref, x_held, sems.at[1])
        load_out(order_ref, out_refs, held, sems.at[0], n, rows, quarter)
        together = jnp.concatenate([m[...] for m in mixed_refs], axis=1)
        pltpu.make_async_copy(held, held, sems.at[0]).wait()
        after_ref[...] = dot(together, held[...], 1, 0)
        arrived(x_held, sems.at[1])

        def finish(i):
            at = tile(i, CHUNK)
            after = x_held[at] + (after_ref[at] + bias_ref[...])
            after_ref[at] = after
            normed_ref[at] = layer_norm(after, gain_ref[...], shift_ref[...]).astype(half)

        loop(count // CHUNK, finish, 13)

    return call(
        kernel,
        "attention_out",
        (order, x_zero, bias, gain, shift, *mixed, *outs),
        [SCALARS, ANYWHERE] + [ON_CHIP] * 7 + [ANYWHERE] * 2,
        [((count, width), full), ((count, width), half)],
        [ON_CHIP] * 2,
        [
            pltpu.VMEM((width, width), half),
            pltpu.VMEM((count, width), full),
            pltpu.SemaphoreType.DMA((2,)),
        ],
    )


def mlp(order, normed, cot, bias, up_all, down_all, down_start, carried=None, ending=None):
    count, width = normed.shape
    n, rows, _ = up_all.shape
    hidden = bias.shape[1]
    share = hidden // n
    step = min(512, hidden)
    steps = hidden // step
    more = [*(carried or []), *(ending[:1] if ending else [])]
    last = list(ending[1:]) if ending else []

    def kernel(order_ref, bias_ref, *refs):
        last_refs, refs = refs[: len(last)], refs[len(last) :]
        normed_ref, cot_ref, up_ref, down_ref, refs = *refs[:4], refs[4:]
        more_refs, refs = refs[: len(more)], refs[len(more) :]
        grad_ref, g_bias_ref, back_ref, end_ref, refs = *refs[:4], refs[4:]
        held, refs = refs[: len(more)], refs[len(more) :]
        rows_in, cots, out, back, up, down, pre, act, act_half, pre_half, g_up, g_down, sems = refs
        bring(normed_ref, rows_in, sems.at[3])
        fetch(
            [up_ref.at[:, :, pl.ds(0, hidden)]],
            None,
            lambda s: up.at[pl.ds(pl.multiple_of(s * rows, rows), rows)],
            sems.at[0],
        )
        bring(cot_ref, cots, sems.at[4])
        fetch(
            [down_ref.at[:, :, pl.ds(down_start, width)]],
            None,
            lambda s: down.at[pl.ds(pl.multiple_of(s * share, share), share)],
            sems.at[1],
        )
        for k in range(len(more)):
            bring(more_refs[k], held[k], sems.at[5 + k])
        arrived(rows_in, sems.at[3])
        arrived(up, sems.at[0])
        for t in range(steps):
            at = pl.ds(t * step, step)
            pre[...] = dot(rows_in[...], up[:, at], 1, 0)
            if not t:
                arrived(cots, sems.at[4])
                arrived(down, sems.at[1])
            act[...] = dot(cots[...], down[at, :], 1, 1)

            def gelu(i, at=at):
                some = tile(i, 2 * CHUNK)
                x = pre[some] + bias_ref[:, at]
                below = 0.5 * (1.0 + lax.erf(x * math.sqrt(0.5)))
                density = jnp.exp(-0.5 * x * x) * (1.0 / math.sqrt(2.0 * math.pi))
                act_half[some] = (x * below).astype(half)
                pre_half[some] = (act[some] * (below + x * density)).astype(half)

            loop(count // CHUNK // 2, gelu)
            p = pre_half[...]
            h = act_half[...]
            more_back = dot(p, up[:, at], 1, 1)
            more_out = dot(h, down[at, :], 1, 0)
            if t:
                back[...] += more_back
                out[...] += more_out
            elif carried:
                arrived(held[0], sems.at[5])
                arrived(held[1], sems.at[6])
                out[...] = held[0][...] + more_out
                back[...] = held[1][...] + more_back
            else:
                out[...] = more_out
                back[...] = more_back
            if t == steps - 1:
                bring(back, back_ref, sems.at[3])
                if not ending:
                    bring(out, end_ref, sems.at[4])
            g_down[at, :] = dot(h, cots[...], 0, 0).astype(half)
            if t == steps - 1:

                def send_down(r):
                    at = pl.multiple_of(order_ref[r] * share, share)
                    bring(g_down.at[pl.ds(at, share)], grad_ref.at[r, 1], sems.at[2])

                loop(n, send_down)
            g_up[:, at] = dot(rows_in[...], p, 0, 0).astype(half)
            g_bias_ref[:, at] = jnp.sum(p.astype(full), axis=0, keepdims=True)

        def send_up(r):
            at = pl.multiple_of(order_ref[r] * rows, rows)
            bring(g_up.at[pl.ds(at, rows)], grad_ref.at[r, 0], sems.at[2])

        loop(n, send_up)
        if ending:
            arrived(held[2], sems.at[7])

            def finish(i):
                at = tile(i, 2 * CHUNK)
                end_ref[at] = (held[2][at] + (out[at] + last_refs[0][...])).astype(half)

            loop(count // CHUNK // 2, finish)
        else:
            arrived(end_ref, sems.at[4])
        arrived(back_ref, sems.at[3])
        arrived(grad_ref, sems.at[2])

    sums = pltpu.VMEM((count, width), full)
    wide = pltpu.VMEM((count, width), half)
    square = pltpu.VMEM((width, hidden), half)
    return call(
        kernel,
        "mlp",
        (order, bias, *last, normed, cot, up_all, down_all, *more),
        [SCALARS] + [ON_CHIP] * (1 + len(last)) + [ANYWHERE] * (4 + len(more)),
        [
            ((n, 2, rows, width), half),
            ((1, hidden), full),
            ((count, width), full),
            ((count, width), half if ending else full),
        ],
        [ANYWHERE, ON_CHIP, ANYWHERE, ON_CHIP if ending else ANYWHERE],
        [
            *([sums] * len(more)),
            wide,
            wide,
            sums,
            sums,
            square,
            pltpu.VMEM((hidden, width), half),
            pltpu.VMEM((count, step), full),
            pltpu.VMEM((count, step), full),
            pltpu.VMEM((count, step), half),
            pltpu.VMEM((count, step), half),
            square,
            pltpu.VMEM((hidden, width), half),
            pltpu.SemaphoreType.DMA((5 + len(more),)),
        ],
    )


def attention_out_back(order, grad, after, cot, gain, mixed, outs):
    count, width = after.shape
    n, rows, _ = outs[0].shape
    quarter = mixed[0].shape[1]

    def kernel(order_ref, grad_ref, after_ref, cot_ref, gain_ref, *refs):
        mixed_refs, out_refs, refs = refs[:4], refs[4:6], refs[6:]
        after_grad_ref, mixed_grad_refs, g_out_ref, sums_ref = refs[0], refs[1:5], refs[5], refs[6]
        held, branch, terms, grad, after, cot, mixes, sems = refs[7:]
        block = count // 4
        for k in range(4):
            some = pl.ds(k * block, block)
            bring(grad_ref.at[some], grad.at[some], sems.at[1 + k])
            bring(after_ref.at[some], after.at[some], sems.at[5 + k])
            bring(cot_ref.at[some], cot.at[some], sems.at[9 + k])
        load_out(order_ref, out_refs, held, sems.at[0], n, rows, quarter)
        for j in range(4):
            bring(mixed_refs[j], mixes.at[j], sems.at[13])
        terms[...] = jnp.zeros_like(terms)

        def fold(value):
            return jnp.sum(value.reshape(CHUNK // 8, 8, width), axis=0)

        def back(i, k):
            at = pl.ds(pl.multiple_of(k * block + i * CHUNK, CHUNK), CHUNK)
            incoming = grad[at]
            part, gain_terms = layer_norm_back(after[at], incoming, gain_ref[...])
            own = cot[at].astype(full)
            total = own + part
            after_grad_ref[at] = total
            rounded = total.astype(half)
            branch[at] = rounded
            terms[0] += fold(rounded.astype(full))
            terms[1] += fold(gain_terms)
            terms[2] += fold(incoming)
            terms[3] += fold(own)

        for k in range(4):
            some = pl.ds(k * block, block)
            arrived(grad.at[some], sems.at[1 + k])
            arrived(after.at[some], sems.at[5 + k])
            arrived(cot.at[some], sems.at[9 + k])
            loop(block // CHUNK, lambda i, k=k: back(i, k), 13)
        for k in range(4):
            sums_ref[k] = jnp.sum(terms[k], axis=0, keepdims=True)
        arrived(held, sems.at[0])
        arrived(mixes, sems.at[13])
        for j in range(4):
            mixed_grad_refs[j][...] = dot(branch[...], held[j * quarter : (j + 1) * quarter], 1, 1).astype(half)
            g_out_ref[j * quarter : (j + 1) * quarter] = dot(mixes[j], branch[...], 0, 0).astype(half)

    return call(
        kernel,
        "attention_out_back",
        (order, grad, after, cot, gain, *mixed, *outs),
        [SCALARS] + [ANYWHERE] * 3 + [ON_CHIP] + [ANYWHERE] * 6,
        [((count, width), full)]
        + [((count, quarter), half)] * 4
        + [((width, width), half), ((4, 1, width), full)],
        [ON_CHIP] * 7,
        [
            pltpu.VMEM((width, width), half),
            pltpu.VMEM((count, width), half),
            pltpu.VMEM((4, 8, width), full),
            pltpu.VMEM((count, width), full),
            pltpu.VMEM((count, width), full),
            pltpu.VMEM((count, width), half),
            pltpu.VMEM((4, count, quarter), half),
            pltpu.SemaphoreType.DMA((14,)),
        ],
    )


def attention_back(order, normed, qkvs, lses, mixed_grads, g_out, which, n_img, patches, factor, n):
    groups = len(qkvs)
    count, width = normed.shape
    wide = qkvs[0].shape[1]
    quarter = wide // 3
    padded = count // n_img
    rows = width // n

    def kernel(order_ref, normed_ref, g_out_ref, *refs):
        qkv_refs, mg_refs, refs = refs[:groups], refs[groups : 2 * groups], refs[2 * groups :]
        lse_refs, refs = refs[:groups], refs[groups:]
        g_w_refs, proj_refs, sums_ref = refs[:groups], refs[groups : 2 * groups], refs[2 * groups]
        g_w, normed_held, g_out_held, sems = refs[2 * groups + 1 :]
        q = order_ref[n]
        bring(g_out_ref, g_out_held, sems.at[groups])
        bring(normed_ref, normed_held, sems.at[groups + 1])
        for g in range(groups):

            def attend(i, g=g):
                at = tile(i // 2, padded)
                lanes = [pl.ds(pl.multiple_of(t * quarter + (i % 2) * 128, 128), 128) for t in range(3)]
                q2 = qkv_refs[g][at, lanes[0]] * factor
                k2 = qkv_refs[g][at, lanes[1]]
                v2 = qkv_refs[g][at, lanes[2]]
                both, scores, first = pair_scores(q2, k2)
                key = lax.broadcasted_iota(jnp.int32, scores.shape, 0)
                probs = jnp.where(key < patches, jnp.exp(scores - lse_refs[g][i]), 0.0)
                o_both = apart(mg_refs[g][at, lanes[0]], first)
                g_probs = dot(v2, o_both, 1, 1)
                weighted = jnp.sum(probs * g_probs, axis=0, keepdims=True)
                g_scores = (probs * (g_probs - weighted)).astype(half)
                g_query = dot(g_scores, k2, 0, 0)
                g_query = jnp.where(first, g_query[:padded], g_query[padded:]) * factor
                proj_refs[g][at, lanes[0]] = g_query.astype(half)
                proj_refs[g][at, lanes[1]] = dot(g_scores, both, 1, 0).astype(half)
                proj_refs[g][at, lanes[2]] = dot(probs.astype(half), o_both, 1, 0).astype(half)

            loop(2 * n_img, attend, 4)
            if not g:
                arrived(g_out_held, sems.at[groups])
                arrived(normed_held, sems.at[groups + 1])

            def send_out(r, g=g):
                at = head_rows(order_ref[r], q, n, rows, quarter)
                column = pl.multiple_of((q ^ which[g]) * quarter, quarter)
                pltpu.make_async_copy(
                    g_out_held.at[pl.ds(at, rows), pl.ds(column, quarter)],
                    g_w_refs[g].at[r, :, pl.ds(wide, quarter)],
                    sems.at[g],
                ).start()

            loop(n, send_out)

            def weigh(t, g=g):
                at = tile(t, quarter)
                some = proj_refs[g][:, at]
                g_w[g, :, at] = dot(normed_held[...], some, 0, 0).astype(half)
                sums_ref[g, :, at] = jnp.sum(some.astype(full), axis=0, keepdims=True)

            loop(3, weigh)

            def send(r, g=g):
                at = pl.multiple_of(order_ref[r] * rows, rows)
                pltpu.make_async_copy(
                    g_w.at[g, pl.ds(at, rows)], g_w_refs[g].at[r, :, pl.ds(0, wide)], sems.at[g]
                ).start()

            loop(n, send)
        for g in range(groups):
            pltpu.make_async_copy(g_w_refs[g], g_w_refs[g], sems.at[g]).wait()

    return call(
        kernel,
        "attention_back",
        (order, normed, g_out, *qkvs, *mixed_grads, *lses),
        [SCALARS] + [ANYWHERE] * 2 + [ON_CHIP] * (3 * groups),
        [((n, rows, wide + quarter), half)] * groups
        + [((count, wide), half)] * groups
        + [((groups, 1, wide), full)],
        [ANYWHERE] * groups + [ON_CHIP] * (groups + 1),
        [
            pltpu.VMEM((groups, width, wide), half),
            pltpu.VMEM((count, width), half),
            pltpu.VMEM((width, width), half),
            pltpu.SemaphoreType.DMA((groups + 2,)),
        ],
    )


def input_back(order, x_zero, after_grad, gain, projs, weights):
    count, width = x_zero.shape
    wide = weights[0][0].shape[2]
    rows = width // sum(part.shape[0] for part in weights[0])
    parts = [part for w in weights for part in w]
    n_parts = len(weights[0])

    def kernel(order_ref, x_ref, after_ref, gain_ref, *refs):
        proj_refs, w_refs = refs[:4], refs[4 : 4 + len(parts)]
        token_ref, sums_ref, held, terms, x_held, after_held, sems = refs[4 + len(parts) :]
        for j in range(4):
            fetch(
                [w.at[:, pl.ds(0, rows)] for w in w_refs[j * n_parts : (j + 1) * n_parts]],
                order_ref,
                lambda s, j=j: held.at[j, pl.ds(pl.multiple_of(s * rows, rows), rows)],
                sems.at[j],
            )
        bring(x_ref, x_held, sems.at[4])
        bring(after_ref, after_held, sems.at[5])
        for j in range(4):
            arrived(held.at[j], sems.at[j])
            product = dot(proj_refs[j][...], held[j], 1, 1)
            if j == 0:
                token_ref[...] = product
            else:
                token_ref[...] += product
        arrived(x_held, sems.at[4])
        arrived(after_held, sems.at[5])
        terms[...] = jnp.zeros_like(terms)

        def fold(value):
            return jnp.sum(value.reshape(ROWS // 8, 8, width), axis=0)

        def back(i):
            at = tile(i, ROWS)
            incoming = token_ref[at]
            part, gain_terms = layer_norm_back(x_held[at], incoming, gain_ref[...])
            token_ref[at] = after_held[at] + part
            terms[0] += fold(gain_terms)
            terms[1] += fold(incoming)

        loop(count // ROWS, back)
        for k in range(2):
            sums_ref[k] = jnp.sum(terms[k], axis=0, keepdims=True)

    return call(
        kernel,
        "input_back",
        (order, x_zero, after_grad, gain, *projs, *parts),
        [SCALARS] + [ANYWHERE] * 2 + [ON_CHIP] * 5 + [ANYWHERE] * len(parts),
        [((count, width), full), ((2, 1, width), full)],
        [ON_CHIP] * 2,
        [
            pltpu.VMEM((4, width, wide), half),
            pltpu.VMEM((2, 8, width), full),
            pltpu.VMEM((count, width), full),
            pltpu.VMEM((count, width), full),
            pltpu.SemaphoreType.DMA((6,)),
        ],
    )


def payloads(which, w_fc1, w_fc2):
    rows, ff = w_fc1.shape
    full_share, width = w_fc2.shape
    share = full_share // 4
    n = ff // full_share
    hidden = n * share
    own, across = which
    if share % 128:
        fc1 = [lax.dynamic_slice(w_fc1, (0, (4 * s + own) * share), (rows, share)) for s in range(n)]
        fc2 = [lax.dynamic_slice(w_fc2, (g * share, 0), (share, width)).astype(half) for g in which]
        rest = jnp.concatenate([*fc1, fc2[0].reshape(rows, -1).astype(full)], axis=1)
        return rest.astype(half), fc2[1]

    def kernel(which_ref, fc1_ref, fc2_ref, rest_ref, two_ref):
        for s in range(n):
            at = pl.ds(pl.multiple_of((4 * s + which_ref[0]) * share, share), share)
            rest_ref[:, s * share : (s + 1) * share] = fc1_ref[:, at].astype(half)
        rest_ref[:, hidden : hidden + width] = fc2_ref[tile(which_ref[0], share), :].astype(half)
        two_ref[...] = fc2_ref[tile(which_ref[1], share), :].astype(half)

    return call(
        kernel,
        "payloads",
        (jnp.stack(which), w_fc1, w_fc2),
        [SCALARS] + [ON_CHIP] * 2,
        [((rows, hidden + width), half), ((share, width), half)],
        [ON_CHIP] * 2,
        [],
    )


def natural_quarters(q, pieces):
    once = [jnp.where((q & 1) == 1, pieces[i ^ 1], pieces[i]) for i in range(4)]
    return [jnp.where(q >= 2, once[i ^ 2], once[i]) for i in range(4)]


def finish_mlp(q, pieces, n):
    _, rows, width = pieces[0].shape
    share = width // n
    if share % 128:
        pieces = natural_quarters(q, pieces)
        fc1 = jnp.stack([p[0].reshape(rows, n, share) for p in pieces], axis=2).reshape(rows, 4 * width)
        return fc1.astype(full), jnp.concatenate([p[1] for p in pieces]).astype(full)

    def kernel(q_ref, *refs):
        fc1_ref, fc2_ref = refs[4:]
        for j in range(4):
            g = q_ref[0] ^ j
            for s in range(n):
                at = pl.ds(pl.multiple_of((4 * s + g) * share, share), share)
                fc1_ref[:, at] = refs[j][0, :, s * share : (s + 1) * share].astype(full)
            fc2_ref[tile(g, rows), :] = refs[j][1].astype(full)

    return call(
        kernel,
        "finish_mlp",
        (q[None], *pieces),
        [SCALARS] + [ON_CHIP] * 4,
        [((rows, 4 * width), full), ((4 * rows, width), full)],
        [ON_CHIP] * 2,
        [],
    )


def finish_attention(q, pieces):
    rows, width = pieces[0].shape
    quarter = width // 4

    def kernel(q_ref, *refs):
        qkv_ref, out_ref = refs[4:]
        for j in range(4):
            g = q_ref[0] ^ j
            for t in range(3):
                at = pl.ds(pl.multiple_of(t * width + g * quarter, quarter), quarter)
                qkv_ref[:, at] = refs[j][:, t * quarter : (t + 1) * quarter].astype(full)
            out_ref[:, tile(g, quarter)] = refs[j][:, 3 * quarter :].astype(full)

    return call(
        kernel,
        "finish_attention",
        (q[None], *pieces),
        [SCALARS] + [ON_CHIP] * 4,
        [((rows, 3 * width), full), ((rows, width), full)],
        [ON_CHIP] * 2,
        [],
    )


BELOW = 16


def first_payload(q, w_qkv, vectors):
    rows, columns = w_qkv.shape
    width = columns // 3
    quarter = width // 4
    wide = 3 * quarter

    def kernel(q_ref, w_ref, *refs):
        out_ref, held, low, sem = refs[len(vectors) :]
        for t in range(3):
            at = pl.multiple_of(t * width + q_ref[0] * quarter, quarter)
            pltpu.make_async_copy(
                w_ref.at[:, pl.ds(at, quarter)], held.at[:, pl.ds(t * quarter, quarter)], sem.at[0]
            ).start()
        low[...] = jnp.zeros_like(low)
        for k, vector in enumerate(refs[: len(vectors)]):
            low[k : k + 1, : vector.shape[1]] = vector[...]
        out_ref[rows:] = low[...].astype(half)
        pltpu.make_async_copy(held, held, sem.at[0]).wait()
        out_ref[:rows] = held[...].astype(half)

    return call(
        kernel,
        "first_payload",
        (q[None], w_qkv, *(v[None] for v in vectors)),
        [SCALARS, ANYWHERE] + [ON_CHIP] * len(vectors),
        [((rows + BELOW, wide), half)],
        [ON_CHIP],
        [pltpu.VMEM((rows, wide), full), pltpu.VMEM((BELOW, wide), full), pltpu.SemaphoreType.DMA((1,))],
    )[0]


def unpack_vectors(order, parts, n, rows, share):
    width = n * rows
    quarter = width // 4
    if rows % 128 or share % 128:
        q = order[n]
        held = jnp.concatenate([p[:, rows:] for p in parts]).astype(full)
        held = held[jnp.zeros((n,), jnp.int32).at[order[:n]].set(jnp.arange(n, dtype=jnp.int32))]
        groups = jnp.arange(4, dtype=jnp.int32) ^ q
        vectors = jnp.stack([held[:, k, :rows].reshape(1, width) for k in range(8)])
        units = held[:, 8, : 4 * share].reshape(n, 4, share).transpose(1, 0, 2)[groups]
        ends = [vectors[k].reshape(4, 1, quarter)[groups] for k in range(2)]
        return vectors, units.reshape(4, 1, width), jnp.concatenate([ends[0], 0 * ends[0], ends[1]], axis=2)

    def kernel(order_ref, *refs):
        part_refs, (vector_ref, fc1_ref, qkv_ref, held, wider, sem) = refs[: len(parts)], refs[len(parts) :]
        base = 0
        for part in part_refs:
            size = part.shape[0]
            pltpu.make_async_copy(part.at[:, pl.ds(rows, BELOW)], held.at[pl.ds(base, size)], sem.at[0]).start()
            base += size
        pltpu.make_async_copy(held, held, sem.at[0]).wait()
        wider[...] = held[...].astype(full)
        q = order_ref[n]
        for r in range(n):
            at = tile(order_ref[r], rows)
            for k in range(8):
                vector_ref[k, :, at] = wider[r, k : k + 1, :rows]
            for j in range(4):
                fc1_ref[j, :, tile(order_ref[r], share)] = wider[r, 8:9, tile(q ^ j, share)]
        for j in range(4):
            at = tile(q ^ j, quarter)
            qkv_ref[j, :, :quarter] = vector_ref[0, :, at]
            qkv_ref[j, :, quarter : 2 * quarter] = jnp.zeros((1, quarter), full)
            qkv_ref[j, :, 2 * quarter :] = vector_ref[1, :, at]

    return call(
        kernel,
        "unpack_vectors",
        (order, *parts),
        [SCALARS] + [ANYWHERE] * len(parts),
        [((8, 1, width), full), ((4, 1, width), full), ((4, 1, 3 * quarter), full)],
        [ON_CHIP] * 3,
        [
            pltpu.VMEM((n, BELOW, 3 * quarter), half),
            pltpu.VMEM((n, BELOW, 3 * quarter), full),
            pltpu.SemaphoreType.DMA((1,)),
        ],
    )


def pack_sums(order, n, rows, share, proj_sums, unit_sums, wide_sums):
    width = n * rows
    quarter = width // 4
    if rows % 128 or share % 128:
        groups = jnp.arange(4, dtype=jnp.int32) ^ order[n]
        proj = jnp.concatenate(proj_sums)[groups]
        units = jnp.concatenate(unit_sums)[groups].reshape(4, n, share)
        flat = [proj[:, :, :quarter].reshape(width), proj[:, :, 2 * quarter :].reshape(width)]
        two, one = wide_sums
        flat += [two[0], one[0], one[1], two[3], two[1], two[2]]
        flat = [v.reshape(n, 1, rows) for v in flat]
        stacked = [jnp.pad(v, ((0, 0), (0, 0), (0, 128 - rows))) for v in flat]
        stacked.append(jnp.pad(units.transpose(1, 0, 2), ((0, 0), (0, 4), (0, 128 - share))))
        return jnp.concatenate(stacked, axis=1)[order[:n]]

    def kernel(order_ref, proj_a, proj_b, unit_a, unit_b, two_ref, one_ref, out_ref, proj, units):
        proj[:2], proj[2:] = proj_a[...], proj_b[...]
        units[:2], units[2:] = unit_a[...], unit_b[...]
        q = order_ref[n]
        per = n // 4
        for r in range(n):
            s = order_ref[r]
            j = (s // per) ^ q
            at = tile(s, rows)
            inside = pl.multiple_of((s % per) * rows, rows)
            out_ref[r, 0:1] = proj[j, :, pl.ds(inside, rows)]
            out_ref[r, 1:2] = proj[j, :, pl.ds(2 * quarter + inside, rows)]
            for k, (ref, row) in enumerate(
                ((two_ref, 0), (one_ref, 0), (one_ref, 1), (two_ref, 3), (two_ref, 1), (two_ref, 2))
            ):
                out_ref[r, 2 + k : 3 + k] = ref[row, :, at]
            for g in range(4):
                out_ref[r, 8 + g : 9 + g] = units[q ^ g, :, tile(s, share)]
            out_ref[r, 12:] = jnp.zeros((4, rows), full)

    sums_two, sums_one = wide_sums
    return call(
        kernel,
        "pack_sums",
        (order, *proj_sums, *unit_sums, sums_two, sums_one),
        [SCALARS] + [ON_CHIP] * 6,
        [((n, 16, rows), full)],
        [ON_CHIP],
        [pltpu.VMEM((4, 1, 3 * quarter), full), pltpu.VMEM((4, 1, width), full)],
    )[0]


def table(codes, width):
    ratio = 0.3 * jnp.exp(codes.astype(full) * (math.log(10.0 / 0.3) / (NSCALE - 1)))
    quarter = width // 4
    omega = jnp.exp(jnp.arange(quarter).astype(full) * (-math.log(10000.0) / quarter))
    steps = jnp.arange(GRID, dtype=jnp.int32).astype(full)
    angle = ratio[:, None, None] * steps[None, :, None] * omega[None, None, :]
    return jnp.concatenate([jnp.sin(angle), jnp.cos(angle)], axis=-1)


def local(
    tokens,
    scale_codes,
    w_qkv,
    b_q,
    b_v,
    w_out,
    b_out,
    gain_one,
    shift_one,
    w_fc1,
    b_fc1,
    w_fc2,
    b_fc2,
    gain_two,
    shift_two,
    cotangent,
):
    n = lax.axis_size("fsdp")
    q = lax.axis_index("dp")
    f = lax.axis_index("fsdp")
    row_count, width = tokens.shape
    rows = width // n
    ff = b_fc1.shape[0] * n
    ffq = ff // n // 4
    hidden = n * ffq
    quarter = width // 4
    n_img = scale_codes.shape[0]
    patches = row_count // n_img
    padded = -(-patches // 16) * 16
    factor = 1.0 / math.sqrt(width // HEADS)
    seq = Order(q)
    bits = list(reversed(range(n.bit_length() - 1)))
    near = min(1, len(bits) - 1)
    shard_order = jnp.asarray(masks(bits), jnp.int32) ^ f
    group_order = jnp.arange(4, dtype=jnp.int32) ^ q
    order = jnp.concatenate([shard_order, q[None]])

    def last_three(chain):
        while len(chain.bits) > 3:
            chain.launch()
            seq.land((), chain)
            chain.join()
        return chain

    small = [b_q, b_v, b_out, gain_one, shift_one, b_fc2, gain_two, shift_two, b_fc1]
    qkv = last_three(Gather(seq, first_payload(q, w_qkv, small), n, bits))
    qkv.launch()
    rest_own, two_own = payloads([seq.at(q), q ^ 2], w_fc1, w_fc2)
    rest_own, two_own = seq.land((rest_own, two_own), qkv)
    rest = Sent(lax.all_gather(rest_own, "fsdp", axis=0, tiled=False))
    two = Sent(lax.all_gather(two_own, "fsdp", axis=0, tiled=False))
    out_own = [lax.dynamic_slice(w_out, (0, g * quarter), (rows, quarter)) for g in (q, q ^ 2)]
    out = last_three(Gather(seq, jnp.concatenate(out_own, axis=1).astype(half), n, bits))

    def spread_rows(value):
        split = value.reshape(n_img, patches, width)
        return jnp.pad(split, ((0, 0), (0, padded - patches), (0, 0)))

    def compact(value):
        return value.reshape(n_img, padded, width)[:, :patches].reshape(row_count, width)

    qkv.join()
    qkv.launch()
    out.launch()
    spread_tokens = seq.land(spread_rows(seq.at(tokens)), qkv)
    qkv_near = qkv.join()
    qkv.launch()
    near_b, near_c = Sent(core_swap(qkv.held)), Sent(x_swap(qkv.held))
    seq.land((), out)
    out.join()
    out.launch()
    places = table(scale_codes, width)
    row_place = jnp.broadcast_to(places[:, :, None], (n_img, GRID, GRID, width // 2))
    col_place = jnp.broadcast_to(places[:, None], (n_img, GRID, GRID, width // 2))
    place = jnp.concatenate([row_place, col_place], axis=-1).reshape(n_img, patches, width)
    place = jnp.pad(place, ((0, 0), (0, padded - patches), (0, 0)))
    x_zero = (seq.at(spread_tokens).astype(full) + place).reshape(-1, width)
    x_zero = seq.land(x_zero, qkv, near_b)
    qkv_far = seq.at(qkv.got)
    far_b, far_c = Sent(core_swap(qkv_far)), Sent(x_swap(qkv_far))
    vectors, bias_fc1, bias_qkv = unpack_vectors(seq.at(order), (qkv_near, qkv_far), n, rows, ffq)
    _, _, full_bout, gain_one_f, shift_one_f, full_bfc2, gain_two_f, shift_two_f = vectors
    normed_one = layer_norm(x_zero, gain_one_f, shift_one_f).astype(half)
    normed_one = seq.land(normed_one, far_b)

    first = attention_forward(
        seq.at(order), normed_one, bias_qkv[:2], ((qkv_near, qkv_far), (near_b.value, far_b.value)),
        n_img, patches, factor,
    )
    first = (seq.land(first[0], near_c, far_c, out), *first[1:])
    near_c, far_c = seq.at((near_c.value, far_c.value))
    near_d, far_d = Sent(core_swap(near_c)), Sent(core_swap(far_c))
    out.join()
    out.launch()
    cot = seq.land(spread_rows(cotangent).reshape(-1, width), near_d, far_d)
    second = attention_forward(
        seq.at(order), normed_one, bias_qkv[2:], ((near_c, far_c), (near_d.value, far_d.value)),
        n_img, patches, factor,
    )
    second = (seq.land(second[0], out), *second[1:])
    out_a = seq.at(out.join())
    out_b = Sent(core_swap(out_a))
    seq.land((), out_b)
    outs = (out_a, out_b.value)
    qkv_parts = (
        (qkv_near, qkv_far), (near_b.value, far_b.value), (near_c, far_c), (near_d.value, far_d.value)
    )
    qkvs = (*first[:2], *second[:2])
    mixed = (*first[2:4], *second[2:4])
    lses = (*first[4:], *second[4:])
    after_attn, normed_two = attention_out(
        seq.at(order), x_zero, mixed, outs, full_bout, gain_two_f, shift_two_f
    )
    normed_two = seq.land(normed_two, rest)
    rest_a = seq.at(rest.value)
    rest_b = Sent(core_swap(rest_a))
    up_c = Sent(x_swap(seq.at(rest_a[:, :, :hidden])))
    seq.land((), rest_b)

    g_1, g_bias_1, back_sum, out_sum = mlp(
        seq.at(order), normed_two, cot, bias_fc1[1], rest_b.value, rest_b.value, hidden
    )
    g_1 = seq.at(g_1)
    got_1 = Sent(core_swap(g_1))
    g_0, g_bias_0, back_sum, out_sum = mlp(
        seq.at(order), normed_two, cot, bias_fc1[0], rest_a, rest_a, hidden, (out_sum, back_sum)
    )
    g_0 = seq.land(g_0, got_1, up_c, two)
    up_c, two = seq.at((up_c.value, two.value))
    up_d, two_d = Sent(core_swap(up_c)), Sent(core_swap(two))
    red = Reduce(seq, (g_0, got_1.value), n)
    red.launch()
    g_2, g_bias_2, back_sum, out_sum = mlp(
        seq.at(order), normed_two, cot, bias_fc1[2], up_c, two, 0, (out_sum, back_sum)
    )
    g_2 = seq.land(g_2, up_d, two_d)
    g_3, g_bias_3, grad_two_in, block = mlp(
        seq.at(order), normed_two, cot, bias_fc1[3], up_d.value, two_d.value, 0,
        (out_sum, back_sum), (after_attn, full_bfc2),
    )
    g_3 = seq.land(g_3, red)
    got_3 = Sent(core_swap(g_3))
    red.launch()
    seq.land((), got_3)
    red_two = Reduce(seq, (g_2, got_3.value), n)
    red_two.launch()

    after_grad, mg0, mg1, mg2, mg3, g_out, sums_two = attention_out_back(
        seq.at(order), grad_two_in, after_attn, cot, gain_two_f, mixed, outs
    )
    mg2 = seq.land(mg2, red)
    red.launch()
    g_w2, g_w3, proj2, proj3, sums_b = attention_back(
        seq.at(order), normed_one, qkvs[2:], lses[2:], (mg2, mg3), g_out, (2, 3), n_img, patches, factor, n
    )
    g_w3 = seq.land(g_w3, red, red_two)
    w_3 = Sent(core_swap(g_w3))
    red_two.launch()
    seq.land((), w_3)
    middle = n // 2
    half_shape = (2,) * (len(bits) - 1)
    w_high = Sent(x_swap(seq.at(rounded_sum([g_w2[middle:], w_3.value[middle:]]))))
    g_w0, g_w1, proj0, proj1, sums_a = attention_back(
        seq.at(order), normed_one, qkvs[:2], lses[:2], (mg0, mg1), g_out, (0, 1), n_img, patches, factor, n
    )
    g_w1 = seq.land(g_w1, red_two, w_high)
    w_1 = Sent(core_swap(g_w1))
    red_two.launch()
    seq.land((), w_1)
    red_w = Reduce(seq, (g_w0, w_1.value), n)
    red_w.launch(0, [w_high.value.reshape(half_shape + w_high.value.shape[1:])])
    w_low = Sent(x_swap(seq.at(rounded_sum([g_w2[:middle], w_3.value[:middle]]))))
    tokens_grad, sums_one = input_back(
        seq.at(order), x_zero, after_grad, gain_one_f, (proj0, proj1, proj2, proj3), qkv_parts
    )
    sums_one = seq.land(sums_one, red_two, red_w, w_low)
    red_w.terms = [*red_w.terms, w_low.value.reshape(half_shape + w_low.value.shape[1:])]
    while len(red_w.axes) > 2:
        red_w.launch()
        seq.land((), red_w)
    red_w.launch()
    cross = Sent(x_swap(seq.at(red_two.rest().piece())))
    packed = pack_sums(
        seq.at(order), n, rows, ffq, (sums_a, sums_b), (jnp.stack([g_bias_0, g_bias_1]), jnp.stack([g_bias_2, g_bias_3])), (sums_two, sums_one)
    )
    packed = seq.at(packed)
    peers = Sent([xor_swap(packed, "dp", 4, m) for m in (1, 2, 3)])
    seq.land((), peers)
    sums = Reduce(seq, (packed, *peers.value), n, full)
    while len(sums.axes) > 1:
        sums.launch()
        if len(sums.axes) > 1:
            seq.land((), sums)
    seq.land((), sums, red_w, cross)
    if red_w.axes:
        red_w.launch()
    mlp_spread = Spread(seq, rounded_sum([*red.rest().terms, cross.value]))
    sums.launch()
    block, tokens_grad = seq.at((block, tokens_grad))
    block_out, grad_tokens = seq.land(
        (compact(block), compact(tokens_grad)), sums, mlp_spread, *([red_w] if len(bits) > 1 else [])
    )
    small_sums = sums.piece()
    w_spread = Spread(seq, red_w.piece())
    mlp_spread.cross()
    small_sums = seq.land(small_sums, mlp_spread)
    mlp_pieces = seq.at(mlp_spread.pieces)
    out_fc1, out_fc2 = finish_mlp(q, mlp_pieces, n)
    out_fc2, small_sums = seq.land((out_fc2, small_sums), w_spread)
    w_spread.cross()
    seq.land((), w_spread)
    out_qkv, out_out = finish_attention(seq.value, w_spread.pieces)
    small_out = [small_sums[k, :rows] for k in range(8)]
    out_bfc1 = small_sums[8:12, :ffq].reshape(-1)
    o_bq, o_bv, o_bout, o_gone, o_sone, o_bfc2, o_gtwo, o_stwo = small_out
    return (
        block_out,
        grad_tokens,
        out_qkv,
        o_bq,
        o_bv,
        out_out,
        o_bout,
        o_gone,
        o_sone,
        out_fc1,
        out_bfc1,
        out_fc2,
        o_bfc2,
        o_gtwo,
        o_stwo,
    )


def solution(mesh):
    rows_split = P(("dp", "fsdp"), None)
    matrix = P("fsdp", None)
    vector = P("fsdp")
    return jax.shard_map(
        local,
        mesh=mesh,
        in_specs=(
            rows_split, P(("dp", "fsdp")), matrix, vector, vector, matrix, vector, vector, vector,
            matrix, vector, matrix, vector, vector, vector, rows_split,
        ),
        out_specs=(
            rows_split, rows_split, matrix, vector, vector, matrix, vector, vector, vector,
            matrix, vector, matrix, vector, vector, vector,
        ),
        check_vma=False,
    )
```

```python
import math

import jax
import jax.numpy as jnp
from jax import lax
from jax.experimental import pallas as pl
from jax.experimental.pallas import tpu as pltpu
from jax.sharding import PartitionSpec as P

HEADS = 16
GRID = 14
NSCALE = 16
norm_eps = 1e-06
half = jnp.bfloat16
full = jnp.float32


def xor_swap(value, axis, size, mask):
    return lax.ppermute(value, axis, [(i, i ^ mask) for i in range(size)])


def core_swap(value):
    return xor_swap(value, "dp", 4, 1)


def x_swap(value):
    return xor_swap(value, "dp", 4, 2)


def masks(bits):
    found = [0]
    for bit in bits:
        found = found + [m | (1 << bit) for m in found]
    return found


class Order:
    def __init__(self, value):
        self.value = value

    def at(self, value):
        value, self.value = lax.optimization_barrier((value, self.value))
        return value

    def land(self, value, *sent):
        value, flights = self.at((value, [s.flight for s in sent]))
        for s, flight in zip(sent, flights, strict=True):
            s.accept(flight)
        return value


class Sent:
    def __init__(self, flight):
        self.flight = flight

    def accept(self, value):
        self.value = value


class Gather:
    def __init__(self, seq, piece, n, bits):
        self.seq, self.held, self.n, self.bits = seq, piece[None], n, list(bits)

    def launch(self):
        self.held = self.seq.at(self.held)
        self.flight = xor_swap(self.held, "fsdp", self.n, 1 << self.bits.pop(0))

    def accept(self, value):
        self.got = value

    def join(self):
        self.held = jnp.concatenate([self.held, self.got])
        return self.held


def rounded_sum(terms, kind=half):
    return sum(t.astype(full) for t in terms).astype(kind)


class Reduce:
    def __init__(self, seq, terms, n, kind=half):
        self.kind = kind
        self.seq, self.n, self.axes = seq, n, list(range(n.bit_length() - 1))
        self.terms = [t.reshape((2,) * len(self.axes) + t.shape[1:]) for t in terms]

    def launch(self, bit=None, more=()):
        bit = self.axes[0] if bit is None else bit
        axis = self.axes.index(bit)
        self.axes.pop(axis)
        low, high = [
            [lax.index_in_dim(t, side, axis, keepdims=False) for t in self.terms] for side in (0, 1)
        ]
        self.terms = low
        self.flight = xor_swap(self.seq.at(rounded_sum([*high, *more], self.kind)), "fsdp", self.n, 1 << bit)

    def accept(self, value):
        self.terms = [*self.terms, value]

    def rest(self):
        while self.axes:
            self.launch()
            self.seq.land((), self)
        return self

    def piece(self):
        return rounded_sum(self.terms, self.kind)


class Spread:
    def __init__(self, seq, piece):
        self.seq, self.pieces = seq, [seq.at(piece)]
        self.flight = [core_swap(self.pieces[0]), x_swap(self.pieces[0])]

    def cross(self):
        self.flight = [core_swap(self.seq.at(self.pieces[2]))]

    def accept(self, value):
        self.pieces += value


ANYWHERE = pl.BlockSpec(memory_space=pl.ANY)
ON_CHIP = pl.BlockSpec(memory_space=pltpu.VMEM)
SCALARS = pl.BlockSpec(memory_space=pltpu.SMEM)


def dot(left, right, dim_left, dim_right):
    return lax.dot_general(
        left, right, (((dim_left,), (dim_right,)), ((), ())), preferred_element_type=full
    )


def call(kernel, name, operands, in_specs, outs, out_specs, scratch):
    return pl.pallas_call(
        kernel,
        out_shape=[jax.ShapeDtypeStruct(shape, kind) for shape, kind in outs],
        in_specs=in_specs,
        out_specs=out_specs,
        scratch_shapes=scratch,
        compiler_params=pltpu.CompilerParams(vmem_limit_bytes=58 * 2**20),
        name=name,
    )(*operands)


def loop(count, body, unroll=1):
    def step(i, carry):
        body(i)
        return carry

    lax.fori_loop(0, count, step, 0, unroll=unroll)


def tile(i, size):
    return pl.ds(pl.multiple_of(i * size, size), size)


def bring(src, dst, sem):
    pltpu.make_async_copy(src, dst, sem).start()


def arrived(dst, sem):
    pltpu.make_async_copy(dst, dst, sem).wait()


def fetch(parts, order_ref, place, sem):
    base = 0
    for part in parts:

        def start(r, part=part, base=base):
            shard = r if order_ref is None else order_ref[base + r]
            pltpu.make_async_copy(part.at[r], place(shard), sem).start()

        loop(part.shape[0], start)
        base += part.shape[0]


def head_rows(s, q, n, rows, quarter):
    per = n // 4
    return pl.multiple_of(((s // per) ^ q) * quarter + (s % per) * rows, rows)


def pair_scores(q2, k2):
    first = lax.broadcasted_iota(jnp.int32, q2.shape, 1) < q2.shape[1] // 2
    both = apart(q2, first)
    return both, dot(k2, both, 1, 1), first


def apart(value, first):
    zero = jnp.zeros_like(value)
    return jnp.concatenate([jnp.where(first, value, zero), jnp.where(first, zero, value)])


def attention_forward(order, normed, bias, weights, n_img, patches, factor):
    groups, n_parts = len(weights), len(weights[0])
    wide = weights[0][0].shape[2]
    count, width = normed.shape
    rows = width // sum(part.shape[0] for part in weights[0])
    padded = count // n_img
    quarter = wide // 3

    def kernel(order_ref, normed_ref, bias_ref, *refs):
        w_refs, refs = refs[: groups * n_parts], refs[groups * n_parts :]
        qkv_refs, mixed_refs, refs = refs[:groups], refs[groups : 2 * groups], refs[2 * groups :]
        lse_refs, (w_held, sems) = refs[:groups], refs[groups:]
        for g in range(groups):
            fetch(
                [w.at[:, pl.ds(0, rows)] for w in w_refs[g * n_parts : (g + 1) * n_parts]],
                order_ref,
                lambda s, g=g: w_held.at[g, pl.ds(pl.multiple_of(s * rows, rows), rows)],
                sems.at[g],
            )
        for g in range(groups):
            pltpu.make_async_copy(w_held.at[g], w_held.at[g], sems.at[g]).wait()

            def project(t, g=g):
                at = tile(t, quarter)
                product = dot(normed_ref[...], w_held[g, :, at], 1, 0)
                qkv_refs[g][:, at] = (product + bias_ref[g, :, at]).astype(half)

            loop(3, project)

            def attend(i, g=g):
                at = tile(i // 2, padded)
                lanes = [pl.ds(pl.multiple_of(t * quarter + (i % 2) * 128, 128), 128) for t in range(3)]
                q2 = qkv_refs[g][at, lanes[0]] * factor
                k2 = qkv_refs[g][at, lanes[1]]
                v2 = qkv_refs[g][at, lanes[2]]
                _, scores, first = pair_scores(q2, k2)
                key = lax.broadcasted_iota(jnp.int32, scores.shape, 0)
                scores = jnp.where(key < patches, scores, -1e30)
                top = jnp.max(scores, axis=0, keepdims=True)
                raised = jnp.exp(scores - top)
                total = jnp.sum(raised, axis=0, keepdims=True)
                lse_refs[g][i] = top + jnp.log(total)
                out = dot((raised * (1.0 / total)).astype(half), v2, 0, 0)
                mixed_refs[g][at, lanes[0]] = jnp.where(first, out[:padded], out[padded:]).astype(half)

            loop(2 * n_img, attend, 2 * n_img)

    return call(
        kernel,
        "attention_forward",
        (order, normed, bias, *(part for w in weights for part in w)),
        [SCALARS, ON_CHIP, ON_CHIP] + [ANYWHERE] * (groups * n_parts),
        [((count, wide), half)] * groups
        + [((count, quarter), half)] * groups
        + [((2 * n_img, 1, 2 * padded), full)] * groups,
        [ON_CHIP] * (3 * groups),
        [pltpu.VMEM((groups, width, wide), half), pltpu.SemaphoreType.DMA((groups,))],
    )


def layer_norm(value, gain, shift):
    center = jnp.mean(value, axis=-1, keepdims=True)
    offset = value - center
    spread = jnp.mean(offset * offset, axis=-1, keepdims=True)
    return offset * lax.rsqrt(spread + norm_eps) * gain + shift


def layer_norm_back(value, grad, gain):
    center = jnp.mean(value, axis=-1, keepdims=True)
    offset = value - center
    scale = lax.rsqrt(jnp.mean(offset * offset, axis=-1, keepdims=True) + norm_eps)
    unit = offset * scale
    scaled = grad * gain
    inner = jnp.mean(scaled * unit, axis=-1, keepdims=True)
    return scale * (scaled - jnp.mean(scaled, axis=-1, keepdims=True) - unit * inner), grad * unit


def load_out(order_ref, out_refs, held, sem, n, rows, quarter):
    q = order_ref[n]
    for j in range(4):
        column = pl.multiple_of((q ^ j) * quarter, quarter)
        fetch(
            [out_refs[j % 2].at[:, :, pl.ds(j // 2 * quarter, quarter)]],
            order_ref,
            lambda s, column=column: held.at[
                pl.ds(head_rows(s, q, n, rows, quarter), rows), pl.ds(column, quarter)
            ],
            sem,
        )


CHUNK = 16
ROWS = 64


def attention_out(order, x_zero, mixed, outs, bias, gain, shift):
    count, width = x_zero.shape
    n, rows, _ = outs[0].shape
    quarter = mixed[0].shape[1]

    def kernel(order_ref, x_ref, bias_ref, gain_ref, shift_ref, *refs):
        mixed_refs, out_refs = refs[:4], refs[4:6]
        after_ref, normed_ref, held, x_held, sems = refs[6:]
        bring(x_ref, x_held, sems.at[1])
        load_out(order_ref, out_refs, held, sems.at[0], n, rows, quarter)
        together = jnp.concatenate([m[...] for m in mixed_refs], axis=1)
        pltpu.make_async_copy(held, held, sems.at[0]).wait()
        after_ref[...] = dot(together, held[...], 1, 0)
        arrived(x_held, sems.at[1])

        def finish(i):
            at = tile(i, CHUNK)
            after = x_held[at] + (after_ref[at] + bias_ref[...])
            after_ref[at] = after
            normed_ref[at] = layer_norm(after, gain_ref[...], shift_ref[...]).astype(half)

        loop(count // CHUNK, finish, 13)

    return call(
        kernel,
        "attention_out",
        (order, x_zero, bias, gain, shift, *mixed, *outs),
        [SCALARS, ANYWHERE] + [ON_CHIP] * 7 + [ANYWHERE] * 2,
        [((count, width), full), ((count, width), half)],
        [ON_CHIP] * 2,
        [
            pltpu.VMEM((width, width), half),
            pltpu.VMEM((count, width), full),
            pltpu.SemaphoreType.DMA((2,)),
        ],
    )


def mlp(order, normed, cot, bias, up_all, down_all, down_start, carried=None, ending=None):
    count, width = normed.shape
    n, rows, _ = up_all.shape
    hidden = bias.shape[1]
    share = hidden // n
    step = min(512, hidden)
    steps = hidden // step
    more = [*(carried or []), *(ending[:1] if ending else [])]
    last = list(ending[1:]) if ending else []

    def kernel(order_ref, bias_ref, *refs):
        last_refs, refs = refs[: len(last)], refs[len(last) :]
        normed_ref, cot_ref, up_ref, down_ref, refs = *refs[:4], refs[4:]
        more_refs, refs = refs[: len(more)], refs[len(more) :]
        g_up_ref, g_down_ref, g_bias_ref, back_ref, end_ref, refs = *refs[:5], refs[5:]
        held, refs = refs[: len(more)], refs[len(more) :]
        rows_in, cots, out, back, up, down, pre, act, act_half, pre_half, g_up, g_down, sems = refs
        bring(normed_ref, rows_in, sems.at[3])
        fetch(
            [up_ref.at[:, :, pl.ds(0, hidden)]],
            None,
            lambda s: up.at[pl.ds(pl.multiple_of(s * rows, rows), rows)],
            sems.at[0],
        )
        bring(cot_ref, cots, sems.at[4])
        fetch(
            [down_ref.at[:, :, pl.ds(down_start, width)]],
            None,
            lambda s: down.at[pl.ds(pl.multiple_of(s * share, share), share)],
            sems.at[1],
        )
        for k in range(len(more)):
            bring(more_refs[k], held[k], sems.at[5 + k])
        arrived(rows_in, sems.at[3])
        arrived(up, sems.at[0])
        for t in range(steps):
            at = pl.ds(t * step, step)
            pre[...] = dot(rows_in[...], up[:, at], 1, 0)
            if not t:
                arrived(cots, sems.at[4])
                arrived(down, sems.at[1])
            act[...] = dot(cots[...], down[at, :], 1, 1)

            def gelu(i, at=at):
                some = tile(i, 2 * CHUNK)
                x = pre[some] + bias_ref[:, at]
                below = 0.5 * (1.0 + lax.erf(x * math.sqrt(0.5)))
                density = jnp.exp(-0.5 * x * x) * (1.0 / math.sqrt(2.0 * math.pi))
                act_half[some] = (x * below).astype(half)
                pre_half[some] = (act[some] * (below + x * density)).astype(half)

            loop(count // CHUNK // 2, gelu)
            p = pre_half[...]
            h = act_half[...]
            more_back = dot(p, up[:, at], 1, 1)
            more_out = dot(h, down[at, :], 1, 0)
            if t:
                back[...] += more_back
                out[...] += more_out
            elif carried:
                arrived(held[0], sems.at[5])
                arrived(held[1], sems.at[6])
                out[...] = held[0][...] + more_out
                back[...] = held[1][...] + more_back
            else:
                out[...] = more_out
                back[...] = more_back
            if t == steps - 1:
                bring(back, back_ref, sems.at[3])
                if not ending:
                    bring(out, end_ref, sems.at[4])
            g_down[at, :] = dot(h, cots[...], 0, 0).astype(half)
            if t == steps - 1:

                def send_down(r):
                    at = pl.multiple_of(order_ref[r] * share, share)
                    bring(g_down.at[pl.ds(at, share)], g_down_ref.at[r], sems.at[2])

                loop(n, send_down)
            g_up[:, at] = dot(rows_in[...], p, 0, 0).astype(half)
            g_bias_ref[:, at] = jnp.sum(p.astype(full), axis=0, keepdims=True)

        def send_up(r):
            at = pl.multiple_of(order_ref[r] * rows, rows)
            bring(g_up.at[pl.ds(at, rows)], g_up_ref.at[r], sems.at[0])

        loop(n, send_up)
        if ending:
            arrived(held[2], sems.at[7])

            def finish(i):
                at = tile(i, 2 * CHUNK)
                end_ref[at] = (held[2][at] + (out[at] + last_refs[0][...])).astype(half)

            loop(count // CHUNK // 2, finish)
        else:
            arrived(end_ref, sems.at[4])
        arrived(back_ref, sems.at[3])
        arrived(g_down_ref, sems.at[2])
        arrived(g_up_ref, sems.at[0])

    sums = pltpu.VMEM((count, width), full)
    wide = pltpu.VMEM((count, width), half)
    square = pltpu.VMEM((width, hidden), half)
    return call(
        kernel,
        "mlp",
        (order, bias, *last, normed, cot, up_all, down_all, *more),
        [SCALARS] + [ON_CHIP] * (1 + len(last)) + [ANYWHERE] * (4 + len(more)),
        [
            ((n, rows, hidden), half),
            ((n, share, width), half),
            ((1, hidden), full),
            ((count, width), full),
            ((count, width), half if ending else full),
        ],
        [ANYWHERE, ANYWHERE, ON_CHIP, ANYWHERE, ON_CHIP if ending else ANYWHERE],
        [
            *([sums] * len(more)),
            wide,
            wide,
            sums,
            sums,
            square,
            pltpu.VMEM((hidden, width), half),
            pltpu.VMEM((count, step), full),
            pltpu.VMEM((count, step), full),
            pltpu.VMEM((count, step), half),
            pltpu.VMEM((count, step), half),
            square,
            pltpu.VMEM((hidden, width), half),
            pltpu.SemaphoreType.DMA((5 + len(more),)),
        ],
    )


def attention_out_back(order, grad, after, cot, gain, mixed, outs):
    count, width = after.shape
    n, rows, _ = outs[0].shape
    quarter = mixed[0].shape[1]

    def kernel(order_ref, grad_ref, after_ref, cot_ref, gain_ref, *refs):
        mixed_refs, out_refs, refs = refs[:4], refs[4:6], refs[6:]
        after_grad_ref, mixed_grad_refs, g_out_ref, sums_ref = refs[0], refs[1:5], refs[5], refs[6]
        held, branch, terms, grad, after, cot, mixes, sems = refs[7:]
        block = count // 4
        for k in range(4):
            some = pl.ds(k * block, block)
            bring(grad_ref.at[some], grad.at[some], sems.at[1 + k])
            bring(after_ref.at[some], after.at[some], sems.at[5 + k])
            bring(cot_ref.at[some], cot.at[some], sems.at[9 + k])
        load_out(order_ref, out_refs, held, sems.at[0], n, rows, quarter)
        for j in range(4):
            bring(mixed_refs[j], mixes.at[j], sems.at[13])
        terms[...] = jnp.zeros_like(terms)

        def fold(value):
            return jnp.sum(value.reshape(CHUNK // 8, 8, width), axis=0)

        def back(i, k):
            at = pl.ds(pl.multiple_of(k * block + i * CHUNK, CHUNK), CHUNK)
            incoming = grad[at]
            part, gain_terms = layer_norm_back(after[at], incoming, gain_ref[...])
            own = cot[at].astype(full)
            total = own + part
            after_grad_ref[at] = total
            rounded = total.astype(half)
            branch[at] = rounded
            terms[0] += fold(rounded.astype(full))
            terms[1] += fold(gain_terms)
            terms[2] += fold(incoming)
            terms[3] += fold(own)

        for k in range(4):
            some = pl.ds(k * block, block)
            arrived(grad.at[some], sems.at[1 + k])
            arrived(after.at[some], sems.at[5 + k])
            arrived(cot.at[some], sems.at[9 + k])
            loop(block // CHUNK, lambda i, k=k: back(i, k), 13)
        for k in range(4):
            sums_ref[k] = jnp.sum(terms[k], axis=0, keepdims=True)
        arrived(held, sems.at[0])
        arrived(mixes, sems.at[13])
        for j in range(4):
            mixed_grad_refs[j][...] = dot(branch[...], held[j * quarter : (j + 1) * quarter], 1, 1).astype(half)
            g_out_ref[j * quarter : (j + 1) * quarter] = dot(mixes[j], branch[...], 0, 0).astype(half)

    return call(
        kernel,
        "attention_out_back",
        (order, grad, after, cot, gain, *mixed, *outs),
        [SCALARS] + [ANYWHERE] * 3 + [ON_CHIP] + [ANYWHERE] * 6,
        [((count, width), full)]
        + [((count, quarter), half)] * 4
        + [((width, width), half), ((4, 1, width), full)],
        [ON_CHIP] * 7,
        [
            pltpu.VMEM((width, width), half),
            pltpu.VMEM((count, width), half),
            pltpu.VMEM((4, 8, width), full),
            pltpu.VMEM((count, width), full),
            pltpu.VMEM((count, width), full),
            pltpu.VMEM((count, width), half),
            pltpu.VMEM((4, count, quarter), half),
            pltpu.SemaphoreType.DMA((14,)),
        ],
    )


def attention_back(order, normed, qkvs, lses, mixed_grads, g_out, which, n_img, patches, factor, n):
    groups = len(qkvs)
    count, width = normed.shape
    wide = qkvs[0].shape[1]
    quarter = wide // 3
    padded = count // n_img
    rows = width // n

    def kernel(order_ref, normed_ref, g_out_ref, *refs):
        qkv_refs, mg_refs, refs = refs[:groups], refs[groups : 2 * groups], refs[2 * groups :]
        lse_refs, refs = refs[:groups], refs[groups:]
        g_w_refs, proj_refs, sums_ref = refs[:groups], refs[groups : 2 * groups], refs[2 * groups]
        g_w, normed_held, g_out_held, sems = refs[2 * groups + 1 :]
        q = order_ref[n]
        bring(g_out_ref, g_out_held, sems.at[groups])
        bring(normed_ref, normed_held, sems.at[groups + 1])
        for g in range(groups):

            def attend(i, g=g):
                at = tile(i // 2, padded)
                lanes = [pl.ds(pl.multiple_of(t * quarter + (i % 2) * 128, 128), 128) for t in range(3)]
                q2 = qkv_refs[g][at, lanes[0]] * factor
                k2 = qkv_refs[g][at, lanes[1]]
                v2 = qkv_refs[g][at, lanes[2]]
                both, scores, first = pair_scores(q2, k2)
                key = lax.broadcasted_iota(jnp.int32, scores.shape, 0)
                probs = jnp.where(key < patches, jnp.exp(scores - lse_refs[g][i]), 0.0)
                o_both = apart(mg_refs[g][at, lanes[0]], first)
                g_probs = dot(v2, o_both, 1, 1)
                weighted = jnp.sum(probs * g_probs, axis=0, keepdims=True)
                g_scores = (probs * (g_probs - weighted)).astype(half)
                g_query = dot(g_scores, k2, 0, 0)
                g_query = jnp.where(first, g_query[:padded], g_query[padded:]) * factor
                proj_refs[g][at, lanes[0]] = g_query.astype(half)
                proj_refs[g][at, lanes[1]] = dot(g_scores, both, 1, 0).astype(half)
                proj_refs[g][at, lanes[2]] = dot(probs.astype(half), o_both, 1, 0).astype(half)

            loop(2 * n_img, attend, 4)
            if not g:
                arrived(g_out_held, sems.at[groups])
                arrived(normed_held, sems.at[groups + 1])

            def send_out(r, g=g):
                at = head_rows(order_ref[r], q, n, rows, quarter)
                column = pl.multiple_of((q ^ which[g]) * quarter, quarter)
                pltpu.make_async_copy(
                    g_out_held.at[pl.ds(at, rows), pl.ds(column, quarter)],
                    g_w_refs[g].at[r, :, pl.ds(wide, quarter)],
                    sems.at[g],
                ).start()

            loop(n, send_out)

            def weigh(t, g=g):
                at = tile(t, quarter)
                some = proj_refs[g][:, at]
                g_w[g, :, at] = dot(normed_held[...], some, 0, 0).astype(half)
                sums_ref[g, :, at] = jnp.sum(some.astype(full), axis=0, keepdims=True)

            loop(3, weigh)

            def send(r, g=g):
                at = pl.multiple_of(order_ref[r] * rows, rows)
                pltpu.make_async_copy(
                    g_w.at[g, pl.ds(at, rows)], g_w_refs[g].at[r, :, pl.ds(0, wide)], sems.at[g]
                ).start()

            loop(n, send)
        for g in range(groups):
            pltpu.make_async_copy(g_w_refs[g], g_w_refs[g], sems.at[g]).wait()

    return call(
        kernel,
        "attention_back",
        (order, normed, g_out, *qkvs, *mixed_grads, *lses),
        [SCALARS] + [ANYWHERE] * 2 + [ON_CHIP] * (3 * groups),
        [((n, rows, wide + quarter), half)] * groups
        + [((count, wide), half)] * groups
        + [((groups, 1, wide), full)],
        [ANYWHERE] * groups + [ON_CHIP] * (groups + 1),
        [
            pltpu.VMEM((groups, width, wide), half),
            pltpu.VMEM((count, width), half),
            pltpu.VMEM((width, width), half),
            pltpu.SemaphoreType.DMA((groups + 2,)),
        ],
    )


def input_back(order, x_zero, after_grad, gain, projs, weights):
    count, width = x_zero.shape
    wide = weights[0][0].shape[2]
    rows = width // sum(part.shape[0] for part in weights[0])
    parts = [part for w in weights for part in w]
    n_parts = len(weights[0])

    def kernel(order_ref, x_ref, after_ref, gain_ref, *refs):
        proj_refs, w_refs = refs[:4], refs[4 : 4 + len(parts)]
        token_ref, sums_ref, held, terms, x_held, after_held, sems = refs[4 + len(parts) :]
        for j in range(4):
            fetch(
                [w.at[:, pl.ds(0, rows)] for w in w_refs[j * n_parts : (j + 1) * n_parts]],
                order_ref,
                lambda s, j=j: held.at[j, pl.ds(pl.multiple_of(s * rows, rows), rows)],
                sems.at[j],
            )
        bring(x_ref, x_held, sems.at[4])
        bring(after_ref, after_held, sems.at[5])
        for j in range(4):
            arrived(held.at[j], sems.at[j])
            product = dot(proj_refs[j][...], held[j], 1, 1)
            if j == 0:
                token_ref[...] = product
            else:
                token_ref[...] += product
        arrived(x_held, sems.at[4])
        arrived(after_held, sems.at[5])
        terms[...] = jnp.zeros_like(terms)

        def fold(value):
            return jnp.sum(value.reshape(ROWS // 8, 8, width), axis=0)

        def back(i):
            at = tile(i, ROWS)
            incoming = token_ref[at]
            part, gain_terms = layer_norm_back(x_held[at], incoming, gain_ref[...])
            token_ref[at] = after_held[at] + part
            terms[0] += fold(gain_terms)
            terms[1] += fold(incoming)

        loop(count // ROWS, back)
        for k in range(2):
            sums_ref[k] = jnp.sum(terms[k], axis=0, keepdims=True)

    return call(
        kernel,
        "input_back",
        (order, x_zero, after_grad, gain, *projs, *parts),
        [SCALARS] + [ANYWHERE] * 2 + [ON_CHIP] * 5 + [ANYWHERE] * len(parts),
        [((count, width), full), ((2, 1, width), full)],
        [ON_CHIP] * 2,
        [
            pltpu.VMEM((4, width, wide), half),
            pltpu.VMEM((2, 8, width), full),
            pltpu.VMEM((count, width), full),
            pltpu.VMEM((count, width), full),
            pltpu.SemaphoreType.DMA((6,)),
        ],
    )


def payloads(which, w_fc1, w_fc2):
    rows, ff = w_fc1.shape
    full_share, width = w_fc2.shape
    share = full_share // 4
    n = ff // full_share
    hidden = n * share
    own, across = which
    if share % 128:
        fc1 = [lax.dynamic_slice(w_fc1, (0, (4 * s + own) * share), (rows, share)) for s in range(n)]
        fc2 = [lax.dynamic_slice(w_fc2, (g * share, 0), (share, width)).astype(half) for g in which]
        rest = jnp.concatenate([*fc1, fc2[0].reshape(rows, -1).astype(full)], axis=1)
        return rest.astype(half), fc2[1]

    def kernel(which_ref, fc1_ref, fc2_ref, rest_ref, two_ref):
        for s in range(n):
            at = pl.ds(pl.multiple_of((4 * s + which_ref[0]) * share, share), share)
            rest_ref[:, s * share : (s + 1) * share] = fc1_ref[:, at].astype(half)
        rest_ref[:, hidden : hidden + width] = fc2_ref[tile(which_ref[0], share), :].astype(half)
        two_ref[...] = fc2_ref[tile(which_ref[1], share), :].astype(half)

    return call(
        kernel,
        "payloads",
        (jnp.stack(which), w_fc1, w_fc2),
        [SCALARS] + [ON_CHIP] * 2,
        [((rows, hidden + width), half), ((share, width), half)],
        [ON_CHIP] * 2,
        [],
    )


def natural_quarters(q, pieces):
    once = [jnp.where((q & 1) == 1, pieces[i ^ 1], pieces[i]) for i in range(4)]
    return [jnp.where(q >= 2, once[i ^ 2], once[i]) for i in range(4)]


def finish_mlp(q, pieces, n):
    _, rows, width = pieces[0].shape
    share = width // n
    if share % 128:
        pieces = natural_quarters(q, pieces)
        fc1 = jnp.stack([p[0].reshape(rows, n, share) for p in pieces], axis=2).reshape(rows, 4 * width)
        return fc1.astype(full), jnp.concatenate([p[1] for p in pieces]).astype(full)

    def kernel(q_ref, *refs):
        fc1_ref, fc2_ref = refs[4:]
        for j in range(4):
            g = q_ref[0] ^ j
            for s in range(n):
                at = pl.ds(pl.multiple_of((4 * s + g) * share, share), share)
                fc1_ref[:, at] = refs[j][0, :, s * share : (s + 1) * share].astype(full)
            fc2_ref[tile(g, rows), :] = refs[j][1].astype(full)

    return call(
        kernel,
        "finish_mlp",
        (q[None], *pieces),
        [SCALARS] + [ON_CHIP] * 4,
        [((rows, 4 * width), full), ((4 * rows, width), full)],
        [ON_CHIP] * 2,
        [],
    )


def finish_attention(q, pieces):
    rows, width = pieces[0].shape
    quarter = width // 4

    def kernel(q_ref, *refs):
        qkv_ref, out_ref = refs[4:]
        for j in range(4):
            g = q_ref[0] ^ j
            for t in range(3):
                at = pl.ds(pl.multiple_of(t * width + g * quarter, quarter), quarter)
                qkv_ref[:, at] = refs[j][:, t * quarter : (t + 1) * quarter].astype(full)
            out_ref[:, tile(g, quarter)] = refs[j][:, 3 * quarter :].astype(full)

    return call(
        kernel,
        "finish_attention",
        (q[None], *pieces),
        [SCALARS] + [ON_CHIP] * 4,
        [((rows, 3 * width), full), ((rows, width), full)],
        [ON_CHIP] * 2,
        [],
    )


BELOW = 16


def first_payload(q, w_qkv, vectors):
    rows, columns = w_qkv.shape
    width = columns // 3
    quarter = width // 4
    wide = 3 * quarter

    def kernel(q_ref, w_ref, *refs):
        out_ref, held, low, sem = refs[len(vectors) :]
        for t in range(3):
            at = pl.multiple_of(t * width + q_ref[0] * quarter, quarter)
            pltpu.make_async_copy(
                w_ref.at[:, pl.ds(at, quarter)], held.at[:, pl.ds(t * quarter, quarter)], sem.at[0]
            ).start()
        low[...] = jnp.zeros_like(low)
        for k, vector in enumerate(refs[: len(vectors)]):
            low[k : k + 1, : vector.shape[1]] = vector[...]
        out_ref[rows:] = low[...].astype(half)
        pltpu.make_async_copy(held, held, sem.at[0]).wait()
        out_ref[:rows] = held[...].astype(half)

    return call(
        kernel,
        "first_payload",
        (q[None], w_qkv, *(v[None] for v in vectors)),
        [SCALARS, ANYWHERE] + [ON_CHIP] * len(vectors),
        [((rows + BELOW, wide), half)],
        [ON_CHIP],
        [pltpu.VMEM((rows, wide), full), pltpu.VMEM((BELOW, wide), full), pltpu.SemaphoreType.DMA((1,))],
    )[0]


def unpack_vectors(order, parts, n, rows, share):
    width = n * rows
    quarter = width // 4
    if rows % 128 or share % 128:
        q = order[n]
        held = jnp.concatenate([p[:, rows:] for p in parts]).astype(full)
        held = held[jnp.zeros((n,), jnp.int32).at[order[:n]].set(jnp.arange(n, dtype=jnp.int32))]
        groups = jnp.arange(4, dtype=jnp.int32) ^ q
        vectors = jnp.stack([held[:, k, :rows].reshape(1, width) for k in range(8)])
        units = held[:, 8, : 4 * share].reshape(n, 4, share).transpose(1, 0, 2)[groups]
        ends = [vectors[k].reshape(4, 1, quarter)[groups] for k in range(2)]
        return vectors, units.reshape(4, 1, width), jnp.concatenate([ends[0], 0 * ends[0], ends[1]], axis=2)

    def kernel(order_ref, *refs):
        part_refs, (vector_ref, fc1_ref, qkv_ref, held, wider, sem) = refs[: len(parts)], refs[len(parts) :]
        base = 0
        for part in part_refs:
            size = part.shape[0]
            pltpu.make_async_copy(part.at[:, pl.ds(rows, BELOW)], held.at[pl.ds(base, size)], sem.at[0]).start()
            base += size
        pltpu.make_async_copy(held, held, sem.at[0]).wait()
        wider[...] = held[...].astype(full)
        q = order_ref[n]
        for r in range(n):
            at = tile(order_ref[r], rows)
            for k in range(8):
                vector_ref[k, :, at] = wider[r, k : k + 1, :rows]
            for j in range(4):
                fc1_ref[j, :, tile(order_ref[r], share)] = wider[r, 8:9, tile(q ^ j, share)]
        for j in range(4):
            at = tile(q ^ j, quarter)
            qkv_ref[j, :, :quarter] = vector_ref[0, :, at]
            qkv_ref[j, :, quarter : 2 * quarter] = jnp.zeros((1, quarter), full)
            qkv_ref[j, :, 2 * quarter :] = vector_ref[1, :, at]

    return call(
        kernel,
        "unpack_vectors",
        (order, *parts),
        [SCALARS] + [ANYWHERE] * len(parts),
        [((8, 1, width), full), ((4, 1, width), full), ((4, 1, 3 * quarter), full)],
        [ON_CHIP] * 3,
        [
            pltpu.VMEM((n, BELOW, 3 * quarter), half),
            pltpu.VMEM((n, BELOW, 3 * quarter), full),
            pltpu.SemaphoreType.DMA((1,)),
        ],
    )


def pack_sums(order, n, rows, share, proj_sums, unit_sums, wide_sums):
    width = n * rows
    quarter = width // 4
    if rows % 128 or share % 128:
        groups = jnp.arange(4, dtype=jnp.int32) ^ order[n]
        proj = jnp.concatenate(proj_sums)[groups]
        units = jnp.concatenate(unit_sums)[groups].reshape(4, n, share)
        flat = [proj[:, :, :quarter].reshape(width), proj[:, :, 2 * quarter :].reshape(width)]
        two, one = wide_sums
        flat += [two[0], one[0], one[1], two[3], two[1], two[2]]
        flat = [v.reshape(n, 1, rows) for v in flat]
        stacked = [jnp.pad(v, ((0, 0), (0, 0), (0, 128 - rows))) for v in flat]
        stacked.append(jnp.pad(units.transpose(1, 0, 2), ((0, 0), (0, 4), (0, 128 - share))))
        return jnp.concatenate(stacked, axis=1)[order[:n]]

    def kernel(order_ref, proj_a, proj_b, unit_a, unit_b, two_ref, one_ref, out_ref, proj, units):
        proj[:2], proj[2:] = proj_a[...], proj_b[...]
        units[:2], units[2:] = unit_a[...], unit_b[...]
        q = order_ref[n]
        per = n // 4
        for r in range(n):
            s = order_ref[r]
            j = (s // per) ^ q
            at = tile(s, rows)
            inside = pl.multiple_of((s % per) * rows, rows)
            out_ref[r, 0:1] = proj[j, :, pl.ds(inside, rows)]
            out_ref[r, 1:2] = proj[j, :, pl.ds(2 * quarter + inside, rows)]
            for k, (ref, row) in enumerate(
                ((two_ref, 0), (one_ref, 0), (one_ref, 1), (two_ref, 3), (two_ref, 1), (two_ref, 2))
            ):
                out_ref[r, 2 + k : 3 + k] = ref[row, :, at]
            for g in range(4):
                out_ref[r, 8 + g : 9 + g] = units[q ^ g, :, tile(s, share)]
            out_ref[r, 12:] = jnp.zeros((4, rows), full)

    sums_two, sums_one = wide_sums
    return call(
        kernel,
        "pack_sums",
        (order, *proj_sums, *unit_sums, sums_two, sums_one),
        [SCALARS] + [ON_CHIP] * 6,
        [((n, 16, rows), full)],
        [ON_CHIP],
        [pltpu.VMEM((4, 1, 3 * quarter), full), pltpu.VMEM((4, 1, width), full)],
    )[0]


def table(codes, width):
    ratio = 0.3 * jnp.exp(codes.astype(full) * (math.log(10.0 / 0.3) / (NSCALE - 1)))
    quarter = width // 4
    omega = jnp.exp(jnp.arange(quarter).astype(full) * (-math.log(10000.0) / quarter))
    steps = jnp.arange(GRID, dtype=jnp.int32).astype(full)
    angle = ratio[:, None, None] * steps[None, :, None] * omega[None, None, :]
    return jnp.concatenate([jnp.sin(angle), jnp.cos(angle)], axis=-1)


def local(
    tokens,
    scale_codes,
    w_qkv,
    b_q,
    b_v,
    w_out,
    b_out,
    gain_one,
    shift_one,
    w_fc1,
    b_fc1,
    w_fc2,
    b_fc2,
    gain_two,
    shift_two,
    cotangent,
):
    n = lax.axis_size("fsdp")
    q = lax.axis_index("dp")
    f = lax.axis_index("fsdp")
    row_count, width = tokens.shape
    rows = width // n
    ff = b_fc1.shape[0] * n
    ffq = ff // n // 4
    hidden = n * ffq
    quarter = width // 4
    n_img = scale_codes.shape[0]
    patches = row_count // n_img
    padded = -(-patches // 16) * 16
    factor = 1.0 / math.sqrt(width // HEADS)
    seq = Order(q)
    bits = list(reversed(range(n.bit_length() - 1)))
    near = min(1, len(bits) - 1)
    shard_order = jnp.asarray(masks(bits), jnp.int32) ^ f
    group_order = jnp.arange(4, dtype=jnp.int32) ^ q
    order = jnp.concatenate([shard_order, q[None]])

    def last_three(chain):
        while len(chain.bits) > 3:
            chain.launch()
            seq.land((), chain)
            chain.join()
        return chain

    small = [b_q, b_v, b_out, gain_one, shift_one, b_fc2, gain_two, shift_two, b_fc1]
    qkv = last_three(Gather(seq, first_payload(q, w_qkv, small), n, bits))
    qkv.launch()
    rest_own, two_own = payloads([seq.at(q), q ^ 2], w_fc1, w_fc2)
    rest_own, two_own = seq.land((rest_own, two_own), qkv)
    rest = Sent(lax.all_gather(rest_own, "fsdp", axis=0, tiled=False))
    two = Sent(lax.all_gather(two_own, "fsdp", axis=0, tiled=False))
    out_own = [lax.dynamic_slice(w_out, (0, g * quarter), (rows, quarter)) for g in (q, q ^ 2)]
    out = last_three(Gather(seq, jnp.concatenate(out_own, axis=1).astype(half), n, bits))

    def spread_rows(value):
        split = value.reshape(n_img, patches, width)
        return jnp.pad(split, ((0, 0), (0, padded - patches), (0, 0)))

    def compact(value):
        return value.reshape(n_img, padded, width)[:, :patches].reshape(row_count, width)

    qkv.join()
    qkv.launch()
    out.launch()
    spread_tokens = seq.land(spread_rows(seq.at(tokens)), qkv)
    qkv_near = qkv.join()
    qkv.launch()
    near_b, near_c = Sent(core_swap(qkv.held)), Sent(x_swap(qkv.held))
    seq.land((), out)
    out.join()
    out.launch()
    places = table(scale_codes, width)
    row_place = jnp.broadcast_to(places[:, :, None], (n_img, GRID, GRID, width // 2))
    col_place = jnp.broadcast_to(places[:, None], (n_img, GRID, GRID, width // 2))
    place = jnp.concatenate([row_place, col_place], axis=-1).reshape(n_img, patches, width)
    place = jnp.pad(place, ((0, 0), (0, padded - patches), (0, 0)))
    x_zero = (seq.at(spread_tokens).astype(full) + place).reshape(-1, width)
    x_zero = seq.land(x_zero, qkv, near_b)
    qkv_far = seq.at(qkv.got)
    far_b, far_c = Sent(core_swap(qkv_far)), Sent(x_swap(qkv_far))
    vectors, bias_fc1, bias_qkv = unpack_vectors(seq.at(order), (qkv_near, qkv_far), n, rows, ffq)
    _, _, full_bout, gain_one_f, shift_one_f, full_bfc2, gain_two_f, shift_two_f = vectors
    normed_one = layer_norm(x_zero, gain_one_f, shift_one_f).astype(half)
    normed_one = seq.land(normed_one, far_b)

    first = attention_forward(
        seq.at(order), normed_one, bias_qkv[:2], ((qkv_near, qkv_far), (near_b.value, far_b.value)),
        n_img, patches, factor,
    )
    first = (seq.land(first[0], near_c, far_c, out), *first[1:])
    near_c, far_c = seq.at((near_c.value, far_c.value))
    near_d, far_d = Sent(core_swap(near_c)), Sent(core_swap(far_c))
    out.join()
    out.launch()
    cot = seq.land(spread_rows(cotangent).reshape(-1, width), near_d, far_d)
    second = attention_forward(
        seq.at(order), normed_one, bias_qkv[2:], ((near_c, far_c), (near_d.value, far_d.value)),
        n_img, patches, factor,
    )
    second = (seq.land(second[0], out), *second[1:])
    out_a = seq.at(out.join())
    out_b = Sent(core_swap(out_a))
    seq.land((), out_b)
    outs = (out_a, out_b.value)
    qkv_parts = (
        (qkv_near, qkv_far), (near_b.value, far_b.value), (near_c, far_c), (near_d.value, far_d.value)
    )
    qkvs = (*first[:2], *second[:2])
    mixed = (*first[2:4], *second[2:4])
    lses = (*first[4:], *second[4:])
    after_attn, normed_two = attention_out(
        seq.at(order), x_zero, mixed, outs, full_bout, gain_two_f, shift_two_f
    )
    normed_two = seq.land(normed_two, rest)
    rest_a = seq.at(rest.value)
    rest_b = Sent(core_swap(rest_a))
    up_c = Sent(x_swap(seq.at(rest_a[:, :, :hidden])))
    seq.land((), rest_b)

    up_g1, down_g1, g_bias_1, back_sum, out_sum = mlp(
        seq.at(order), normed_two, cot, bias_fc1[1], rest_b.value, rest_b.value, hidden
    )
    up_g0, down_g0, g_bias_0, back_sum, out_sum = mlp(
        order, normed_two, cot, bias_fc1[0], rest_a, rest_a, hidden, (out_sum, back_sum)
    )
    up_g0 = seq.land(up_g0, up_c, two)
    up_g1 = seq.at(up_g1)
    up_got = Sent(core_swap(up_g1))
    down_g1 = seq.at(down_g1)
    down_got = Sent(core_swap(down_g1))
    up_c, two = seq.at((up_c.value, two.value))
    up_d, two_d = Sent(core_swap(up_c)), Sent(core_swap(two))
    seq.land((), up_got)
    red_up = Reduce(seq, (up_g0, up_got.value), n)
    red_up.launch()
    seq.land((), down_got)
    red_down = Reduce(seq, (down_g0, down_got.value), n)
    red_down.launch(near)
    up_g2, down_g2, g_bias_2, back_sum, out_sum = mlp(
        seq.at(order), normed_two, cot, bias_fc1[2], up_c, two, 0, (out_sum, back_sum)
    )
    up_g2 = seq.land(up_g2, up_d, two_d, red_up, red_down)
    red_up.launch()
    red_down.launch()
    up_g3, down_g3, g_bias_3, grad_two_in, block = mlp(
        seq.at(order), normed_two, cot, bias_fc1[3], up_d.value, two_d.value, 0,
        (out_sum, back_sum), (after_attn, full_bfc2),
    )
    up_g3 = seq.land(up_g3, red_up, red_down)
    up_got = Sent(core_swap(up_g3))
    down_g3 = seq.at(down_g3)
    down_got = Sent(core_swap(down_g3))
    red_up.launch()
    red_down.launch()
    seq.land((), up_got)
    two_up = Reduce(seq, (up_g2, up_got.value), n)
    two_up.launch()
    seq.land((), down_got)
    two_down = Reduce(seq, (down_g2, down_got.value), n)
    two_down.launch(near)

    after_grad, mg0, mg1, mg2, mg3, g_out, sums_two = attention_out_back(
        seq.at(order), grad_two_in, after_attn, cot, gain_two_f, mixed, outs
    )
    mg2 = seq.at(mg2)
    g_w2, g_w3, proj2, proj3, sums_b = attention_back(
        seq.at(order), normed_one, qkvs[2:], lses[2:], (mg2, mg3), g_out, (2, 3), n_img, patches, factor, n
    )
    g_w3 = seq.land(g_w3, red_up, red_down, two_up, two_down)
    w_3 = Sent(core_swap(g_w3))
    two_up.launch()
    two_down.launch()
    seq.land((), w_3)
    middle = n // 2
    half_shape = (2,) * (len(bits) - 1)
    w_high = Sent(x_swap(seq.at(rounded_sum([g_w2[middle:], w_3.value[middle:]]))))
    g_w0, g_w1, proj0, proj1, sums_a = attention_back(
        seq.at(order), normed_one, qkvs[:2], lses[:2], (mg0, mg1), g_out, (0, 1), n_img, patches, factor, n
    )
    g_w1 = seq.land(g_w1, two_up, two_down, w_high)
    w_1 = Sent(core_swap(g_w1))
    two_up.launch()
    two_down.launch()
    seq.land((), w_1)
    red_w = Reduce(seq, (g_w0, w_1.value), n)
    red_w.launch(0, [w_high.value.reshape(half_shape + w_high.value.shape[1:])])
    w_low = Sent(x_swap(seq.at(rounded_sum([g_w2[:middle], w_3.value[:middle]]))))
    tokens_grad, sums_one = input_back(
        seq.at(order), x_zero, after_grad, gain_one_f, (proj0, proj1, proj2, proj3), qkv_parts
    )
    sums_one = seq.land(sums_one, two_up, two_down, red_w, w_low)
    red_w.terms = [*red_w.terms, w_low.value.reshape(half_shape + w_low.value.shape[1:])]
    while len(red_w.axes) > 2:
        red_w.launch()
        seq.land((), red_w)
    red_w.launch()
    cross = Sent(x_swap(seq.at(jnp.stack([two_up.rest().piece(), two_down.rest().piece()]))))
    packed = pack_sums(
        seq.at(order), n, rows, ffq, (sums_a, sums_b), (jnp.stack([g_bias_0, g_bias_1]), jnp.stack([g_bias_2, g_bias_3])), (sums_two, sums_one)
    )
    packed = seq.at(packed)
    peers = Sent([xor_swap(packed, "dp", 4, m) for m in (1, 2, 3)])
    seq.land((), peers)
    sums = Reduce(seq, (packed, *peers.value), n, full)
    while len(sums.axes) > 1:
        sums.launch()
        if len(sums.axes) > 1:
            seq.land((), sums)
    seq.land((), sums, red_w, cross)
    if red_w.axes:
        red_w.launch()
    owned = [rounded_sum([*red_up.rest().terms, cross.value[0]]), rounded_sum([*red_down.rest().terms, cross.value[1]])]
    mlp_spread = Spread(seq, jnp.stack(owned))
    sums.launch()
    block, tokens_grad = seq.at((block, tokens_grad))
    block_out, grad_tokens = seq.land(
        (compact(block), compact(tokens_grad)), sums, mlp_spread, *([red_w] if len(bits) > 1 else [])
    )
    small_sums = sums.piece()
    w_spread = Spread(seq, red_w.piece())
    mlp_spread.cross()
    small_sums = seq.land(small_sums, mlp_spread)
    mlp_pieces = seq.at(mlp_spread.pieces)
    out_fc1, out_fc2 = finish_mlp(q, mlp_pieces, n)
    out_fc2, small_sums = seq.land((out_fc2, small_sums), w_spread)
    w_spread.cross()
    seq.land((), w_spread)
    out_qkv, out_out = finish_attention(seq.value, w_spread.pieces)
    small_out = [small_sums[k, :rows] for k in range(8)]
    out_bfc1 = small_sums[8:12, :ffq].reshape(-1)
    o_bq, o_bv, o_bout, o_gone, o_sone, o_bfc2, o_gtwo, o_stwo = small_out
    return (
        block_out,
        grad_tokens,
        out_qkv,
        o_bq,
        o_bv,
        out_out,
        o_bout,
        o_gone,
        o_sone,
        out_fc1,
        out_bfc1,
        out_fc2,
        o_bfc2,
        o_gtwo,
        o_stwo,
    )


def solution(mesh):
    rows_split = P(("dp", "fsdp"), None)
    matrix = P("fsdp", None)
    vector = P("fsdp")
    return jax.shard_map(
        local,
        mesh=mesh,
        in_specs=(
            rows_split, P(("dp", "fsdp")), matrix, vector, vector, matrix, vector, vector, vector,
            matrix, vector, matrix, vector, vector, vector, rows_split,
        ),
        out_specs=(
            rows_split, rows_split, matrix, vector, vector, matrix, vector, vector, vector,
            matrix, vector, matrix, vector, vector, vector,
        ),
        check_vma=False,
    )
```

```python
import math

import jax
import jax.numpy as jnp
from jax import lax
from jax.experimental import pallas as pl
from jax.experimental.pallas import tpu as pltpu
from jax.sharding import PartitionSpec as P

HEADS = 16
GRID = 14
NSCALE = 16
norm_eps = 1e-06
half = jnp.bfloat16
full = jnp.float32


def xor_swap(value, axis, size, mask):
    return lax.ppermute(value, axis, [(i, i ^ mask) for i in range(size)])


def core_swap(value):
    return xor_swap(value, "dp", 4, 1)


def x_swap(value):
    return xor_swap(value, "dp", 4, 2)


def masks(bits):
    found = [0]
    for bit in bits:
        found = found + [m | (1 << bit) for m in found]
    return found


class Order:
    def __init__(self, value):
        self.value = value

    def at(self, value):
        value, self.value = lax.optimization_barrier((value, self.value))
        return value

    def land(self, value, *sent):
        value, flights = self.at((value, [s.flight for s in sent]))
        for s, flight in zip(sent, flights, strict=True):
            s.accept(flight)
        return value


class Sent:
    def __init__(self, flight):
        self.flight = flight

    def accept(self, value):
        self.value = value


class Gather:
    def __init__(self, seq, piece, n, bits):
        self.seq, self.held, self.n, self.bits = seq, piece[None], n, list(bits)

    def launch(self):
        self.held = self.seq.at(self.held)
        self.flight = xor_swap(self.held, "fsdp", self.n, 1 << self.bits.pop(0))

    def accept(self, value):
        self.got = value

    def join(self):
        self.held = jnp.concatenate([self.held, self.got])
        return self.held


def rounded_sum(terms, kind=half):
    return sum(t.astype(full) for t in terms).astype(kind)


class Reduce:
    def __init__(self, seq, terms, n, kind=half):
        self.kind = kind
        self.seq, self.n, self.axes = seq, n, list(range(n.bit_length() - 1))
        self.terms = [t.reshape((2,) * len(self.axes) + t.shape[1:]) for t in terms]

    def launch(self, bit=None, more=()):
        bit = self.axes[0] if bit is None else bit
        axis = self.axes.index(bit)
        self.axes.pop(axis)
        low, high = [
            [lax.index_in_dim(t, side, axis, keepdims=False) for t in self.terms] for side in (0, 1)
        ]
        self.terms = low
        self.flight = xor_swap(self.seq.at(rounded_sum([*high, *more], self.kind)), "fsdp", self.n, 1 << bit)

    def accept(self, value):
        self.terms = [*self.terms, value]

    def rest(self):
        while self.axes:
            self.launch()
            self.seq.land((), self)
        return self

    def piece(self):
        return rounded_sum(self.terms, self.kind)


class Spread:
    def __init__(self, seq, piece):
        self.seq, self.pieces = seq, [seq.at(piece)]
        self.flight = [core_swap(self.pieces[0]), x_swap(self.pieces[0])]

    def cross(self):
        self.flight = [core_swap(self.seq.at(self.pieces[2]))]

    def accept(self, value):
        self.pieces += value


ANYWHERE = pl.BlockSpec(memory_space=pl.ANY)
ON_CHIP = pl.BlockSpec(memory_space=pltpu.VMEM)
SCALARS = pl.BlockSpec(memory_space=pltpu.SMEM)


def dot(left, right, dim_left, dim_right):
    return lax.dot_general(
        left, right, (((dim_left,), (dim_right,)), ((), ())), preferred_element_type=full
    )


def call(kernel, name, operands, in_specs, outs, out_specs, scratch):
    return pl.pallas_call(
        kernel,
        out_shape=[jax.ShapeDtypeStruct(shape, kind) for shape, kind in outs],
        in_specs=in_specs,
        out_specs=out_specs,
        scratch_shapes=scratch,
        compiler_params=pltpu.CompilerParams(vmem_limit_bytes=58 * 2**20),
        name=name,
    )(*operands)


def loop(count, body, unroll=1):
    def step(i, carry):
        body(i)
        return carry

    lax.fori_loop(0, count, step, 0, unroll=unroll)


def tile(i, size):
    return pl.ds(pl.multiple_of(i * size, size), size)


def bring(src, dst, sem):
    pltpu.make_async_copy(src, dst, sem).start()


def arrived(dst, sem):
    pltpu.make_async_copy(dst, dst, sem).wait()


def fetch(parts, order_ref, place, sem):
    base = 0
    for part in parts:

        def start(r, part=part, base=base):
            shard = r if order_ref is None else order_ref[base + r]
            pltpu.make_async_copy(part.at[r], place(shard), sem).start()

        loop(part.shape[0], start)
        base += part.shape[0]


def head_rows(s, q, n, rows, quarter):
    per = n // 4
    return pl.multiple_of(((s // per) ^ q) * quarter + (s % per) * rows, rows)


def pair_scores(q2, k2):
    first = lax.broadcasted_iota(jnp.int32, q2.shape, 1) < q2.shape[1] // 2
    both = apart(q2, first)
    return both, dot(k2, both, 1, 1), first


def apart(value, first):
    zero = jnp.zeros_like(value)
    return jnp.concatenate([jnp.where(first, value, zero), jnp.where(first, zero, value)])


def attention_forward(order, normed, bias, weights, n_img, patches, factor):
    groups, n_parts = len(weights), len(weights[0])
    wide = weights[0][0].shape[2]
    count, width = normed.shape
    rows = width // sum(part.shape[0] for part in weights[0])
    padded = count // n_img
    quarter = wide // 3

    def kernel(order_ref, normed_ref, bias_ref, *refs):
        w_refs, refs = refs[: groups * n_parts], refs[groups * n_parts :]
        qkv_refs, mixed_refs, refs = refs[:groups], refs[groups : 2 * groups], refs[2 * groups :]
        lse_refs, (w_held, sems) = refs[:groups], refs[groups:]
        for g in range(groups):
            fetch(
                [w.at[:, pl.ds(0, rows)] for w in w_refs[g * n_parts : (g + 1) * n_parts]],
                order_ref,
                lambda s, g=g: w_held.at[g, pl.ds(pl.multiple_of(s * rows, rows), rows)],
                sems.at[g],
            )
        for g in range(groups):
            pltpu.make_async_copy(w_held.at[g], w_held.at[g], sems.at[g]).wait()

            def project(t, g=g):
                at = tile(t, quarter)
                product = dot(normed_ref[...], w_held[g, :, at], 1, 0)
                qkv_refs[g][:, at] = (product + bias_ref[g, :, at]).astype(half)

            loop(3, project)

            def attend(i, g=g):
                at = tile(i // 2, padded)
                lanes = [pl.ds(pl.multiple_of(t * quarter + (i % 2) * 128, 128), 128) for t in range(3)]
                q2 = qkv_refs[g][at, lanes[0]] * factor
                k2 = qkv_refs[g][at, lanes[1]]
                v2 = qkv_refs[g][at, lanes[2]]
                _, scores, first = pair_scores(q2, k2)
                key = lax.broadcasted_iota(jnp.int32, scores.shape, 0)
                scores = jnp.where(key < patches, scores, -1e30)
                top = jnp.max(scores, axis=0, keepdims=True)
                raised = jnp.exp(scores - top)
                total = jnp.sum(raised, axis=0, keepdims=True)
                lse_refs[g][i] = top + jnp.log(total)
                out = dot((raised * (1.0 / total)).astype(half), v2, 0, 0)
                mixed_refs[g][at, lanes[0]] = jnp.where(first, out[:padded], out[padded:]).astype(half)

            loop(2 * n_img, attend, 2 * n_img)

    return call(
        kernel,
        "attention_forward",
        (order, normed, bias, *(part for w in weights for part in w)),
        [SCALARS, ON_CHIP, ON_CHIP] + [ANYWHERE] * (groups * n_parts),
        [((count, wide), half)] * groups
        + [((count, quarter), half)] * groups
        + [((2 * n_img, 1, 2 * padded), full)] * groups,
        [ON_CHIP] * (3 * groups),
        [pltpu.VMEM((groups, width, wide), half), pltpu.SemaphoreType.DMA((groups,))],
    )


def layer_norm(value, gain, shift):
    center = jnp.mean(value, axis=-1, keepdims=True)
    offset = value - center
    spread = jnp.mean(offset * offset, axis=-1, keepdims=True)
    return offset * lax.rsqrt(spread + norm_eps) * gain + shift


def layer_norm_back(value, grad, gain):
    center = jnp.mean(value, axis=-1, keepdims=True)
    offset = value - center
    scale = lax.rsqrt(jnp.mean(offset * offset, axis=-1, keepdims=True) + norm_eps)
    unit = offset * scale
    scaled = grad * gain
    inner = jnp.mean(scaled * unit, axis=-1, keepdims=True)
    return scale * (scaled - jnp.mean(scaled, axis=-1, keepdims=True) - unit * inner), grad * unit


def load_out(order_ref, out_refs, held, sem, n, rows, quarter):
    q = order_ref[n]
    for j in range(4):
        column = pl.multiple_of((q ^ j) * quarter, quarter)
        fetch(
            [out_refs[j % 2].at[:, :, pl.ds(j // 2 * quarter, quarter)]],
            order_ref,
            lambda s, column=column: held.at[
                pl.ds(head_rows(s, q, n, rows, quarter), rows), pl.ds(column, quarter)
            ],
            sem,
        )


CHUNK = 16
ROWS = 64


def attention_out(order, x_zero, mixed, outs, bias, gain, shift):
    count, width = x_zero.shape
    n, rows, _ = outs[0].shape
    quarter = mixed[0].shape[1]

    def kernel(order_ref, x_ref, bias_ref, gain_ref, shift_ref, *refs):
        mixed_refs, out_refs = refs[:4], refs[4:6]
        after_ref, normed_ref, held, x_held, sems = refs[6:]
        bring(x_ref, x_held, sems.at[1])
        load_out(order_ref, out_refs, held, sems.at[0], n, rows, quarter)
        together = jnp.concatenate([m[...] for m in mixed_refs], axis=1)
        pltpu.make_async_copy(held, held, sems.at[0]).wait()
        after_ref[...] = dot(together, held[...], 1, 0)
        arrived(x_held, sems.at[1])

        def finish(i):
            at = tile(i, CHUNK)
            after = x_held[at] + (after_ref[at] + bias_ref[...])
            after_ref[at] = after
            normed_ref[at] = layer_norm(after, gain_ref[...], shift_ref[...]).astype(half)

        loop(count // CHUNK, finish, 13)

    return call(
        kernel,
        "attention_out",
        (order, x_zero, bias, gain, shift, *mixed, *outs),
        [SCALARS, ANYWHERE] + [ON_CHIP] * 7 + [ANYWHERE] * 2,
        [((count, width), full), ((count, width), half)],
        [ON_CHIP] * 2,
        [
            pltpu.VMEM((width, width), half),
            pltpu.VMEM((count, width), full),
            pltpu.SemaphoreType.DMA((2,)),
        ],
    )


def mlp(order, normed, cot, bias, up_all, down_all, down_start, carried=None, ending=None):
    count, width = normed.shape
    n, rows, _ = up_all.shape
    hidden = bias.shape[1]
    share = hidden // n
    step = min(512, hidden)
    steps = hidden // step
    more = [*(carried or []), *(ending[:1] if ending else [])]
    last = list(ending[1:]) if ending else []

    def kernel(order_ref, bias_ref, *refs):
        last_refs, refs = refs[: len(last)], refs[len(last) :]
        normed_ref, cot_ref, up_ref, down_ref, refs = *refs[:4], refs[4:]
        more_refs, refs = refs[: len(more)], refs[len(more) :]
        g_up_ref, g_down_ref, g_bias_ref, back_ref, end_ref, refs = *refs[:5], refs[5:]
        held, refs = refs[: len(more)], refs[len(more) :]
        rows_in, cots, out, back, up, down, pre, act, act_half, pre_half, g_up, g_down, sems = refs
        bring(normed_ref, rows_in, sems.at[3])
        fetch(
            [up_ref.at[:, :, pl.ds(0, hidden)]],
            None,
            lambda s: up.at[pl.ds(pl.multiple_of(s * rows, rows), rows)],
            sems.at[0],
        )
        bring(cot_ref, cots, sems.at[4])
        fetch(
            [down_ref.at[:, :, pl.ds(down_start, width)]],
            None,
            lambda s: down.at[pl.ds(pl.multiple_of(s * share, share), share)],
            sems.at[1],
        )
        for k in range(len(more)):
            bring(more_refs[k], held[k], sems.at[5 + k])
        arrived(rows_in, sems.at[3])
        arrived(up, sems.at[0])
        for t in range(steps):
            at = pl.ds(t * step, step)
            pre[...] = dot(rows_in[...], up[:, at], 1, 0)
            if not t:
                arrived(cots, sems.at[4])
                arrived(down, sems.at[1])
            act[...] = dot(cots[...], down[at, :], 1, 1)

            def gelu(i, at=at):
                some = tile(i, 2 * CHUNK)
                x = pre[some] + bias_ref[:, at]
                below = 0.5 * (1.0 + lax.erf(x * math.sqrt(0.5)))
                density = jnp.exp(-0.5 * x * x) * (1.0 / math.sqrt(2.0 * math.pi))
                act_half[some] = (x * below).astype(half)
                pre_half[some] = (act[some] * (below + x * density)).astype(half)

            loop(count // CHUNK // 2, gelu)
            p = pre_half[...]
            h = act_half[...]
            more_back = dot(p, up[:, at], 1, 1)
            more_out = dot(h, down[at, :], 1, 0)
            if t:
                back[...] += more_back
                out[...] += more_out
            elif carried:
                arrived(held[0], sems.at[5])
                arrived(held[1], sems.at[6])
                out[...] = held[0][...] + more_out
                back[...] = held[1][...] + more_back
            else:
                out[...] = more_out
                back[...] = more_back
            if t == steps - 1:
                bring(back, back_ref, sems.at[3])
                if not ending:
                    bring(out, end_ref, sems.at[4])
            g_down[at, :] = dot(h, cots[...], 0, 0).astype(half)
            if t == steps - 1:

                def send_down(r):
                    at = pl.multiple_of(order_ref[r] * share, share)
                    bring(g_down.at[pl.ds(at, share)], g_down_ref.at[r], sems.at[2])

                loop(n, send_down)
            g_up[:, at] = dot(rows_in[...], p, 0, 0).astype(half)
            g_bias_ref[:, at] = jnp.sum(p.astype(full), axis=0, keepdims=True)

        def send_up(r):
            at = pl.multiple_of(order_ref[r] * rows, rows)
            bring(g_up.at[pl.ds(at, rows)], g_up_ref.at[r], sems.at[0])

        loop(n, send_up)
        if ending:
            arrived(held[2], sems.at[7])

            def finish(i):
                at = tile(i, 2 * CHUNK)
                end_ref[at] = (held[2][at] + (out[at] + last_refs[0][...])).astype(half)

            loop(count // CHUNK // 2, finish)
        else:
            arrived(end_ref, sems.at[4])
        arrived(back_ref, sems.at[3])
        arrived(g_down_ref, sems.at[2])
        arrived(g_up_ref, sems.at[0])

    sums = pltpu.VMEM((count, width), full)
    wide = pltpu.VMEM((count, width), half)
    square = pltpu.VMEM((width, hidden), half)
    return call(
        kernel,
        "mlp",
        (order, bias, *last, normed, cot, up_all, down_all, *more),
        [SCALARS] + [ON_CHIP] * (1 + len(last)) + [ANYWHERE] * (4 + len(more)),
        [
            ((n, rows, hidden), half),
            ((n, share, width), half),
            ((1, hidden), full),
            ((count, width), full),
            ((count, width), half if ending else full),
        ],
        [ANYWHERE, ANYWHERE, ON_CHIP, ANYWHERE, ON_CHIP if ending else ANYWHERE],
        [
            *([sums] * len(more)),
            wide,
            wide,
            sums,
            sums,
            square,
            pltpu.VMEM((hidden, width), half),
            pltpu.VMEM((count, step), full),
            pltpu.VMEM((count, step), full),
            pltpu.VMEM((count, step), half),
            pltpu.VMEM((count, step), half),
            square,
            pltpu.VMEM((hidden, width), half),
            pltpu.SemaphoreType.DMA((5 + len(more),)),
        ],
    )


def attention_out_back(order, grad, after, cot, gain, mixed, outs):
    count, width = after.shape
    n, rows, _ = outs[0].shape
    quarter = mixed[0].shape[1]

    def kernel(order_ref, grad_ref, after_ref, cot_ref, gain_ref, *refs):
        mixed_refs, out_refs, refs = refs[:4], refs[4:6], refs[6:]
        after_grad_ref, mixed_grad_refs, g_out_ref, sums_ref = refs[0], refs[1:5], refs[5], refs[6]
        held, branch, terms, grad, after, cot, mixes, sems = refs[7:]
        block = count // 4
        for k in range(4):
            some = pl.ds(k * block, block)
            bring(grad_ref.at[some], grad.at[some], sems.at[1 + k])
            bring(after_ref.at[some], after.at[some], sems.at[5 + k])
            bring(cot_ref.at[some], cot.at[some], sems.at[9 + k])
        load_out(order_ref, out_refs, held, sems.at[0], n, rows, quarter)
        for j in range(4):
            bring(mixed_refs[j], mixes.at[j], sems.at[13])
        terms[...] = jnp.zeros_like(terms)

        def fold(value):
            return jnp.sum(value.reshape(CHUNK // 8, 8, width), axis=0)

        def back(i, k):
            at = pl.ds(pl.multiple_of(k * block + i * CHUNK, CHUNK), CHUNK)
            incoming = grad[at]
            part, gain_terms = layer_norm_back(after[at], incoming, gain_ref[...])
            own = cot[at].astype(full)
            total = own + part
            after_grad_ref[at] = total
            rounded = total.astype(half)
            branch[at] = rounded
            terms[0] += fold(rounded.astype(full))
            terms[1] += fold(gain_terms)
            terms[2] += fold(incoming)
            terms[3] += fold(own)

        for k in range(4):
            some = pl.ds(k * block, block)
            arrived(grad.at[some], sems.at[1 + k])
            arrived(after.at[some], sems.at[5 + k])
            arrived(cot.at[some], sems.at[9 + k])
            loop(block // CHUNK, lambda i, k=k: back(i, k), 13)
        for k in range(4):
            sums_ref[k] = jnp.sum(terms[k], axis=0, keepdims=True)
        arrived(held, sems.at[0])
        arrived(mixes, sems.at[13])
        for j in range(4):
            mixed_grad_refs[j][...] = dot(branch[...], held[j * quarter : (j + 1) * quarter], 1, 1).astype(half)
            g_out_ref[j * quarter : (j + 1) * quarter] = dot(mixes[j], branch[...], 0, 0).astype(half)

    return call(
        kernel,
        "attention_out_back",
        (order, grad, after, cot, gain, *mixed, *outs),
        [SCALARS] + [ANYWHERE] * 3 + [ON_CHIP] + [ANYWHERE] * 6,
        [((count, width), full)]
        + [((count, quarter), half)] * 4
        + [((width, width), half), ((4, 1, width), full)],
        [ON_CHIP] * 7,
        [
            pltpu.VMEM((width, width), half),
            pltpu.VMEM((count, width), half),
            pltpu.VMEM((4, 8, width), full),
            pltpu.VMEM((count, width), full),
            pltpu.VMEM((count, width), full),
            pltpu.VMEM((count, width), half),
            pltpu.VMEM((4, count, quarter), half),
            pltpu.SemaphoreType.DMA((14,)),
        ],
    )


def attention_back(order, normed, qkvs, lses, mixed_grads, g_out, which, n_img, patches, factor, n):
    groups = len(qkvs)
    count, width = normed.shape
    wide = qkvs[0].shape[1]
    quarter = wide // 3
    padded = count // n_img
    rows = width // n

    def kernel(order_ref, normed_ref, g_out_ref, *refs):
        qkv_refs, mg_refs, refs = refs[:groups], refs[groups : 2 * groups], refs[2 * groups :]
        lse_refs, refs = refs[:groups], refs[groups:]
        g_w_refs, proj_refs, sums_ref = refs[:groups], refs[groups : 2 * groups], refs[2 * groups]
        g_w, normed_held, g_out_held, sems = refs[2 * groups + 1 :]
        q = order_ref[n]
        bring(g_out_ref, g_out_held, sems.at[groups])
        bring(normed_ref, normed_held, sems.at[groups + 1])
        for g in range(groups):

            def attend(i, g=g):
                at = tile(i // 2, padded)
                lanes = [pl.ds(pl.multiple_of(t * quarter + (i % 2) * 128, 128), 128) for t in range(3)]
                q2 = qkv_refs[g][at, lanes[0]] * factor
                k2 = qkv_refs[g][at, lanes[1]]
                v2 = qkv_refs[g][at, lanes[2]]
                both, scores, first = pair_scores(q2, k2)
                key = lax.broadcasted_iota(jnp.int32, scores.shape, 0)
                probs = jnp.where(key < patches, jnp.exp(scores - lse_refs[g][i]), 0.0)
                o_both = apart(mg_refs[g][at, lanes[0]], first)
                g_probs = dot(v2, o_both, 1, 1)
                weighted = jnp.sum(probs * g_probs, axis=0, keepdims=True)
                g_scores = (probs * (g_probs - weighted)).astype(half)
                g_query = dot(g_scores, k2, 0, 0)
                g_query = jnp.where(first, g_query[:padded], g_query[padded:]) * factor
                proj_refs[g][at, lanes[0]] = g_query.astype(half)
                proj_refs[g][at, lanes[1]] = dot(g_scores, both, 1, 0).astype(half)
                proj_refs[g][at, lanes[2]] = dot(probs.astype(half), o_both, 1, 0).astype(half)

            loop(2 * n_img, attend, 4)
            if not g:
                arrived(g_out_held, sems.at[groups])
                arrived(normed_held, sems.at[groups + 1])

            def send_out(r, g=g):
                at = head_rows(order_ref[r], q, n, rows, quarter)
                column = pl.multiple_of((q ^ which[g]) * quarter, quarter)
                pltpu.make_async_copy(
                    g_out_held.at[pl.ds(at, rows), pl.ds(column, quarter)],
                    g_w_refs[g].at[r, :, pl.ds(wide, quarter)],
                    sems.at[g],
                ).start()

            loop(n, send_out)

            def weigh(t, g=g):
                at = tile(t, quarter)
                some = proj_refs[g][:, at]
                g_w[g, :, at] = dot(normed_held[...], some, 0, 0).astype(half)
                sums_ref[g, :, at] = jnp.sum(some.astype(full), axis=0, keepdims=True)

            loop(3, weigh)

            def send(r, g=g):
                at = pl.multiple_of(order_ref[r] * rows, rows)
                pltpu.make_async_copy(
                    g_w.at[g, pl.ds(at, rows)], g_w_refs[g].at[r, :, pl.ds(0, wide)], sems.at[g]
                ).start()

            loop(n, send)
        for g in range(groups):
            pltpu.make_async_copy(g_w_refs[g], g_w_refs[g], sems.at[g]).wait()

    return call(
        kernel,
        "attention_back",
        (order, normed, g_out, *qkvs, *mixed_grads, *lses),
        [SCALARS] + [ANYWHERE] * 2 + [ON_CHIP] * (3 * groups),
        [((n, rows, wide + quarter), half)] * groups
        + [((count, wide), half)] * groups
        + [((groups, 1, wide), full)],
        [ANYWHERE] * groups + [ON_CHIP] * (groups + 1),
        [
            pltpu.VMEM((groups, width, wide), half),
            pltpu.VMEM((count, width), half),
            pltpu.VMEM((width, width), half),
            pltpu.SemaphoreType.DMA((groups + 2,)),
        ],
    )


def input_back(order, x_zero, after_grad, gain, projs, weights):
    count, width = x_zero.shape
    wide = weights[0][0].shape[2]
    rows = width // sum(part.shape[0] for part in weights[0])
    parts = [part for w in weights for part in w]
    n_parts = len(weights[0])

    def kernel(order_ref, x_ref, after_ref, gain_ref, *refs):
        proj_refs, w_refs = refs[:4], refs[4 : 4 + len(parts)]
        token_ref, sums_ref, held, terms, x_held, after_held, sems = refs[4 + len(parts) :]
        for j in range(4):
            fetch(
                [w.at[:, pl.ds(0, rows)] for w in w_refs[j * n_parts : (j + 1) * n_parts]],
                order_ref,
                lambda s, j=j: held.at[j, pl.ds(pl.multiple_of(s * rows, rows), rows)],
                sems.at[j],
            )
        bring(x_ref, x_held, sems.at[4])
        bring(after_ref, after_held, sems.at[5])
        for j in range(4):
            arrived(held.at[j], sems.at[j])
            product = dot(proj_refs[j][...], held[j], 1, 1)
            if j == 0:
                token_ref[...] = product
            else:
                token_ref[...] += product
        arrived(x_held, sems.at[4])
        arrived(after_held, sems.at[5])
        terms[...] = jnp.zeros_like(terms)

        def fold(value):
            return jnp.sum(value.reshape(ROWS // 8, 8, width), axis=0)

        def back(i):
            at = tile(i, ROWS)
            incoming = token_ref[at]
            part, gain_terms = layer_norm_back(x_held[at], incoming, gain_ref[...])
            token_ref[at] = after_held[at] + part
            terms[0] += fold(gain_terms)
            terms[1] += fold(incoming)

        loop(count // ROWS, back)
        for k in range(2):
            sums_ref[k] = jnp.sum(terms[k], axis=0, keepdims=True)

    return call(
        kernel,
        "input_back",
        (order, x_zero, after_grad, gain, *projs, *parts),
        [SCALARS] + [ANYWHERE] * 2 + [ON_CHIP] * 5 + [ANYWHERE] * len(parts),
        [((count, width), full), ((2, 1, width), full)],
        [ON_CHIP] * 2,
        [
            pltpu.VMEM((4, width, wide), half),
            pltpu.VMEM((2, 8, width), full),
            pltpu.VMEM((count, width), full),
            pltpu.VMEM((count, width), full),
            pltpu.SemaphoreType.DMA((6,)),
        ],
    )


def payloads(which, w_fc1, w_fc2):
    rows, ff = w_fc1.shape
    full_share, width = w_fc2.shape
    share = full_share // 4
    n = ff // full_share
    hidden = n * share
    own, across = which
    if share % 128:
        fc1 = [lax.dynamic_slice(w_fc1, (0, (4 * s + own) * share), (rows, share)) for s in range(n)]
        fc2 = [lax.dynamic_slice(w_fc2, (g * share, 0), (share, width)).astype(half) for g in which]
        rest = jnp.concatenate([*fc1, fc2[0].reshape(rows, -1).astype(full)], axis=1)
        return rest.astype(half), fc2[1]

    def kernel(which_ref, fc1_ref, fc2_ref, rest_ref, two_ref):
        for s in range(n):
            at = pl.ds(pl.multiple_of((4 * s + which_ref[0]) * share, share), share)
            rest_ref[:, s * share : (s + 1) * share] = fc1_ref[:, at].astype(half)
        rest_ref[:, hidden : hidden + width] = fc2_ref[tile(which_ref[0], share), :].astype(half)
        two_ref[...] = fc2_ref[tile(which_ref[1], share), :].astype(half)

    return call(
        kernel,
        "payloads",
        (jnp.stack(which), w_fc1, w_fc2),
        [SCALARS] + [ON_CHIP] * 2,
        [((rows, hidden + width), half), ((share, width), half)],
        [ON_CHIP] * 2,
        [],
    )


def natural_quarters(q, pieces):
    once = [jnp.where((q & 1) == 1, pieces[i ^ 1], pieces[i]) for i in range(4)]
    return [jnp.where(q >= 2, once[i ^ 2], once[i]) for i in range(4)]


def finish_mlp(q, pieces, n):
    _, rows, width = pieces[0].shape
    share = width // n
    if share % 128:
        pieces = natural_quarters(q, pieces)
        fc1 = jnp.stack([p[0].reshape(rows, n, share) for p in pieces], axis=2).reshape(rows, 4 * width)
        return fc1.astype(full), jnp.concatenate([p[1] for p in pieces]).astype(full)

    def kernel(q_ref, *refs):
        fc1_ref, fc2_ref = refs[4:]
        for j in range(4):
            g = q_ref[0] ^ j
            for s in range(n):
                at = pl.ds(pl.multiple_of((4 * s + g) * share, share), share)
                fc1_ref[:, at] = refs[j][0, :, s * share : (s + 1) * share].astype(full)
            fc2_ref[tile(g, rows), :] = refs[j][1].astype(full)

    return call(
        kernel,
        "finish_mlp",
        (q[None], *pieces),
        [SCALARS] + [ON_CHIP] * 4,
        [((rows, 4 * width), full), ((4 * rows, width), full)],
        [ON_CHIP] * 2,
        [],
    )


def finish_attention(q, pieces):
    rows, width = pieces[0].shape
    quarter = width // 4

    def kernel(q_ref, *refs):
        qkv_ref, out_ref = refs[4:]
        for j in range(4):
            g = q_ref[0] ^ j
            for t in range(3):
                at = pl.ds(pl.multiple_of(t * width + g * quarter, quarter), quarter)
                qkv_ref[:, at] = refs[j][:, t * quarter : (t + 1) * quarter].astype(full)
            out_ref[:, tile(g, quarter)] = refs[j][:, 3 * quarter :].astype(full)

    return call(
        kernel,
        "finish_attention",
        (q[None], *pieces),
        [SCALARS] + [ON_CHIP] * 4,
        [((rows, 3 * width), full), ((rows, width), full)],
        [ON_CHIP] * 2,
        [],
    )


BELOW = 16


def first_payload(q, w_qkv, vectors):
    rows, columns = w_qkv.shape
    width = columns // 3
    quarter = width // 4
    wide = 3 * quarter

    def kernel(q_ref, w_ref, *refs):
        out_ref, held, low, sem = refs[len(vectors) :]
        for t in range(3):
            at = pl.multiple_of(t * width + q_ref[0] * quarter, quarter)
            pltpu.make_async_copy(
                w_ref.at[:, pl.ds(at, quarter)], held.at[:, pl.ds(t * quarter, quarter)], sem.at[0]
            ).start()
        low[...] = jnp.zeros_like(low)
        for k, vector in enumerate(refs[: len(vectors)]):
            low[k : k + 1, : vector.shape[1]] = vector[...]
        out_ref[rows:] = low[...].astype(half)
        pltpu.make_async_copy(held, held, sem.at[0]).wait()
        out_ref[:rows] = held[...].astype(half)

    return call(
        kernel,
        "first_payload",
        (q[None], w_qkv, *(v[None] for v in vectors)),
        [SCALARS, ANYWHERE] + [ON_CHIP] * len(vectors),
        [((rows + BELOW, wide), half)],
        [ON_CHIP],
        [pltpu.VMEM((rows, wide), full), pltpu.VMEM((BELOW, wide), full), pltpu.SemaphoreType.DMA((1,))],
    )[0]


def unpack_vectors(order, parts, n, rows, share):
    width = n * rows
    quarter = width // 4
    if rows % 128 or share % 128:
        q = order[n]
        held = jnp.concatenate([p[:, rows:] for p in parts]).astype(full)
        held = held[jnp.zeros((n,), jnp.int32).at[order[:n]].set(jnp.arange(n, dtype=jnp.int32))]
        groups = jnp.arange(4, dtype=jnp.int32) ^ q
        vectors = jnp.stack([held[:, k, :rows].reshape(1, width) for k in range(8)])
        units = held[:, 8, : 4 * share].reshape(n, 4, share).transpose(1, 0, 2)[groups]
        ends = [vectors[k].reshape(4, 1, quarter)[groups] for k in range(2)]
        return vectors, units.reshape(4, 1, width), jnp.concatenate([ends[0], 0 * ends[0], ends[1]], axis=2)

    def kernel(order_ref, *refs):
        part_refs, (vector_ref, fc1_ref, qkv_ref, held, wider, sem) = refs[: len(parts)], refs[len(parts) :]
        base = 0
        for part in part_refs:
            size = part.shape[0]
            pltpu.make_async_copy(part.at[:, pl.ds(rows, BELOW)], held.at[pl.ds(base, size)], sem.at[0]).start()
            base += size
        pltpu.make_async_copy(held, held, sem.at[0]).wait()
        wider[...] = held[...].astype(full)
        q = order_ref[n]
        for r in range(n):
            at = tile(order_ref[r], rows)
            for k in range(8):
                vector_ref[k, :, at] = wider[r, k : k + 1, :rows]
            for j in range(4):
                fc1_ref[j, :, tile(order_ref[r], share)] = wider[r, 8:9, tile(q ^ j, share)]
        for j in range(4):
            at = tile(q ^ j, quarter)
            qkv_ref[j, :, :quarter] = vector_ref[0, :, at]
            qkv_ref[j, :, quarter : 2 * quarter] = jnp.zeros((1, quarter), full)
            qkv_ref[j, :, 2 * quarter :] = vector_ref[1, :, at]

    return call(
        kernel,
        "unpack_vectors",
        (order, *parts),
        [SCALARS] + [ANYWHERE] * len(parts),
        [((8, 1, width), full), ((4, 1, width), full), ((4, 1, 3 * quarter), full)],
        [ON_CHIP] * 3,
        [
            pltpu.VMEM((n, BELOW, 3 * quarter), half),
            pltpu.VMEM((n, BELOW, 3 * quarter), full),
            pltpu.SemaphoreType.DMA((1,)),
        ],
    )


def pack_sums(order, n, rows, share, proj_sums, unit_sums, wide_sums):
    width = n * rows
    quarter = width // 4
    if rows % 128 or share % 128:
        groups = jnp.arange(4, dtype=jnp.int32) ^ order[n]
        proj = jnp.concatenate(proj_sums)[groups]
        units = jnp.concatenate(unit_sums)[groups].reshape(4, n, share)
        flat = [proj[:, :, :quarter].reshape(width), proj[:, :, 2 * quarter :].reshape(width)]
        two, one = wide_sums
        flat += [two[0], one[0], one[1], two[3], two[1], two[2]]
        flat = [v.reshape(n, 1, rows) for v in flat]
        stacked = [jnp.pad(v, ((0, 0), (0, 0), (0, 128 - rows))) for v in flat]
        stacked.append(jnp.pad(units.transpose(1, 0, 2), ((0, 0), (0, 4), (0, 128 - share))))
        return jnp.concatenate(stacked, axis=1)[order[:n]]

    def kernel(order_ref, proj_a, proj_b, unit_a, unit_b, two_ref, one_ref, out_ref, proj, units):
        proj[:2], proj[2:] = proj_a[...], proj_b[...]
        units[:2], units[2:] = unit_a[...], unit_b[...]
        q = order_ref[n]
        per = n // 4
        for r in range(n):
            s = order_ref[r]
            j = (s // per) ^ q
            at = tile(s, rows)
            inside = pl.multiple_of((s % per) * rows, rows)
            out_ref[r, 0:1] = proj[j, :, pl.ds(inside, rows)]
            out_ref[r, 1:2] = proj[j, :, pl.ds(2 * quarter + inside, rows)]
            for k, (ref, row) in enumerate(
                ((two_ref, 0), (one_ref, 0), (one_ref, 1), (two_ref, 3), (two_ref, 1), (two_ref, 2))
            ):
                out_ref[r, 2 + k : 3 + k] = ref[row, :, at]
            for g in range(4):
                out_ref[r, 8 + g : 9 + g] = units[q ^ g, :, tile(s, share)]
            out_ref[r, 12:] = jnp.zeros((4, rows), full)

    sums_two, sums_one = wide_sums
    return call(
        kernel,
        "pack_sums",
        (order, *proj_sums, *unit_sums, sums_two, sums_one),
        [SCALARS] + [ON_CHIP] * 6,
        [((n, 16, rows), full)],
        [ON_CHIP],
        [pltpu.VMEM((4, 1, 3 * quarter), full), pltpu.VMEM((4, 1, width), full)],
    )[0]


def table(codes, width):
    ratio = 0.3 * jnp.exp(codes.astype(full) * (math.log(10.0 / 0.3) / (NSCALE - 1)))
    quarter = width // 4
    omega = jnp.exp(jnp.arange(quarter).astype(full) * (-math.log(10000.0) / quarter))
    steps = jnp.arange(GRID, dtype=jnp.int32).astype(full)
    angle = ratio[:, None, None] * steps[None, :, None] * omega[None, None, :]
    return jnp.concatenate([jnp.sin(angle), jnp.cos(angle)], axis=-1)


def local(
    tokens,
    scale_codes,
    w_qkv,
    b_q,
    b_v,
    w_out,
    b_out,
    gain_one,
    shift_one,
    w_fc1,
    b_fc1,
    w_fc2,
    b_fc2,
    gain_two,
    shift_two,
    cotangent,
):
    n = lax.axis_size("fsdp")
    q = lax.axis_index("dp")
    f = lax.axis_index("fsdp")
    row_count, width = tokens.shape
    rows = width // n
    ff = b_fc1.shape[0] * n
    ffq = ff // n // 4
    hidden = n * ffq
    quarter = width // 4
    n_img = scale_codes.shape[0]
    patches = row_count // n_img
    padded = -(-patches // 16) * 16
    factor = 1.0 / math.sqrt(width // HEADS)
    seq = Order(q)
    bits = list(reversed(range(n.bit_length() - 1)))
    near = min(1, len(bits) - 1)
    shard_order = jnp.asarray(masks(bits), jnp.int32) ^ f
    group_order = jnp.arange(4, dtype=jnp.int32) ^ q
    order = jnp.concatenate([shard_order, q[None]])

    def last_three(chain):
        while len(chain.bits) > 3:
            chain.launch()
            seq.land((), chain)
            chain.join()
        return chain

    small = [b_q, b_v, b_out, gain_one, shift_one, b_fc2, gain_two, shift_two, b_fc1]
    qkv = last_three(Gather(seq, first_payload(q, w_qkv, small), n, bits))
    qkv.launch()
    rest_own, two_own = payloads([seq.at(q), q ^ 2], w_fc1, w_fc2)
    rest_own, two_own = seq.land((rest_own, two_own), qkv)
    rest = Sent(lax.all_gather(rest_own, "fsdp", axis=0, tiled=False))
    two = Sent(lax.all_gather(two_own, "fsdp", axis=0, tiled=False))
    out_own = [lax.dynamic_slice(w_out, (0, g * quarter), (rows, quarter)) for g in (q, q ^ 2)]
    out = last_three(Gather(seq, jnp.concatenate(out_own, axis=1).astype(half), n, bits))

    def spread_rows(value):
        split = value.reshape(n_img, patches, width)
        return jnp.pad(split, ((0, 0), (0, padded - patches), (0, 0)))

    def compact(value):
        return value.reshape(n_img, padded, width)[:, :patches].reshape(row_count, width)

    qkv.join()
    qkv.launch()
    spread_tokens = seq.land(spread_rows(seq.at(tokens)), qkv)
    qkv_near = qkv.join()
    qkv.launch()
    near_b, near_c = Sent(core_swap(qkv.held)), Sent(x_swap(qkv.held))
    out.launch()
    places = table(scale_codes, width)
    row_place = jnp.broadcast_to(places[:, :, None], (n_img, GRID, GRID, width // 2))
    col_place = jnp.broadcast_to(places[:, None], (n_img, GRID, GRID, width // 2))
    place = jnp.concatenate([row_place, col_place], axis=-1).reshape(n_img, patches, width)
    place = jnp.pad(place, ((0, 0), (0, padded - patches), (0, 0)))
    x_zero = (seq.at(spread_tokens).astype(full) + place).reshape(-1, width)
    x_zero = seq.land(x_zero, qkv, near_b, out)
    qkv_far = seq.at(qkv.got)
    far_b, far_c = Sent(core_swap(qkv_far)), Sent(x_swap(qkv_far))
    out.join()
    out.launch()
    vectors, bias_fc1, bias_qkv = unpack_vectors(seq.at(order), (qkv_near, qkv_far), n, rows, ffq)
    _, _, full_bout, gain_one_f, shift_one_f, full_bfc2, gain_two_f, shift_two_f = vectors
    normed_one = layer_norm(x_zero, gain_one_f, shift_one_f).astype(half)
    normed_one = seq.land(normed_one, far_b)

    first = attention_forward(
        seq.at(order), normed_one, bias_qkv[:2], ((qkv_near, qkv_far), (near_b.value, far_b.value)),
        n_img, patches, factor,
    )
    first = (seq.land(first[0], near_c, far_c, out), *first[1:])
    near_c, far_c = seq.at((near_c.value, far_c.value))
    near_d, far_d = Sent(core_swap(near_c)), Sent(core_swap(far_c))
    out.join()
    out.launch()
    cot = seq.land(spread_rows(cotangent).reshape(-1, width), near_d, far_d)
    second = attention_forward(
        seq.at(order), normed_one, bias_qkv[2:], ((near_c, far_c), (near_d.value, far_d.value)),
        n_img, patches, factor,
    )
    second = (seq.land(second[0], out), *second[1:])
    out_a = seq.at(out.join())
    out_b = Sent(core_swap(out_a))
    seq.land((), out_b)
    outs = (out_a, out_b.value)
    qkv_parts = (
        (qkv_near, qkv_far), (near_b.value, far_b.value), (near_c, far_c), (near_d.value, far_d.value)
    )
    qkvs = (*first[:2], *second[:2])
    mixed = (*first[2:4], *second[2:4])
    lses = (*first[4:], *second[4:])
    after_attn, normed_two = attention_out(
        seq.at(order), x_zero, mixed, outs, full_bout, gain_two_f, shift_two_f
    )
    normed_two = seq.land(normed_two, rest)
    rest_a = seq.at(rest.value)
    rest_b = Sent(core_swap(rest_a))
    up_c = Sent(x_swap(seq.at(rest_a[:, :, :hidden])))
    seq.land((), rest_b)

    up_g1, down_g1, g_bias_1, back_sum, out_sum = mlp(
        seq.at(order), normed_two, cot, bias_fc1[1], rest_b.value, rest_b.value, hidden
    )
    up_g0, down_g0, g_bias_0, back_sum, out_sum = mlp(
        order, normed_two, cot, bias_fc1[0], rest_a, rest_a, hidden, (out_sum, back_sum)
    )
    up_g0 = seq.land(up_g0, up_c, two)
    up_g1 = seq.at(up_g1)
    up_got = Sent(core_swap(up_g1))
    down_g1 = seq.at(down_g1)
    down_got = Sent(core_swap(down_g1))
    seq.land((), up_got)
    red_up = Reduce(seq, (up_g0, up_got.value), n)
    red_up.launch()
    seq.land((), down_got)
    red_down = Reduce(seq, (down_g0, down_got.value), n)
    red_down.launch(near)
    up_c, two = seq.at((up_c.value, two.value))
    up_d, two_d = Sent(core_swap(up_c)), Sent(core_swap(two))
    up_g2, down_g2, g_bias_2, back_sum, out_sum = mlp(
        seq.at(order), normed_two, cot, bias_fc1[2], up_c, two, 0, (out_sum, back_sum)
    )
    up_g2 = seq.land(up_g2, up_d, two_d, red_up, red_down)
    red_up.launch()
    red_down.launch()
    up_g3, down_g3, g_bias_3, grad_two_in, block = mlp(
        seq.at(order), normed_two, cot, bias_fc1[3], up_d.value, two_d.value, 0,
        (out_sum, back_sum), (after_attn, full_bfc2),
    )
    up_g3 = seq.land(up_g3, red_up, red_down)
    up_got = Sent(core_swap(up_g3))
    down_g3 = seq.at(down_g3)
    down_got = Sent(core_swap(down_g3))
    red_up.launch()
    red_down.launch()
    seq.land((), up_got)
    two_up = Reduce(seq, (up_g2, up_got.value), n)
    two_up.launch()
    seq.land((), down_got)
    two_down = Reduce(seq, (down_g2, down_got.value), n)
    two_down.launch(near)

    after_grad, mg0, mg1, mg2, mg3, g_out, sums_two = attention_out_back(
        seq.at(order), grad_two_in, after_attn, cot, gain_two_f, mixed, outs
    )
    mg2 = seq.at(mg2)
    g_w2, g_w3, proj2, proj3, sums_b = attention_back(
        seq.at(order), normed_one, qkvs[2:], lses[2:], (mg2, mg3), g_out, (2, 3), n_img, patches, factor, n
    )
    g_w3 = seq.land(g_w3, red_up, red_down, two_up, two_down)
    w_3 = Sent(core_swap(g_w3))
    two_up.launch()
    two_down.launch()
    seq.land((), w_3)
    middle = n // 2
    half_shape = (2,) * (len(bits) - 1)
    w_high = Sent(x_swap(seq.at(rounded_sum([g_w2[middle:], w_3.value[middle:]]))))
    g_w0, g_w1, proj0, proj1, sums_a = attention_back(
        seq.at(order), normed_one, qkvs[:2], lses[:2], (mg0, mg1), g_out, (0, 1), n_img, patches, factor, n
    )
    g_w1 = seq.land(g_w1, two_up, two_down, w_high)
    w_1 = Sent(core_swap(g_w1))
    two_up.launch()
    two_down.launch()
    seq.land((), w_1)
    red_w = Reduce(seq, (g_w0, w_1.value), n)
    red_w.launch(0, [w_high.value.reshape(half_shape + w_high.value.shape[1:])])
    w_low = Sent(x_swap(seq.at(rounded_sum([g_w2[:middle], w_3.value[:middle]]))))
    tokens_grad, sums_one = input_back(
        seq.at(order), x_zero, after_grad, gain_one_f, (proj0, proj1, proj2, proj3), qkv_parts
    )
    sums_one = seq.land(sums_one, two_up, two_down, red_w, w_low)
    red_w.terms = [*red_w.terms, w_low.value.reshape(half_shape + w_low.value.shape[1:])]
    while len(red_w.axes) > 2:
        red_w.launch()
        seq.land((), red_w)
    red_w.launch()
    packed = pack_sums(
        seq.at(order),
        n,
        rows,
        ffq,
        (sums_a, sums_b),
        (jnp.stack([g_bias_0, g_bias_1]), jnp.stack([g_bias_2, g_bias_3])),
        (sums_two, sums_one),
    )
    packed = seq.at(packed)
    peers = Sent([xor_swap(packed, "dp", 4, m) for m in (1, 2, 3)])
    crossing = jnp.stack([two_up.rest().piece(), two_down.rest().piece()])
    cross = Sent(x_swap(seq.at(crossing)))
    seq.land((), peers, red_w)
    if red_w.axes:
        red_w.launch()
    sums = Reduce(seq, (packed, *peers.value), n, full)
    while len(sums.axes) > 2:
        sums.launch()
        seq.land((), sums)
    if len(sums.axes) > 1:
        sums.launch()
        seq.land((), sums, cross)
    else:
        seq.land((), cross)
    owned = [rounded_sum([*red_up.rest().terms, cross.value[0]]), rounded_sum([*red_down.rest().terms, cross.value[1]])]
    mlp_spread = Spread(seq, jnp.stack(owned))
    sums.launch()
    seq.land((), sums, *([red_w] if len(bits) > 1 else []))
    w_spread = Spread(seq, red_w.piece())
    small_sums = sums.piece()
    block, tokens_grad = seq.at((block, tokens_grad))
    block_out, grad_tokens = seq.land((compact(block), compact(tokens_grad)), mlp_spread)
    mlp_spread.cross()
    small_sums = seq.land(small_sums, mlp_spread, w_spread)
    w_spread.cross()
    mlp_pieces = seq.at(mlp_spread.pieces)
    out_fc1, out_fc2 = finish_mlp(q, mlp_pieces, n)
    out_fc2 = seq.land(out_fc2, w_spread)
    out_qkv, out_out = finish_attention(seq.value, w_spread.pieces)
    small_out = [small_sums[k, :rows] for k in range(8)]
    out_bfc1 = small_sums[8:12, :ffq].reshape(-1)
    o_bq, o_bv, o_bout, o_gone, o_sone, o_bfc2, o_gtwo, o_stwo = small_out
    return (
        block_out,
        grad_tokens,
        out_qkv,
        o_bq,
        o_bv,
        out_out,
        o_bout,
        o_gone,
        o_sone,
        out_fc1,
        out_bfc1,
        out_fc2,
        o_bfc2,
        o_gtwo,
        o_stwo,
    )


def solution(mesh):
    rows_split = P(("dp", "fsdp"), None)
    matrix = P("fsdp", None)
    vector = P("fsdp")
    return jax.shard_map(
        local,
        mesh=mesh,
        in_specs=(
            rows_split, P(("dp", "fsdp")), matrix, vector, vector, matrix, vector, vector, vector,
            matrix, vector, matrix, vector, vector, vector, rows_split,
        ),
        out_specs=(
            rows_split, rows_split, matrix, vector, vector, matrix, vector, vector, vector,
            matrix, vector, matrix, vector, vector, vector,
        ),
        check_vma=False,
    )
```

```python
import math

import jax
import jax.numpy as jnp
from jax import lax
from jax.experimental import pallas as pl
from jax.experimental.pallas import tpu as pltpu
from jax.sharding import PartitionSpec as P

HEADS = 16
GRID = 14
NSCALE = 16
norm_eps = 1e-06
half = jnp.bfloat16
full = jnp.float32


def xor_swap(value, axis, size, mask):
    return lax.ppermute(value, axis, [(i, i ^ mask) for i in range(size)])


def core_swap(value):
    return xor_swap(value, "dp", 4, 1)


def x_swap(value):
    return xor_swap(value, "dp", 4, 2)


def masks(bits):
    found = [0]
    for bit in bits:
        found = found + [m | (1 << bit) for m in found]
    return found


class Order:
    def __init__(self, value):
        self.value = value

    def at(self, value):
        value, self.value = lax.optimization_barrier((value, self.value))
        return value

    def land(self, value, *sent):
        value, flights = self.at((value, [s.flight for s in sent]))
        for s, flight in zip(sent, flights, strict=True):
            s.accept(flight)
        return value


class Sent:
    def __init__(self, flight):
        self.flight = flight

    def accept(self, value):
        self.value = value


class Gather:
    def __init__(self, seq, piece, n, bits):
        self.seq, self.held, self.n, self.bits = seq, piece[None], n, list(bits)

    def launch(self):
        self.held = self.seq.at(self.held)
        self.flight = xor_swap(self.held, "fsdp", self.n, 1 << self.bits.pop(0))

    def accept(self, value):
        self.got = value

    def join(self):
        self.held = jnp.concatenate([self.held, self.got])
        return self.held


def rounded_sum(terms, kind=half):
    return sum(t.astype(full) for t in terms).astype(kind)


class Reduce:
    def __init__(self, seq, terms, n, kind=half):
        self.kind = kind
        self.seq, self.n, self.axes = seq, n, list(range(n.bit_length() - 1))
        self.terms = [t.reshape((2,) * len(self.axes) + t.shape[1:]) for t in terms]

    def launch(self, bit=None, more=()):
        bit = self.axes[0] if bit is None else bit
        axis = self.axes.index(bit)
        self.axes.pop(axis)
        low, high = [
            [lax.index_in_dim(t, side, axis, keepdims=False) for t in self.terms] for side in (0, 1)
        ]
        self.terms = low
        self.flight = xor_swap(self.seq.at(rounded_sum([*high, *more], self.kind)), "fsdp", self.n, 1 << bit)

    def accept(self, value):
        self.terms = [*self.terms, value]

    def rest(self):
        while self.axes:
            self.launch()
            self.seq.land((), self)
        return self

    def piece(self):
        return rounded_sum(self.terms, self.kind)


class Spread:
    def __init__(self, seq, piece):
        self.seq, self.pieces = seq, [seq.at(piece)]
        self.flight = [core_swap(self.pieces[0]), x_swap(self.pieces[0])]

    def cross(self):
        self.flight = [core_swap(self.seq.at(self.pieces[2]))]

    def accept(self, value):
        self.pieces += value


ANYWHERE = pl.BlockSpec(memory_space=pl.ANY)
ON_CHIP = pl.BlockSpec(memory_space=pltpu.VMEM)
SCALARS = pl.BlockSpec(memory_space=pltpu.SMEM)


def dot(left, right, dim_left, dim_right):
    return lax.dot_general(
        left, right, (((dim_left,), (dim_right,)), ((), ())), preferred_element_type=full
    )


def call(kernel, name, operands, in_specs, outs, out_specs, scratch):
    return pl.pallas_call(
        kernel,
        out_shape=[jax.ShapeDtypeStruct(shape, kind) for shape, kind in outs],
        in_specs=in_specs,
        out_specs=out_specs,
        scratch_shapes=scratch,
        compiler_params=pltpu.CompilerParams(vmem_limit_bytes=58 * 2**20),
        name=name,
    )(*operands)


def loop(count, body, unroll=1):
    def step(i, carry):
        body(i)
        return carry

    lax.fori_loop(0, count, step, 0, unroll=unroll)


def tile(i, size):
    return pl.ds(pl.multiple_of(i * size, size), size)


def bring(src, dst, sem):
    pltpu.make_async_copy(src, dst, sem).start()


def arrived(dst, sem):
    pltpu.make_async_copy(dst, dst, sem).wait()


def fetch(parts, order_ref, place, sem):
    base = 0
    for part in parts:

        def start(r, part=part, base=base):
            shard = r if order_ref is None else order_ref[base + r]
            pltpu.make_async_copy(part.at[r], place(shard), sem).start()

        loop(part.shape[0], start)
        base += part.shape[0]


def head_rows(s, q, n, rows, quarter):
    per = n // 4
    return pl.multiple_of(((s // per) ^ q) * quarter + (s % per) * rows, rows)


def pair_scores(q2, k2):
    first = lax.broadcasted_iota(jnp.int32, q2.shape, 1) < q2.shape[1] // 2
    both = apart(q2, first)
    return both, dot(k2, both, 1, 1), first


def apart(value, first):
    zero = jnp.zeros_like(value)
    return jnp.concatenate([jnp.where(first, value, zero), jnp.where(first, zero, value)])


def attention_forward(order, normed, bias, weights, n_img, patches, factor):
    groups, n_parts = len(weights), len(weights[0])
    wide = weights[0][0].shape[2]
    count, width = normed.shape
    rows = width // sum(part.shape[0] for part in weights[0])
    padded = count // n_img
    quarter = wide // 3

    def kernel(order_ref, normed_ref, bias_ref, *refs):
        w_refs, refs = refs[: groups * n_parts], refs[groups * n_parts :]
        qkv_refs, mixed_refs, refs = refs[:groups], refs[groups : 2 * groups], refs[2 * groups :]
        lse_refs, (w_held, sems) = refs[:groups], refs[groups:]
        for g in range(groups):
            fetch(
                [w.at[:, pl.ds(0, rows)] for w in w_refs[g * n_parts : (g + 1) * n_parts]],
                order_ref,
                lambda s, g=g: w_held.at[g, pl.ds(pl.multiple_of(s * rows, rows), rows)],
                sems.at[g],
            )
        for g in range(groups):
            pltpu.make_async_copy(w_held.at[g], w_held.at[g], sems.at[g]).wait()

            def project(t, g=g):
                at = tile(t, quarter)
                product = dot(normed_ref[...], w_held[g, :, at], 1, 0)
                qkv_refs[g][:, at] = (product + bias_ref[g, :, at]).astype(half)

            loop(3, project)

            def attend(i, g=g):
                at = tile(i // 2, padded)
                lanes = [pl.ds(pl.multiple_of(t * quarter + (i % 2) * 128, 128), 128) for t in range(3)]
                q2 = qkv_refs[g][at, lanes[0]] * factor
                k2 = qkv_refs[g][at, lanes[1]]
                v2 = qkv_refs[g][at, lanes[2]]
                _, scores, first = pair_scores(q2, k2)
                key = lax.broadcasted_iota(jnp.int32, scores.shape, 0)
                scores = jnp.where(key < patches, scores, -1e30)
                top = jnp.max(scores, axis=0, keepdims=True)
                raised = jnp.exp(scores - top)
                total = jnp.sum(raised, axis=0, keepdims=True)
                lse_refs[g][i] = top + jnp.log(total)
                out = dot((raised * (1.0 / total)).astype(half), v2, 0, 0)
                mixed_refs[g][at, lanes[0]] = jnp.where(first, out[:padded], out[padded:]).astype(half)

            loop(2 * n_img, attend, 2 * n_img)

    return call(
        kernel,
        "attention_forward",
        (order, normed, bias, *(part for w in weights for part in w)),
        [SCALARS, ON_CHIP, ON_CHIP] + [ANYWHERE] * (groups * n_parts),
        [((count, wide), half)] * groups
        + [((count, quarter), half)] * groups
        + [((2 * n_img, 1, 2 * padded), full)] * groups,
        [ON_CHIP] * (3 * groups),
        [pltpu.VMEM((groups, width, wide), half), pltpu.SemaphoreType.DMA((groups,))],
    )


def layer_norm(value, gain, shift):
    center = jnp.mean(value, axis=-1, keepdims=True)
    offset = value - center
    spread = jnp.mean(offset * offset, axis=-1, keepdims=True)
    return offset * lax.rsqrt(spread + norm_eps) * gain + shift


def layer_norm_back(value, grad, gain):
    center = jnp.mean(value, axis=-1, keepdims=True)
    offset = value - center
    scale = lax.rsqrt(jnp.mean(offset * offset, axis=-1, keepdims=True) + norm_eps)
    unit = offset * scale
    scaled = grad * gain
    inner = jnp.mean(scaled * unit, axis=-1, keepdims=True)
    return scale * (scaled - jnp.mean(scaled, axis=-1, keepdims=True) - unit * inner), grad * unit


def load_out(order_ref, out_refs, held, sem, n, rows, quarter):
    q = order_ref[n]
    for j in range(4):
        column = pl.multiple_of((q ^ j) * quarter, quarter)
        fetch(
            [out_refs[j % 2].at[:, :, pl.ds(j // 2 * quarter, quarter)]],
            order_ref,
            lambda s, column=column: held.at[
                pl.ds(head_rows(s, q, n, rows, quarter), rows), pl.ds(column, quarter)
            ],
            sem,
        )


CHUNK = 16
ROWS = 64


def attention_out(order, x_zero, mixed, outs, bias, gain, shift):
    count, width = x_zero.shape
    n, rows, _ = outs[0].shape
    quarter = mixed[0].shape[1]

    def kernel(order_ref, x_ref, bias_ref, gain_ref, shift_ref, *refs):
        mixed_refs, out_refs = refs[:4], refs[4:6]
        after_ref, normed_ref, held, x_held, sems = refs[6:]
        bring(x_ref, x_held, sems.at[1])
        load_out(order_ref, out_refs, held, sems.at[0], n, rows, quarter)
        together = jnp.concatenate([m[...] for m in mixed_refs], axis=1)
        pltpu.make_async_copy(held, held, sems.at[0]).wait()
        after_ref[...] = dot(together, held[...], 1, 0)
        arrived(x_held, sems.at[1])

        def finish(i):
            at = tile(i, CHUNK)
            after = x_held[at] + (after_ref[at] + bias_ref[...])
            after_ref[at] = after
            normed_ref[at] = layer_norm(after, gain_ref[...], shift_ref[...]).astype(half)

        loop(count // CHUNK, finish, 13)

    return call(
        kernel,
        "attention_out",
        (order, x_zero, bias, gain, shift, *mixed, *outs),
        [SCALARS, ANYWHERE] + [ON_CHIP] * 7 + [ANYWHERE] * 2,
        [((count, width), full), ((count, width), half)],
        [ON_CHIP] * 2,
        [
            pltpu.VMEM((width, width), half),
            pltpu.VMEM((count, width), full),
            pltpu.SemaphoreType.DMA((2,)),
        ],
    )


def mlp(order, normed, cot, bias, up_all, down_all, down_start, carried=None, ending=None):
    count, width = normed.shape
    n, rows, _ = up_all.shape
    hidden = bias.shape[1]
    share = hidden // n
    step = min(512, hidden)
    steps = hidden // step
    more = [*(carried or []), *(ending[:1] if ending else [])]
    last = list(ending[1:]) if ending else []

    def kernel(order_ref, bias_ref, *refs):
        last_refs, refs = refs[: len(last)], refs[len(last) :]
        normed_ref, cot_ref, up_ref, down_ref, refs = *refs[:4], refs[4:]
        more_refs, refs = refs[: len(more)], refs[len(more) :]
        g_up_ref, g_down_ref, g_bias_ref, back_ref, end_ref, refs = *refs[:5], refs[5:]
        held, refs = refs[: len(more)], refs[len(more) :]
        rows_in, cots, out, back, up, down, pre, act, act_half, pre_half, g_up, g_down, sems = refs
        bring(normed_ref, rows_in, sems.at[3])
        fetch(
            [up_ref.at[:, :, pl.ds(0, hidden)]],
            None,
            lambda s: up.at[pl.ds(pl.multiple_of(s * rows, rows), rows)],
            sems.at[0],
        )
        bring(cot_ref, cots, sems.at[4])
        fetch(
            [down_ref.at[:, :, pl.ds(down_start, width)]],
            None,
            lambda s: down.at[pl.ds(pl.multiple_of(s * share, share), share)],
            sems.at[1],
        )
        for k in range(len(more)):
            bring(more_refs[k], held[k], sems.at[5 + k])
        arrived(rows_in, sems.at[3])
        arrived(up, sems.at[0])
        for t in range(steps):
            at = pl.ds(t * step, step)
            pre[...] = dot(rows_in[...], up[:, at], 1, 0)
            if not t:
                arrived(cots, sems.at[4])
                arrived(down, sems.at[1])
            act[...] = dot(cots[...], down[at, :], 1, 1)

            def gelu(i, at=at):
                some = tile(i, 2 * CHUNK)
                x = pre[some] + bias_ref[:, at]
                below = 0.5 * (1.0 + lax.erf(x * math.sqrt(0.5)))
                density = jnp.exp(-0.5 * x * x) * (1.0 / math.sqrt(2.0 * math.pi))
                act_half[some] = (x * below).astype(half)
                pre_half[some] = (act[some] * (below + x * density)).astype(half)

            loop(count // CHUNK // 2, gelu)
            p = pre_half[...]
            h = act_half[...]
            more_back = dot(p, up[:, at], 1, 1)
            more_out = dot(h, down[at, :], 1, 0)
            if t:
                back[...] += more_back
                out[...] += more_out
            elif carried:
                arrived(held[0], sems.at[5])
                arrived(held[1], sems.at[6])
                out[...] = held[0][...] + more_out
                back[...] = held[1][...] + more_back
            else:
                out[...] = more_out
                back[...] = more_back
            if t == steps - 1:
                bring(back, back_ref, sems.at[3])
                if not ending:
                    bring(out, end_ref, sems.at[4])
            g_down[at, :] = dot(h, cots[...], 0, 0).astype(half)
            if t == steps - 1:

                def send_down(r):
                    at = pl.multiple_of(order_ref[r] * share, share)
                    bring(g_down.at[pl.ds(at, share)], g_down_ref.at[r], sems.at[2])

                loop(n, send_down)
            g_up[:, at] = dot(rows_in[...], p, 0, 0).astype(half)
            g_bias_ref[:, at] = jnp.sum(p.astype(full), axis=0, keepdims=True)

        def send_up(r):
            at = pl.multiple_of(order_ref[r] * rows, rows)
            bring(g_up.at[pl.ds(at, rows)], g_up_ref.at[r], sems.at[0])

        loop(n, send_up)
        if ending:
            arrived(held[2], sems.at[7])

            def finish(i):
                at = tile(i, 2 * CHUNK)
                end_ref[at] = (held[2][at] + (out[at] + last_refs[0][...])).astype(half)

            loop(count // CHUNK // 2, finish)
        else:
            arrived(end_ref, sems.at[4])
        arrived(back_ref, sems.at[3])
        arrived(g_down_ref, sems.at[2])
        arrived(g_up_ref, sems.at[0])

    sums = pltpu.VMEM((count, width), full)
    wide = pltpu.VMEM((count, width), half)
    square = pltpu.VMEM((width, hidden), half)
    return call(
        kernel,
        "mlp",
        (order, bias, *last, normed, cot, up_all, down_all, *more),
        [SCALARS] + [ON_CHIP] * (1 + len(last)) + [ANYWHERE] * (4 + len(more)),
        [
            ((n, rows, hidden), half),
            ((n, share, width), half),
            ((1, hidden), full),
            ((count, width), full),
            ((count, width), half if ending else full),
        ],
        [ANYWHERE, ANYWHERE, ON_CHIP, ANYWHERE, ON_CHIP if ending else ANYWHERE],
        [
            *([sums] * len(more)),
            wide,
            wide,
            sums,
            sums,
            square,
            pltpu.VMEM((hidden, width), half),
            pltpu.VMEM((count, step), full),
            pltpu.VMEM((count, step), full),
            pltpu.VMEM((count, step), half),
            pltpu.VMEM((count, step), half),
            square,
            pltpu.VMEM((hidden, width), half),
            pltpu.SemaphoreType.DMA((5 + len(more),)),
        ],
    )


def attention_out_back(order, grad, after, cot, gain, mixed, outs):
    count, width = after.shape
    n, rows, _ = outs[0].shape
    quarter = mixed[0].shape[1]

    def kernel(order_ref, grad_ref, after_ref, cot_ref, gain_ref, *refs):
        mixed_refs, out_refs, refs = refs[:4], refs[4:6], refs[6:]
        after_grad_ref, mixed_grad_refs, g_out_ref, sums_ref = refs[0], refs[1:5], refs[5], refs[6]
        held, branch, terms, grad, after, cot, mixes, sems = refs[7:]
        block = count // 4
        for k in range(4):
            some = pl.ds(k * block, block)
            bring(grad_ref.at[some], grad.at[some], sems.at[1 + k])
            bring(after_ref.at[some], after.at[some], sems.at[5 + k])
            bring(cot_ref.at[some], cot.at[some], sems.at[9 + k])
        load_out(order_ref, out_refs, held, sems.at[0], n, rows, quarter)
        for j in range(4):
            bring(mixed_refs[j], mixes.at[j], sems.at[13])
        terms[...] = jnp.zeros_like(terms)

        def fold(value):
            return jnp.sum(value.reshape(CHUNK // 8, 8, width), axis=0)

        def back(i, k):
            at = pl.ds(pl.multiple_of(k * block + i * CHUNK, CHUNK), CHUNK)
            incoming = grad[at]
            part, gain_terms = layer_norm_back(after[at], incoming, gain_ref[...])
            own = cot[at].astype(full)
            total = own + part
            after_grad_ref[at] = total
            rounded = total.astype(half)
            branch[at] = rounded
            terms[0] += fold(rounded.astype(full))
            terms[1] += fold(gain_terms)
            terms[2] += fold(incoming)
            terms[3] += fold(own)

        for k in range(4):
            some = pl.ds(k * block, block)
            arrived(grad.at[some], sems.at[1 + k])
            arrived(after.at[some], sems.at[5 + k])
            arrived(cot.at[some], sems.at[9 + k])
            loop(block // CHUNK, lambda i, k=k: back(i, k), 13)
        for k in range(4):
            sums_ref[k] = jnp.sum(terms[k], axis=0, keepdims=True)
        arrived(held, sems.at[0])
        arrived(mixes, sems.at[13])
        for j in range(4):
            mixed_grad_refs[j][...] = dot(branch[...], held[j * quarter : (j + 1) * quarter], 1, 1).astype(half)
            g_out_ref[j * quarter : (j + 1) * quarter] = dot(mixes[j], branch[...], 0, 0).astype(half)

    return call(
        kernel,
        "attention_out_back",
        (order, grad, after, cot, gain, *mixed, *outs),
        [SCALARS] + [ANYWHERE] * 3 + [ON_CHIP] + [ANYWHERE] * 6,
        [((count, width), full)]
        + [((count, quarter), half)] * 4
        + [((width, width), half), ((4, 1, width), full)],
        [ON_CHIP] * 7,
        [
            pltpu.VMEM((width, width), half),
            pltpu.VMEM((count, width), half),
            pltpu.VMEM((4, 8, width), full),
            pltpu.VMEM((count, width), full),
            pltpu.VMEM((count, width), full),
            pltpu.VMEM((count, width), half),
            pltpu.VMEM((4, count, quarter), half),
            pltpu.SemaphoreType.DMA((14,)),
        ],
    )


def attention_back(order, normed, qkvs, lses, mixed_grads, g_out, which, n_img, patches, factor, n):
    groups = len(qkvs)
    count, width = normed.shape
    wide = qkvs[0].shape[1]
    quarter = wide // 3
    padded = count // n_img
    rows = width // n

    def kernel(order_ref, normed_ref, g_out_ref, *refs):
        qkv_refs, mg_refs, refs = refs[:groups], refs[groups : 2 * groups], refs[2 * groups :]
        lse_refs, refs = refs[:groups], refs[groups:]
        g_w_refs, proj_refs, sums_ref = refs[:groups], refs[groups : 2 * groups], refs[2 * groups]
        g_w, normed_held, g_out_held, sems = refs[2 * groups + 1 :]
        q = order_ref[n]
        bring(g_out_ref, g_out_held, sems.at[groups])
        bring(normed_ref, normed_held, sems.at[groups + 1])
        for g in range(groups):

            def attend(i, g=g):
                at = tile(i // 2, padded)
                lanes = [pl.ds(pl.multiple_of(t * quarter + (i % 2) * 128, 128), 128) for t in range(3)]
                q2 = qkv_refs[g][at, lanes[0]] * factor
                k2 = qkv_refs[g][at, lanes[1]]
                v2 = qkv_refs[g][at, lanes[2]]
                both, scores, first = pair_scores(q2, k2)
                key = lax.broadcasted_iota(jnp.int32, scores.shape, 0)
                probs = jnp.where(key < patches, jnp.exp(scores - lse_refs[g][i]), 0.0)
                o_both = apart(mg_refs[g][at, lanes[0]], first)
                g_probs = dot(v2, o_both, 1, 1)
                weighted = jnp.sum(probs * g_probs, axis=0, keepdims=True)
                g_scores = (probs * (g_probs - weighted)).astype(half)
                g_query = dot(g_scores, k2, 0, 0)
                g_query = jnp.where(first, g_query[:padded], g_query[padded:]) * factor
                proj_refs[g][at, lanes[0]] = g_query.astype(half)
                proj_refs[g][at, lanes[1]] = dot(g_scores, both, 1, 0).astype(half)
                proj_refs[g][at, lanes[2]] = dot(probs.astype(half), o_both, 1, 0).astype(half)

            loop(2 * n_img, attend, 4)
            if not g:
                arrived(g_out_held, sems.at[groups])
                arrived(normed_held, sems.at[groups + 1])

            def send_out(r, g=g):
                at = head_rows(order_ref[r], q, n, rows, quarter)
                column = pl.multiple_of((q ^ which[g]) * quarter, quarter)
                pltpu.make_async_copy(
                    g_out_held.at[pl.ds(at, rows), pl.ds(column, quarter)],
                    g_w_refs[g].at[r, :, pl.ds(wide, quarter)],
                    sems.at[g],
                ).start()

            loop(n, send_out)

            def weigh(t, g=g):
                at = tile(t, quarter)
                some = proj_refs[g][:, at]
                g_w[g, :, at] = dot(normed_held[...], some, 0, 0).astype(half)
                sums_ref[g, :, at] = jnp.sum(some.astype(full), axis=0, keepdims=True)

            loop(3, weigh)

            def send(r, g=g):
                at = pl.multiple_of(order_ref[r] * rows, rows)
                pltpu.make_async_copy(
                    g_w.at[g, pl.ds(at, rows)], g_w_refs[g].at[r, :, pl.ds(0, wide)], sems.at[g]
                ).start()

            loop(n, send)
        for g in range(groups):
            pltpu.make_async_copy(g_w_refs[g], g_w_refs[g], sems.at[g]).wait()

    return call(
        kernel,
        "attention_back",
        (order, normed, g_out, *qkvs, *mixed_grads, *lses),
        [SCALARS] + [ANYWHERE] * 2 + [ON_CHIP] * (3 * groups),
        [((n, rows, wide + quarter), half)] * groups
        + [((count, wide), half)] * groups
        + [((groups, 1, wide), full)],
        [ANYWHERE] * groups + [ON_CHIP] * (groups + 1),
        [
            pltpu.VMEM((groups, width, wide), half),
            pltpu.VMEM((count, width), half),
            pltpu.VMEM((width, width), half),
            pltpu.SemaphoreType.DMA((groups + 2,)),
        ],
    )


def input_back(order, x_zero, after_grad, gain, projs, weights):
    count, width = x_zero.shape
    wide = weights[0][0].shape[2]
    rows = width // sum(part.shape[0] for part in weights[0])
    parts = [part for w in weights for part in w]
    n_parts = len(weights[0])

    def kernel(order_ref, x_ref, after_ref, gain_ref, *refs):
        proj_refs, w_refs = refs[:4], refs[4 : 4 + len(parts)]
        token_ref, sums_ref, held, terms, x_held, after_held, sems = refs[4 + len(parts) :]
        for j in range(4):
            fetch(
                [w.at[:, pl.ds(0, rows)] for w in w_refs[j * n_parts : (j + 1) * n_parts]],
                order_ref,
                lambda s, j=j: held.at[j, pl.ds(pl.multiple_of(s * rows, rows), rows)],
                sems.at[j],
            )
        bring(x_ref, x_held, sems.at[4])
        bring(after_ref, after_held, sems.at[5])
        for j in range(4):
            arrived(held.at[j], sems.at[j])
            product = dot(proj_refs[j][...], held[j], 1, 1)
            if j == 0:
                token_ref[...] = product
            else:
                token_ref[...] += product
        arrived(x_held, sems.at[4])
        arrived(after_held, sems.at[5])
        terms[...] = jnp.zeros_like(terms)

        def fold(value):
            return jnp.sum(value.reshape(ROWS // 8, 8, width), axis=0)

        def back(i):
            at = tile(i, ROWS)
            incoming = token_ref[at]
            part, gain_terms = layer_norm_back(x_held[at], incoming, gain_ref[...])
            token_ref[at] = after_held[at] + part
            terms[0] += fold(gain_terms)
            terms[1] += fold(incoming)

        loop(count // ROWS, back)
        for k in range(2):
            sums_ref[k] = jnp.sum(terms[k], axis=0, keepdims=True)

    return call(
        kernel,
        "input_back",
        (order, x_zero, after_grad, gain, *projs, *parts),
        [SCALARS] + [ANYWHERE] * 2 + [ON_CHIP] * 5 + [ANYWHERE] * len(parts),
        [((count, width), full), ((2, 1, width), full)],
        [ON_CHIP] * 2,
        [
            pltpu.VMEM((4, width, wide), half),
            pltpu.VMEM((2, 8, width), full),
            pltpu.VMEM((count, width), full),
            pltpu.VMEM((count, width), full),
            pltpu.SemaphoreType.DMA((6,)),
        ],
    )


def payloads(which, w_fc1, w_fc2):
    rows, ff = w_fc1.shape
    full_share, width = w_fc2.shape
    share = full_share // 4
    n = ff // full_share
    hidden = n * share
    own, across = which
    if share % 128:
        fc1 = [lax.dynamic_slice(w_fc1, (0, (4 * s + own) * share), (rows, share)) for s in range(n)]
        fc2 = [lax.dynamic_slice(w_fc2, (g * share, 0), (share, width)).astype(half) for g in which]
        rest = jnp.concatenate([*fc1, fc2[0].reshape(rows, -1).astype(full)], axis=1)
        return rest.astype(half), fc2[1]

    def kernel(which_ref, fc1_ref, fc2_ref, rest_ref, two_ref):
        for s in range(n):
            at = pl.ds(pl.multiple_of((4 * s + which_ref[0]) * share, share), share)
            rest_ref[:, s * share : (s + 1) * share] = fc1_ref[:, at].astype(half)
        rest_ref[:, hidden : hidden + width] = fc2_ref[tile(which_ref[0], share), :].astype(half)
        two_ref[...] = fc2_ref[tile(which_ref[1], share), :].astype(half)

    return call(
        kernel,
        "payloads",
        (jnp.stack(which), w_fc1, w_fc2),
        [SCALARS] + [ON_CHIP] * 2,
        [((rows, hidden + width), half), ((share, width), half)],
        [ON_CHIP] * 2,
        [],
    )


def natural_quarters(q, pieces):
    once = [jnp.where((q & 1) == 1, pieces[i ^ 1], pieces[i]) for i in range(4)]
    return [jnp.where(q >= 2, once[i ^ 2], once[i]) for i in range(4)]


def finish_mlp(q, pieces, n):
    _, rows, width = pieces[0].shape
    share = width // n
    if share % 128:
        pieces = natural_quarters(q, pieces)
        fc1 = jnp.stack([p[0].reshape(rows, n, share) for p in pieces], axis=2).reshape(rows, 4 * width)
        return fc1.astype(full), jnp.concatenate([p[1] for p in pieces]).astype(full)

    def kernel(q_ref, *refs):
        fc1_ref, fc2_ref = refs[4:]
        for j in range(4):
            g = q_ref[0] ^ j
            for s in range(n):
                at = pl.ds(pl.multiple_of((4 * s + g) * share, share), share)
                fc1_ref[:, at] = refs[j][0, :, s * share : (s + 1) * share].astype(full)
            fc2_ref[tile(g, rows), :] = refs[j][1].astype(full)

    return call(
        kernel,
        "finish_mlp",
        (q[None], *pieces),
        [SCALARS] + [ON_CHIP] * 4,
        [((rows, 4 * width), full), ((4 * rows, width), full)],
        [ON_CHIP] * 2,
        [],
    )


def finish_attention(q, pieces):
    rows, width = pieces[0].shape
    quarter = width // 4

    def kernel(q_ref, *refs):
        qkv_ref, out_ref = refs[4:]
        for j in range(4):
            g = q_ref[0] ^ j
            for t in range(3):
                at = pl.ds(pl.multiple_of(t * width + g * quarter, quarter), quarter)
                qkv_ref[:, at] = refs[j][:, t * quarter : (t + 1) * quarter].astype(full)
            out_ref[:, tile(g, quarter)] = refs[j][:, 3 * quarter :].astype(full)

    return call(
        kernel,
        "finish_attention",
        (q[None], *pieces),
        [SCALARS] + [ON_CHIP] * 4,
        [((rows, 3 * width), full), ((rows, width), full)],
        [ON_CHIP] * 2,
        [],
    )


BELOW = 16


def first_payload(q, w_qkv, vectors):
    rows, columns = w_qkv.shape
    width = columns // 3
    quarter = width // 4
    wide = 3 * quarter

    def kernel(q_ref, w_ref, *refs):
        out_ref, held, low, sem = refs[len(vectors) :]
        for t in range(3):
            at = pl.multiple_of(t * width + q_ref[0] * quarter, quarter)
            pltpu.make_async_copy(
                w_ref.at[:, pl.ds(at, quarter)], held.at[:, pl.ds(t * quarter, quarter)], sem.at[0]
            ).start()
        low[...] = jnp.zeros_like(low)
        for k, vector in enumerate(refs[: len(vectors)]):
            low[k : k + 1, : vector.shape[1]] = vector[...]
        out_ref[rows:] = low[...].astype(half)
        pltpu.make_async_copy(held, held, sem.at[0]).wait()
        out_ref[:rows] = held[...].astype(half)

    return call(
        kernel,
        "first_payload",
        (q[None], w_qkv, *(v[None] for v in vectors)),
        [SCALARS, ANYWHERE] + [ON_CHIP] * len(vectors),
        [((rows + BELOW, wide), half)],
        [ON_CHIP],
        [pltpu.VMEM((rows, wide), full), pltpu.VMEM((BELOW, wide), full), pltpu.SemaphoreType.DMA((1,))],
    )[0]


def unpack_vectors(order, parts, n, rows, share):
    width = n * rows
    quarter = width // 4
    if rows % 128 or share % 128:
        q = order[n]
        held = jnp.concatenate([p[:, rows:] for p in parts]).astype(full)
        held = held[jnp.zeros((n,), jnp.int32).at[order[:n]].set(jnp.arange(n, dtype=jnp.int32))]
        groups = jnp.arange(4, dtype=jnp.int32) ^ q
        vectors = jnp.stack([held[:, k, :rows].reshape(1, width) for k in range(8)])
        units = held[:, 8, : 4 * share].reshape(n, 4, share).transpose(1, 0, 2)[groups]
        ends = [vectors[k].reshape(4, 1, quarter)[groups] for k in range(2)]
        return vectors, units.reshape(4, 1, width), jnp.concatenate([ends[0], 0 * ends[0], ends[1]], axis=2)

    def kernel(order_ref, *refs):
        part_refs, (vector_ref, fc1_ref, qkv_ref, held, wider, sem) = refs[: len(parts)], refs[len(parts) :]
        base = 0
        for part in part_refs:
            size = part.shape[0]
            pltpu.make_async_copy(part.at[:, pl.ds(rows, BELOW)], held.at[pl.ds(base, size)], sem.at[0]).start()
            base += size
        pltpu.make_async_copy(held, held, sem.at[0]).wait()
        wider[...] = held[...].astype(full)
        q = order_ref[n]
        for r in range(n):
            at = tile(order_ref[r], rows)
            for k in range(8):
                vector_ref[k, :, at] = wider[r, k : k + 1, :rows]
            for j in range(4):
                fc1_ref[j, :, tile(order_ref[r], share)] = wider[r, 8:9, tile(q ^ j, share)]
        for j in range(4):
            at = tile(q ^ j, quarter)
            qkv_ref[j, :, :quarter] = vector_ref[0, :, at]
            qkv_ref[j, :, quarter : 2 * quarter] = jnp.zeros((1, quarter), full)
            qkv_ref[j, :, 2 * quarter :] = vector_ref[1, :, at]

    return call(
        kernel,
        "unpack_vectors",
        (order, *parts),
        [SCALARS] + [ANYWHERE] * len(parts),
        [((8, 1, width), full), ((4, 1, width), full), ((4, 1, 3 * quarter), full)],
        [ON_CHIP] * 3,
        [
            pltpu.VMEM((n, BELOW, 3 * quarter), half),
            pltpu.VMEM((n, BELOW, 3 * quarter), full),
            pltpu.SemaphoreType.DMA((1,)),
        ],
    )


def pack_sums(order, n, rows, share, proj_sums, unit_sums, wide_sums):
    width = n * rows
    quarter = width // 4
    if rows % 128 or share % 128:
        groups = jnp.arange(4, dtype=jnp.int32) ^ order[n]
        proj = jnp.concatenate(proj_sums)[groups]
        units = jnp.concatenate(unit_sums)[groups].reshape(4, n, share)
        flat = [proj[:, :, :quarter].reshape(width), proj[:, :, 2 * quarter :].reshape(width)]
        two, one = wide_sums
        flat += [two[0], one[0], one[1], two[3], two[1], two[2]]
        flat = [v.reshape(n, 1, rows) for v in flat]
        stacked = [jnp.pad(v, ((0, 0), (0, 0), (0, 128 - rows))) for v in flat]
        stacked.append(jnp.pad(units.transpose(1, 0, 2), ((0, 0), (0, 4), (0, 128 - share))))
        return jnp.concatenate(stacked, axis=1)[order[:n]]

    def kernel(order_ref, proj_a, proj_b, unit_a, unit_b, two_ref, one_ref, out_ref, proj, units):
        proj[:2], proj[2:] = proj_a[...], proj_b[...]
        units[:2], units[2:] = unit_a[...], unit_b[...]
        q = order_ref[n]
        per = n // 4
        for r in range(n):
            s = order_ref[r]
            j = (s // per) ^ q
            at = tile(s, rows)
            inside = pl.multiple_of((s % per) * rows, rows)
            out_ref[r, 0:1] = proj[j, :, pl.ds(inside, rows)]
            out_ref[r, 1:2] = proj[j, :, pl.ds(2 * quarter + inside, rows)]
            for k, (ref, row) in enumerate(
                ((two_ref, 0), (one_ref, 0), (one_ref, 1), (two_ref, 3), (two_ref, 1), (two_ref, 2))
            ):
                out_ref[r, 2 + k : 3 + k] = ref[row, :, at]
            for g in range(4):
                out_ref[r, 8 + g : 9 + g] = units[q ^ g, :, tile(s, share)]
            out_ref[r, 12:] = jnp.zeros((4, rows), full)

    sums_two, sums_one = wide_sums
    return call(
        kernel,
        "pack_sums",
        (order, *proj_sums, *unit_sums, sums_two, sums_one),
        [SCALARS] + [ON_CHIP] * 6,
        [((n, 16, rows), full)],
        [ON_CHIP],
        [pltpu.VMEM((4, 1, 3 * quarter), full), pltpu.VMEM((4, 1, width), full)],
    )[0]


def table(codes, width):
    ratio = 0.3 * jnp.exp(codes.astype(full) * (math.log(10.0 / 0.3) / (NSCALE - 1)))
    quarter = width // 4
    omega = jnp.exp(jnp.arange(quarter).astype(full) * (-math.log(10000.0) / quarter))
    steps = jnp.arange(GRID, dtype=jnp.int32).astype(full)
    angle = ratio[:, None, None] * steps[None, :, None] * omega[None, None, :]
    return jnp.concatenate([jnp.sin(angle), jnp.cos(angle)], axis=-1)


def local(
    tokens,
    scale_codes,
    w_qkv,
    b_q,
    b_v,
    w_out,
    b_out,
    gain_one,
    shift_one,
    w_fc1,
    b_fc1,
    w_fc2,
    b_fc2,
    gain_two,
    shift_two,
    cotangent,
):
    n = lax.axis_size("fsdp")
    q = lax.axis_index("dp")
    f = lax.axis_index("fsdp")
    row_count, width = tokens.shape
    rows = width // n
    ff = b_fc1.shape[0] * n
    ffq = ff // n // 4
    hidden = n * ffq
    quarter = width // 4
    n_img = scale_codes.shape[0]
    patches = row_count // n_img
    padded = -(-patches // 16) * 16
    factor = 1.0 / math.sqrt(width // HEADS)
    seq = Order(q)
    bits = list(reversed(range(n.bit_length() - 1)))
    near = min(1, len(bits) - 1)
    shard_order = jnp.asarray(masks(bits), jnp.int32) ^ f
    group_order = jnp.arange(4, dtype=jnp.int32) ^ q
    order = jnp.concatenate([shard_order, q[None]])

    def last_three(chain):
        while len(chain.bits) > 3:
            chain.launch()
            seq.land((), chain)
            chain.join()
        return chain

    small = [b_q, b_v, b_out, gain_one, shift_one, b_fc2, gain_two, shift_two, b_fc1]
    qkv = last_three(Gather(seq, first_payload(q, w_qkv, small), n, bits))
    qkv.launch()
    rest_own, two_own = payloads([seq.at(q), q ^ 2], w_fc1, w_fc2)
    rest_own, two_own = seq.land((rest_own, two_own), qkv)
    rest = Sent(lax.all_gather(rest_own, "fsdp", axis=0, tiled=False))
    two = Sent(lax.all_gather(two_own, "fsdp", axis=0, tiled=False))
    out_own = [lax.dynamic_slice(w_out, (0, g * quarter), (rows, quarter)) for g in (q, q ^ 2)]
    out = last_three(Gather(seq, jnp.concatenate(out_own, axis=1).astype(half), n, bits))

    def spread_rows(value):
        split = value.reshape(n_img, patches, width)
        return jnp.pad(split, ((0, 0), (0, padded - patches), (0, 0)))

    def compact(value):
        return value.reshape(n_img, padded, width)[:, :patches].reshape(row_count, width)

    qkv.join()
    qkv.launch()
    spread_tokens = seq.land(spread_rows(seq.at(tokens)), qkv)
    qkv_near = qkv.join()
    qkv.launch()
    near_b, near_c = Sent(core_swap(qkv.held)), Sent(x_swap(qkv.held))
    out.launch()
    places = table(scale_codes, width)
    row_place = jnp.broadcast_to(places[:, :, None], (n_img, GRID, GRID, width // 2))
    col_place = jnp.broadcast_to(places[:, None], (n_img, GRID, GRID, width // 2))
    place = jnp.concatenate([row_place, col_place], axis=-1).reshape(n_img, patches, width)
    place = jnp.pad(place, ((0, 0), (0, padded - patches), (0, 0)))
    x_zero = (seq.at(spread_tokens).astype(full) + place).reshape(-1, width)
    x_zero = seq.land(x_zero, qkv, near_b, out)
    qkv_far = seq.at(qkv.got)
    far_b, far_c = Sent(core_swap(qkv_far)), Sent(x_swap(qkv_far))
    out.join()
    out.launch()
    vectors, bias_fc1, bias_qkv = unpack_vectors(seq.at(order), (qkv_near, qkv_far), n, rows, ffq)
    _, _, full_bout, gain_one_f, shift_one_f, full_bfc2, gain_two_f, shift_two_f = vectors
    normed_one = layer_norm(x_zero, gain_one_f, shift_one_f).astype(half)
    normed_one = seq.land(normed_one, far_b)

    first = attention_forward(
        seq.at(order), normed_one, bias_qkv[:2], ((qkv_near, qkv_far), (near_b.value, far_b.value)),
        n_img, patches, factor,
    )
    first = (seq.land(first[0], near_c, far_c, out), *first[1:])
    near_c, far_c = seq.at((near_c.value, far_c.value))
    near_d, far_d = Sent(core_swap(near_c)), Sent(core_swap(far_c))
    out.join()
    out.launch()
    cot = seq.land(spread_rows(cotangent).reshape(-1, width), near_d, far_d)
    second = attention_forward(
        seq.at(order), normed_one, bias_qkv[2:], ((near_c, far_c), (near_d.value, far_d.value)),
        n_img, patches, factor,
    )
    second = (seq.land(second[0], out, rest), *second[1:])
    out_a = seq.at(out.join())
    out_b = Sent(core_swap(out_a))
    seq.land((), out_b)
    rest_a = seq.at(rest.value)
    rest_b = Sent(core_swap(rest_a))
    up_c = Sent(x_swap(seq.at(rest_a[:, :, :hidden])))
    outs = (out_a, out_b.value)
    qkv_parts = (
        (qkv_near, qkv_far), (near_b.value, far_b.value), (near_c, far_c), (near_d.value, far_d.value)
    )
    qkvs = (*first[:2], *second[:2])
    mixed = (*first[2:4], *second[2:4])
    lses = (*first[4:], *second[4:])
    after_attn, normed_two = attention_out(
        seq.at(order), x_zero, mixed, outs, full_bout, gain_two_f, shift_two_f
    )
    normed_two = seq.land(normed_two, rest_b)

    up_g1, down_g1, g_bias_1, back_sum, out_sum = mlp(
        seq.at(order), normed_two, cot, bias_fc1[1], rest_b.value, rest_b.value, hidden
    )
    up_g0, down_g0, g_bias_0, back_sum, out_sum = mlp(
        order, normed_two, cot, bias_fc1[0], rest_a, rest_a, hidden, (out_sum, back_sum)
    )
    up_g0 = seq.land(up_g0, up_c, two)
    up_g1 = seq.at(up_g1)
    up_got = Sent(core_swap(up_g1))
    down_g1 = seq.at(down_g1)
    down_got = Sent(core_swap(down_g1))
    seq.land((), up_got)
    red_up = Reduce(seq, (up_g0, up_got.value), n)
    red_up.launch()
    seq.land((), down_got)
    red_down = Reduce(seq, (down_g0, down_got.value), n)
    red_down.launch(near)
    up_c, two = seq.at((up_c.value, two.value))
    up_d, two_d = Sent(core_swap(up_c)), Sent(core_swap(two))
    up_g2, down_g2, g_bias_2, back_sum, out_sum = mlp(
        seq.at(order), normed_two, cot, bias_fc1[2], up_c, two, 0, (out_sum, back_sum)
    )
    up_g2 = seq.land(up_g2, up_d, two_d, red_up, red_down)
    red_up.launch()
    red_down.launch()
    up_g3, down_g3, g_bias_3, grad_two_in, block = mlp(
        seq.at(order), normed_two, cot, bias_fc1[3], up_d.value, two_d.value, 0,
        (out_sum, back_sum), (after_attn, full_bfc2),
    )
    up_g3 = seq.land(up_g3, red_up, red_down)
    up_got = Sent(core_swap(up_g3))
    down_g3 = seq.at(down_g3)
    down_got = Sent(core_swap(down_g3))
    red_up.launch()
    red_down.launch()
    seq.land((), up_got)
    two_up = Reduce(seq, (up_g2, up_got.value), n)
    two_up.launch()
    seq.land((), down_got)
    two_down = Reduce(seq, (down_g2, down_got.value), n)
    two_down.launch(near)

    after_grad, mg0, mg1, mg2, mg3, g_out, sums_two = attention_out_back(
        seq.at(order), grad_two_in, after_attn, cot, gain_two_f, mixed, outs
    )
    mg2 = seq.at(mg2)
    g_w2, g_w3, proj2, proj3, sums_b = attention_back(
        seq.at(order), normed_one, qkvs[2:], lses[2:], (mg2, mg3), g_out, (2, 3), n_img, patches, factor, n
    )
    g_w3 = seq.land(g_w3, red_up, red_down, two_up, two_down)
    w_3 = Sent(core_swap(g_w3))
    two_up.launch()
    two_down.launch()
    seq.land((), w_3)
    middle = n // 2
    half_shape = (2,) * (len(bits) - 1)
    w_high = Sent(x_swap(seq.at(rounded_sum([g_w2[middle:], w_3.value[middle:]]))))
    g_w0, g_w1, proj0, proj1, sums_a = attention_back(
        seq.at(order), normed_one, qkvs[:2], lses[:2], (mg0, mg1), g_out, (0, 1), n_img, patches, factor, n
    )
    g_w1 = seq.land(g_w1, two_up, two_down, w_high)
    w_1 = Sent(core_swap(g_w1))
    two_up.launch()
    two_down.launch()
    seq.land((), w_1)
    red_w = Reduce(seq, (g_w0, w_1.value), n)
    red_w.launch(0, [w_high.value.reshape(half_shape + w_high.value.shape[1:])])
    w_low = Sent(x_swap(seq.at(rounded_sum([g_w2[:middle], w_3.value[:middle]]))))
    tokens_grad, sums_one = input_back(
        seq.at(order), x_zero, after_grad, gain_one_f, (proj0, proj1, proj2, proj3), qkv_parts
    )
    sums_one = seq.land(sums_one, two_up, two_down, red_w, w_low)
    red_w.terms = [*red_w.terms, w_low.value.reshape(half_shape + w_low.value.shape[1:])]
    while len(red_w.axes) > 2:
        red_w.launch()
        seq.land((), red_w)
    red_w.launch()
    packed = pack_sums(
        seq.at(order),
        n,
        rows,
        ffq,
        (sums_a, sums_b),
        (jnp.stack([g_bias_0, g_bias_1]), jnp.stack([g_bias_2, g_bias_3])),
        (sums_two, sums_one),
    )
    packed = seq.at(packed)
    peers = Sent([xor_swap(packed, "dp", 4, m) for m in (1, 2, 3)])
    crossing = jnp.stack([two_up.rest().piece(), two_down.rest().piece()])
    cross = Sent(x_swap(seq.at(crossing)))
    seq.land((), peers, red_w, cross)
    if red_w.axes:
        red_w.launch()
    owned = [rounded_sum([*red_up.rest().terms, cross.value[0]]), rounded_sum([*red_down.rest().terms, cross.value[1]])]
    mlp_spread = Spread(seq, jnp.stack(owned))
    sums = Reduce(seq, (packed, *peers.value), n, full)
    while len(sums.axes) > 1:
        sums.launch()
        if len(sums.axes) > 1:
            seq.land((), sums)
    seq.land((), *([sums, red_w] if len(bits) > 1 else []))
    w_spread = Spread(seq, red_w.piece())
    sums.launch()
    block, tokens_grad = seq.at((block, tokens_grad))
    block_out, grad_tokens = seq.land((compact(block), compact(tokens_grad)), sums, mlp_spread)
    mlp_spread.cross()
    small_sums = seq.land(sums.piece(), mlp_spread)
    mlp_pieces = seq.at(mlp_spread.pieces)
    out_fc1, out_fc2 = finish_mlp(q, mlp_pieces, n)
    out_fc2 = seq.land(out_fc2, w_spread)
    w_spread.cross()
    seq.land((), w_spread)
    out_qkv, out_out = finish_attention(seq.value, w_spread.pieces)
    small_out = [small_sums[k, :rows] for k in range(8)]
    out_bfc1 = small_sums[8:12, :ffq].reshape(-1)
    o_bq, o_bv, o_bout, o_gone, o_sone, o_bfc2, o_gtwo, o_stwo = small_out
    return (
        block_out,
        grad_tokens,
        out_qkv,
        o_bq,
        o_bv,
        out_out,
        o_bout,
        o_gone,
        o_sone,
        out_fc1,
        out_bfc1,
        out_fc2,
        o_bfc2,
        o_gtwo,
        o_stwo,
    )


def solution(mesh):
    rows_split = P(("dp", "fsdp"), None)
    matrix = P("fsdp", None)
    vector = P("fsdp")
    return jax.shard_map(
        local,
        mesh=mesh,
        in_specs=(
            rows_split, P(("dp", "fsdp")), matrix, vector, vector, matrix, vector, vector, vector,
            matrix, vector, matrix, vector, vector, vector, rows_split,
        ),
        out_specs=(
            rows_split, rows_split, matrix, vector, vector, matrix, vector, vector, vector,
            matrix, vector, matrix, vector, vector, vector,
        ),
        check_vma=False,
    )
```

```python
import math

import jax
import jax.numpy as jnp
from jax import lax
from jax.experimental import pallas as pl
from jax.experimental.pallas import tpu as pltpu
from jax.sharding import PartitionSpec as P

HEADS = 16
GRID = 14
NSCALE = 16
norm_eps = 1e-06
half = jnp.bfloat16
full = jnp.float32


def xor_swap(value, axis, size, mask):
    return lax.ppermute(value, axis, [(i, i ^ mask) for i in range(size)])


def core_swap(value):
    return xor_swap(value, "dp", 4, 1)


def x_swap(value):
    return xor_swap(value, "dp", 4, 2)


def masks(bits):
    found = [0]
    for bit in bits:
        found = found + [m | (1 << bit) for m in found]
    return found


class Order:
    def __init__(self, value):
        self.value = value

    def at(self, value):
        value, self.value = lax.optimization_barrier((value, self.value))
        return value

    def land(self, value, *sent):
        value, flights = self.at((value, [s.flight for s in sent]))
        for s, flight in zip(sent, flights, strict=True):
            s.accept(flight)
        return value


class Sent:
    def __init__(self, flight):
        self.flight = flight

    def accept(self, value):
        self.value = value


class Gather:
    def __init__(self, seq, piece, n, bits):
        self.seq, self.held, self.n, self.bits = seq, piece[None], n, list(bits)

    def launch(self):
        self.held = self.seq.at(self.held)
        self.flight = xor_swap(self.held, "fsdp", self.n, 1 << self.bits.pop(0))

    def accept(self, value):
        self.got = value

    def join(self):
        self.held = jnp.concatenate([self.held, self.got])
        return self.held


def rounded_sum(terms, kind=half):
    return sum(t.astype(full) for t in terms).astype(kind)


class Reduce:
    def __init__(self, seq, terms, n, kind=half):
        self.kind = kind
        self.seq, self.n, self.axes = seq, n, list(range(n.bit_length() - 1))
        self.terms = [t.reshape((2,) * len(self.axes) + t.shape[1:]) for t in terms]

    def launch(self, bit=None, more=()):
        bit = self.axes[0] if bit is None else bit
        axis = self.axes.index(bit)
        self.axes.pop(axis)
        low, high = [
            [lax.index_in_dim(t, side, axis, keepdims=False) for t in self.terms] for side in (0, 1)
        ]
        self.terms = low
        self.flight = xor_swap(self.seq.at(rounded_sum([*high, *more], self.kind)), "fsdp", self.n, 1 << bit)

    def accept(self, value):
        self.terms = [*self.terms, value]

    def rest(self):
        while self.axes:
            self.launch()
            self.seq.land((), self)
        return self

    def piece(self):
        return rounded_sum(self.terms, self.kind)


class Spread:
    def __init__(self, seq, piece):
        self.seq, self.pieces = seq, [seq.at(piece)]
        self.flight = [core_swap(self.pieces[0]), x_swap(self.pieces[0])]

    def cross(self):
        self.flight = [core_swap(self.seq.at(self.pieces[2]))]

    def accept(self, value):
        self.pieces += value


ANYWHERE = pl.BlockSpec(memory_space=pl.ANY)
ON_CHIP = pl.BlockSpec(memory_space=pltpu.VMEM)
SCALARS = pl.BlockSpec(memory_space=pltpu.SMEM)


def dot(left, right, dim_left, dim_right):
    return lax.dot_general(
        left, right, (((dim_left,), (dim_right,)), ((), ())), preferred_element_type=full
    )


def call(kernel, name, operands, in_specs, outs, out_specs, scratch):
    return pl.pallas_call(
        kernel,
        out_shape=[jax.ShapeDtypeStruct(shape, kind) for shape, kind in outs],
        in_specs=in_specs,
        out_specs=out_specs,
        scratch_shapes=scratch,
        compiler_params=pltpu.CompilerParams(vmem_limit_bytes=58 * 2**20),
        name=name,
    )(*operands)


def loop(count, body, unroll=1):
    def step(i, carry):
        body(i)
        return carry

    lax.fori_loop(0, count, step, 0, unroll=unroll)


def tile(i, size):
    return pl.ds(pl.multiple_of(i * size, size), size)


def bring(src, dst, sem):
    pltpu.make_async_copy(src, dst, sem).start()


def arrived(dst, sem):
    pltpu.make_async_copy(dst, dst, sem).wait()


def fetch(parts, order_ref, place, sem):
    base = 0
    for part in parts:

        def start(r, part=part, base=base):
            shard = r if order_ref is None else order_ref[base + r]
            pltpu.make_async_copy(part.at[r], place(shard), sem).start()

        loop(part.shape[0], start)
        base += part.shape[0]


def head_rows(s, q, n, rows, quarter):
    per = n // 4
    return pl.multiple_of(((s // per) ^ q) * quarter + (s % per) * rows, rows)


def pair_scores(q2, k2):
    first = lax.broadcasted_iota(jnp.int32, q2.shape, 1) < q2.shape[1] // 2
    both = apart(q2, first)
    return both, dot(k2, both, 1, 1), first


def apart(value, first):
    zero = jnp.zeros_like(value)
    return jnp.concatenate([jnp.where(first, value, zero), jnp.where(first, zero, value)])


def attention_forward(order, normed, bias, weights, n_img, patches, factor):
    groups, n_parts = len(weights), len(weights[0])
    wide = weights[0][0].shape[2]
    count, width = normed.shape
    rows = width // sum(part.shape[0] for part in weights[0])
    padded = count // n_img
    quarter = wide // 3

    def kernel(order_ref, normed_ref, bias_ref, *refs):
        w_refs, refs = refs[: groups * n_parts], refs[groups * n_parts :]
        qkv_refs, mixed_refs, refs = refs[:groups], refs[groups : 2 * groups], refs[2 * groups :]
        lse_refs, (w_held, sems) = refs[:groups], refs[groups:]
        for g in range(groups):
            fetch(
                [w.at[:, pl.ds(0, rows)] for w in w_refs[g * n_parts : (g + 1) * n_parts]],
                order_ref,
                lambda s, g=g: w_held.at[g, pl.ds(pl.multiple_of(s * rows, rows), rows)],
                sems.at[g],
            )
        for g in range(groups):
            pltpu.make_async_copy(w_held.at[g], w_held.at[g], sems.at[g]).wait()

            def project(t, g=g):
                at = tile(t, quarter)
                product = dot(normed_ref[...], w_held[g, :, at], 1, 0)
                qkv_refs[g][:, at] = (product + bias_ref[g, :, at]).astype(half)

            loop(3, project)

            def attend(i, g=g):
                at = tile(i // 2, padded)
                lanes = [pl.ds(pl.multiple_of(t * quarter + (i % 2) * 128, 128), 128) for t in range(3)]
                q2 = qkv_refs[g][at, lanes[0]] * factor
                k2 = qkv_refs[g][at, lanes[1]]
                v2 = qkv_refs[g][at, lanes[2]]
                _, scores, first = pair_scores(q2, k2)
                key = lax.broadcasted_iota(jnp.int32, scores.shape, 0)
                scores = jnp.where(key < patches, scores, -1e30)
                top = jnp.max(scores, axis=0, keepdims=True)
                raised = jnp.exp(scores - top)
                total = jnp.sum(raised, axis=0, keepdims=True)
                lse_refs[g][i] = top + jnp.log(total)
                out = dot((raised * (1.0 / total)).astype(half), v2, 0, 0)
                mixed_refs[g][at, lanes[0]] = jnp.where(first, out[:padded], out[padded:]).astype(half)

            loop(2 * n_img, attend, 2 * n_img)

    return call(
        kernel,
        "attention_forward",
        (order, normed, bias, *(part for w in weights for part in w)),
        [SCALARS, ON_CHIP, ON_CHIP] + [ANYWHERE] * (groups * n_parts),
        [((count, wide), half)] * groups
        + [((count, quarter), half)] * groups
        + [((2 * n_img, 1, 2 * padded), full)] * groups,
        [ON_CHIP] * (3 * groups),
        [pltpu.VMEM((groups, width, wide), half), pltpu.SemaphoreType.DMA((groups,))],
    )


def layer_norm(value, gain, shift):
    center = jnp.mean(value, axis=-1, keepdims=True)
    offset = value - center
    spread = jnp.mean(offset * offset, axis=-1, keepdims=True)
    return offset * lax.rsqrt(spread + norm_eps) * gain + shift


def layer_norm_back(value, grad, gain):
    center = jnp.mean(value, axis=-1, keepdims=True)
    offset = value - center
    scale = lax.rsqrt(jnp.mean(offset * offset, axis=-1, keepdims=True) + norm_eps)
    unit = offset * scale
    scaled = grad * gain
    inner = jnp.mean(scaled * unit, axis=-1, keepdims=True)
    return scale * (scaled - jnp.mean(scaled, axis=-1, keepdims=True) - unit * inner), grad * unit


def load_out(order_ref, out_refs, held, sem, n, rows, quarter):
    q = order_ref[n]
    for j in range(4):
        column = pl.multiple_of((q ^ j) * quarter, quarter)
        fetch(
            [out_refs[j % 2].at[:, :, pl.ds(j // 2 * quarter, quarter)]],
            order_ref,
            lambda s, column=column: held.at[
                pl.ds(head_rows(s, q, n, rows, quarter), rows), pl.ds(column, quarter)
            ],
            sem,
        )


CHUNK = 16
ROWS = 64


def attention_out(order, x_zero, mixed, outs, bias, gain, shift):
    count, width = x_zero.shape
    n, rows, _ = outs[0].shape
    quarter = mixed[0].shape[1]

    def kernel(order_ref, x_ref, bias_ref, gain_ref, shift_ref, *refs):
        mixed_refs, out_refs = refs[:4], refs[4:6]
        after_ref, normed_ref, held, x_held, sems = refs[6:]
        bring(x_ref, x_held, sems.at[1])
        load_out(order_ref, out_refs, held, sems.at[0], n, rows, quarter)
        together = jnp.concatenate([m[...] for m in mixed_refs], axis=1)
        pltpu.make_async_copy(held, held, sems.at[0]).wait()
        after_ref[...] = dot(together, held[...], 1, 0)
        arrived(x_held, sems.at[1])

        def finish(i):
            at = tile(i, CHUNK)
            after = x_held[at] + (after_ref[at] + bias_ref[...])
            after_ref[at] = after
            normed_ref[at] = layer_norm(after, gain_ref[...], shift_ref[...]).astype(half)

        loop(count // CHUNK, finish, 13)

    return call(
        kernel,
        "attention_out",
        (order, x_zero, bias, gain, shift, *mixed, *outs),
        [SCALARS, ANYWHERE] + [ON_CHIP] * 7 + [ANYWHERE] * 2,
        [((count, width), full), ((count, width), half)],
        [ON_CHIP] * 2,
        [
            pltpu.VMEM((width, width), half),
            pltpu.VMEM((count, width), full),
            pltpu.SemaphoreType.DMA((2,)),
        ],
    )


def mlp(order, normed, cot, bias, up_all, down_all, down_start, carried=None, ending=None):
    count, width = normed.shape
    n, rows, _ = up_all.shape
    hidden = bias.shape[1]
    share = hidden // n
    step = min(512, hidden)
    steps = hidden // step
    more = [*(carried or []), *(ending[:1] if ending else [])]
    last = list(ending[1:]) if ending else []

    def kernel(order_ref, bias_ref, *refs):
        last_refs, refs = refs[: len(last)], refs[len(last) :]
        normed_ref, cot_ref, up_ref, down_ref, refs = *refs[:4], refs[4:]
        more_refs, refs = refs[: len(more)], refs[len(more) :]
        g_up_ref, g_down_ref, g_bias_ref, back_ref, end_ref, refs = *refs[:5], refs[5:]
        held, refs = refs[: len(more)], refs[len(more) :]
        rows_in, cots, out, back, up, down, pre, act, act_half, pre_half, g_up, g_down, sems = refs
        bring(normed_ref, rows_in, sems.at[3])
        fetch(
            [up_ref.at[:, :, pl.ds(0, hidden)]],
            None,
            lambda s: up.at[pl.ds(pl.multiple_of(s * rows, rows), rows)],
            sems.at[0],
        )
        bring(cot_ref, cots, sems.at[4])
        fetch(
            [down_ref.at[:, :, pl.ds(down_start, width)]],
            None,
            lambda s: down.at[pl.ds(pl.multiple_of(s * share, share), share)],
            sems.at[1],
        )
        for k in range(len(more)):
            bring(more_refs[k], held[k], sems.at[5 + k])
        arrived(rows_in, sems.at[3])
        arrived(up, sems.at[0])
        for t in range(steps):
            at = pl.ds(t * step, step)
            pre[...] = dot(rows_in[...], up[:, at], 1, 0)
            if not t:
                arrived(cots, sems.at[4])
                arrived(down, sems.at[1])
            act[...] = dot(cots[...], down[at, :], 1, 1)

            def gelu(i, at=at):
                some = tile(i, 2 * CHUNK)
                x = pre[some] + bias_ref[:, at]
                below = 0.5 * (1.0 + lax.erf(x * math.sqrt(0.5)))
                density = jnp.exp(-0.5 * x * x) * (1.0 / math.sqrt(2.0 * math.pi))
                act_half[some] = (x * below).astype(half)
                pre_half[some] = (act[some] * (below + x * density)).astype(half)

            loop(count // CHUNK // 2, gelu)
            p = pre_half[...]
            h = act_half[...]
            more_back = dot(p, up[:, at], 1, 1)
            more_out = dot(h, down[at, :], 1, 0)
            if t:
                back[...] += more_back
                out[...] += more_out
            elif carried:
                arrived(held[0], sems.at[5])
                arrived(held[1], sems.at[6])
                out[...] = held[0][...] + more_out
                back[...] = held[1][...] + more_back
            else:
                out[...] = more_out
                back[...] = more_back
            if t == steps - 1:
                bring(back, back_ref, sems.at[3])
                if not ending:
                    bring(out, end_ref, sems.at[4])
            g_down[at, :] = dot(h, cots[...], 0, 0).astype(half)
            if t == steps - 1:

                def send_down(r):
                    at = pl.multiple_of(order_ref[r] * share, share)
                    bring(g_down.at[pl.ds(at, share)], g_down_ref.at[r], sems.at[2])

                loop(n, send_down)
            g_up[:, at] = dot(rows_in[...], p, 0, 0).astype(half)
            g_bias_ref[:, at] = jnp.sum(p.astype(full), axis=0, keepdims=True)

        def send_up(r):
            at = pl.multiple_of(order_ref[r] * rows, rows)
            bring(g_up.at[pl.ds(at, rows)], g_up_ref.at[r], sems.at[0])

        loop(n, send_up)
        if ending:
            arrived(held[2], sems.at[7])

            def finish(i):
                at = tile(i, 2 * CHUNK)
                end_ref[at] = (held[2][at] + (out[at] + last_refs[0][...])).astype(half)

            loop(count // CHUNK // 2, finish)
        else:
            arrived(end_ref, sems.at[4])
        arrived(back_ref, sems.at[3])
        arrived(g_down_ref, sems.at[2])
        arrived(g_up_ref, sems.at[0])

    sums = pltpu.VMEM((count, width), full)
    wide = pltpu.VMEM((count, width), half)
    square = pltpu.VMEM((width, hidden), half)
    return call(
        kernel,
        "mlp",
        (order, bias, *last, normed, cot, up_all, down_all, *more),
        [SCALARS] + [ON_CHIP] * (1 + len(last)) + [ANYWHERE] * (4 + len(more)),
        [
            ((n, rows, hidden), half),
            ((n, share, width), half),
            ((1, hidden), full),
            ((count, width), full),
            ((count, width), half if ending else full),
        ],
        [ANYWHERE, ANYWHERE, ON_CHIP, ANYWHERE, ON_CHIP if ending else ANYWHERE],
        [
            *([sums] * len(more)),
            wide,
            wide,
            sums,
            sums,
            square,
            pltpu.VMEM((hidden, width), half),
            pltpu.VMEM((count, step), full),
            pltpu.VMEM((count, step), full),
            pltpu.VMEM((count, step), half),
            pltpu.VMEM((count, step), half),
            square,
            pltpu.VMEM((hidden, width), half),
            pltpu.SemaphoreType.DMA((5 + len(more),)),
        ],
    )


def attention_out_back(order, grad, after, cot, gain, mixed, outs):
    count, width = after.shape
    n, rows, _ = outs[0].shape
    quarter = mixed[0].shape[1]

    def kernel(order_ref, grad_ref, after_ref, cot_ref, gain_ref, *refs):
        mixed_refs, out_refs, refs = refs[:4], refs[4:6], refs[6:]
        after_grad_ref, mixed_grad_refs, g_out_ref, sums_ref = refs[0], refs[1:5], refs[5], refs[6]
        held, branch, terms, grad, after, cot, mixes, sems = refs[7:]
        block = count // 4
        for k in range(4):
            some = pl.ds(k * block, block)
            bring(grad_ref.at[some], grad.at[some], sems.at[1 + k])
            bring(after_ref.at[some], after.at[some], sems.at[5 + k])
            bring(cot_ref.at[some], cot.at[some], sems.at[9 + k])
        load_out(order_ref, out_refs, held, sems.at[0], n, rows, quarter)
        for j in range(4):
            bring(mixed_refs[j], mixes.at[j], sems.at[13])
        terms[...] = jnp.zeros_like(terms)

        def fold(value):
            return jnp.sum(value.reshape(CHUNK // 8, 8, width), axis=0)

        def back(i, k):
            at = pl.ds(pl.multiple_of(k * block + i * CHUNK, CHUNK), CHUNK)
            incoming = grad[at]
            part, gain_terms = layer_norm_back(after[at], incoming, gain_ref[...])
            own = cot[at].astype(full)
            total = own + part
            after_grad_ref[at] = total
            rounded = total.astype(half)
            branch[at] = rounded
            terms[0] += fold(rounded.astype(full))
            terms[1] += fold(gain_terms)
            terms[2] += fold(incoming)
            terms[3] += fold(own)

        for k in range(4):
            some = pl.ds(k * block, block)
            arrived(grad.at[some], sems.at[1 + k])
            arrived(after.at[some], sems.at[5 + k])
            arrived(cot.at[some], sems.at[9 + k])
            loop(block // CHUNK, lambda i, k=k: back(i, k), 13)
        for k in range(4):
            sums_ref[k] = jnp.sum(terms[k], axis=0, keepdims=True)
        arrived(held, sems.at[0])
        arrived(mixes, sems.at[13])
        for j in range(4):
            mixed_grad_refs[j][...] = dot(branch[...], held[j * quarter : (j + 1) * quarter], 1, 1).astype(half)
            g_out_ref[j * quarter : (j + 1) * quarter] = dot(mixes[j], branch[...], 0, 0).astype(half)

    return call(
        kernel,
        "attention_out_back",
        (order, grad, after, cot, gain, *mixed, *outs),
        [SCALARS] + [ANYWHERE] * 3 + [ON_CHIP] + [ANYWHERE] * 6,
        [((count, width), full)]
        + [((count, quarter), half)] * 4
        + [((width, width), half), ((4, 1, width), full)],
        [ON_CHIP] * 7,
        [
            pltpu.VMEM((width, width), half),
            pltpu.VMEM((count, width), half),
            pltpu.VMEM((4, 8, width), full),
            pltpu.VMEM((count, width), full),
            pltpu.VMEM((count, width), full),
            pltpu.VMEM((count, width), half),
            pltpu.VMEM((4, count, quarter), half),
            pltpu.SemaphoreType.DMA((14,)),
        ],
    )


def attention_back(order, normed, qkvs, lses, mixed_grads, g_out, which, n_img, patches, factor, n):
    groups = len(qkvs)
    count, width = normed.shape
    wide = qkvs[0].shape[1]
    quarter = wide // 3
    padded = count // n_img
    rows = width // n

    def kernel(order_ref, normed_ref, g_out_ref, *refs):
        qkv_refs, mg_refs, refs = refs[:groups], refs[groups : 2 * groups], refs[2 * groups :]
        lse_refs, refs = refs[:groups], refs[groups:]
        g_w_refs, proj_refs, sums_ref = refs[:groups], refs[groups : 2 * groups], refs[2 * groups]
        g_w, normed_held, g_out_held, sems = refs[2 * groups + 1 :]
        q = order_ref[n]
        bring(g_out_ref, g_out_held, sems.at[groups])
        bring(normed_ref, normed_held, sems.at[groups + 1])
        for g in range(groups):

            def attend(i, g=g):
                at = tile(i // 2, padded)
                lanes = [pl.ds(pl.multiple_of(t * quarter + (i % 2) * 128, 128), 128) for t in range(3)]
                q2 = qkv_refs[g][at, lanes[0]] * factor
                k2 = qkv_refs[g][at, lanes[1]]
                v2 = qkv_refs[g][at, lanes[2]]
                both, scores, first = pair_scores(q2, k2)
                key = lax.broadcasted_iota(jnp.int32, scores.shape, 0)
                probs = jnp.where(key < patches, jnp.exp(scores - lse_refs[g][i]), 0.0)
                o_both = apart(mg_refs[g][at, lanes[0]], first)
                g_probs = dot(v2, o_both, 1, 1)
                weighted = jnp.sum(probs * g_probs, axis=0, keepdims=True)
                g_scores = (probs * (g_probs - weighted)).astype(half)
                g_query = dot(g_scores, k2, 0, 0)
                g_query = jnp.where(first, g_query[:padded], g_query[padded:]) * factor
                proj_refs[g][at, lanes[0]] = g_query.astype(half)
                proj_refs[g][at, lanes[1]] = dot(g_scores, both, 1, 0).astype(half)
                proj_refs[g][at, lanes[2]] = dot(probs.astype(half), o_both, 1, 0).astype(half)

            loop(2 * n_img, attend, 4)
            if not g:
                arrived(g_out_held, sems.at[groups])
                arrived(normed_held, sems.at[groups + 1])

            def send_out(r, g=g):
                at = head_rows(order_ref[r], q, n, rows, quarter)
                column = pl.multiple_of((q ^ which[g]) * quarter, quarter)
                pltpu.make_async_copy(
                    g_out_held.at[pl.ds(at, rows), pl.ds(column, quarter)],
                    g_w_refs[g].at[r, :, pl.ds(wide, quarter)],
                    sems.at[g],
                ).start()

            loop(n, send_out)

            def weigh(t, g=g):
                at = tile(t, quarter)
                some = proj_refs[g][:, at]
                g_w[g, :, at] = dot(normed_held[...], some, 0, 0).astype(half)
                sums_ref[g, :, at] = jnp.sum(some.astype(full), axis=0, keepdims=True)

            loop(3, weigh)

            def send(r, g=g):
                at = pl.multiple_of(order_ref[r] * rows, rows)
                pltpu.make_async_copy(
                    g_w.at[g, pl.ds(at, rows)], g_w_refs[g].at[r, :, pl.ds(0, wide)], sems.at[g]
                ).start()

            loop(n, send)
        for g in range(groups):
            pltpu.make_async_copy(g_w_refs[g], g_w_refs[g], sems.at[g]).wait()

    return call(
        kernel,
        "attention_back",
        (order, normed, g_out, *qkvs, *mixed_grads, *lses),
        [SCALARS] + [ANYWHERE] * 2 + [ON_CHIP] * (3 * groups),
        [((n, rows, wide + quarter), half)] * groups
        + [((count, wide), half)] * groups
        + [((groups, 1, wide), full)],
        [ANYWHERE] * groups + [ON_CHIP] * (groups + 1),
        [
            pltpu.VMEM((groups, width, wide), half),
            pltpu.VMEM((count, width), half),
            pltpu.VMEM((width, width), half),
            pltpu.SemaphoreType.DMA((groups + 2,)),
        ],
    )


def input_back(order, x_zero, after_grad, gain, projs, weights):
    count, width = x_zero.shape
    wide = weights[0][0].shape[2]
    rows = width // sum(part.shape[0] for part in weights[0])
    parts = [part for w in weights for part in w]
    n_parts = len(weights[0])

    def kernel(order_ref, x_ref, after_ref, gain_ref, *refs):
        proj_refs, w_refs = refs[:4], refs[4 : 4 + len(parts)]
        token_ref, sums_ref, held, terms, x_held, after_held, sems = refs[4 + len(parts) :]
        for j in range(4):
            fetch(
                [w.at[:, pl.ds(0, rows)] for w in w_refs[j * n_parts : (j + 1) * n_parts]],
                order_ref,
                lambda s, j=j: held.at[j, pl.ds(pl.multiple_of(s * rows, rows), rows)],
                sems.at[j],
            )
        bring(x_ref, x_held, sems.at[4])
        bring(after_ref, after_held, sems.at[5])
        for j in range(4):
            arrived(held.at[j], sems.at[j])
            product = dot(proj_refs[j][...], held[j], 1, 1)
            if j == 0:
                token_ref[...] = product
            else:
                token_ref[...] += product
        arrived(x_held, sems.at[4])
        arrived(after_held, sems.at[5])
        terms[...] = jnp.zeros_like(terms)

        def fold(value):
            return jnp.sum(value.reshape(ROWS // 8, 8, width), axis=0)

        def back(i):
            at = tile(i, ROWS)
            incoming = token_ref[at]
            part, gain_terms = layer_norm_back(x_held[at], incoming, gain_ref[...])
            token_ref[at] = after_held[at] + part
            terms[0] += fold(gain_terms)
            terms[1] += fold(incoming)

        loop(count // ROWS, back)
        for k in range(2):
            sums_ref[k] = jnp.sum(terms[k], axis=0, keepdims=True)

    return call(
        kernel,
        "input_back",
        (order, x_zero, after_grad, gain, *projs, *parts),
        [SCALARS] + [ANYWHERE] * 2 + [ON_CHIP] * 5 + [ANYWHERE] * len(parts),
        [((count, width), full), ((2, 1, width), full)],
        [ON_CHIP] * 2,
        [
            pltpu.VMEM((4, width, wide), half),
            pltpu.VMEM((2, 8, width), full),
            pltpu.VMEM((count, width), full),
            pltpu.VMEM((count, width), full),
            pltpu.SemaphoreType.DMA((6,)),
        ],
    )


def payloads(which, w_fc1, w_fc2):
    rows, ff = w_fc1.shape
    full_share, width = w_fc2.shape
    share = full_share // 4
    n = ff // full_share
    hidden = n * share
    own, across = which
    if share % 128:
        fc1 = [lax.dynamic_slice(w_fc1, (0, (4 * s + own) * share), (rows, share)) for s in range(n)]
        fc2 = [lax.dynamic_slice(w_fc2, (g * share, 0), (share, width)).astype(half) for g in which]
        rest = jnp.concatenate([*fc1, fc2[0].reshape(rows, -1).astype(full)], axis=1)
        return rest.astype(half), fc2[1]

    def kernel(which_ref, fc1_ref, fc2_ref, rest_ref, two_ref):
        for s in range(n):
            at = pl.ds(pl.multiple_of((4 * s + which_ref[0]) * share, share), share)
            rest_ref[:, s * share : (s + 1) * share] = fc1_ref[:, at].astype(half)
        rest_ref[:, hidden : hidden + width] = fc2_ref[tile(which_ref[0], share), :].astype(half)
        two_ref[...] = fc2_ref[tile(which_ref[1], share), :].astype(half)

    return call(
        kernel,
        "payloads",
        (jnp.stack(which), w_fc1, w_fc2),
        [SCALARS] + [ON_CHIP] * 2,
        [((rows, hidden + width), half), ((share, width), half)],
        [ON_CHIP] * 2,
        [],
    )


def natural_quarters(q, pieces):
    once = [jnp.where((q & 1) == 1, pieces[i ^ 1], pieces[i]) for i in range(4)]
    return [jnp.where(q >= 2, once[i ^ 2], once[i]) for i in range(4)]


def finish_mlp(q, pieces, n):
    _, rows, width = pieces[0].shape
    share = width // n
    if share % 128:
        pieces = natural_quarters(q, pieces)
        fc1 = jnp.stack([p[0].reshape(rows, n, share) for p in pieces], axis=2).reshape(rows, 4 * width)
        return fc1.astype(full), jnp.concatenate([p[1] for p in pieces]).astype(full)

    def kernel(q_ref, *refs):
        fc1_ref, fc2_ref = refs[4:]
        for j in range(4):
            g = q_ref[0] ^ j
            for s in range(n):
                at = pl.ds(pl.multiple_of((4 * s + g) * share, share), share)
                fc1_ref[:, at] = refs[j][0, :, s * share : (s + 1) * share].astype(full)
            fc2_ref[tile(g, rows), :] = refs[j][1].astype(full)

    return call(
        kernel,
        "finish_mlp",
        (q[None], *pieces),
        [SCALARS] + [ON_CHIP] * 4,
        [((rows, 4 * width), full), ((4 * rows, width), full)],
        [ON_CHIP] * 2,
        [],
    )


def finish_attention(q, pieces):
    rows, width = pieces[0].shape
    quarter = width // 4

    def kernel(q_ref, *refs):
        qkv_ref, out_ref = refs[4:]
        for j in range(4):
            g = q_ref[0] ^ j
            for t in range(3):
                at = pl.ds(pl.multiple_of(t * width + g * quarter, quarter), quarter)
                qkv_ref[:, at] = refs[j][:, t * quarter : (t + 1) * quarter].astype(full)
            out_ref[:, tile(g, quarter)] = refs[j][:, 3 * quarter :].astype(full)

    return call(
        kernel,
        "finish_attention",
        (q[None], *pieces),
        [SCALARS] + [ON_CHIP] * 4,
        [((rows, 3 * width), full), ((rows, width), full)],
        [ON_CHIP] * 2,
        [],
    )


BELOW = 16


def first_payload(q, w_qkv, vectors):
    rows, columns = w_qkv.shape
    width = columns // 3
    quarter = width // 4
    wide = 3 * quarter

    def kernel(q_ref, w_ref, *refs):
        out_ref, held, low, sem = refs[len(vectors) :]
        for t in range(3):
            at = pl.multiple_of(t * width + q_ref[0] * quarter, quarter)
            pltpu.make_async_copy(
                w_ref.at[:, pl.ds(at, quarter)], held.at[:, pl.ds(t * quarter, quarter)], sem.at[0]
            ).start()
        low[...] = jnp.zeros_like(low)
        for k, vector in enumerate(refs[: len(vectors)]):
            low[k : k + 1, : vector.shape[1]] = vector[...]
        out_ref[rows:] = low[...].astype(half)
        pltpu.make_async_copy(held, held, sem.at[0]).wait()
        out_ref[:rows] = held[...].astype(half)

    return call(
        kernel,
        "first_payload",
        (q[None], w_qkv, *(v[None] for v in vectors)),
        [SCALARS, ANYWHERE] + [ON_CHIP] * len(vectors),
        [((rows + BELOW, wide), half)],
        [ON_CHIP],
        [pltpu.VMEM((rows, wide), full), pltpu.VMEM((BELOW, wide), full), pltpu.SemaphoreType.DMA((1,))],
    )[0]


def unpack_vectors(order, parts, n, rows, share):
    width = n * rows
    quarter = width // 4
    if rows % 128 or share % 128:
        q = order[n]
        held = jnp.concatenate([p[:, rows:] for p in parts]).astype(full)
        held = held[jnp.zeros((n,), jnp.int32).at[order[:n]].set(jnp.arange(n, dtype=jnp.int32))]
        groups = jnp.arange(4, dtype=jnp.int32) ^ q
        vectors = jnp.stack([held[:, k, :rows].reshape(1, width) for k in range(8)])
        units = held[:, 8, : 4 * share].reshape(n, 4, share).transpose(1, 0, 2)[groups]
        ends = [vectors[k].reshape(4, 1, quarter)[groups] for k in range(2)]
        return vectors, units.reshape(4, 1, width), jnp.concatenate([ends[0], 0 * ends[0], ends[1]], axis=2)

    def kernel(order_ref, *refs):
        part_refs, (vector_ref, fc1_ref, qkv_ref, held, wider, sem) = refs[: len(parts)], refs[len(parts) :]
        base = 0
        for part in part_refs:
            size = part.shape[0]
            pltpu.make_async_copy(part.at[:, pl.ds(rows, BELOW)], held.at[pl.ds(base, size)], sem.at[0]).start()
            base += size
        pltpu.make_async_copy(held, held, sem.at[0]).wait()
        wider[...] = held[...].astype(full)
        q = order_ref[n]
        for r in range(n):
            at = tile(order_ref[r], rows)
            for k in range(8):
                vector_ref[k, :, at] = wider[r, k : k + 1, :rows]
            for j in range(4):
                fc1_ref[j, :, tile(order_ref[r], share)] = wider[r, 8:9, tile(q ^ j, share)]
        for j in range(4):
            at = tile(q ^ j, quarter)
            qkv_ref[j, :, :quarter] = vector_ref[0, :, at]
            qkv_ref[j, :, quarter : 2 * quarter] = jnp.zeros((1, quarter), full)
            qkv_ref[j, :, 2 * quarter :] = vector_ref[1, :, at]

    return call(
        kernel,
        "unpack_vectors",
        (order, *parts),
        [SCALARS] + [ANYWHERE] * len(parts),
        [((8, 1, width), full), ((4, 1, width), full), ((4, 1, 3 * quarter), full)],
        [ON_CHIP] * 3,
        [
            pltpu.VMEM((n, BELOW, 3 * quarter), half),
            pltpu.VMEM((n, BELOW, 3 * quarter), full),
            pltpu.SemaphoreType.DMA((1,)),
        ],
    )


def pack_sums(order, n, rows, share, proj_sums, unit_sums, wide_sums):
    width = n * rows
    quarter = width // 4
    if rows % 128 or share % 128:
        groups = jnp.arange(4, dtype=jnp.int32) ^ order[n]
        proj = jnp.concatenate(proj_sums)[groups]
        units = jnp.concatenate(unit_sums)[groups].reshape(4, n, share)
        flat = [proj[:, :, :quarter].reshape(width), proj[:, :, 2 * quarter :].reshape(width)]
        two, one = wide_sums
        flat += [two[0], one[0], one[1], two[3], two[1], two[2]]
        flat = [v.reshape(n, 1, rows) for v in flat]
        stacked = [jnp.pad(v, ((0, 0), (0, 0), (0, 128 - rows))) for v in flat]
        stacked.append(jnp.pad(units.transpose(1, 0, 2), ((0, 0), (0, 4), (0, 128 - share))))
        return jnp.concatenate(stacked, axis=1)[order[:n]]

    def kernel(order_ref, proj_a, proj_b, unit_a, unit_b, two_ref, one_ref, out_ref, proj, units):
        proj[:2], proj[2:] = proj_a[...], proj_b[...]
        units[:2], units[2:] = unit_a[...], unit_b[...]
        q = order_ref[n]
        per = n // 4
        for r in range(n):
            s = order_ref[r]
            j = (s // per) ^ q
            at = tile(s, rows)
            inside = pl.multiple_of((s % per) * rows, rows)
            out_ref[r, 0:1] = proj[j, :, pl.ds(inside, rows)]
            out_ref[r, 1:2] = proj[j, :, pl.ds(2 * quarter + inside, rows)]
            for k, (ref, row) in enumerate(
                ((two_ref, 0), (one_ref, 0), (one_ref, 1), (two_ref, 3), (two_ref, 1), (two_ref, 2))
            ):
                out_ref[r, 2 + k : 3 + k] = ref[row, :, at]
            for g in range(4):
                out_ref[r, 8 + g : 9 + g] = units[q ^ g, :, tile(s, share)]
            out_ref[r, 12:] = jnp.zeros((4, rows), full)

    sums_two, sums_one = wide_sums
    return call(
        kernel,
        "pack_sums",
        (order, *proj_sums, *unit_sums, sums_two, sums_one),
        [SCALARS] + [ON_CHIP] * 6,
        [((n, 16, rows), full)],
        [ON_CHIP],
        [pltpu.VMEM((4, 1, 3 * quarter), full), pltpu.VMEM((4, 1, width), full)],
    )[0]


def table(codes, width):
    ratio = 0.3 * jnp.exp(codes.astype(full) * (math.log(10.0 / 0.3) / (NSCALE - 1)))
    quarter = width // 4
    omega = jnp.exp(jnp.arange(quarter).astype(full) * (-math.log(10000.0) / quarter))
    steps = jnp.arange(GRID, dtype=jnp.int32).astype(full)
    angle = ratio[:, None, None] * steps[None, :, None] * omega[None, None, :]
    return jnp.concatenate([jnp.sin(angle), jnp.cos(angle)], axis=-1)


def local(
    tokens,
    scale_codes,
    w_qkv,
    b_q,
    b_v,
    w_out,
    b_out,
    gain_one,
    shift_one,
    w_fc1,
    b_fc1,
    w_fc2,
    b_fc2,
    gain_two,
    shift_two,
    cotangent,
):
    n = lax.axis_size("fsdp")
    q = lax.axis_index("dp")
    f = lax.axis_index("fsdp")
    row_count, width = tokens.shape
    rows = width // n
    ff = b_fc1.shape[0] * n
    ffq = ff // n // 4
    hidden = n * ffq
    quarter = width // 4
    n_img = scale_codes.shape[0]
    patches = row_count // n_img
    padded = -(-patches // 16) * 16
    factor = 1.0 / math.sqrt(width // HEADS)
    seq = Order(q)
    bits = list(reversed(range(n.bit_length() - 1)))
    near = min(1, len(bits) - 1)
    shard_order = jnp.asarray(masks(bits), jnp.int32) ^ f
    group_order = jnp.arange(4, dtype=jnp.int32) ^ q
    order = jnp.concatenate([shard_order, q[None]])

    def last_three(chain):
        while len(chain.bits) > 3:
            chain.launch()
            seq.land((), chain)
            chain.join()
        return chain

    small = [b_q, b_v, b_out, gain_one, shift_one, b_fc2, gain_two, shift_two, b_fc1]
    qkv = last_three(Gather(seq, first_payload(q, w_qkv, small), n, bits))
    qkv.launch()
    rest_own, two_own = payloads([seq.at(q), q ^ 2], w_fc1, w_fc2)
    rest_own, two_own = seq.land((rest_own, two_own), qkv)
    rest = Sent(lax.all_gather(rest_own, "fsdp", axis=0, tiled=False))
    two = Sent(lax.all_gather(two_own, "fsdp", axis=0, tiled=False))
    out_own = [lax.dynamic_slice(w_out, (0, g * quarter), (rows, quarter)) for g in (q, q ^ 2)]
    out = last_three(Gather(seq, jnp.concatenate(out_own, axis=1).astype(half), n, bits))

    def spread_rows(value):
        split = value.reshape(n_img, patches, width)
        return jnp.pad(split, ((0, 0), (0, padded - patches), (0, 0)))

    def compact(value):
        return value.reshape(n_img, padded, width)[:, :patches].reshape(row_count, width)

    qkv.join()
    qkv.launch()
    spread_tokens = seq.land(spread_rows(seq.at(tokens)), qkv)
    qkv_near = qkv.join()
    qkv.launch()
    near_b, near_c = Sent(core_swap(qkv.held)), Sent(x_swap(qkv.held))
    out.launch()
    places = table(scale_codes, width)
    row_place = jnp.broadcast_to(places[:, :, None], (n_img, GRID, GRID, width // 2))
    col_place = jnp.broadcast_to(places[:, None], (n_img, GRID, GRID, width // 2))
    place = jnp.concatenate([row_place, col_place], axis=-1).reshape(n_img, patches, width)
    place = jnp.pad(place, ((0, 0), (0, padded - patches), (0, 0)))
    x_zero = (seq.at(spread_tokens).astype(full) + place).reshape(-1, width)
    x_zero = seq.land(x_zero, qkv, near_b, out)
    qkv_far = seq.at(qkv.got)
    far_b, far_c = Sent(core_swap(qkv_far)), Sent(x_swap(qkv_far))
    out.join()
    out.launch()
    vectors, bias_fc1, bias_qkv = unpack_vectors(seq.at(order), (qkv_near, qkv_far), n, rows, ffq)
    _, _, full_bout, gain_one_f, shift_one_f, full_bfc2, gain_two_f, shift_two_f = vectors
    normed_one = layer_norm(x_zero, gain_one_f, shift_one_f).astype(half)
    normed_one = seq.land(normed_one, far_b)

    first = attention_forward(
        seq.at(order), normed_one, bias_qkv[:2], ((qkv_near, qkv_far), (near_b.value, far_b.value)),
        n_img, patches, factor,
    )
    first = (seq.land(first[0], near_c, far_c, out), *first[1:])
    near_c, far_c = seq.at((near_c.value, far_c.value))
    near_d, far_d = Sent(core_swap(near_c)), Sent(core_swap(far_c))
    out.join()
    out.launch()
    cot = seq.land(spread_rows(cotangent).reshape(-1, width), near_d, far_d)
    second = attention_forward(
        seq.at(order), normed_one, bias_qkv[2:], ((near_c, far_c), (near_d.value, far_d.value)),
        n_img, patches, factor,
    )
    second = (seq.land(second[0], out, rest), *second[1:])
    out_a = seq.at(out.join())
    out_b = Sent(core_swap(out_a))
    seq.land((), out_b)
    rest_a = seq.at(rest.value)
    rest_b = Sent(core_swap(rest_a))
    up_c = Sent(x_swap(seq.at(rest_a[:, :, :hidden])))
    outs = (out_a, out_b.value)
    qkv_parts = (
        (qkv_near, qkv_far), (near_b.value, far_b.value), (near_c, far_c), (near_d.value, far_d.value)
    )
    qkvs = (*first[:2], *second[:2])
    mixed = (*first[2:4], *second[2:4])
    lses = (*first[4:], *second[4:])
    after_attn, normed_two = attention_out(
        seq.at(order), x_zero, mixed, outs, full_bout, gain_two_f, shift_two_f
    )
    normed_two = seq.land(normed_two, rest_b)

    up_g1, down_g1, g_bias_1, back_sum, out_sum = mlp(
        seq.at(order), normed_two, cot, bias_fc1[1], rest_b.value, rest_b.value, hidden
    )
    up_g0, down_g0, g_bias_0, back_sum, out_sum = mlp(
        order, normed_two, cot, bias_fc1[0], rest_a, rest_a, hidden, (out_sum, back_sum)
    )
    up_g0 = seq.land(up_g0, up_c, two)
    up_g1 = seq.at(up_g1)
    up_got = Sent(core_swap(up_g1))
    down_g1 = seq.at(down_g1)
    down_got = Sent(core_swap(down_g1))
    seq.land((), up_got)
    red_up = Reduce(seq, (up_g0, up_got.value), n)
    red_up.launch()
    seq.land((), down_got)
    red_down = Reduce(seq, (down_g0, down_got.value), n)
    red_down.launch(near)
    up_c, two = seq.at((up_c.value, two.value))
    up_d, two_d = Sent(core_swap(up_c)), Sent(core_swap(two))
    up_g2, down_g2, g_bias_2, back_sum, out_sum = mlp(
        seq.at(order), normed_two, cot, bias_fc1[2], up_c, two, 0, (out_sum, back_sum)
    )
    up_g2 = seq.land(up_g2, up_d, two_d, red_up, red_down)
    red_up.launch()
    red_down.launch()
    up_g3, down_g3, g_bias_3, grad_two_in, block = mlp(
        seq.at(order), normed_two, cot, bias_fc1[3], up_d.value, two_d.value, 0,
        (out_sum, back_sum), (after_attn, full_bfc2),
    )
    up_g3 = seq.land(up_g3, red_up, red_down)
    up_got = Sent(core_swap(up_g3))
    down_g3 = seq.at(down_g3)
    down_got = Sent(core_swap(down_g3))
    red_up.launch()
    red_down.launch()
    seq.land((), up_got)
    two_up = Reduce(seq, (up_g2, up_got.value), n)
    two_up.launch()
    seq.land((), down_got)
    two_down = Reduce(seq, (down_g2, down_got.value), n)
    two_down.launch(near)

    after_grad, mg0, mg1, mg2, mg3, g_out, sums_two = attention_out_back(
        seq.at(order), grad_two_in, after_attn, cot, gain_two_f, mixed, outs
    )
    mg2 = seq.at(mg2)
    g_w2, g_w3, proj2, proj3, sums_b = attention_back(
        seq.at(order), normed_one, qkvs[2:], lses[2:], (mg2, mg3), g_out, (2, 3), n_img, patches, factor, n
    )
    g_w3 = seq.land(g_w3, red_up, red_down, two_up, two_down)
    w_3 = Sent(core_swap(g_w3))
    two_up.launch()
    two_down.launch()
    seq.land((), w_3)
    middle = n // 2
    half_shape = (2,) * (len(bits) - 1)
    w_high = Sent(x_swap(seq.at(rounded_sum([g_w2[middle:], w_3.value[middle:]]))))
    g_w0, g_w1, proj0, proj1, sums_a = attention_back(
        seq.at(order), normed_one, qkvs[:2], lses[:2], (mg0, mg1), g_out, (0, 1), n_img, patches, factor, n
    )
    g_w1 = seq.land(g_w1, two_up, two_down, w_high)
    w_1 = Sent(core_swap(g_w1))
    two_up.launch()
    two_down.launch()
    seq.land((), w_1)
    red_w = Reduce(seq, (g_w0, w_1.value), n)
    red_w.launch(0, [w_high.value.reshape(half_shape + w_high.value.shape[1:])])
    w_low = Sent(x_swap(seq.at(rounded_sum([g_w2[:middle], w_3.value[:middle]]))))
    tokens_grad, sums_one = input_back(
        seq.at(order), x_zero, after_grad, gain_one_f, (proj0, proj1, proj2, proj3), qkv_parts
    )
    sums_one = seq.land(sums_one, two_up, two_down, red_w, w_low)
    red_w.terms = [*red_w.terms, w_low.value.reshape(half_shape + w_low.value.shape[1:])]
    while len(red_w.axes) > 2:
        red_w.launch()
        seq.land((), red_w)
    red_w.launch()
    two_up.terms, two_down.terms, sums_one = seq.at((two_up.terms, two_down.terms, sums_one))
    packed = pack_sums(
        order,
        n,
        rows,
        ffq,
        (sums_a, sums_b),
        (jnp.stack([g_bias_0, g_bias_1]), jnp.stack([g_bias_2, g_bias_3])),
        (sums_two, sums_one),
    )
    packed = seq.at(packed)
    peers = Sent([xor_swap(packed, "dp", 4, m) for m in (1, 2, 3)])
    crossing = jnp.stack([two_up.rest().piece(), two_down.rest().piece()])
    cross = Sent(x_swap(seq.at(crossing)))
    seq.land((), peers, red_w)
    if red_w.axes:
        red_w.launch()
    seq.land((), cross)
    red_up.rest()
    red_down.rest()
    red_up.terms, red_down.terms, cross.value = seq.at((red_up.terms, red_down.terms, cross.value))
    owned = [rounded_sum([*red_up.terms, cross.value[0]]), rounded_sum([*red_down.terms, cross.value[1]])]
    mlp_spread = Spread(seq, jnp.stack(owned))
    sums = Reduce(seq, (packed, *peers.value), n, full)
    sums.launch()
    seq.land((), *([sums, red_w] if len(bits) > 1 else [sums]))
    w_spread = Spread(seq, red_w.piece())
    while len(sums.axes) > 1:
        sums.launch()
        if len(sums.axes) > 1:
            seq.land((), sums)
    block, tokens_grad = seq.at((block, tokens_grad))
    block_out, grad_tokens = seq.land(
        (compact(block), compact(tokens_grad)), *([sums] if len(bits) > 1 else []), mlp_spread, w_spread
    )
    mlp_spread.cross()
    w_spread.cross()
    if sums.axes:
        sums.launch()
    seq.land((), mlp_spread, w_spread, *([sums] if len(bits) > 2 else []))
    small_sums = sums.piece()
    mlp_pieces = seq.at(mlp_spread.pieces)
    out_fc1, out_fc2 = finish_mlp(q, mlp_pieces, n)
    out_qkv, out_out = finish_attention(seq.value, w_spread.pieces)
    small_out = [small_sums[k, :rows] for k in range(8)]
    out_bfc1 = small_sums[8:12, :ffq].reshape(-1)
    o_bq, o_bv, o_bout, o_gone, o_sone, o_bfc2, o_gtwo, o_stwo = small_out
    return (
        block_out,
        grad_tokens,
        out_qkv,
        o_bq,
        o_bv,
        out_out,
        o_bout,
        o_gone,
        o_sone,
        out_fc1,
        out_bfc1,
        out_fc2,
        o_bfc2,
        o_gtwo,
        o_stwo,
    )


def solution(mesh):
    rows_split = P(("dp", "fsdp"), None)
    matrix = P("fsdp", None)
    vector = P("fsdp")
    return jax.shard_map(
        local,
        mesh=mesh,
        in_specs=(
            rows_split, P(("dp", "fsdp")), matrix, vector, vector, matrix, vector, vector, vector,
            matrix, vector, matrix, vector, vector, vector, rows_split,
        ),
        out_specs=(
            rows_split, rows_split, matrix, vector, vector, matrix, vector, vector, vector,
            matrix, vector, matrix, vector, vector, vector,
        ),
        check_vma=False,
    )
```

```python
import math

import jax
import jax.numpy as jnp
from jax import lax
from jax.experimental import pallas as pl
from jax.experimental.pallas import tpu as pltpu
from jax.sharding import PartitionSpec as P

HEADS = 16
GRID = 14
NSCALE = 16
norm_eps = 1e-06
half = jnp.bfloat16
full = jnp.float32


def xor_swap(value, axis, size, mask):
    return lax.ppermute(value, axis, [(i, i ^ mask) for i in range(size)])


def core_swap(value):
    return xor_swap(value, "dp", 4, 1)


def x_swap(value):
    return xor_swap(value, "dp", 4, 2)


def masks(bits):
    found = [0]
    for bit in bits:
        found = found + [m | (1 << bit) for m in found]
    return found


class Order:
    def __init__(self, value):
        self.value = value

    def at(self, value):
        value, self.value = lax.optimization_barrier((value, self.value))
        return value

    def land(self, value, *sent):
        value, flights = self.at((value, [s.flight for s in sent]))
        for s, flight in zip(sent, flights, strict=True):
            s.accept(flight)
        return value


class Sent:
    def __init__(self, flight):
        self.flight = flight

    def accept(self, value):
        self.value = value


class Gather:
    def __init__(self, seq, piece, n, bits):
        self.seq, self.held, self.n, self.bits = seq, piece[None], n, list(bits)

    def launch(self):
        self.held = self.seq.at(self.held)
        self.flight = xor_swap(self.held, "fsdp", self.n, 1 << self.bits.pop(0))

    def accept(self, value):
        self.got = value

    def join(self):
        self.held = jnp.concatenate([self.held, self.got])
        return self.held


def rounded_sum(terms, kind=half):
    return sum(t.astype(full) for t in terms).astype(kind)


class Reduce:
    def __init__(self, seq, terms, n, kind=half):
        self.kind = kind
        self.seq, self.n, self.axes = seq, n, list(range(n.bit_length() - 1))
        self.terms = [t.reshape((2,) * len(self.axes) + t.shape[1:]) for t in terms]

    def launch(self, bit=None, more=()):
        bit = self.axes[0] if bit is None else bit
        axis = self.axes.index(bit)
        self.axes.pop(axis)
        low, high = [
            [lax.index_in_dim(t, side, axis, keepdims=False) for t in self.terms] for side in (0, 1)
        ]
        self.terms = low
        self.flight = xor_swap(self.seq.at(rounded_sum([*high, *more], self.kind)), "fsdp", self.n, 1 << bit)

    def accept(self, value):
        self.terms = [*self.terms, value]

    def rest(self):
        while self.axes:
            self.launch()
            self.seq.land((), self)
        return self

    def piece(self):
        return rounded_sum(self.terms, self.kind)


class Spread:
    def __init__(self, seq, piece):
        self.seq, self.pieces = seq, [seq.at(piece)]
        self.flight = [core_swap(self.pieces[0]), x_swap(self.pieces[0])]

    def cross(self):
        self.flight = [core_swap(self.seq.at(self.pieces[2]))]

    def accept(self, value):
        self.pieces += value


ANYWHERE = pl.BlockSpec(memory_space=pl.ANY)
ON_CHIP = pl.BlockSpec(memory_space=pltpu.VMEM)
SCALARS = pl.BlockSpec(memory_space=pltpu.SMEM)


def dot(left, right, dim_left, dim_right):
    return lax.dot_general(
        left, right, (((dim_left,), (dim_right,)), ((), ())), preferred_element_type=full
    )


def call(kernel, name, operands, in_specs, outs, out_specs, scratch):
    return pl.pallas_call(
        kernel,
        out_shape=[jax.ShapeDtypeStruct(shape, kind) for shape, kind in outs],
        in_specs=in_specs,
        out_specs=out_specs,
        scratch_shapes=scratch,
        compiler_params=pltpu.CompilerParams(vmem_limit_bytes=58 * 2**20),
        name=name,
    )(*operands)


def loop(count, body, unroll=1):
    def step(i, carry):
        body(i)
        return carry

    lax.fori_loop(0, count, step, 0, unroll=unroll)


def tile(i, size):
    return pl.ds(pl.multiple_of(i * size, size), size)


def bring(src, dst, sem):
    pltpu.make_async_copy(src, dst, sem).start()


def arrived(dst, sem):
    pltpu.make_async_copy(dst, dst, sem).wait()


def fetch(parts, order_ref, place, sem):
    base = 0
    for part in parts:

        def start(r, part=part, base=base):
            shard = r if order_ref is None else order_ref[base + r]
            pltpu.make_async_copy(part.at[r], place(shard), sem).start()

        loop(part.shape[0], start)
        base += part.shape[0]


def head_rows(s, q, n, rows, quarter):
    per = n // 4
    return pl.multiple_of(((s // per) ^ q) * quarter + (s % per) * rows, rows)


def pair_scores(q2, k2):
    first = lax.broadcasted_iota(jnp.int32, q2.shape, 1) < q2.shape[1] // 2
    both = apart(q2, first)
    return both, dot(k2, both, 1, 1), first


def apart(value, first):
    zero = jnp.zeros_like(value)
    return jnp.concatenate([jnp.where(first, value, zero), jnp.where(first, zero, value)])


def attention_forward(order, normed, bias, weights, n_img, patches, factor):
    groups, n_parts = len(weights), len(weights[0])
    wide = weights[0][0].shape[2]
    count, width = normed.shape
    rows = width // sum(part.shape[0] for part in weights[0])
    padded = count // n_img
    quarter = wide // 3

    def kernel(order_ref, normed_ref, bias_ref, *refs):
        w_refs, refs = refs[: groups * n_parts], refs[groups * n_parts :]
        qkv_refs, mixed_refs, refs = refs[:groups], refs[groups : 2 * groups], refs[2 * groups :]
        lse_refs, (w_held, sems) = refs[:groups], refs[groups:]
        for g in range(groups):
            fetch(
                [w.at[:, pl.ds(0, rows)] for w in w_refs[g * n_parts : (g + 1) * n_parts]],
                order_ref,
                lambda s, g=g: w_held.at[g, pl.ds(pl.multiple_of(s * rows, rows), rows)],
                sems.at[g],
            )
        for g in range(groups):
            pltpu.make_async_copy(w_held.at[g], w_held.at[g], sems.at[g]).wait()

            def project(t, g=g):
                at = tile(t, quarter)
                product = dot(normed_ref[...], w_held[g, :, at], 1, 0)
                qkv_refs[g][:, at] = (product + bias_ref[g, :, at]).astype(half)

            loop(3, project)

            def attend(i, g=g):
                at = tile(i // 2, padded)
                lanes = [pl.ds(pl.multiple_of(t * quarter + (i % 2) * 128, 128), 128) for t in range(3)]
                q2 = qkv_refs[g][at, lanes[0]] * factor
                k2 = qkv_refs[g][at, lanes[1]]
                v2 = qkv_refs[g][at, lanes[2]]
                _, scores, first = pair_scores(q2, k2)
                key = lax.broadcasted_iota(jnp.int32, scores.shape, 0)
                scores = jnp.where(key < patches, scores, -1e30)
                top = jnp.max(scores, axis=0, keepdims=True)
                raised = jnp.exp(scores - top)
                total = jnp.sum(raised, axis=0, keepdims=True)
                lse_refs[g][i] = top + jnp.log(total)
                out = dot((raised * (1.0 / total)).astype(half), v2, 0, 0)
                mixed_refs[g][at, lanes[0]] = jnp.where(first, out[:padded], out[padded:]).astype(half)

            loop(2 * n_img, attend, 2 * n_img)

    return call(
        kernel,
        "attention_forward",
        (order, normed, bias, *(part for w in weights for part in w)),
        [SCALARS, ON_CHIP, ON_CHIP] + [ANYWHERE] * (groups * n_parts),
        [((count, wide), half)] * groups
        + [((count, quarter), half)] * groups
        + [((2 * n_img, 1, 2 * padded), full)] * groups,
        [ON_CHIP] * (3 * groups),
        [pltpu.VMEM((groups, width, wide), half), pltpu.SemaphoreType.DMA((groups,))],
    )


def layer_norm(value, gain, shift):
    center = jnp.mean(value, axis=-1, keepdims=True)
    offset = value - center
    spread = jnp.mean(offset * offset, axis=-1, keepdims=True)
    return offset * lax.rsqrt(spread + norm_eps) * gain + shift


def layer_norm_back(value, grad, gain):
    center = jnp.mean(value, axis=-1, keepdims=True)
    offset = value - center
    scale = lax.rsqrt(jnp.mean(offset * offset, axis=-1, keepdims=True) + norm_eps)
    unit = offset * scale
    scaled = grad * gain
    inner = jnp.mean(scaled * unit, axis=-1, keepdims=True)
    return scale * (scaled - jnp.mean(scaled, axis=-1, keepdims=True) - unit * inner), grad * unit


def load_out(order_ref, out_refs, held, sem, n, rows, quarter):
    q = order_ref[n]
    for j in range(4):
        column = pl.multiple_of((q ^ j) * quarter, quarter)
        fetch(
            [out_refs[j % 2].at[:, :, pl.ds(j // 2 * quarter, quarter)]],
            order_ref,
            lambda s, column=column: held.at[
                pl.ds(head_rows(s, q, n, rows, quarter), rows), pl.ds(column, quarter)
            ],
            sem,
        )


CHUNK = 16
ROWS = 64


def attention_out(order, x_zero, mixed, outs, bias, gain, shift):
    count, width = x_zero.shape
    n, rows, _ = outs[0].shape
    quarter = mixed[0].shape[1]

    def kernel(order_ref, x_ref, bias_ref, gain_ref, shift_ref, *refs):
        mixed_refs, out_refs = refs[:4], refs[4:6]
        after_ref, normed_ref, held, x_held, sems = refs[6:]
        bring(x_ref, x_held, sems.at[1])
        load_out(order_ref, out_refs, held, sems.at[0], n, rows, quarter)
        together = jnp.concatenate([m[...] for m in mixed_refs], axis=1)
        pltpu.make_async_copy(held, held, sems.at[0]).wait()
        after_ref[...] = dot(together, held[...], 1, 0)
        arrived(x_held, sems.at[1])

        def finish(i):
            at = tile(i, CHUNK)
            after = x_held[at] + (after_ref[at] + bias_ref[...])
            after_ref[at] = after
            normed_ref[at] = layer_norm(after, gain_ref[...], shift_ref[...]).astype(half)

        loop(count // CHUNK, finish, 13)

    return call(
        kernel,
        "attention_out",
        (order, x_zero, bias, gain, shift, *mixed, *outs),
        [SCALARS, ANYWHERE] + [ON_CHIP] * 7 + [ANYWHERE] * 2,
        [((count, width), full), ((count, width), half)],
        [ON_CHIP] * 2,
        [
            pltpu.VMEM((width, width), half),
            pltpu.VMEM((count, width), full),
            pltpu.SemaphoreType.DMA((2,)),
        ],
    )


def mlp(order, normed, cot, bias, up_all, down_all, down_start, carried=None, ending=None):
    count, width = normed.shape
    n, rows, _ = up_all.shape
    hidden = bias.shape[1]
    share = hidden // n
    step = min(512, hidden)
    steps = hidden // step
    more = [*(carried or []), *(ending[:1] if ending else [])]
    last = list(ending[1:]) if ending else []

    def kernel(order_ref, bias_ref, *refs):
        last_refs, refs = refs[: len(last)], refs[len(last) :]
        normed_ref, cot_ref, up_ref, down_ref, refs = *refs[:4], refs[4:]
        more_refs, refs = refs[: len(more)], refs[len(more) :]
        g_up_ref, g_down_ref, g_bias_ref, back_ref, end_ref, refs = *refs[:5], refs[5:]
        held, refs = refs[: len(more)], refs[len(more) :]
        rows_in, cots, out, back, up, down, pre, act, act_half, pre_half, g_up, g_down, sems = refs
        bring(normed_ref, rows_in, sems.at[3])
        fetch(
            [up_ref.at[:, :, pl.ds(0, hidden)]],
            None,
            lambda s: up.at[pl.ds(pl.multiple_of(s * rows, rows), rows)],
            sems.at[0],
        )
        bring(cot_ref, cots, sems.at[4])
        fetch(
            [down_ref.at[:, :, pl.ds(down_start, width)]],
            None,
            lambda s: down.at[pl.ds(pl.multiple_of(s * share, share), share)],
            sems.at[1],
        )
        for k in range(len(more)):
            bring(more_refs[k], held[k], sems.at[5 + k])
        arrived(rows_in, sems.at[3])
        arrived(up, sems.at[0])
        for t in range(steps):
            at = pl.ds(t * step, step)
            pre[...] = dot(rows_in[...], up[:, at], 1, 0)
            if not t:
                arrived(cots, sems.at[4])
                arrived(down, sems.at[1])
            act[...] = dot(cots[...], down[at, :], 1, 1)

            def gelu(i, at=at):
                some = tile(i, 2 * CHUNK)
                x = pre[some] + bias_ref[:, at]
                below = 0.5 * (1.0 + lax.erf(x * math.sqrt(0.5)))
                density = jnp.exp(-0.5 * x * x) * (1.0 / math.sqrt(2.0 * math.pi))
                act_half[some] = (x * below).astype(half)
                pre_half[some] = (act[some] * (below + x * density)).astype(half)

            loop(count // CHUNK // 2, gelu)
            p = pre_half[...]
            h = act_half[...]
            more_back = dot(p, up[:, at], 1, 1)
            more_out = dot(h, down[at, :], 1, 0)
            if t:
                back[...] += more_back
                out[...] += more_out
            elif carried:
                arrived(held[0], sems.at[5])
                arrived(held[1], sems.at[6])
                out[...] = held[0][...] + more_out
                back[...] = held[1][...] + more_back
            else:
                out[...] = more_out
                back[...] = more_back
            if t == steps - 1:
                bring(back, back_ref, sems.at[3])
                if not ending:
                    bring(out, end_ref, sems.at[4])
            g_down[at, :] = dot(h, cots[...], 0, 0).astype(half)
            if t == steps - 1:

                def send_down(r):
                    at = pl.multiple_of(order_ref[r] * share, share)
                    bring(g_down.at[pl.ds(at, share)], g_down_ref.at[r], sems.at[2])

                loop(n, send_down)
            g_up[:, at] = dot(rows_in[...], p, 0, 0).astype(half)
            g_bias_ref[:, at] = jnp.sum(p.astype(full), axis=0, keepdims=True)

        def send_up(r):
            at = pl.multiple_of(order_ref[r] * rows, rows)
            bring(g_up.at[pl.ds(at, rows)], g_up_ref.at[r], sems.at[0])

        loop(n, send_up)
        if ending:
            arrived(held[2], sems.at[7])

            def finish(i):
                at = tile(i, 2 * CHUNK)
                end_ref[at] = (held[2][at] + (out[at] + last_refs[0][...])).astype(half)

            loop(count // CHUNK // 2, finish)
        else:
            arrived(end_ref, sems.at[4])
        arrived(back_ref, sems.at[3])
        arrived(g_down_ref, sems.at[2])
        arrived(g_up_ref, sems.at[0])

    sums = pltpu.VMEM((count, width), full)
    wide = pltpu.VMEM((count, width), half)
    square = pltpu.VMEM((width, hidden), half)
    return call(
        kernel,
        "mlp",
        (order, bias, *last, normed, cot, up_all, down_all, *more),
        [SCALARS] + [ON_CHIP] * (1 + len(last)) + [ANYWHERE] * (4 + len(more)),
        [
            ((n, rows, hidden), half),
            ((n, share, width), half),
            ((1, hidden), full),
            ((count, width), full),
            ((count, width), half if ending else full),
        ],
        [ANYWHERE, ANYWHERE, ON_CHIP, ANYWHERE, ON_CHIP if ending else ANYWHERE],
        [
            *([sums] * len(more)),
            wide,
            wide,
            sums,
            sums,
            square,
            pltpu.VMEM((hidden, width), half),
            pltpu.VMEM((count, step), full),
            pltpu.VMEM((count, step), full),
            pltpu.VMEM((count, step), half),
            pltpu.VMEM((count, step), half),
            square,
            pltpu.VMEM((hidden, width), half),
            pltpu.SemaphoreType.DMA((5 + len(more),)),
        ],
    )


def attention_out_back(order, grad, after, cot, gain, mixed, outs):
    count, width = after.shape
    n, rows, _ = outs[0].shape
    quarter = mixed[0].shape[1]

    def kernel(order_ref, grad_ref, after_ref, cot_ref, gain_ref, *refs):
        mixed_refs, out_refs, refs = refs[:4], refs[4:6], refs[6:]
        after_grad_ref, mixed_grad_refs, g_out_ref, sums_ref = refs[0], refs[1:5], refs[5], refs[6]
        held, branch, terms, grad, after, cot, mixes, sems = refs[7:]
        block = count // 4
        for k in range(4):
            some = pl.ds(k * block, block)
            bring(grad_ref.at[some], grad.at[some], sems.at[1 + k])
            bring(after_ref.at[some], after.at[some], sems.at[5 + k])
            bring(cot_ref.at[some], cot.at[some], sems.at[9 + k])
        load_out(order_ref, out_refs, held, sems.at[0], n, rows, quarter)
        for j in range(4):
            bring(mixed_refs[j], mixes.at[j], sems.at[13])
        terms[...] = jnp.zeros_like(terms)

        def fold(value):
            return jnp.sum(value.reshape(CHUNK // 8, 8, width), axis=0)

        def back(i, k):
            at = pl.ds(pl.multiple_of(k * block + i * CHUNK, CHUNK), CHUNK)
            incoming = grad[at]
            part, gain_terms = layer_norm_back(after[at], incoming, gain_ref[...])
            own = cot[at].astype(full)
            total = own + part
            after_grad_ref[at] = total
            rounded = total.astype(half)
            branch[at] = rounded
            terms[0] += fold(rounded.astype(full))
            terms[1] += fold(gain_terms)
            terms[2] += fold(incoming)
            terms[3] += fold(own)

        for k in range(4):
            some = pl.ds(k * block, block)
            arrived(grad.at[some], sems.at[1 + k])
            arrived(after.at[some], sems.at[5 + k])
            arrived(cot.at[some], sems.at[9 + k])
            loop(block // CHUNK, lambda i, k=k: back(i, k), 13)
        for k in range(4):
            sums_ref[k] = jnp.sum(terms[k], axis=0, keepdims=True)
        arrived(held, sems.at[0])
        arrived(mixes, sems.at[13])
        for j in range(4):
            mixed_grad_refs[j][...] = dot(branch[...], held[j * quarter : (j + 1) * quarter], 1, 1).astype(half)
            g_out_ref[j * quarter : (j + 1) * quarter] = dot(mixes[j], branch[...], 0, 0).astype(half)

    return call(
        kernel,
        "attention_out_back",
        (order, grad, after, cot, gain, *mixed, *outs),
        [SCALARS] + [ANYWHERE] * 3 + [ON_CHIP] + [ANYWHERE] * 6,
        [((count, width), full)]
        + [((count, quarter), half)] * 4
        + [((width, width), half), ((4, 1, width), full)],
        [ON_CHIP] * 7,
        [
            pltpu.VMEM((width, width), half),
            pltpu.VMEM((count, width), half),
            pltpu.VMEM((4, 8, width), full),
            pltpu.VMEM((count, width), full),
            pltpu.VMEM((count, width), full),
            pltpu.VMEM((count, width), half),
            pltpu.VMEM((4, count, quarter), half),
            pltpu.SemaphoreType.DMA((14,)),
        ],
    )


def attention_back(order, normed, qkvs, lses, mixed_grads, g_out, which, n_img, patches, factor, n):
    groups = len(qkvs)
    count, width = normed.shape
    wide = qkvs[0].shape[1]
    quarter = wide // 3
    padded = count // n_img
    rows = width // n

    def kernel(order_ref, normed_ref, g_out_ref, *refs):
        qkv_refs, mg_refs, refs = refs[:groups], refs[groups : 2 * groups], refs[2 * groups :]
        lse_refs, refs = refs[:groups], refs[groups:]
        g_w_refs, proj_refs, sums_ref = refs[:groups], refs[groups : 2 * groups], refs[2 * groups]
        g_w, normed_held, g_out_held, sems = refs[2 * groups + 1 :]
        q = order_ref[n]
        bring(g_out_ref, g_out_held, sems.at[groups])
        bring(normed_ref, normed_held, sems.at[groups + 1])
        for g in range(groups):

            def attend(i, g=g):
                at = tile(i // 2, padded)
                lanes = [pl.ds(pl.multiple_of(t * quarter + (i % 2) * 128, 128), 128) for t in range(3)]
                q2 = qkv_refs[g][at, lanes[0]] * factor
                k2 = qkv_refs[g][at, lanes[1]]
                v2 = qkv_refs[g][at, lanes[2]]
                both, scores, first = pair_scores(q2, k2)
                key = lax.broadcasted_iota(jnp.int32, scores.shape, 0)
                probs = jnp.where(key < patches, jnp.exp(scores - lse_refs[g][i]), 0.0)
                o_both = apart(mg_refs[g][at, lanes[0]], first)
                g_probs = dot(v2, o_both, 1, 1)
                weighted = jnp.sum(probs * g_probs, axis=0, keepdims=True)
                g_scores = (probs * (g_probs - weighted)).astype(half)
                g_query = dot(g_scores, k2, 0, 0)
                g_query = jnp.where(first, g_query[:padded], g_query[padded:]) * factor
                proj_refs[g][at, lanes[0]] = g_query.astype(half)
                proj_refs[g][at, lanes[1]] = dot(g_scores, both, 1, 0).astype(half)
                proj_refs[g][at, lanes[2]] = dot(probs.astype(half), o_both, 1, 0).astype(half)

            loop(2 * n_img, attend, 4)
            if not g:
                arrived(g_out_held, sems.at[groups])
                arrived(normed_held, sems.at[groups + 1])

            def send_out(r, g=g):
                at = head_rows(order_ref[r], q, n, rows, quarter)
                column = pl.multiple_of((q ^ which[g]) * quarter, quarter)
                pltpu.make_async_copy(
                    g_out_held.at[pl.ds(at, rows), pl.ds(column, quarter)],
                    g_w_refs[g].at[r, :, pl.ds(wide, quarter)],
                    sems.at[g],
                ).start()

            loop(n, send_out)

            def weigh(t, g=g):
                at = tile(t, quarter)
                some = proj_refs[g][:, at]
                g_w[g, :, at] = dot(normed_held[...], some, 0, 0).astype(half)
                sums_ref[g, :, at] = jnp.sum(some.astype(full), axis=0, keepdims=True)

            loop(3, weigh)

            def send(r, g=g):
                at = pl.multiple_of(order_ref[r] * rows, rows)
                pltpu.make_async_copy(
                    g_w.at[g, pl.ds(at, rows)], g_w_refs[g].at[r, :, pl.ds(0, wide)], sems.at[g]
                ).start()

            loop(n, send)
        for g in range(groups):
            pltpu.make_async_copy(g_w_refs[g], g_w_refs[g], sems.at[g]).wait()

    return call(
        kernel,
        "attention_back",
        (order, normed, g_out, *qkvs, *mixed_grads, *lses),
        [SCALARS] + [ANYWHERE] * 2 + [ON_CHIP] * (3 * groups),
        [((n, rows, wide + quarter), half)] * groups
        + [((count, wide), half)] * groups
        + [((groups, 1, wide), full)],
        [ANYWHERE] * groups + [ON_CHIP] * (groups + 1),
        [
            pltpu.VMEM((groups, width, wide), half),
            pltpu.VMEM((count, width), half),
            pltpu.VMEM((width, width), half),
            pltpu.SemaphoreType.DMA((groups + 2,)),
        ],
    )


def input_back(order, x_zero, after_grad, gain, projs, weights):
    count, width = x_zero.shape
    wide = weights[0][0].shape[2]
    rows = width // sum(part.shape[0] for part in weights[0])
    parts = [part for w in weights for part in w]
    n_parts = len(weights[0])

    def kernel(order_ref, x_ref, after_ref, gain_ref, *refs):
        proj_refs, w_refs = refs[:4], refs[4 : 4 + len(parts)]
        token_ref, sums_ref, held, terms, x_held, after_held, sems = refs[4 + len(parts) :]
        for j in range(4):
            fetch(
                [w.at[:, pl.ds(0, rows)] for w in w_refs[j * n_parts : (j + 1) * n_parts]],
                order_ref,
                lambda s, j=j: held.at[j, pl.ds(pl.multiple_of(s * rows, rows), rows)],
                sems.at[j],
            )
        bring(x_ref, x_held, sems.at[4])
        bring(after_ref, after_held, sems.at[5])
        for j in range(4):
            arrived(held.at[j], sems.at[j])
            product = dot(proj_refs[j][...], held[j], 1, 1)
            if j == 0:
                token_ref[...] = product
            else:
                token_ref[...] += product
        arrived(x_held, sems.at[4])
        arrived(after_held, sems.at[5])
        terms[...] = jnp.zeros_like(terms)

        def fold(value):
            return jnp.sum(value.reshape(ROWS // 8, 8, width), axis=0)

        def back(i):
            at = tile(i, ROWS)
            incoming = token_ref[at]
            part, gain_terms = layer_norm_back(x_held[at], incoming, gain_ref[...])
            token_ref[at] = after_held[at] + part
            terms[0] += fold(gain_terms)
            terms[1] += fold(incoming)

        loop(count // ROWS, back)
        for k in range(2):
            sums_ref[k] = jnp.sum(terms[k], axis=0, keepdims=True)

    return call(
        kernel,
        "input_back",
        (order, x_zero, after_grad, gain, *projs, *parts),
        [SCALARS] + [ANYWHERE] * 2 + [ON_CHIP] * 5 + [ANYWHERE] * len(parts),
        [((count, width), full), ((2, 1, width), full)],
        [ON_CHIP] * 2,
        [
            pltpu.VMEM((4, width, wide), half),
            pltpu.VMEM((2, 8, width), full),
            pltpu.VMEM((count, width), full),
            pltpu.VMEM((count, width), full),
            pltpu.SemaphoreType.DMA((6,)),
        ],
    )


def payloads(which, w_fc1, w_fc2):
    rows, ff = w_fc1.shape
    full_share, width = w_fc2.shape
    share = full_share // 4
    n = ff // full_share
    hidden = n * share
    own, across = which
    if share % 128:
        fc1 = [lax.dynamic_slice(w_fc1, (0, (4 * s + own) * share), (rows, share)) for s in range(n)]
        fc2 = [lax.dynamic_slice(w_fc2, (g * share, 0), (share, width)).astype(half) for g in which]
        rest = jnp.concatenate([*fc1, fc2[0].reshape(rows, -1).astype(full)], axis=1)
        return rest.astype(half), fc2[1]

    def kernel(which_ref, fc1_ref, fc2_ref, rest_ref, two_ref):
        for s in range(n):
            at = pl.ds(pl.multiple_of((4 * s + which_ref[0]) * share, share), share)
            rest_ref[:, s * share : (s + 1) * share] = fc1_ref[:, at].astype(half)
        rest_ref[:, hidden : hidden + width] = fc2_ref[tile(which_ref[0], share), :].astype(half)
        two_ref[...] = fc2_ref[tile(which_ref[1], share), :].astype(half)

    return call(
        kernel,
        "payloads",
        (jnp.stack(which), w_fc1, w_fc2),
        [SCALARS] + [ON_CHIP] * 2,
        [((rows, hidden + width), half), ((share, width), half)],
        [ON_CHIP] * 2,
        [],
    )


def natural_quarters(q, pieces):
    once = [jnp.where((q & 1) == 1, pieces[i ^ 1], pieces[i]) for i in range(4)]
    return [jnp.where(q >= 2, once[i ^ 2], once[i]) for i in range(4)]


def finish_mlp(q, pieces, n):
    _, rows, width = pieces[0].shape
    share = width // n
    if share % 128:
        pieces = natural_quarters(q, pieces)
        fc1 = jnp.stack([p[0].reshape(rows, n, share) for p in pieces], axis=2).reshape(rows, 4 * width)
        return fc1.astype(full), jnp.concatenate([p[1] for p in pieces]).astype(full)

    def kernel(q_ref, *refs):
        fc1_ref, fc2_ref = refs[4:]
        for j in range(4):
            g = q_ref[0] ^ j
            for s in range(n):
                at = pl.ds(pl.multiple_of((4 * s + g) * share, share), share)
                fc1_ref[:, at] = refs[j][0, :, s * share : (s + 1) * share].astype(full)
            fc2_ref[tile(g, rows), :] = refs[j][1].astype(full)

    return call(
        kernel,
        "finish_mlp",
        (q[None], *pieces),
        [SCALARS] + [ON_CHIP] * 4,
        [((rows, 4 * width), full), ((4 * rows, width), full)],
        [ON_CHIP] * 2,
        [],
    )


def finish_attention(q, pieces):
    rows, width = pieces[0].shape
    quarter = width // 4

    def kernel(q_ref, *refs):
        qkv_ref, out_ref = refs[4:]
        for j in range(4):
            g = q_ref[0] ^ j
            for t in range(3):
                at = pl.ds(pl.multiple_of(t * width + g * quarter, quarter), quarter)
                qkv_ref[:, at] = refs[j][:, t * quarter : (t + 1) * quarter].astype(full)
            out_ref[:, tile(g, quarter)] = refs[j][:, 3 * quarter :].astype(full)

    return call(
        kernel,
        "finish_attention",
        (q[None], *pieces),
        [SCALARS] + [ON_CHIP] * 4,
        [((rows, 3 * width), full), ((rows, width), full)],
        [ON_CHIP] * 2,
        [],
    )


BELOW = 16


def first_payload(q, w_qkv, vectors):
    rows, columns = w_qkv.shape
    width = columns // 3
    quarter = width // 4
    wide = 3 * quarter

    def kernel(q_ref, w_ref, *refs):
        out_ref, held, low, sem = refs[len(vectors) :]
        for t in range(3):
            at = pl.multiple_of(t * width + q_ref[0] * quarter, quarter)
            pltpu.make_async_copy(
                w_ref.at[:, pl.ds(at, quarter)], held.at[:, pl.ds(t * quarter, quarter)], sem.at[0]
            ).start()
        low[...] = jnp.zeros_like(low)
        for k, vector in enumerate(refs[: len(vectors)]):
            low[k : k + 1, : vector.shape[1]] = vector[...]
        out_ref[rows:] = low[...].astype(half)
        pltpu.make_async_copy(held, held, sem.at[0]).wait()
        out_ref[:rows] = held[...].astype(half)

    return call(
        kernel,
        "first_payload",
        (q[None], w_qkv, *(v[None] for v in vectors)),
        [SCALARS, ANYWHERE] + [ON_CHIP] * len(vectors),
        [((rows + BELOW, wide), half)],
        [ON_CHIP],
        [pltpu.VMEM((rows, wide), full), pltpu.VMEM((BELOW, wide), full), pltpu.SemaphoreType.DMA((1,))],
    )[0]


def unpack_vectors(order, parts, n, rows, share):
    width = n * rows
    quarter = width // 4
    if rows % 128 or share % 128:
        q = order[n]
        held = jnp.concatenate([p[:, rows:] for p in parts]).astype(full)
        held = held[jnp.zeros((n,), jnp.int32).at[order[:n]].set(jnp.arange(n, dtype=jnp.int32))]
        groups = jnp.arange(4, dtype=jnp.int32) ^ q
        vectors = jnp.stack([held[:, k, :rows].reshape(1, width) for k in range(8)])
        units = held[:, 8, : 4 * share].reshape(n, 4, share).transpose(1, 0, 2)[groups]
        ends = [vectors[k].reshape(4, 1, quarter)[groups] for k in range(2)]
        return vectors, units.reshape(4, 1, width), jnp.concatenate([ends[0], 0 * ends[0], ends[1]], axis=2)

    def kernel(order_ref, *refs):
        part_refs, (vector_ref, fc1_ref, qkv_ref, held, wider, sem) = refs[: len(parts)], refs[len(parts) :]
        base = 0
        for part in part_refs:
            size = part.shape[0]
            pltpu.make_async_copy(part.at[:, pl.ds(rows, BELOW)], held.at[pl.ds(base, size)], sem.at[0]).start()
            base += size
        pltpu.make_async_copy(held, held, sem.at[0]).wait()
        wider[...] = held[...].astype(full)
        q = order_ref[n]
        for r in range(n):
            at = tile(order_ref[r], rows)
            for k in range(8):
                vector_ref[k, :, at] = wider[r, k : k + 1, :rows]
            for j in range(4):
                fc1_ref[j, :, tile(order_ref[r], share)] = wider[r, 8:9, tile(q ^ j, share)]
        for j in range(4):
            at = tile(q ^ j, quarter)
            qkv_ref[j, :, :quarter] = vector_ref[0, :, at]
            qkv_ref[j, :, quarter : 2 * quarter] = jnp.zeros((1, quarter), full)
            qkv_ref[j, :, 2 * quarter :] = vector_ref[1, :, at]

    return call(
        kernel,
        "unpack_vectors",
        (order, *parts),
        [SCALARS] + [ANYWHERE] * len(parts),
        [((8, 1, width), full), ((4, 1, width), full), ((4, 1, 3 * quarter), full)],
        [ON_CHIP] * 3,
        [
            pltpu.VMEM((n, BELOW, 3 * quarter), half),
            pltpu.VMEM((n, BELOW, 3 * quarter), full),
            pltpu.SemaphoreType.DMA((1,)),
        ],
    )


def pack_sums(order, n, rows, share, proj_sums, unit_sums, wide_sums):
    width = n * rows
    quarter = width // 4
    if rows % 128 or share % 128:
        groups = jnp.arange(4, dtype=jnp.int32) ^ order[n]
        proj = jnp.concatenate(proj_sums)[groups]
        units = jnp.concatenate(unit_sums)[groups].reshape(4, n, share)
        flat = [proj[:, :, :quarter].reshape(width), proj[:, :, 2 * quarter :].reshape(width)]
        two, one = wide_sums
        flat += [two[0], one[0], one[1], two[3], two[1], two[2]]
        flat = [v.reshape(n, 1, rows) for v in flat]
        stacked = [jnp.pad(v, ((0, 0), (0, 0), (0, 128 - rows))) for v in flat]
        stacked.append(jnp.pad(units.transpose(1, 0, 2), ((0, 0), (0, 4), (0, 128 - share))))
        return jnp.concatenate(stacked, axis=1)[order[:n]]

    def kernel(order_ref, proj_a, proj_b, unit_a, unit_b, two_ref, one_ref, out_ref, proj, units):
        proj[:2], proj[2:] = proj_a[...], proj_b[...]
        units[:2], units[2:] = unit_a[...], unit_b[...]
        q = order_ref[n]
        per = n // 4
        for r in range(n):
            s = order_ref[r]
            j = (s // per) ^ q
            at = tile(s, rows)
            inside = pl.multiple_of((s % per) * rows, rows)
            out_ref[r, 0:1] = proj[j, :, pl.ds(inside, rows)]
            out_ref[r, 1:2] = proj[j, :, pl.ds(2 * quarter + inside, rows)]
            for k, (ref, row) in enumerate(
                ((two_ref, 0), (one_ref, 0), (one_ref, 1), (two_ref, 3), (two_ref, 1), (two_ref, 2))
            ):
                out_ref[r, 2 + k : 3 + k] = ref[row, :, at]
            for g in range(4):
                out_ref[r, 8 + g : 9 + g] = units[q ^ g, :, tile(s, share)]
            out_ref[r, 12:] = jnp.zeros((4, rows), full)

    sums_two, sums_one = wide_sums
    return call(
        kernel,
        "pack_sums",
        (order, *proj_sums, *unit_sums, sums_two, sums_one),
        [SCALARS] + [ON_CHIP] * 6,
        [((n, 16, rows), full)],
        [ON_CHIP],
        [pltpu.VMEM((4, 1, 3 * quarter), full), pltpu.VMEM((4, 1, width), full)],
    )[0]


def table(codes, width):
    ratio = 0.3 * jnp.exp(codes.astype(full) * (math.log(10.0 / 0.3) / (NSCALE - 1)))
    quarter = width // 4
    omega = jnp.exp(jnp.arange(quarter).astype(full) * (-math.log(10000.0) / quarter))
    steps = jnp.arange(GRID, dtype=jnp.int32).astype(full)
    angle = ratio[:, None, None] * steps[None, :, None] * omega[None, None, :]
    return jnp.concatenate([jnp.sin(angle), jnp.cos(angle)], axis=-1)


def local(
    tokens,
    scale_codes,
    w_qkv,
    b_q,
    b_v,
    w_out,
    b_out,
    gain_one,
    shift_one,
    w_fc1,
    b_fc1,
    w_fc2,
    b_fc2,
    gain_two,
    shift_two,
    cotangent,
):
    n = lax.axis_size("fsdp")
    q = lax.axis_index("dp")
    f = lax.axis_index("fsdp")
    row_count, width = tokens.shape
    rows = width // n
    ff = b_fc1.shape[0] * n
    ffq = ff // n // 4
    hidden = n * ffq
    quarter = width // 4
    n_img = scale_codes.shape[0]
    patches = row_count // n_img
    padded = -(-patches // 16) * 16
    factor = 1.0 / math.sqrt(width // HEADS)
    seq = Order(q)
    bits = list(reversed(range(n.bit_length() - 1)))
    near = min(1, len(bits) - 1)
    shard_order = jnp.asarray(masks(bits), jnp.int32) ^ f
    group_order = jnp.arange(4, dtype=jnp.int32) ^ q
    order = jnp.concatenate([shard_order, q[None]])

    def last_three(chain):
        while len(chain.bits) > 3:
            chain.launch()
            seq.land((), chain)
            chain.join()
        return chain

    small = [b_q, b_v, b_out, gain_one, shift_one, b_fc2, gain_two, shift_two, b_fc1]
    qkv = last_three(Gather(seq, first_payload(q, w_qkv, small), n, bits))
    qkv.launch()
    rest_own, two_own = payloads([seq.at(q), q ^ 2], w_fc1, w_fc2)
    rest_own, two_own = seq.land((rest_own, two_own), qkv)
    rest = Sent(lax.all_gather(rest_own, "fsdp", axis=0, tiled=False))
    two = Sent(lax.all_gather(two_own, "fsdp", axis=0, tiled=False))
    out_own = [lax.dynamic_slice(w_out, (0, g * quarter), (rows, quarter)) for g in (q, q ^ 2)]
    out = last_three(Gather(seq, jnp.concatenate(out_own, axis=1).astype(half), n, bits))

    def spread_rows(value):
        split = value.reshape(n_img, patches, width)
        return jnp.pad(split, ((0, 0), (0, padded - patches), (0, 0)))

    def compact(value):
        return value.reshape(n_img, padded, width)[:, :patches].reshape(row_count, width)

    qkv.join()
    qkv.launch()
    spread_tokens = seq.land(spread_rows(seq.at(tokens)), qkv)
    qkv_near = qkv.join()
    qkv.launch()
    near_b, near_c = Sent(core_swap(qkv.held)), Sent(x_swap(qkv.held))
    out.launch()
    places = table(scale_codes, width)
    row_place = jnp.broadcast_to(places[:, :, None], (n_img, GRID, GRID, width // 2))
    col_place = jnp.broadcast_to(places[:, None], (n_img, GRID, GRID, width // 2))
    place = jnp.concatenate([row_place, col_place], axis=-1).reshape(n_img, patches, width)
    place = jnp.pad(place, ((0, 0), (0, padded - patches), (0, 0)))
    x_zero = (seq.at(spread_tokens).astype(full) + place).reshape(-1, width)
    x_zero = seq.land(x_zero, qkv, near_b, out)
    qkv_far = seq.at(qkv.got)
    far_b, far_c = Sent(core_swap(qkv_far)), Sent(x_swap(qkv_far))
    out.join()
    out.launch()
    vectors, bias_fc1, bias_qkv = unpack_vectors(seq.at(order), (qkv_near, qkv_far), n, rows, ffq)
    _, _, full_bout, gain_one_f, shift_one_f, full_bfc2, gain_two_f, shift_two_f = vectors
    normed_one = layer_norm(x_zero, gain_one_f, shift_one_f).astype(half)
    normed_one = seq.land(normed_one, far_b)

    first = attention_forward(
        seq.at(order), normed_one, bias_qkv[:2], ((qkv_near, qkv_far), (near_b.value, far_b.value)),
        n_img, patches, factor,
    )
    first = (seq.land(first[0], near_c, far_c, out), *first[1:])
    near_c, far_c = seq.at((near_c.value, far_c.value))
    near_d, far_d = Sent(core_swap(near_c)), Sent(core_swap(far_c))
    out.join()
    out.launch()
    cot = seq.land(spread_rows(cotangent).reshape(-1, width), near_d, far_d)
    second = attention_forward(
        seq.at(order), normed_one, bias_qkv[2:], ((near_c, far_c), (near_d.value, far_d.value)),
        n_img, patches, factor,
    )
    second = (seq.land(second[0], out, rest), *second[1:])
    out_a = seq.at(out.join())
    out_b = Sent(core_swap(out_a))
    seq.land((), out_b)
    rest_a = seq.at(rest.value)
    rest_b = Sent(core_swap(rest_a))
    up_c = Sent(x_swap(seq.at(rest_a[:, :, :hidden])))
    outs = (out_a, out_b.value)
    qkv_parts = (
        (qkv_near, qkv_far), (near_b.value, far_b.value), (near_c, far_c), (near_d.value, far_d.value)
    )
    qkvs = (*first[:2], *second[:2])
    mixed = (*first[2:4], *second[2:4])
    lses = (*first[4:], *second[4:])
    after_attn, normed_two = attention_out(
        seq.at(order), x_zero, mixed, outs, full_bout, gain_two_f, shift_two_f
    )
    normed_two = seq.land(normed_two, rest_b)

    up_g1, down_g1, g_bias_1, back_sum, out_sum = mlp(
        seq.at(order), normed_two, cot, bias_fc1[1], rest_b.value, rest_b.value, hidden
    )
    up_g0, down_g0, g_bias_0, back_sum, out_sum = mlp(
        order, normed_two, cot, bias_fc1[0], rest_a, rest_a, hidden, (out_sum, back_sum)
    )
    up_g0 = seq.land(up_g0, up_c, two)
    up_g1 = seq.at(up_g1)
    up_got = Sent(core_swap(up_g1))
    down_g1 = seq.at(down_g1)
    down_got = Sent(core_swap(down_g1))
    seq.land((), up_got)
    red_up = Reduce(seq, (up_g0, up_got.value), n)
    red_up.launch()
    seq.land((), down_got)
    red_down = Reduce(seq, (down_g0, down_got.value), n)
    red_down.launch(near)
    up_c, two = seq.at((up_c.value, two.value))
    up_d, two_d = Sent(core_swap(up_c)), Sent(core_swap(two))
    up_g2, down_g2, g_bias_2, back_sum, out_sum = mlp(
        seq.at(order), normed_two, cot, bias_fc1[2], up_c, two, 0, (out_sum, back_sum)
    )
    up_g2 = seq.land(up_g2, up_d, two_d, red_up, red_down)
    red_up.launch()
    red_down.launch()
    up_g3, down_g3, g_bias_3, grad_two_in, block = mlp(
        seq.at(order), normed_two, cot, bias_fc1[3], up_d.value, two_d.value, 0,
        (out_sum, back_sum), (after_attn, full_bfc2),
    )
    up_g3 = seq.land(up_g3, red_up, red_down)
    up_got = Sent(core_swap(up_g3))
    down_g3 = seq.at(down_g3)
    down_got = Sent(core_swap(down_g3))
    red_up.launch()
    red_down.launch()
    seq.land((), up_got)
    two_up = Reduce(seq, (up_g2, up_got.value), n)
    two_up.launch()
    seq.land((), down_got)
    two_down = Reduce(seq, (down_g2, down_got.value), n)
    two_down.launch(near)

    after_grad, mg0, mg1, mg2, mg3, g_out, sums_two = attention_out_back(
        seq.at(order), grad_two_in, after_attn, cot, gain_two_f, mixed, outs
    )
    mg2 = seq.at(mg2)
    g_w2, g_w3, proj2, proj3, sums_b = attention_back(
        seq.at(order), normed_one, qkvs[2:], lses[2:], (mg2, mg3), g_out, (2, 3), n_img, patches, factor, n
    )
    g_w3 = seq.land(g_w3, red_up, red_down, two_up, two_down)
    w_3 = Sent(core_swap(g_w3))
    two_up.launch()
    two_down.launch()
    seq.land((), w_3)
    middle = n // 2
    half_shape = (2,) * (len(bits) - 1)
    w_high = Sent(x_swap(seq.at(rounded_sum([g_w2[middle:], w_3.value[middle:]]))))
    g_w0, g_w1, proj0, proj1, sums_a = attention_back(
        seq.at(order), normed_one, qkvs[:2], lses[:2], (mg0, mg1), g_out, (0, 1), n_img, patches, factor, n
    )
    g_w1 = seq.land(g_w1, two_up, two_down, w_high)
    w_1 = Sent(core_swap(g_w1))
    two_up.launch()
    two_down.launch()
    seq.land((), w_1)
    red_w = Reduce(seq, (g_w0, w_1.value), n)
    red_w.launch(0, [w_high.value.reshape(half_shape + w_high.value.shape[1:])])
    w_low = Sent(x_swap(seq.at(rounded_sum([g_w2[:middle], w_3.value[:middle]]))))
    tokens_grad, sums_one = input_back(
        seq.at(order), x_zero, after_grad, gain_one_f, (proj0, proj1, proj2, proj3), qkv_parts
    )
    sums_one = seq.land(sums_one, two_up, two_down, red_w, w_low)
    red_w.terms = [*red_w.terms, w_low.value.reshape(half_shape + w_low.value.shape[1:])]
    while len(red_w.axes) > 2:
        red_w.launch()
        seq.land((), red_w)
    red_w.launch()
    two_up.terms[-1], two_down.terms[-1], sums_one = seq.at((two_up.terms[-1], two_down.terms[-1], sums_one))
    packed = pack_sums(
        order,
        n,
        rows,
        ffq,
        (sums_a, sums_b),
        (jnp.stack([g_bias_0, g_bias_1]), jnp.stack([g_bias_2, g_bias_3])),
        (sums_two, sums_one),
    )
    packed = seq.at(packed)
    peers = Sent([xor_swap(packed, "dp", 4, m) for m in (1, 2, 3)])
    crossing = jnp.stack([two_up.rest().piece(), two_down.rest().piece()])
    cross = Sent(x_swap(seq.at(crossing)))
    seq.land((), red_w)
    if red_w.axes:
        red_w.launch()
    seq.land((), peers, cross)
    owned = [
        rounded_sum([*red_up.rest().terms, cross.value[0]]),
        rounded_sum([*red_down.rest().terms, cross.value[1]]),
    ]
    mlp_spread = Spread(seq, jnp.stack(owned))
    sums = Reduce(seq, (packed, *peers.value), n, full)
    while len(sums.axes) > 1:
        sums.launch()
        if len(sums.axes) > 1:
            seq.land((), sums)
    seq.land((), *([sums, red_w] if len(bits) > 1 else []))
    w_spread = Spread(seq, red_w.piece())
    sums.launch()
    block, tokens_grad = seq.at((block, tokens_grad))
    block_out, grad_tokens = seq.land((compact(block), compact(tokens_grad)), sums, mlp_spread, w_spread)
    mlp_spread.cross()
    w_spread.cross()
    small_sums = seq.land(sums.piece(), mlp_spread, w_spread)
    out_fc1, out_fc2 = finish_mlp(q, mlp_spread.pieces, n)
    out_qkv, out_out = finish_attention(seq.value, w_spread.pieces)
    small_out = [small_sums[k, :rows] for k in range(8)]
    out_bfc1 = small_sums[8:12, :ffq].reshape(-1)
    o_bq, o_bv, o_bout, o_gone, o_sone, o_bfc2, o_gtwo, o_stwo = small_out
    return (
        block_out,
        grad_tokens,
        out_qkv,
        o_bq,
        o_bv,
        out_out,
        o_bout,
        o_gone,
        o_sone,
        out_fc1,
        out_bfc1,
        out_fc2,
        o_bfc2,
        o_gtwo,
        o_stwo,
    )


def solution(mesh):
    rows_split = P(("dp", "fsdp"), None)
    matrix = P("fsdp", None)
    vector = P("fsdp")
    return jax.shard_map(
        local,
        mesh=mesh,
        in_specs=(
            rows_split, P(("dp", "fsdp")), matrix, vector, vector, matrix, vector, vector, vector,
            matrix, vector, matrix, vector, vector, vector, rows_split,
        ),
        out_specs=(
            rows_split, rows_split, matrix, vector, vector, matrix, vector, vector, vector,
            matrix, vector, matrix, vector, vector, vector,
        ),
        check_vma=False,
    )
```

```python
import math

import jax
import jax.numpy as jnp
from jax import lax
from jax.experimental import pallas as pl
from jax.experimental.pallas import tpu as pltpu
from jax.sharding import PartitionSpec as P

HEADS = 16
GRID = 14
NSCALE = 16
norm_eps = 1e-06
half = jnp.bfloat16
full = jnp.float32


def xor_swap(value, axis, size, mask):
    return lax.ppermute(value, axis, [(i, i ^ mask) for i in range(size)])


def core_swap(value):
    return xor_swap(value, "dp", 4, 1)


def x_swap(value):
    return xor_swap(value, "dp", 4, 2)


def masks(bits):
    found = [0]
    for bit in bits:
        found = found + [m | (1 << bit) for m in found]
    return found


class Order:
    def __init__(self, value):
        self.value = value

    def at(self, value):
        value, self.value = lax.optimization_barrier((value, self.value))
        return value

    def land(self, value, *sent):
        value, flights = self.at((value, [s.flight for s in sent]))
        for s, flight in zip(sent, flights, strict=True):
            s.accept(flight)
        return value


class Sent:
    def __init__(self, flight):
        self.flight = flight

    def accept(self, value):
        self.value = value


class Gather:
    def __init__(self, seq, piece, n, bits):
        self.seq, self.held, self.n, self.bits = seq, piece[None], n, list(bits)

    def launch(self):
        self.held = self.seq.at(self.held)
        self.flight = xor_swap(self.held, "fsdp", self.n, 1 << self.bits.pop(0))

    def accept(self, value):
        self.got = value

    def join(self):
        self.held = jnp.concatenate([self.held, self.got])
        return self.held


def rounded_sum(terms, kind=half):
    return sum(t.astype(full) for t in terms).astype(kind)


class Reduce:
    def __init__(self, seq, terms, n, kind=half):
        self.kind = kind
        self.seq, self.n, self.axes = seq, n, list(range(n.bit_length() - 1))
        self.terms = [t.reshape((2,) * len(self.axes) + t.shape[1:]) for t in terms]

    def launch(self, bit=None, more=()):
        bit = self.axes[0] if bit is None else bit
        axis = self.axes.index(bit)
        self.axes.pop(axis)
        low, high = [
            [lax.index_in_dim(t, side, axis, keepdims=False) for t in self.terms] for side in (0, 1)
        ]
        self.terms = low
        self.flight = xor_swap(self.seq.at(rounded_sum([*high, *more], self.kind)), "fsdp", self.n, 1 << bit)

    def accept(self, value):
        self.terms = [*self.terms, value]

    def rest(self):
        while self.axes:
            self.launch()
            self.seq.land((), self)
        return self

    def piece(self):
        return rounded_sum(self.terms, self.kind)


class Spread:
    def __init__(self, seq, piece):
        self.seq, self.pieces = seq, [seq.at(piece)]
        self.flight = [core_swap(self.pieces[0]), x_swap(self.pieces[0])]

    def cross(self):
        self.flight = [core_swap(self.seq.at(self.pieces[2]))]

    def accept(self, value):
        self.pieces += value


ANYWHERE = pl.BlockSpec(memory_space=pl.ANY)
ON_CHIP = pl.BlockSpec(memory_space=pltpu.VMEM)
SCALARS = pl.BlockSpec(memory_space=pltpu.SMEM)


def dot(left, right, dim_left, dim_right):
    return lax.dot_general(
        left, right, (((dim_left,), (dim_right,)), ((), ())), preferred_element_type=full
    )


def call(kernel, name, operands, in_specs, outs, out_specs, scratch):
    return pl.pallas_call(
        kernel,
        out_shape=[jax.ShapeDtypeStruct(shape, kind) for shape, kind in outs],
        in_specs=in_specs,
        out_specs=out_specs,
        scratch_shapes=scratch,
        compiler_params=pltpu.CompilerParams(vmem_limit_bytes=58 * 2**20),
        name=name,
    )(*operands)


def loop(count, body, unroll=1):
    def step(i, carry):
        body(i)
        return carry

    lax.fori_loop(0, count, step, 0, unroll=unroll)


def tile(i, size):
    return pl.ds(pl.multiple_of(i * size, size), size)


def bring(src, dst, sem):
    pltpu.make_async_copy(src, dst, sem).start()


def arrived(dst, sem):
    pltpu.make_async_copy(dst, dst, sem).wait()


def fetch(parts, order_ref, place, sem):
    base = 0
    for part in parts:

        def start(r, part=part, base=base):
            shard = r if order_ref is None else order_ref[base + r]
            pltpu.make_async_copy(part.at[r], place(shard), sem).start()

        loop(part.shape[0], start)
        base += part.shape[0]


def head_rows(s, q, n, rows, quarter):
    per = n // 4
    return pl.multiple_of(((s // per) ^ q) * quarter + (s % per) * rows, rows)


def pair_scores(q2, k2):
    first = lax.broadcasted_iota(jnp.int32, q2.shape, 1) < q2.shape[1] // 2
    both = apart(q2, first)
    return both, dot(k2, both, 1, 1), first


def apart(value, first):
    zero = jnp.zeros_like(value)
    return jnp.concatenate([jnp.where(first, value, zero), jnp.where(first, zero, value)])


def attention_forward(order, normed, bias, weights, n_img, patches, factor):
    groups, n_parts = len(weights), len(weights[0])
    wide = weights[0][0].shape[2]
    count, width = normed.shape
    rows = width // sum(part.shape[0] for part in weights[0])
    padded = count // n_img
    quarter = wide // 3

    def kernel(order_ref, normed_ref, bias_ref, *refs):
        w_refs, refs = refs[: groups * n_parts], refs[groups * n_parts :]
        qkv_refs, mixed_refs, refs = refs[:groups], refs[groups : 2 * groups], refs[2 * groups :]
        lse_refs, (w_held, sems) = refs[:groups], refs[groups:]
        for g in range(groups):
            fetch(
                [w.at[:, pl.ds(0, rows)] for w in w_refs[g * n_parts : (g + 1) * n_parts]],
                order_ref,
                lambda s, g=g: w_held.at[g, pl.ds(pl.multiple_of(s * rows, rows), rows)],
                sems.at[g],
            )
        for g in range(groups):
            pltpu.make_async_copy(w_held.at[g], w_held.at[g], sems.at[g]).wait()

            def project(t, g=g):
                at = tile(t, quarter)
                product = dot(normed_ref[...], w_held[g, :, at], 1, 0)
                qkv_refs[g][:, at] = (product + bias_ref[g, :, at]).astype(half)

            loop(3, project)

            def attend(i, g=g):
                at = tile(i // 2, padded)
                lanes = [pl.ds(pl.multiple_of(t * quarter + (i % 2) * 128, 128), 128) for t in range(3)]
                q2 = qkv_refs[g][at, lanes[0]] * factor
                k2 = qkv_refs[g][at, lanes[1]]
                v2 = qkv_refs[g][at, lanes[2]]
                _, scores, first = pair_scores(q2, k2)
                key = lax.broadcasted_iota(jnp.int32, scores.shape, 0)
                scores = jnp.where(key < patches, scores, -1e30)
                top = jnp.max(scores, axis=0, keepdims=True)
                raised = jnp.exp(scores - top)
                total = jnp.sum(raised, axis=0, keepdims=True)
                lse_refs[g][i] = top + jnp.log(total)
                out = dot((raised * (1.0 / total)).astype(half), v2, 0, 0)
                mixed_refs[g][at, lanes[0]] = jnp.where(first, out[:padded], out[padded:]).astype(half)

            loop(2 * n_img, attend, 2 * n_img)

    return call(
        kernel,
        "attention_forward",
        (order, normed, bias, *(part for w in weights for part in w)),
        [SCALARS, ON_CHIP, ON_CHIP] + [ANYWHERE] * (groups * n_parts),
        [((count, wide), half)] * groups
        + [((count, quarter), half)] * groups
        + [((2 * n_img, 1, 2 * padded), full)] * groups,
        [ON_CHIP] * (3 * groups),
        [pltpu.VMEM((groups, width, wide), half), pltpu.SemaphoreType.DMA((groups,))],
    )


def layer_norm(value, gain, shift):
    center = jnp.mean(value, axis=-1, keepdims=True)
    offset = value - center
    spread = jnp.mean(offset * offset, axis=-1, keepdims=True)
    return offset * lax.rsqrt(spread + norm_eps) * gain + shift


def layer_norm_back(value, grad, gain):
    center = jnp.mean(value, axis=-1, keepdims=True)
    offset = value - center
    scale = lax.rsqrt(jnp.mean(offset * offset, axis=-1, keepdims=True) + norm_eps)
    unit = offset * scale
    scaled = grad * gain
    inner = jnp.mean(scaled * unit, axis=-1, keepdims=True)
    return scale * (scaled - jnp.mean(scaled, axis=-1, keepdims=True) - unit * inner), grad * unit


def load_out(order_ref, out_refs, held, sem, n, rows, quarter):
    q = order_ref[n]
    for j in range(4):
        column = pl.multiple_of((q ^ j) * quarter, quarter)
        fetch(
            [out_refs[j % 2].at[:, :, pl.ds(j // 2 * quarter, quarter)]],
            order_ref,
            lambda s, column=column: held.at[
                pl.ds(head_rows(s, q, n, rows, quarter), rows), pl.ds(column, quarter)
            ],
            sem,
        )


CHUNK = 16
ROWS = 64


def attention_out(order, x_zero, mixed, outs, bias, gain, shift):
    count, width = x_zero.shape
    n, rows, _ = outs[0].shape
    quarter = mixed[0].shape[1]

    def kernel(order_ref, x_ref, bias_ref, gain_ref, shift_ref, *refs):
        mixed_refs, out_refs = refs[:4], refs[4:6]
        after_ref, normed_ref, held, x_held, sems = refs[6:]
        bring(x_ref, x_held, sems.at[1])
        load_out(order_ref, out_refs, held, sems.at[0], n, rows, quarter)
        together = jnp.concatenate([m[...] for m in mixed_refs], axis=1)
        pltpu.make_async_copy(held, held, sems.at[0]).wait()
        after_ref[...] = dot(together, held[...], 1, 0)
        arrived(x_held, sems.at[1])

        def finish(i):
            at = tile(i, CHUNK)
            after = x_held[at] + (after_ref[at] + bias_ref[...])
            after_ref[at] = after
            normed_ref[at] = layer_norm(after, gain_ref[...], shift_ref[...]).astype(half)

        loop(count // CHUNK, finish, 13)

    return call(
        kernel,
        "attention_out",
        (order, x_zero, bias, gain, shift, *mixed, *outs),
        [SCALARS, ANYWHERE] + [ON_CHIP] * 7 + [ANYWHERE] * 2,
        [((count, width), full), ((count, width), half)],
        [ON_CHIP] * 2,
        [
            pltpu.VMEM((width, width), half),
            pltpu.VMEM((count, width), full),
            pltpu.SemaphoreType.DMA((2,)),
        ],
    )


def mlp(order, normed, cot, bias, up_all, down_all, down_start, carried=None, ending=None):
    count, width = normed.shape
    n, rows, _ = up_all.shape
    hidden = bias.shape[1]
    share = hidden // n
    step = min(512, hidden)
    steps = hidden // step
    more = [*(carried or []), *(ending[:1] if ending else [])]
    last = list(ending[1:]) if ending else []

    def kernel(order_ref, bias_ref, *refs):
        last_refs, refs = refs[: len(last)], refs[len(last) :]
        normed_ref, cot_ref, up_ref, down_ref, refs = *refs[:4], refs[4:]
        more_refs, refs = refs[: len(more)], refs[len(more) :]
        g_up_ref, g_down_ref, g_bias_ref, back_ref, end_ref, refs = *refs[:5], refs[5:]
        held, refs = refs[: len(more)], refs[len(more) :]
        rows_in, cots, out, back, up, down, pre, act, act_half, pre_half, g_up, g_down, sems = refs
        bring(normed_ref, rows_in, sems.at[3])
        fetch(
            [up_ref.at[:, :, pl.ds(0, hidden)]],
            None,
            lambda s: up.at[pl.ds(pl.multiple_of(s * rows, rows), rows)],
            sems.at[0],
        )
        bring(cot_ref, cots, sems.at[4])
        fetch(
            [down_ref.at[:, :, pl.ds(down_start, width)]],
            None,
            lambda s: down.at[pl.ds(pl.multiple_of(s * share, share), share)],
            sems.at[1],
        )
        for k in range(len(more)):
            bring(more_refs[k], held[k], sems.at[5 + k])
        arrived(rows_in, sems.at[3])
        arrived(up, sems.at[0])
        for t in range(steps):
            at = pl.ds(t * step, step)
            pre[...] = dot(rows_in[...], up[:, at], 1, 0)
            if not t:
                arrived(cots, sems.at[4])
                arrived(down, sems.at[1])
            act[...] = dot(cots[...], down[at, :], 1, 1)

            def gelu(i, at=at):
                some = tile(i, 2 * CHUNK)
                x = pre[some] + bias_ref[:, at]
                below = 0.5 * (1.0 + lax.erf(x * math.sqrt(0.5)))
                density = jnp.exp(-0.5 * x * x) * (1.0 / math.sqrt(2.0 * math.pi))
                act_half[some] = (x * below).astype(half)
                pre_half[some] = (act[some] * (below + x * density)).astype(half)

            loop(count // CHUNK // 2, gelu)
            p = pre_half[...]
            h = act_half[...]
            more_back = dot(p, up[:, at], 1, 1)
            more_out = dot(h, down[at, :], 1, 0)
            if t:
                back[...] += more_back
                out[...] += more_out
            elif carried:
                arrived(held[0], sems.at[5])
                arrived(held[1], sems.at[6])
                out[...] = held[0][...] + more_out
                back[...] = held[1][...] + more_back
            else:
                out[...] = more_out
                back[...] = more_back
            if t == steps - 1:
                bring(back, back_ref, sems.at[3])
                if not ending:
                    bring(out, end_ref, sems.at[4])
            g_down[at, :] = dot(h, cots[...], 0, 0).astype(half)
            if t == steps - 1:

                def send_down(r):
                    at = pl.multiple_of(order_ref[r] * share, share)
                    bring(g_down.at[pl.ds(at, share)], g_down_ref.at[r], sems.at[2])

                loop(n, send_down)
            g_up[:, at] = dot(rows_in[...], p, 0, 0).astype(half)
            g_bias_ref[:, at] = jnp.sum(p.astype(full), axis=0, keepdims=True)

        def send_up(r):
            at = pl.multiple_of(order_ref[r] * rows, rows)
            bring(g_up.at[pl.ds(at, rows)], g_up_ref.at[r], sems.at[0])

        loop(n, send_up)
        if ending:
            arrived(held[2], sems.at[7])

            def finish(i):
                at = tile(i, 2 * CHUNK)
                end_ref[at] = (held[2][at] + (out[at] + last_refs[0][...])).astype(half)

            loop(count // CHUNK // 2, finish)
        else:
            arrived(end_ref, sems.at[4])
        arrived(back_ref, sems.at[3])
        arrived(g_down_ref, sems.at[2])
        arrived(g_up_ref, sems.at[0])

    sums = pltpu.VMEM((count, width), full)
    wide = pltpu.VMEM((count, width), half)
    square = pltpu.VMEM((width, hidden), half)
    return call(
        kernel,
        "mlp",
        (order, bias, *last, normed, cot, up_all, down_all, *more),
        [SCALARS] + [ON_CHIP] * (1 + len(last)) + [ANYWHERE] * (4 + len(more)),
        [
            ((n, rows, hidden), half),
            ((n, share, width), half),
            ((1, hidden), full),
            ((count, width), full),
            ((count, width), half if ending else full),
        ],
        [ANYWHERE, ANYWHERE, ON_CHIP, ANYWHERE, ON_CHIP if ending else ANYWHERE],
        [
            *([sums] * len(more)),
            wide,
            wide,
            sums,
            sums,
            square,
            pltpu.VMEM((hidden, width), half),
            pltpu.VMEM((count, step), full),
            pltpu.VMEM((count, step), full),
            pltpu.VMEM((count, step), half),
            pltpu.VMEM((count, step), half),
            square,
            pltpu.VMEM((hidden, width), half),
            pltpu.SemaphoreType.DMA((5 + len(more),)),
        ],
    )


def attention_out_back(order, grad, after, cot, gain, mixed, outs):
    count, width = after.shape
    n, rows, _ = outs[0].shape
    quarter = mixed[0].shape[1]

    def kernel(order_ref, grad_ref, after_ref, cot_ref, gain_ref, *refs):
        mixed_refs, out_refs, refs = refs[:4], refs[4:6], refs[6:]
        after_grad_ref, mixed_grad_refs, g_out_ref, sums_ref = refs[0], refs[1:5], refs[5], refs[6]
        held, branch, terms, grad, after, cot, mixes, sems = refs[7:]
        block = count // 4
        for k in range(4):
            some = pl.ds(k * block, block)
            bring(grad_ref.at[some], grad.at[some], sems.at[1 + k])
            bring(after_ref.at[some], after.at[some], sems.at[5 + k])
            bring(cot_ref.at[some], cot.at[some], sems.at[9 + k])
        load_out(order_ref, out_refs, held, sems.at[0], n, rows, quarter)
        for j in range(4):
            bring(mixed_refs[j], mixes.at[j], sems.at[13])
        terms[...] = jnp.zeros_like(terms)

        def fold(value):
            return jnp.sum(value.reshape(CHUNK // 8, 8, width), axis=0)

        def back(i, k):
            at = pl.ds(pl.multiple_of(k * block + i * CHUNK, CHUNK), CHUNK)
            incoming = grad[at]
            part, gain_terms = layer_norm_back(after[at], incoming, gain_ref[...])
            own = cot[at].astype(full)
            total = own + part
            after_grad_ref[at] = total
            rounded = total.astype(half)
            branch[at] = rounded
            terms[0] += fold(rounded.astype(full))
            terms[1] += fold(gain_terms)
            terms[2] += fold(incoming)
            terms[3] += fold(own)

        for k in range(4):
            some = pl.ds(k * block, block)
            arrived(grad.at[some], sems.at[1 + k])
            arrived(after.at[some], sems.at[5 + k])
            arrived(cot.at[some], sems.at[9 + k])
            loop(block // CHUNK, lambda i, k=k: back(i, k), 13)
        for k in range(4):
            sums_ref[k] = jnp.sum(terms[k], axis=0, keepdims=True)
        arrived(held, sems.at[0])
        arrived(mixes, sems.at[13])
        for j in range(4):
            mixed_grad_refs[j][...] = dot(branch[...], held[j * quarter : (j + 1) * quarter], 1, 1).astype(half)
            g_out_ref[j * quarter : (j + 1) * quarter] = dot(mixes[j], branch[...], 0, 0).astype(half)

    return call(
        kernel,
        "attention_out_back",
        (order, grad, after, cot, gain, *mixed, *outs),
        [SCALARS] + [ANYWHERE] * 3 + [ON_CHIP] + [ANYWHERE] * 6,
        [((count, width), full)]
        + [((count, quarter), half)] * 4
        + [((width, width), half), ((4, 1, width), full)],
        [ON_CHIP] * 7,
        [
            pltpu.VMEM((width, width), half),
            pltpu.VMEM((count, width), half),
            pltpu.VMEM((4, 8, width), full),
            pltpu.VMEM((count, width), full),
            pltpu.VMEM((count, width), full),
            pltpu.VMEM((count, width), half),
            pltpu.VMEM((4, count, quarter), half),
            pltpu.SemaphoreType.DMA((14,)),
        ],
    )


def attention_back(order, normed, qkvs, lses, mixed_grads, g_out, which, n_img, patches, factor, n):
    groups = len(qkvs)
    count, width = normed.shape
    wide = qkvs[0].shape[1]
    quarter = wide // 3
    padded = count // n_img
    rows = width // n

    def kernel(order_ref, normed_ref, g_out_ref, *refs):
        qkv_refs, mg_refs, refs = refs[:groups], refs[groups : 2 * groups], refs[2 * groups :]
        lse_refs, refs = refs[:groups], refs[groups:]
        g_w_refs, proj_refs, sums_ref = refs[:groups], refs[groups : 2 * groups], refs[2 * groups]
        g_w, normed_held, g_out_held, sems = refs[2 * groups + 1 :]
        q = order_ref[n]
        bring(g_out_ref, g_out_held, sems.at[groups])
        bring(normed_ref, normed_held, sems.at[groups + 1])
        for g in range(groups):

            def attend(i, g=g):
                at = tile(i // 2, padded)
                lanes = [pl.ds(pl.multiple_of(t * quarter + (i % 2) * 128, 128), 128) for t in range(3)]
                q2 = qkv_refs[g][at, lanes[0]] * factor
                k2 = qkv_refs[g][at, lanes[1]]
                v2 = qkv_refs[g][at, lanes[2]]
                both, scores, first = pair_scores(q2, k2)
                key = lax.broadcasted_iota(jnp.int32, scores.shape, 0)
                probs = jnp.where(key < patches, jnp.exp(scores - lse_refs[g][i]), 0.0)
                o_both = apart(mg_refs[g][at, lanes[0]], first)
                g_probs = dot(v2, o_both, 1, 1)
                weighted = jnp.sum(probs * g_probs, axis=0, keepdims=True)
                g_scores = (probs * (g_probs - weighted)).astype(half)
                g_query = dot(g_scores, k2, 0, 0)
                g_query = jnp.where(first, g_query[:padded], g_query[padded:]) * factor
                proj_refs[g][at, lanes[0]] = g_query.astype(half)
                proj_refs[g][at, lanes[1]] = dot(g_scores, both, 1, 0).astype(half)
                proj_refs[g][at, lanes[2]] = dot(probs.astype(half), o_both, 1, 0).astype(half)

            loop(2 * n_img, attend, 4)
            if not g:
                arrived(g_out_held, sems.at[groups])
                arrived(normed_held, sems.at[groups + 1])

            def send_out(r, g=g):
                at = head_rows(order_ref[r], q, n, rows, quarter)
                column = pl.multiple_of((q ^ which[g]) * quarter, quarter)
                pltpu.make_async_copy(
                    g_out_held.at[pl.ds(at, rows), pl.ds(column, quarter)],
                    g_w_refs[g].at[r, :, pl.ds(wide, quarter)],
                    sems.at[g],
                ).start()

            loop(n, send_out)

            def weigh(t, g=g):
                at = tile(t, quarter)
                some = proj_refs[g][:, at]
                g_w[g, :, at] = dot(normed_held[...], some, 0, 0).astype(half)
                sums_ref[g, :, at] = jnp.sum(some.astype(full), axis=0, keepdims=True)

            loop(3, weigh)

            def send(r, g=g):
                at = pl.multiple_of(order_ref[r] * rows, rows)
                pltpu.make_async_copy(
                    g_w.at[g, pl.ds(at, rows)], g_w_refs[g].at[r, :, pl.ds(0, wide)], sems.at[g]
                ).start()

            loop(n, send)
        for g in range(groups):
            pltpu.make_async_copy(g_w_refs[g], g_w_refs[g], sems.at[g]).wait()

    return call(
        kernel,
        "attention_back",
        (order, normed, g_out, *qkvs, *mixed_grads, *lses),
        [SCALARS] + [ANYWHERE] * 2 + [ON_CHIP] * (3 * groups),
        [((n, rows, wide + quarter), half)] * groups
        + [((count, wide), half)] * groups
        + [((groups, 1, wide), full)],
        [ANYWHERE] * groups + [ON_CHIP] * (groups + 1),
        [
            pltpu.VMEM((groups, width, wide), half),
            pltpu.VMEM((count, width), half),
            pltpu.VMEM((width, width), half),
            pltpu.SemaphoreType.DMA((groups + 2,)),
        ],
    )


def input_back(order, x_zero, after_grad, gain, projs, weights):
    count, width = x_zero.shape
    wide = weights[0][0].shape[2]
    rows = width // sum(part.shape[0] for part in weights[0])
    parts = [part for w in weights for part in w]
    n_parts = len(weights[0])

    def kernel(order_ref, x_ref, after_ref, gain_ref, *refs):
        proj_refs, w_refs = refs[:4], refs[4 : 4 + len(parts)]
        token_ref, sums_ref, held, terms, x_held, after_held, sems = refs[4 + len(parts) :]
        for j in range(4):
            fetch(
                [w.at[:, pl.ds(0, rows)] for w in w_refs[j * n_parts : (j + 1) * n_parts]],
                order_ref,
                lambda s, j=j: held.at[j, pl.ds(pl.multiple_of(s * rows, rows), rows)],
                sems.at[j],
            )
        bring(x_ref, x_held, sems.at[4])
        bring(after_ref, after_held, sems.at[5])
        for j in range(4):
            arrived(held.at[j], sems.at[j])
            product = dot(proj_refs[j][...], held[j], 1, 1)
            if j == 0:
                token_ref[...] = product
            else:
                token_ref[...] += product
        arrived(x_held, sems.at[4])
        arrived(after_held, sems.at[5])
        terms[...] = jnp.zeros_like(terms)

        def fold(value):
            return jnp.sum(value.reshape(ROWS // 8, 8, width), axis=0)

        def back(i):
            at = tile(i, ROWS)
            incoming = token_ref[at]
            part, gain_terms = layer_norm_back(x_held[at], incoming, gain_ref[...])
            token_ref[at] = after_held[at] + part
            terms[0] += fold(gain_terms)
            terms[1] += fold(incoming)

        loop(count // ROWS, back)
        for k in range(2):
            sums_ref[k] = jnp.sum(terms[k], axis=0, keepdims=True)

    return call(
        kernel,
        "input_back",
        (order, x_zero, after_grad, gain, *projs, *parts),
        [SCALARS] + [ANYWHERE] * 2 + [ON_CHIP] * 5 + [ANYWHERE] * len(parts),
        [((count, width), full), ((2, 1, width), full)],
        [ON_CHIP] * 2,
        [
            pltpu.VMEM((4, width, wide), half),
            pltpu.VMEM((2, 8, width), full),
            pltpu.VMEM((count, width), full),
            pltpu.VMEM((count, width), full),
            pltpu.SemaphoreType.DMA((6,)),
        ],
    )


def payloads(which, w_fc1, w_fc2):
    rows, ff = w_fc1.shape
    full_share, width = w_fc2.shape
    share = full_share // 4
    n = ff // full_share
    hidden = n * share
    own, across = which
    if share % 128:
        fc1 = [lax.dynamic_slice(w_fc1, (0, (4 * s + own) * share), (rows, share)) for s in range(n)]
        fc2 = [lax.dynamic_slice(w_fc2, (g * share, 0), (share, width)).astype(half) for g in which]
        rest = jnp.concatenate([*fc1, fc2[0].reshape(rows, -1).astype(full)], axis=1)
        return rest.astype(half), fc2[1]

    def kernel(which_ref, fc1_ref, fc2_ref, rest_ref, two_ref):
        for s in range(n):
            at = pl.ds(pl.multiple_of((4 * s + which_ref[0]) * share, share), share)
            rest_ref[:, s * share : (s + 1) * share] = fc1_ref[:, at].astype(half)
        rest_ref[:, hidden : hidden + width] = fc2_ref[tile(which_ref[0], share), :].astype(half)
        two_ref[...] = fc2_ref[tile(which_ref[1], share), :].astype(half)

    return call(
        kernel,
        "payloads",
        (jnp.stack(which), w_fc1, w_fc2),
        [SCALARS] + [ON_CHIP] * 2,
        [((rows, hidden + width), half), ((share, width), half)],
        [ON_CHIP] * 2,
        [],
    )


def natural_quarters(q, pieces):
    once = [jnp.where((q & 1) == 1, pieces[i ^ 1], pieces[i]) for i in range(4)]
    return [jnp.where(q >= 2, once[i ^ 2], once[i]) for i in range(4)]


def finish_mlp(q, pieces, n):
    _, rows, width = pieces[0].shape
    share = width // n
    if share % 128:
        pieces = natural_quarters(q, pieces)
        fc1 = jnp.stack([p[0].reshape(rows, n, share) for p in pieces], axis=2).reshape(rows, 4 * width)
        return fc1.astype(full), jnp.concatenate([p[1] for p in pieces]).astype(full)

    def kernel(q_ref, *refs):
        fc1_ref, fc2_ref = refs[4:]
        for j in range(4):
            g = q_ref[0] ^ j
            for s in range(n):
                at = pl.ds(pl.multiple_of((4 * s + g) * share, share), share)
                fc1_ref[:, at] = refs[j][0, :, s * share : (s + 1) * share].astype(full)
            fc2_ref[tile(g, rows), :] = refs[j][1].astype(full)

    return call(
        kernel,
        "finish_mlp",
        (q[None], *pieces),
        [SCALARS] + [ON_CHIP] * 4,
        [((rows, 4 * width), full), ((4 * rows, width), full)],
        [ON_CHIP] * 2,
        [],
    )


def finish_attention(q, pieces):
    rows, width = pieces[0].shape
    quarter = width // 4

    def kernel(q_ref, *refs):
        qkv_ref, out_ref = refs[4:]
        for j in range(4):
            g = q_ref[0] ^ j
            for t in range(3):
                at = pl.ds(pl.multiple_of(t * width + g * quarter, quarter), quarter)
                qkv_ref[:, at] = refs[j][:, t * quarter : (t + 1) * quarter].astype(full)
            out_ref[:, tile(g, quarter)] = refs[j][:, 3 * quarter :].astype(full)

    return call(
        kernel,
        "finish_attention",
        (q[None], *pieces),
        [SCALARS] + [ON_CHIP] * 4,
        [((rows, 3 * width), full), ((rows, width), full)],
        [ON_CHIP] * 2,
        [],
    )


BELOW = 16


def first_payload(q, w_qkv, vectors):
    rows, columns = w_qkv.shape
    width = columns // 3
    quarter = width // 4
    wide = 3 * quarter

    def kernel(q_ref, w_ref, *refs):
        out_ref, held, low, sem = refs[len(vectors) :]
        for t in range(3):
            at = pl.multiple_of(t * width + q_ref[0] * quarter, quarter)
            pltpu.make_async_copy(
                w_ref.at[:, pl.ds(at, quarter)], held.at[:, pl.ds(t * quarter, quarter)], sem.at[0]
            ).start()
        low[...] = jnp.zeros_like(low)
        for k, vector in enumerate(refs[: len(vectors)]):
            low[k : k + 1, : vector.shape[1]] = vector[...]
        out_ref[rows:] = low[...].astype(half)
        pltpu.make_async_copy(held, held, sem.at[0]).wait()
        out_ref[:rows] = held[...].astype(half)

    return call(
        kernel,
        "first_payload",
        (q[None], w_qkv, *(v[None] for v in vectors)),
        [SCALARS, ANYWHERE] + [ON_CHIP] * len(vectors),
        [((rows + BELOW, wide), half)],
        [ON_CHIP],
        [pltpu.VMEM((rows, wide), full), pltpu.VMEM((BELOW, wide), full), pltpu.SemaphoreType.DMA((1,))],
    )[0]


def unpack_vectors(order, parts, n, rows, share):
    width = n * rows
    quarter = width // 4
    if rows % 128 or share % 128:
        q = order[n]
        held = jnp.concatenate([p[:, rows:] for p in parts]).astype(full)
        held = held[jnp.zeros((n,), jnp.int32).at[order[:n]].set(jnp.arange(n, dtype=jnp.int32))]
        groups = jnp.arange(4, dtype=jnp.int32) ^ q
        vectors = jnp.stack([held[:, k, :rows].reshape(1, width) for k in range(8)])
        units = held[:, 8, : 4 * share].reshape(n, 4, share).transpose(1, 0, 2)[groups]
        ends = [vectors[k].reshape(4, 1, quarter)[groups] for k in range(2)]
        return vectors, units.reshape(4, 1, width), jnp.concatenate([ends[0], 0 * ends[0], ends[1]], axis=2)

    def kernel(order_ref, *refs):
        part_refs, (vector_ref, fc1_ref, qkv_ref, held, wider, sem) = refs[: len(parts)], refs[len(parts) :]
        base = 0
        for part in part_refs:
            size = part.shape[0]
            pltpu.make_async_copy(part.at[:, pl.ds(rows, BELOW)], held.at[pl.ds(base, size)], sem.at[0]).start()
            base += size
        pltpu.make_async_copy(held, held, sem.at[0]).wait()
        wider[...] = held[...].astype(full)
        q = order_ref[n]
        for r in range(n):
            at = tile(order_ref[r], rows)
            for k in range(8):
                vector_ref[k, :, at] = wider[r, k : k + 1, :rows]
            for j in range(4):
                fc1_ref[j, :, tile(order_ref[r], share)] = wider[r, 8:9, tile(q ^ j, share)]
        for j in range(4):
            at = tile(q ^ j, quarter)
            qkv_ref[j, :, :quarter] = vector_ref[0, :, at]
            qkv_ref[j, :, quarter : 2 * quarter] = jnp.zeros((1, quarter), full)
            qkv_ref[j, :, 2 * quarter :] = vector_ref[1, :, at]

    return call(
        kernel,
        "unpack_vectors",
        (order, *parts),
        [SCALARS] + [ANYWHERE] * len(parts),
        [((8, 1, width), full), ((4, 1, width), full), ((4, 1, 3 * quarter), full)],
        [ON_CHIP] * 3,
        [
            pltpu.VMEM((n, BELOW, 3 * quarter), half),
            pltpu.VMEM((n, BELOW, 3 * quarter), full),
            pltpu.SemaphoreType.DMA((1,)),
        ],
    )


def pack_sums(order, n, rows, share, proj_sums, unit_sums, wide_sums):
    width = n * rows
    quarter = width // 4
    if rows % 128 or share % 128:
        groups = jnp.arange(4, dtype=jnp.int32) ^ order[n]
        proj = jnp.concatenate(proj_sums)[groups]
        units = jnp.concatenate(unit_sums)[groups].reshape(4, n, share)
        flat = [proj[:, :, :quarter].reshape(width), proj[:, :, 2 * quarter :].reshape(width)]
        two, one = wide_sums
        flat += [two[0], one[0], one[1], two[3], two[1], two[2]]
        flat = [v.reshape(n, 1, rows) for v in flat]
        stacked = [jnp.pad(v, ((0, 0), (0, 0), (0, 128 - rows))) for v in flat]
        stacked.append(jnp.pad(units.transpose(1, 0, 2), ((0, 0), (0, 4), (0, 128 - share))))
        return jnp.concatenate(stacked, axis=1)[order[:n]]

    def kernel(order_ref, proj_a, proj_b, unit_a, unit_b, two_ref, one_ref, out_ref, proj, units):
        proj[:2], proj[2:] = proj_a[...], proj_b[...]
        units[:2], units[2:] = unit_a[...], unit_b[...]
        q = order_ref[n]
        per = n // 4
        for r in range(n):
            s = order_ref[r]
            j = (s // per) ^ q
            at = tile(s, rows)
            inside = pl.multiple_of((s % per) * rows, rows)
            out_ref[r, 0:1] = proj[j, :, pl.ds(inside, rows)]
            out_ref[r, 1:2] = proj[j, :, pl.ds(2 * quarter + inside, rows)]
            for k, (ref, row) in enumerate(
                ((two_ref, 0), (one_ref, 0), (one_ref, 1), (two_ref, 3), (two_ref, 1), (two_ref, 2))
            ):
                out_ref[r, 2 + k : 3 + k] = ref[row, :, at]
            for g in range(4):
                out_ref[r, 8 + g : 9 + g] = units[q ^ g, :, tile(s, share)]
            out_ref[r, 12:] = jnp.zeros((4, rows), full)

    sums_two, sums_one = wide_sums
    return call(
        kernel,
        "pack_sums",
        (order, *proj_sums, *unit_sums, sums_two, sums_one),
        [SCALARS] + [ON_CHIP] * 6,
        [((n, 16, rows), full)],
        [ON_CHIP],
        [pltpu.VMEM((4, 1, 3 * quarter), full), pltpu.VMEM((4, 1, width), full)],
    )[0]


def table(codes, width):
    ratio = 0.3 * jnp.exp(codes.astype(full) * (math.log(10.0 / 0.3) / (NSCALE - 1)))
    quarter = width // 4
    omega = jnp.exp(jnp.arange(quarter).astype(full) * (-math.log(10000.0) / quarter))
    steps = jnp.arange(GRID, dtype=jnp.int32).astype(full)
    angle = ratio[:, None, None] * steps[None, :, None] * omega[None, None, :]
    return jnp.concatenate([jnp.sin(angle), jnp.cos(angle)], axis=-1)


def local(
    tokens,
    scale_codes,
    w_qkv,
    b_q,
    b_v,
    w_out,
    b_out,
    gain_one,
    shift_one,
    w_fc1,
    b_fc1,
    w_fc2,
    b_fc2,
    gain_two,
    shift_two,
    cotangent,
):
    n = lax.axis_size("fsdp")
    q = lax.axis_index("dp")
    f = lax.axis_index("fsdp")
    row_count, width = tokens.shape
    rows = width // n
    ff = b_fc1.shape[0] * n
    ffq = ff // n // 4
    hidden = n * ffq
    quarter = width // 4
    n_img = scale_codes.shape[0]
    patches = row_count // n_img
    padded = -(-patches // 16) * 16
    factor = 1.0 / math.sqrt(width // HEADS)
    seq = Order(q)
    bits = list(reversed(range(n.bit_length() - 1)))
    near = min(1, len(bits) - 1)
    shard_order = jnp.asarray(masks(bits), jnp.int32) ^ f
    group_order = jnp.arange(4, dtype=jnp.int32) ^ q
    order = jnp.concatenate([shard_order, q[None]])

    def last_three(chain):
        while len(chain.bits) > 3:
            chain.launch()
            seq.land((), chain)
            chain.join()
        return chain

    small = [b_q, b_v, b_out, gain_one, shift_one, b_fc2, gain_two, shift_two, b_fc1]
    qkv = last_three(Gather(seq, first_payload(q, w_qkv, small), n, bits))
    qkv.launch()
    rest_own, two_own = payloads([seq.at(q), q ^ 2], w_fc1, w_fc2)
    rest_own, two_own = seq.land((rest_own, two_own), qkv)
    rest = Sent(lax.all_gather(rest_own, "fsdp", axis=0, tiled=False))
    two = Sent(lax.all_gather(two_own, "fsdp", axis=0, tiled=False))
    out_own = [lax.dynamic_slice(w_out, (0, g * quarter), (rows, quarter)) for g in (q, q ^ 2)]
    out = last_three(Gather(seq, jnp.concatenate(out_own, axis=1).astype(half), n, bits))

    def spread_rows(value):
        split = value.reshape(n_img, patches, width)
        return jnp.pad(split, ((0, 0), (0, padded - patches), (0, 0)))

    def compact(value):
        return value.reshape(n_img, padded, width)[:, :patches].reshape(row_count, width)

    qkv.join()
    qkv.launch()
    spread_tokens = seq.land(spread_rows(seq.at(tokens)), qkv)
    qkv_near = qkv.join()
    qkv.launch()
    near_b, near_c = Sent(core_swap(qkv.held)), Sent(x_swap(qkv.held))
    out.launch()
    places = table(scale_codes, width)
    row_place = jnp.broadcast_to(places[:, :, None], (n_img, GRID, GRID, width // 2))
    col_place = jnp.broadcast_to(places[:, None], (n_img, GRID, GRID, width // 2))
    place = jnp.concatenate([row_place, col_place], axis=-1).reshape(n_img, patches, width)
    place = jnp.pad(place, ((0, 0), (0, padded - patches), (0, 0)))
    x_zero = (seq.at(spread_tokens).astype(full) + place).reshape(-1, width)
    x_zero = seq.land(x_zero, qkv, near_b, out)
    qkv_far = seq.at(qkv.got)
    far_b, far_c = Sent(core_swap(qkv_far)), Sent(x_swap(qkv_far))
    out.join()
    out.launch()
    vectors, bias_fc1, bias_qkv = unpack_vectors(seq.at(order), (qkv_near, qkv_far), n, rows, ffq)
    _, _, full_bout, gain_one_f, shift_one_f, full_bfc2, gain_two_f, shift_two_f = vectors
    normed_one = layer_norm(x_zero, gain_one_f, shift_one_f).astype(half)
    normed_one = seq.land(normed_one, far_b)

    first = attention_forward(
        seq.at(order), normed_one, bias_qkv[:2], ((qkv_near, qkv_far), (near_b.value, far_b.value)),
        n_img, patches, factor,
    )
    first = (seq.land(first[0], near_c, far_c, out), *first[1:])
    near_c, far_c = seq.at((near_c.value, far_c.value))
    near_d, far_d = Sent(core_swap(near_c)), Sent(core_swap(far_c))
    out.join()
    out.launch()
    cot = seq.land(spread_rows(cotangent).reshape(-1, width), near_d, far_d)
    second = attention_forward(
        seq.at(order), normed_one, bias_qkv[2:], ((near_c, far_c), (near_d.value, far_d.value)),
        n_img, patches, factor,
    )
    second = (seq.land(second[0], out, rest), *second[1:])
    out_a = seq.at(out.join())
    out_b = Sent(core_swap(out_a))
    seq.land((), out_b)
    rest_a = seq.at(rest.value)
    rest_b = Sent(core_swap(rest_a))
    up_c = Sent(x_swap(seq.at(rest_a[:, :, :hidden])))
    outs = (out_a, out_b.value)
    qkv_parts = (
        (qkv_near, qkv_far), (near_b.value, far_b.value), (near_c, far_c), (near_d.value, far_d.value)
    )
    qkvs = (*first[:2], *second[:2])
    mixed = (*first[2:4], *second[2:4])
    lses = (*first[4:], *second[4:])
    after_attn, normed_two = attention_out(
        seq.at(order), x_zero, mixed, outs, full_bout, gain_two_f, shift_two_f
    )
    normed_two = seq.land(normed_two, rest_b)

    up_g1, down_g1, g_bias_1, back_sum, out_sum = mlp(
        seq.at(order), normed_two, cot, bias_fc1[1], rest_b.value, rest_b.value, hidden
    )
    up_g0, down_g0, g_bias_0, back_sum, out_sum = mlp(
        order, normed_two, cot, bias_fc1[0], rest_a, rest_a, hidden, (out_sum, back_sum)
    )
    up_g0 = seq.land(up_g0, up_c, two)
    up_g1 = seq.at(up_g1)
    up_got = Sent(core_swap(up_g1))
    down_g1 = seq.at(down_g1)
    down_got = Sent(core_swap(down_g1))
    seq.land((), up_got)
    red_up = Reduce(seq, (up_g0, up_got.value), n)
    red_up.launch()
    seq.land((), down_got)
    red_down = Reduce(seq, (down_g0, down_got.value), n)
    red_down.launch(near)
    up_c, two = seq.at((up_c.value, two.value))
    up_d, two_d = Sent(core_swap(up_c)), Sent(core_swap(two))
    up_g2, down_g2, g_bias_2, back_sum, out_sum = mlp(
        seq.at(order), normed_two, cot, bias_fc1[2], up_c, two, 0, (out_sum, back_sum)
    )
    up_g2 = seq.land(up_g2, up_d, two_d, red_up, red_down)
    red_up.launch()
    red_down.launch()
    up_g3, down_g3, g_bias_3, grad_two_in, block = mlp(
        seq.at(order), normed_two, cot, bias_fc1[3], up_d.value, two_d.value, 0,
        (out_sum, back_sum), (after_attn, full_bfc2),
    )
    up_g3 = seq.land(up_g3, red_up, red_down)
    up_got = Sent(core_swap(up_g3))
    down_g3 = seq.at(down_g3)
    down_got = Sent(core_swap(down_g3))
    red_up.launch()
    red_down.launch()
    seq.land((), up_got)
    two_up = Reduce(seq, (up_g2, up_got.value), n)
    two_up.launch()
    seq.land((), down_got)
    two_down = Reduce(seq, (down_g2, down_got.value), n)
    two_down.launch(near)

    after_grad, mg0, mg1, mg2, mg3, g_out, sums_two = attention_out_back(
        seq.at(order), grad_two_in, after_attn, cot, gain_two_f, mixed, outs
    )
    mg2 = seq.at(mg2)
    g_w2, g_w3, proj2, proj3, sums_b = attention_back(
        seq.at(order), normed_one, qkvs[2:], lses[2:], (mg2, mg3), g_out, (2, 3), n_img, patches, factor, n
    )
    g_w3 = seq.land(g_w3, red_up, red_down, two_up, two_down)
    w_3 = Sent(core_swap(g_w3))
    two_up.launch()
    two_down.launch()
    seq.land((), w_3)
    middle = n // 2
    half_shape = (2,) * (len(bits) - 1)
    w_high = Sent(x_swap(seq.at(rounded_sum([g_w2[middle:], w_3.value[middle:]]))))
    g_w0, g_w1, proj0, proj1, sums_a = attention_back(
        seq.at(order), normed_one, qkvs[:2], lses[:2], (mg0, mg1), g_out, (0, 1), n_img, patches, factor, n
    )
    g_w1 = seq.land(g_w1, two_up, two_down, w_high)
    w_1 = Sent(core_swap(g_w1))
    two_up.launch()
    two_down.launch()
    seq.land((), w_1)
    red_w = Reduce(seq, (g_w0, w_1.value), n)
    red_w.launch(0, [w_high.value.reshape(half_shape + w_high.value.shape[1:])])
    w_low = Sent(x_swap(seq.at(rounded_sum([g_w2[:middle], w_3.value[:middle]]))))
    tokens_grad, sums_one = input_back(
        seq.at(order), x_zero, after_grad, gain_one_f, (proj0, proj1, proj2, proj3), qkv_parts
    )
    sums_one = seq.land(sums_one, two_up, two_down, red_w, w_low)
    red_w.terms = [*red_w.terms, w_low.value.reshape(half_shape + w_low.value.shape[1:])]
    while len(red_w.axes) > 2:
        red_w.launch()
        seq.land((), red_w)
    red_w.launch()
    packed = pack_sums(
        seq.at(order),
        n,
        rows,
        ffq,
        (sums_a, sums_b),
        (jnp.stack([g_bias_0, g_bias_1]), jnp.stack([g_bias_2, g_bias_3])),
        (sums_two, sums_one),
    )
    sums = Reduce(seq, (packed,), n, full)
    while len(sums.axes) > 3:
        sums.launch()
        seq.land((), sums)
    sums.launch()
    crossing = jnp.stack([two_up.rest().piece(), two_down.rest().piece()])
    cross = Sent(x_swap(seq.at(crossing)))
    seq.land((), red_w, sums)
    red_w.launch()
    sums.launch()
    seq.land((), cross)
    owned = [
        rounded_sum([*red_up.rest().terms, cross.value[0]]),
        rounded_sum([*red_down.rest().terms, cross.value[1]]),
    ]
    mlp_spread = Spread(seq, jnp.stack(owned))
    seq.land((), sums, red_w)
    w_spread = Spread(seq, red_w.piece())
    sums.launch()
    block, tokens_grad = seq.at((block, tokens_grad))
    block_out, grad_tokens = seq.land((compact(block), compact(tokens_grad)), sums, mlp_spread, w_spread)
    mlp_spread.cross()
    w_spread.cross()
    packed = seq.at(sums.piece())
    peers = Sent([xor_swap(packed, "dp", 4, m) for m in (1, 2, 3)])
    seq.land((), mlp_spread, w_spread, peers)
    beside, across, opposite = peers.value
    small_sums = (packed + beside) + (across + opposite)
    out_fc1, out_fc2 = finish_mlp(q, mlp_spread.pieces, n)
    out_qkv, out_out = finish_attention(seq.value, w_spread.pieces)
    small_out = [small_sums[k, :rows] for k in range(8)]
    out_bfc1 = small_sums[8:12, :ffq].reshape(-1)
    o_bq, o_bv, o_bout, o_gone, o_sone, o_bfc2, o_gtwo, o_stwo = small_out
    return (
        block_out,
        grad_tokens,
        out_qkv,
        o_bq,
        o_bv,
        out_out,
        o_bout,
        o_gone,
        o_sone,
        out_fc1,
        out_bfc1,
        out_fc2,
        o_bfc2,
        o_gtwo,
        o_stwo,
    )


def solution(mesh):
    rows_split = P(("dp", "fsdp"), None)
    matrix = P("fsdp", None)
    vector = P("fsdp")
    return jax.shard_map(
        local,
        mesh=mesh,
        in_specs=(
            rows_split, P(("dp", "fsdp")), matrix, vector, vector, matrix, vector, vector, vector,
            matrix, vector, matrix, vector, vector, vector, rows_split,
        ),
        out_specs=(
            rows_split, rows_split, matrix, vector, vector, matrix, vector, vector, vector,
            matrix, vector, matrix, vector, vector, vector,
        ),
        check_vma=False,
    )
```

```python
import math

import jax
import jax.numpy as jnp
from jax import lax
from jax.experimental import pallas as pl
from jax.experimental.pallas import tpu as pltpu
from jax.sharding import PartitionSpec as P

HEADS = 16
GRID = 14
NSCALE = 16
norm_eps = 1e-06
half = jnp.bfloat16
full = jnp.float32


def xor_swap(value, axis, size, mask):
    return lax.ppermute(value, axis, [(i, i ^ mask) for i in range(size)])


def core_swap(value):
    return xor_swap(value, "dp", 4, 1)


def x_swap(value):
    return xor_swap(value, "dp", 4, 2)


def masks(bits):
    found = [0]
    for bit in bits:
        found = found + [m | (1 << bit) for m in found]
    return found


class Order:
    def __init__(self, value):
        self.value = value

    def at(self, value):
        value, self.value = lax.optimization_barrier((value, self.value))
        return value

    def land(self, value, *sent):
        value, flights = self.at((value, [s.flight for s in sent]))
        for s, flight in zip(sent, flights, strict=True):
            s.accept(flight)
        return value


class Sent:
    def __init__(self, flight):
        self.flight = flight

    def accept(self, value):
        self.value = value


class Gather:
    def __init__(self, seq, piece, n, bits):
        self.seq, self.held, self.n, self.bits = seq, piece[None], n, list(bits)

    def launch(self):
        self.held = self.seq.at(self.held)
        self.flight = xor_swap(self.held, "fsdp", self.n, 1 << self.bits.pop(0))

    def accept(self, value):
        self.got = value

    def join(self):
        self.held = jnp.concatenate([self.held, self.got])
        return self.held


def rounded_sum(terms, kind=half):
    return sum(t.astype(full) for t in terms).astype(kind)


class Reduce:
    def __init__(self, seq, terms, n, kind=half):
        self.kind = kind
        self.seq, self.n, self.axes = seq, n, list(range(n.bit_length() - 1))
        self.terms = [t.reshape((2,) * len(self.axes) + t.shape[1:]) for t in terms]

    def launch(self, bit=None, more=()):
        bit = self.axes[0] if bit is None else bit
        axis = self.axes.index(bit)
        self.axes.pop(axis)
        low, high = [
            [lax.index_in_dim(t, side, axis, keepdims=False) for t in self.terms] for side in (0, 1)
        ]
        self.terms = low
        self.flight = xor_swap(self.seq.at(rounded_sum([*high, *more], self.kind)), "fsdp", self.n, 1 << bit)

    def accept(self, value):
        self.terms = [*self.terms, value]

    def rest(self):
        while self.axes:
            self.launch()
            self.seq.land((), self)
        return self

    def piece(self):
        return rounded_sum(self.terms, self.kind)


class Spread:
    def __init__(self, seq, piece):
        self.seq, self.pieces = seq, [seq.at(piece)]
        self.flight = [core_swap(self.pieces[0]), x_swap(self.pieces[0])]

    def cross(self):
        self.flight = [core_swap(self.seq.at(self.pieces[2]))]

    def accept(self, value):
        self.pieces += value


ANYWHERE = pl.BlockSpec(memory_space=pl.ANY)
ON_CHIP = pl.BlockSpec(memory_space=pltpu.VMEM)
SCALARS = pl.BlockSpec(memory_space=pltpu.SMEM)


def dot(left, right, dim_left, dim_right):
    return lax.dot_general(
        left, right, (((dim_left,), (dim_right,)), ((), ())), preferred_element_type=full
    )


def call(kernel, name, operands, in_specs, outs, out_specs, scratch):
    return pl.pallas_call(
        kernel,
        out_shape=[jax.ShapeDtypeStruct(shape, kind) for shape, kind in outs],
        in_specs=in_specs,
        out_specs=out_specs,
        scratch_shapes=scratch,
        compiler_params=pltpu.CompilerParams(vmem_limit_bytes=58 * 2**20),
        name=name,
    )(*operands)


def loop(count, body, unroll=1):
    def step(i, carry):
        body(i)
        return carry

    lax.fori_loop(0, count, step, 0, unroll=unroll)


def tile(i, size):
    return pl.ds(pl.multiple_of(i * size, size), size)


def bring(src, dst, sem):
    pltpu.make_async_copy(src, dst, sem).start()


def arrived(dst, sem):
    pltpu.make_async_copy(dst, dst, sem).wait()


def fetch(parts, order_ref, place, sem):
    base = 0
    for part in parts:

        def start(r, part=part, base=base):
            shard = r if order_ref is None else order_ref[base + r]
            pltpu.make_async_copy(part.at[r], place(shard), sem).start()

        loop(part.shape[0], start)
        base += part.shape[0]


def head_rows(s, q, n, rows, quarter):
    per = n // 4
    return pl.multiple_of(((s // per) ^ q) * quarter + (s % per) * rows, rows)


def pair_scores(q2, k2):
    first = lax.broadcasted_iota(jnp.int32, q2.shape, 1) < q2.shape[1] // 2
    both = apart(q2, first)
    return both, dot(k2, both, 1, 1), first


def apart(value, first):
    zero = jnp.zeros_like(value)
    return jnp.concatenate([jnp.where(first, value, zero), jnp.where(first, zero, value)])


def attention_forward(order, normed, bias, weights, n_img, patches, factor):
    groups, n_parts = len(weights), len(weights[0])
    wide = weights[0][0].shape[2]
    count, width = normed.shape
    rows = width // sum(part.shape[0] for part in weights[0])
    padded = count // n_img
    quarter = wide // 3

    def kernel(order_ref, normed_ref, bias_ref, *refs):
        w_refs, refs = refs[: groups * n_parts], refs[groups * n_parts :]
        qkv_refs, mixed_refs, refs = refs[:groups], refs[groups : 2 * groups], refs[2 * groups :]
        lse_refs, (w_held, sems) = refs[:groups], refs[groups:]
        for g in range(groups):
            fetch(
                [w.at[:, pl.ds(0, rows)] for w in w_refs[g * n_parts : (g + 1) * n_parts]],
                order_ref,
                lambda s, g=g: w_held.at[g, pl.ds(pl.multiple_of(s * rows, rows), rows)],
                sems.at[g],
            )
        for g in range(groups):
            pltpu.make_async_copy(w_held.at[g], w_held.at[g], sems.at[g]).wait()

            def project(t, g=g):
                at = tile(t, quarter)
                product = dot(normed_ref[...], w_held[g, :, at], 1, 0)
                qkv_refs[g][:, at] = (product + bias_ref[g, :, at]).astype(half)

            loop(3, project)

            def attend(i, g=g):
                at = tile(i // 2, padded)
                lanes = [pl.ds(pl.multiple_of(t * quarter + (i % 2) * 128, 128), 128) for t in range(3)]
                q2 = qkv_refs[g][at, lanes[0]] * factor
                k2 = qkv_refs[g][at, lanes[1]]
                v2 = qkv_refs[g][at, lanes[2]]
                _, scores, first = pair_scores(q2, k2)
                key = lax.broadcasted_iota(jnp.int32, scores.shape, 0)
                scores = jnp.where(key < patches, scores, -1e30)
                top = jnp.max(scores, axis=0, keepdims=True)
                raised = jnp.exp(scores - top)
                total = jnp.sum(raised, axis=0, keepdims=True)
                lse_refs[g][i] = top + jnp.log(total)
                out = dot((raised * (1.0 / total)).astype(half), v2, 0, 0)
                mixed_refs[g][at, lanes[0]] = jnp.where(first, out[:padded], out[padded:]).astype(half)

            loop(2 * n_img, attend, 2 * n_img)

    return call(
        kernel,
        "attention_forward",
        (order, normed, bias, *(part for w in weights for part in w)),
        [SCALARS, ON_CHIP, ON_CHIP] + [ANYWHERE] * (groups * n_parts),
        [((count, wide), half)] * groups
        + [((count, quarter), half)] * groups
        + [((2 * n_img, 1, 2 * padded), full)] * groups,
        [ON_CHIP] * (3 * groups),
        [pltpu.VMEM((groups, width, wide), half), pltpu.SemaphoreType.DMA((groups,))],
    )


def layer_norm(value, gain, shift):
    center = jnp.mean(value, axis=-1, keepdims=True)
    offset = value - center
    spread = jnp.mean(offset * offset, axis=-1, keepdims=True)
    return offset * lax.rsqrt(spread + norm_eps) * gain + shift


def layer_norm_back(value, grad, gain):
    center = jnp.mean(value, axis=-1, keepdims=True)
    offset = value - center
    scale = lax.rsqrt(jnp.mean(offset * offset, axis=-1, keepdims=True) + norm_eps)
    unit = offset * scale
    scaled = grad * gain
    inner = jnp.mean(scaled * unit, axis=-1, keepdims=True)
    return scale * (scaled - jnp.mean(scaled, axis=-1, keepdims=True) - unit * inner), grad * unit


def load_out(order_ref, out_refs, held, sem, n, rows, quarter):
    q = order_ref[n]
    for j in range(4):
        column = pl.multiple_of((q ^ j) * quarter, quarter)
        fetch(
            [out_refs[j % 2].at[:, :, pl.ds(j // 2 * quarter, quarter)]],
            order_ref,
            lambda s, column=column: held.at[
                pl.ds(head_rows(s, q, n, rows, quarter), rows), pl.ds(column, quarter)
            ],
            sem,
        )


CHUNK = 16
ROWS = 64


def attention_out(order, x_zero, mixed, outs, bias, gain, shift):
    count, width = x_zero.shape
    n, rows, _ = outs[0].shape
    quarter = mixed[0].shape[1]

    def kernel(order_ref, x_ref, bias_ref, gain_ref, shift_ref, *refs):
        mixed_refs, out_refs = refs[:4], refs[4:6]
        after_ref, normed_ref, held, x_held, sems = refs[6:]
        bring(x_ref, x_held, sems.at[1])
        load_out(order_ref, out_refs, held, sems.at[0], n, rows, quarter)
        together = jnp.concatenate([m[...] for m in mixed_refs], axis=1)
        pltpu.make_async_copy(held, held, sems.at[0]).wait()
        after_ref[...] = dot(together, held[...], 1, 0)
        arrived(x_held, sems.at[1])

        def finish(i):
            at = tile(i, CHUNK)
            after = x_held[at] + (after_ref[at] + bias_ref[...])
            after_ref[at] = after
            normed_ref[at] = layer_norm(after, gain_ref[...], shift_ref[...]).astype(half)

        loop(count // CHUNK, finish, 13)

    return call(
        kernel,
        "attention_out",
        (order, x_zero, bias, gain, shift, *mixed, *outs),
        [SCALARS, ANYWHERE] + [ON_CHIP] * 7 + [ANYWHERE] * 2,
        [((count, width), full), ((count, width), half)],
        [ON_CHIP] * 2,
        [
            pltpu.VMEM((width, width), half),
            pltpu.VMEM((count, width), full),
            pltpu.SemaphoreType.DMA((2,)),
        ],
    )


def mlp(order, normed, cot, bias, up_all, down_all, down_start, carried=None, ending=None):
    count, width = normed.shape
    n, rows, _ = up_all.shape
    hidden = bias.shape[1]
    share = hidden // n
    step = min(512, hidden)
    steps = hidden // step
    more = [*(carried or []), *(ending[:1] if ending else [])]
    last = list(ending[1:]) if ending else []

    def kernel(order_ref, bias_ref, *refs):
        last_refs, refs = refs[: len(last)], refs[len(last) :]
        normed_ref, cot_ref, up_ref, down_ref, refs = *refs[:4], refs[4:]
        more_refs, refs = refs[: len(more)], refs[len(more) :]
        g_up_ref, g_down_ref, g_bias_ref, back_ref, end_ref, refs = *refs[:5], refs[5:]
        held, refs = refs[: len(more)], refs[len(more) :]
        rows_in, cots, out, back, up, down, pre, act, act_half, pre_half, g_up, g_down, sems = refs
        bring(normed_ref, rows_in, sems.at[3])
        fetch(
            [up_ref.at[:, :, pl.ds(0, hidden)]],
            None,
            lambda s: up.at[pl.ds(pl.multiple_of(s * rows, rows), rows)],
            sems.at[0],
        )
        bring(cot_ref, cots, sems.at[4])
        fetch(
            [down_ref.at[:, :, pl.ds(down_start, width)]],
            None,
            lambda s: down.at[pl.ds(pl.multiple_of(s * share, share), share)],
            sems.at[1],
        )
        for k in range(len(more)):
            bring(more_refs[k], held[k], sems.at[5 + k])
        arrived(rows_in, sems.at[3])
        arrived(up, sems.at[0])
        for t in range(steps):
            at = pl.ds(t * step, step)
            pre[...] = dot(rows_in[...], up[:, at], 1, 0)
            if not t:
                arrived(cots, sems.at[4])
                arrived(down, sems.at[1])
            act[...] = dot(cots[...], down[at, :], 1, 1)

            def gelu(i, at=at):
                some = tile(i, 2 * CHUNK)
                x = pre[some] + bias_ref[:, at]
                below = 0.5 * (1.0 + lax.erf(x * math.sqrt(0.5)))
                density = jnp.exp(-0.5 * x * x) * (1.0 / math.sqrt(2.0 * math.pi))
                act_half[some] = (x * below).astype(half)
                pre_half[some] = (act[some] * (below + x * density)).astype(half)

            loop(count // CHUNK // 2, gelu)
            p = pre_half[...]
            h = act_half[...]
            more_back = dot(p, up[:, at], 1, 1)
            more_out = dot(h, down[at, :], 1, 0)
            if t:
                back[...] += more_back
                out[...] += more_out
            elif carried:
                arrived(held[0], sems.at[5])
                arrived(held[1], sems.at[6])
                out[...] = held[0][...] + more_out
                back[...] = held[1][...] + more_back
            else:
                out[...] = more_out
                back[...] = more_back
            if t == steps - 1:
                bring(back, back_ref, sems.at[3])
                if not ending:
                    bring(out, end_ref, sems.at[4])
            g_down[at, :] = dot(h, cots[...], 0, 0).astype(half)
            if t == steps - 1:

                def send_down(r):
                    at = pl.multiple_of(order_ref[r] * share, share)
                    bring(g_down.at[pl.ds(at, share)], g_down_ref.at[r], sems.at[2])

                loop(n, send_down)
            g_up[:, at] = dot(rows_in[...], p, 0, 0).astype(half)
            g_bias_ref[:, at] = jnp.sum(p.astype(full), axis=0, keepdims=True)

        def send_up(r):
            at = pl.multiple_of(order_ref[r] * rows, rows)
            bring(g_up.at[pl.ds(at, rows)], g_up_ref.at[r], sems.at[0])

        loop(n, send_up)
        if ending:
            arrived(held[2], sems.at[7])

            def finish(i):
                at = tile(i, 2 * CHUNK)
                end_ref[at] = (held[2][at] + (out[at] + last_refs[0][...])).astype(half)

            loop(count // CHUNK // 2, finish)
        else:
            arrived(end_ref, sems.at[4])
        arrived(back_ref, sems.at[3])
        arrived(g_down_ref, sems.at[2])
        arrived(g_up_ref, sems.at[0])

    sums = pltpu.VMEM((count, width), full)
    wide = pltpu.VMEM((count, width), half)
    square = pltpu.VMEM((width, hidden), half)
    return call(
        kernel,
        "mlp",
        (order, bias, *last, normed, cot, up_all, down_all, *more),
        [SCALARS] + [ON_CHIP] * (1 + len(last)) + [ANYWHERE] * (4 + len(more)),
        [
            ((n, rows, hidden), half),
            ((n, share, width), half),
            ((1, hidden), full),
            ((count, width), full),
            ((count, width), half if ending else full),
        ],
        [ANYWHERE, ANYWHERE, ON_CHIP, ANYWHERE, ON_CHIP if ending else ANYWHERE],
        [
            *([sums] * len(more)),
            wide,
            wide,
            sums,
            sums,
            square,
            pltpu.VMEM((hidden, width), half),
            pltpu.VMEM((count, step), full),
            pltpu.VMEM((count, step), full),
            pltpu.VMEM((count, step), half),
            pltpu.VMEM((count, step), half),
            square,
            pltpu.VMEM((hidden, width), half),
            pltpu.SemaphoreType.DMA((5 + len(more),)),
        ],
    )


def attention_out_back(order, grad, after, cot, gain, mixed, outs):
    count, width = after.shape
    n, rows, _ = outs[0].shape
    quarter = mixed[0].shape[1]

    def kernel(order_ref, grad_ref, after_ref, cot_ref, gain_ref, *refs):
        mixed_refs, out_refs, refs = refs[:4], refs[4:6], refs[6:]
        after_grad_ref, mixed_grad_refs, g_out_ref, sums_ref = refs[0], refs[1:5], refs[5], refs[6]
        held, branch, terms, grad, after, cot, mixes, sems = refs[7:]
        block = count // 4
        for k in range(4):
            some = pl.ds(k * block, block)
            bring(grad_ref.at[some], grad.at[some], sems.at[1 + k])
            bring(after_ref.at[some], after.at[some], sems.at[5 + k])
            bring(cot_ref.at[some], cot.at[some], sems.at[9 + k])
        load_out(order_ref, out_refs, held, sems.at[0], n, rows, quarter)
        for j in range(4):
            bring(mixed_refs[j], mixes.at[j], sems.at[13])
        terms[...] = jnp.zeros_like(terms)

        def fold(value):
            return jnp.sum(value.reshape(CHUNK // 8, 8, width), axis=0)

        def back(i, k):
            at = pl.ds(pl.multiple_of(k * block + i * CHUNK, CHUNK), CHUNK)
            incoming = grad[at]
            part, gain_terms = layer_norm_back(after[at], incoming, gain_ref[...])
            own = cot[at].astype(full)
            total = own + part
            after_grad_ref[at] = total
            rounded = total.astype(half)
            branch[at] = rounded
            terms[0] += fold(rounded.astype(full))
            terms[1] += fold(gain_terms)
            terms[2] += fold(incoming)
            terms[3] += fold(own)

        for k in range(4):
            some = pl.ds(k * block, block)
            arrived(grad.at[some], sems.at[1 + k])
            arrived(after.at[some], sems.at[5 + k])
            arrived(cot.at[some], sems.at[9 + k])
            loop(block // CHUNK, lambda i, k=k: back(i, k), 13)
        for k in range(4):
            sums_ref[k] = jnp.sum(terms[k], axis=0, keepdims=True)
        arrived(held, sems.at[0])
        arrived(mixes, sems.at[13])
        for j in range(4):
            mixed_grad_refs[j][...] = dot(branch[...], held[j * quarter : (j + 1) * quarter], 1, 1).astype(half)
            g_out_ref[j * quarter : (j + 1) * quarter] = dot(mixes[j], branch[...], 0, 0).astype(half)

    return call(
        kernel,
        "attention_out_back",
        (order, grad, after, cot, gain, *mixed, *outs),
        [SCALARS] + [ANYWHERE] * 3 + [ON_CHIP] + [ANYWHERE] * 6,
        [((count, width), full)]
        + [((count, quarter), half)] * 4
        + [((width, width), half), ((4, 1, width), full)],
        [ON_CHIP] * 7,
        [
            pltpu.VMEM((width, width), half),
            pltpu.VMEM((count, width), half),
            pltpu.VMEM((4, 8, width), full),
            pltpu.VMEM((count, width), full),
            pltpu.VMEM((count, width), full),
            pltpu.VMEM((count, width), half),
            pltpu.VMEM((4, count, quarter), half),
            pltpu.SemaphoreType.DMA((14,)),
        ],
    )


def attention_back(order, normed, qkvs, lses, mixed_grads, g_out, which, n_img, patches, factor, n):
    groups = len(qkvs)
    count, width = normed.shape
    wide = qkvs[0].shape[1]
    quarter = wide // 3
    padded = count // n_img
    rows = width // n

    def kernel(order_ref, normed_ref, g_out_ref, *refs):
        qkv_refs, mg_refs, refs = refs[:groups], refs[groups : 2 * groups], refs[2 * groups :]
        lse_refs, refs = refs[:groups], refs[groups:]
        g_w_refs, proj_refs, sums_ref = refs[:groups], refs[groups : 2 * groups], refs[2 * groups]
        g_w, normed_held, g_out_held, sems = refs[2 * groups + 1 :]
        q = order_ref[n]
        bring(g_out_ref, g_out_held, sems.at[groups])
        bring(normed_ref, normed_held, sems.at[groups + 1])
        for g in range(groups):

            def attend(i, g=g):
                at = tile(i // 2, padded)
                lanes = [pl.ds(pl.multiple_of(t * quarter + (i % 2) * 128, 128), 128) for t in range(3)]
                q2 = qkv_refs[g][at, lanes[0]] * factor
                k2 = qkv_refs[g][at, lanes[1]]
                v2 = qkv_refs[g][at, lanes[2]]
                both, scores, first = pair_scores(q2, k2)
                key = lax.broadcasted_iota(jnp.int32, scores.shape, 0)
                probs = jnp.where(key < patches, jnp.exp(scores - lse_refs[g][i]), 0.0)
                o_both = apart(mg_refs[g][at, lanes[0]], first)
                g_probs = dot(v2, o_both, 1, 1)
                weighted = jnp.sum(probs * g_probs, axis=0, keepdims=True)
                g_scores = (probs * (g_probs - weighted)).astype(half)
                g_query = dot(g_scores, k2, 0, 0)
                g_query = jnp.where(first, g_query[:padded], g_query[padded:]) * factor
                proj_refs[g][at, lanes[0]] = g_query.astype(half)
                proj_refs[g][at, lanes[1]] = dot(g_scores, both, 1, 0).astype(half)
                proj_refs[g][at, lanes[2]] = dot(probs.astype(half), o_both, 1, 0).astype(half)

            loop(2 * n_img, attend, 4)
            if not g:
                arrived(g_out_held, sems.at[groups])
                arrived(normed_held, sems.at[groups + 1])

            def send_out(r, g=g):
                at = head_rows(order_ref[r], q, n, rows, quarter)
                column = pl.multiple_of((q ^ which[g]) * quarter, quarter)
                pltpu.make_async_copy(
                    g_out_held.at[pl.ds(at, rows), pl.ds(column, quarter)],
                    g_w_refs[g].at[r, :, pl.ds(wide, quarter)],
                    sems.at[g],
                ).start()

            loop(n, send_out)

            def weigh(t, g=g):
                at = tile(t, quarter)
                some = proj_refs[g][:, at]
                g_w[g, :, at] = dot(normed_held[...], some, 0, 0).astype(half)
                sums_ref[g, :, at] = jnp.sum(some.astype(full), axis=0, keepdims=True)

            loop(3, weigh)

            def send(r, g=g):
                at = pl.multiple_of(order_ref[r] * rows, rows)
                pltpu.make_async_copy(
                    g_w.at[g, pl.ds(at, rows)], g_w_refs[g].at[r, :, pl.ds(0, wide)], sems.at[g]
                ).start()

            loop(n, send)
        for g in range(groups):
            pltpu.make_async_copy(g_w_refs[g], g_w_refs[g], sems.at[g]).wait()

    return call(
        kernel,
        "attention_back",
        (order, normed, g_out, *qkvs, *mixed_grads, *lses),
        [SCALARS] + [ANYWHERE] * 2 + [ON_CHIP] * (3 * groups),
        [((n, rows, wide + quarter), half)] * groups
        + [((count, wide), half)] * groups
        + [((groups, 1, wide), full)],
        [ANYWHERE] * groups + [ON_CHIP] * (groups + 1),
        [
            pltpu.VMEM((groups, width, wide), half),
            pltpu.VMEM((count, width), half),
            pltpu.VMEM((width, width), half),
            pltpu.SemaphoreType.DMA((groups + 2,)),
        ],
    )


def input_back(order, x_zero, after_grad, gain, projs, weights):
    count, width = x_zero.shape
    wide = weights[0][0].shape[2]
    rows = width // sum(part.shape[0] for part in weights[0])
    parts = [part for w in weights for part in w]
    n_parts = len(weights[0])

    def kernel(order_ref, x_ref, after_ref, gain_ref, *refs):
        proj_refs, w_refs = refs[:4], refs[4 : 4 + len(parts)]
        token_ref, sums_ref, held, terms, x_held, after_held, sems = refs[4 + len(parts) :]
        for j in range(4):
            fetch(
                [w.at[:, pl.ds(0, rows)] for w in w_refs[j * n_parts : (j + 1) * n_parts]],
                order_ref,
                lambda s, j=j: held.at[j, pl.ds(pl.multiple_of(s * rows, rows), rows)],
                sems.at[j],
            )
        bring(x_ref, x_held, sems.at[4])
        bring(after_ref, after_held, sems.at[5])
        for j in range(4):
            arrived(held.at[j], sems.at[j])
            product = dot(proj_refs[j][...], held[j], 1, 1)
            if j == 0:
                token_ref[...] = product
            else:
                token_ref[...] += product
        arrived(x_held, sems.at[4])
        arrived(after_held, sems.at[5])
        terms[...] = jnp.zeros_like(terms)

        def fold(value):
            return jnp.sum(value.reshape(ROWS // 8, 8, width), axis=0)

        def back(i):
            at = tile(i, ROWS)
            incoming = token_ref[at]
            part, gain_terms = layer_norm_back(x_held[at], incoming, gain_ref[...])
            token_ref[at] = after_held[at] + part
            terms[0] += fold(gain_terms)
            terms[1] += fold(incoming)

        loop(count // ROWS, back)
        for k in range(2):
            sums_ref[k] = jnp.sum(terms[k], axis=0, keepdims=True)

    return call(
        kernel,
        "input_back",
        (order, x_zero, after_grad, gain, *projs, *parts),
        [SCALARS] + [ANYWHERE] * 2 + [ON_CHIP] * 5 + [ANYWHERE] * len(parts),
        [((count, width), full), ((2, 1, width), full)],
        [ON_CHIP] * 2,
        [
            pltpu.VMEM((4, width, wide), half),
            pltpu.VMEM((2, 8, width), full),
            pltpu.VMEM((count, width), full),
            pltpu.VMEM((count, width), full),
            pltpu.SemaphoreType.DMA((6,)),
        ],
    )


def payloads(which, w_fc1, w_fc2):
    rows, ff = w_fc1.shape
    full_share, width = w_fc2.shape
    share = full_share // 4
    n = ff // full_share
    hidden = n * share
    own, across = which
    if share % 128:
        fc1 = [lax.dynamic_slice(w_fc1, (0, (4 * s + own) * share), (rows, share)) for s in range(n)]
        fc2 = [lax.dynamic_slice(w_fc2, (g * share, 0), (share, width)).astype(half) for g in which]
        rest = jnp.concatenate([*fc1, fc2[0].reshape(rows, -1).astype(full)], axis=1)
        return rest.astype(half), fc2[1]

    def kernel(which_ref, fc1_ref, fc2_ref, rest_ref, two_ref):
        for s in range(n):
            at = pl.ds(pl.multiple_of((4 * s + which_ref[0]) * share, share), share)
            rest_ref[:, s * share : (s + 1) * share] = fc1_ref[:, at].astype(half)
        rest_ref[:, hidden : hidden + width] = fc2_ref[tile(which_ref[0], share), :].astype(half)
        two_ref[...] = fc2_ref[tile(which_ref[1], share), :].astype(half)

    return call(
        kernel,
        "payloads",
        (jnp.stack(which), w_fc1, w_fc2),
        [SCALARS] + [ON_CHIP] * 2,
        [((rows, hidden + width), half), ((share, width), half)],
        [ON_CHIP] * 2,
        [],
    )


def natural_quarters(q, pieces):
    once = [jnp.where((q & 1) == 1, pieces[i ^ 1], pieces[i]) for i in range(4)]
    return [jnp.where(q >= 2, once[i ^ 2], once[i]) for i in range(4)]


def finish_mlp(q, pieces, n):
    _, rows, width = pieces[0].shape
    share = width // n
    if share % 128:
        pieces = natural_quarters(q, pieces)
        fc1 = jnp.stack([p[0].reshape(rows, n, share) for p in pieces], axis=2).reshape(rows, 4 * width)
        return fc1.astype(full), jnp.concatenate([p[1] for p in pieces]).astype(full)

    def kernel(q_ref, *refs):
        fc1_ref, fc2_ref = refs[4:]
        for j in range(4):
            g = q_ref[0] ^ j
            for s in range(n):
                at = pl.ds(pl.multiple_of((4 * s + g) * share, share), share)
                fc1_ref[:, at] = refs[j][0, :, s * share : (s + 1) * share].astype(full)
            fc2_ref[tile(g, rows), :] = refs[j][1].astype(full)

    return call(
        kernel,
        "finish_mlp",
        (q[None], *pieces),
        [SCALARS] + [ON_CHIP] * 4,
        [((rows, 4 * width), full), ((4 * rows, width), full)],
        [ON_CHIP] * 2,
        [],
    )


def finish_attention(q, pieces):
    rows, width = pieces[0].shape
    quarter = width // 4

    def kernel(q_ref, *refs):
        qkv_ref, out_ref = refs[4:]
        for j in range(4):
            g = q_ref[0] ^ j
            for t in range(3):
                at = pl.ds(pl.multiple_of(t * width + g * quarter, quarter), quarter)
                qkv_ref[:, at] = refs[j][:, t * quarter : (t + 1) * quarter].astype(full)
            out_ref[:, tile(g, quarter)] = refs[j][:, 3 * quarter :].astype(full)

    return call(
        kernel,
        "finish_attention",
        (q[None], *pieces),
        [SCALARS] + [ON_CHIP] * 4,
        [((rows, 3 * width), full), ((rows, width), full)],
        [ON_CHIP] * 2,
        [],
    )


BELOW = 16


def first_payload(q, w_qkv, vectors):
    rows, columns = w_qkv.shape
    width = columns // 3
    quarter = width // 4
    wide = 3 * quarter

    def kernel(q_ref, w_ref, *refs):
        out_ref, held, low, sem = refs[len(vectors) :]
        for t in range(3):
            at = pl.multiple_of(t * width + q_ref[0] * quarter, quarter)
            pltpu.make_async_copy(
                w_ref.at[:, pl.ds(at, quarter)], held.at[:, pl.ds(t * quarter, quarter)], sem.at[0]
            ).start()
        low[...] = jnp.zeros_like(low)
        for k, vector in enumerate(refs[: len(vectors)]):
            low[k : k + 1, : vector.shape[1]] = vector[...]
        out_ref[rows:] = low[...].astype(half)
        pltpu.make_async_copy(held, held, sem.at[0]).wait()
        out_ref[:rows] = held[...].astype(half)

    return call(
        kernel,
        "first_payload",
        (q[None], w_qkv, *(v[None] for v in vectors)),
        [SCALARS, ANYWHERE] + [ON_CHIP] * len(vectors),
        [((rows + BELOW, wide), half)],
        [ON_CHIP],
        [pltpu.VMEM((rows, wide), full), pltpu.VMEM((BELOW, wide), full), pltpu.SemaphoreType.DMA((1,))],
    )[0]


def unpack_vectors(order, parts, n, rows, share):
    width = n * rows
    quarter = width // 4
    if rows % 128 or share % 128:
        q = order[n]
        held = jnp.concatenate([p[:, rows:] for p in parts]).astype(full)
        held = held[jnp.zeros((n,), jnp.int32).at[order[:n]].set(jnp.arange(n, dtype=jnp.int32))]
        groups = jnp.arange(4, dtype=jnp.int32) ^ q
        vectors = jnp.stack([held[:, k, :rows].reshape(1, width) for k in range(8)])
        units = held[:, 8, : 4 * share].reshape(n, 4, share).transpose(1, 0, 2)[groups]
        ends = [vectors[k].reshape(4, 1, quarter)[groups] for k in range(2)]
        return vectors, units.reshape(4, 1, width), jnp.concatenate([ends[0], 0 * ends[0], ends[1]], axis=2)

    def kernel(order_ref, *refs):
        part_refs, (vector_ref, fc1_ref, qkv_ref, held, wider, sem) = refs[: len(parts)], refs[len(parts) :]
        base = 0
        for part in part_refs:
            size = part.shape[0]
            pltpu.make_async_copy(part.at[:, pl.ds(rows, BELOW)], held.at[pl.ds(base, size)], sem.at[0]).start()
            base += size
        pltpu.make_async_copy(held, held, sem.at[0]).wait()
        wider[...] = held[...].astype(full)
        q = order_ref[n]
        for r in range(n):
            at = tile(order_ref[r], rows)
            for k in range(8):
                vector_ref[k, :, at] = wider[r, k : k + 1, :rows]
            for j in range(4):
                fc1_ref[j, :, tile(order_ref[r], share)] = wider[r, 8:9, tile(q ^ j, share)]
        for j in range(4):
            at = tile(q ^ j, quarter)
            qkv_ref[j, :, :quarter] = vector_ref[0, :, at]
            qkv_ref[j, :, quarter : 2 * quarter] = jnp.zeros((1, quarter), full)
            qkv_ref[j, :, 2 * quarter :] = vector_ref[1, :, at]

    return call(
        kernel,
        "unpack_vectors",
        (order, *parts),
        [SCALARS] + [ANYWHERE] * len(parts),
        [((8, 1, width), full), ((4, 1, width), full), ((4, 1, 3 * quarter), full)],
        [ON_CHIP] * 3,
        [
            pltpu.VMEM((n, BELOW, 3 * quarter), half),
            pltpu.VMEM((n, BELOW, 3 * quarter), full),
            pltpu.SemaphoreType.DMA((1,)),
        ],
    )


def pack_sums(order, n, rows, share, proj_sums, unit_sums, wide_sums):
    width = n * rows
    quarter = width // 4
    if rows % 128 or share % 128:
        groups = jnp.arange(4, dtype=jnp.int32) ^ order[n]
        proj = jnp.concatenate(proj_sums)[groups]
        units = jnp.concatenate(unit_sums)[groups].reshape(4, n, share)
        flat = [proj[:, :, :quarter].reshape(width), proj[:, :, 2 * quarter :].reshape(width)]
        two, one = wide_sums
        flat += [two[0], one[0], one[1], two[3], two[1], two[2]]
        flat = [v.reshape(n, 1, rows) for v in flat]
        stacked = [jnp.pad(v, ((0, 0), (0, 0), (0, 128 - rows))) for v in flat]
        stacked.append(jnp.pad(units.transpose(1, 0, 2), ((0, 0), (0, 4), (0, 128 - share))))
        return jnp.concatenate(stacked, axis=1)[order[:n]]

    def kernel(order_ref, proj_a, proj_b, unit_a, unit_b, two_ref, one_ref, out_ref, proj, units):
        proj[:2], proj[2:] = proj_a[...], proj_b[...]
        units[:2], units[2:] = unit_a[...], unit_b[...]
        q = order_ref[n]
        per = n // 4
        for r in range(n):
            s = order_ref[r]
            j = (s // per) ^ q
            at = tile(s, rows)
            inside = pl.multiple_of((s % per) * rows, rows)
            out_ref[r, 0:1] = proj[j, :, pl.ds(inside, rows)]
            out_ref[r, 1:2] = proj[j, :, pl.ds(2 * quarter + inside, rows)]
            for k, (ref, row) in enumerate(
                ((two_ref, 0), (one_ref, 0), (one_ref, 1), (two_ref, 3), (two_ref, 1), (two_ref, 2))
            ):
                out_ref[r, 2 + k : 3 + k] = ref[row, :, at]
            for g in range(4):
                out_ref[r, 8 + g : 9 + g] = units[q ^ g, :, tile(s, share)]
            out_ref[r, 12:] = jnp.zeros((4, rows), full)

    sums_two, sums_one = wide_sums
    return call(
        kernel,
        "pack_sums",
        (order, *proj_sums, *unit_sums, sums_two, sums_one),
        [SCALARS] + [ON_CHIP] * 6,
        [((n, 16, rows), full)],
        [ON_CHIP],
        [pltpu.VMEM((4, 1, 3 * quarter), full), pltpu.VMEM((4, 1, width), full)],
    )[0]


def table(codes, width):
    ratio = 0.3 * jnp.exp(codes.astype(full) * (math.log(10.0 / 0.3) / (NSCALE - 1)))
    quarter = width // 4
    omega = jnp.exp(jnp.arange(quarter).astype(full) * (-math.log(10000.0) / quarter))
    steps = jnp.arange(GRID, dtype=jnp.int32).astype(full)
    angle = ratio[:, None, None] * steps[None, :, None] * omega[None, None, :]
    return jnp.concatenate([jnp.sin(angle), jnp.cos(angle)], axis=-1)


def local(
    tokens,
    scale_codes,
    w_qkv,
    b_q,
    b_v,
    w_out,
    b_out,
    gain_one,
    shift_one,
    w_fc1,
    b_fc1,
    w_fc2,
    b_fc2,
    gain_two,
    shift_two,
    cotangent,
):
    n = lax.axis_size("fsdp")
    q = lax.axis_index("dp")
    f = lax.axis_index("fsdp")
    row_count, width = tokens.shape
    rows = width // n
    ff = b_fc1.shape[0] * n
    ffq = ff // n // 4
    hidden = n * ffq
    quarter = width // 4
    n_img = scale_codes.shape[0]
    patches = row_count // n_img
    padded = -(-patches // 16) * 16
    factor = 1.0 / math.sqrt(width // HEADS)
    seq = Order(q)
    bits = list(reversed(range(n.bit_length() - 1)))
    near = min(1, len(bits) - 1)
    shard_order = jnp.asarray(masks(bits), jnp.int32) ^ f
    group_order = jnp.arange(4, dtype=jnp.int32) ^ q
    order = jnp.concatenate([shard_order, q[None]])

    def last_three(chain):
        while len(chain.bits) > 3:
            chain.launch()
            seq.land((), chain)
            chain.join()
        return chain

    small = [b_q, b_v, b_out, gain_one, shift_one, b_fc2, gain_two, shift_two, b_fc1]
    qkv = last_three(Gather(seq, first_payload(q, w_qkv, small), n, bits))
    qkv.launch()
    rest_own, two_own = payloads([seq.at(q), q ^ 2], w_fc1, w_fc2)
    rest_own, two_own = seq.land((rest_own, two_own), qkv)
    rest = Sent(lax.all_gather(rest_own, "fsdp", axis=0, tiled=False))
    two = Sent(lax.all_gather(two_own, "fsdp", axis=0, tiled=False))
    out_own = [lax.dynamic_slice(w_out, (0, g * quarter), (rows, quarter)) for g in (q, q ^ 2)]
    out = last_three(Gather(seq, jnp.concatenate(out_own, axis=1).astype(half), n, bits))

    def spread_rows(value):
        split = value.reshape(n_img, patches, width)
        return jnp.pad(split, ((0, 0), (0, padded - patches), (0, 0)))

    def compact(value):
        return value.reshape(n_img, padded, width)[:, :patches].reshape(row_count, width)

    qkv.join()
    qkv.launch()
    spread_tokens = seq.land(spread_rows(seq.at(tokens)), qkv)
    qkv_near = qkv.join()
    qkv.launch()
    near_b, near_c = Sent(core_swap(qkv.held)), Sent(x_swap(qkv.held))
    out.launch()
    places = table(scale_codes, width)
    row_place = jnp.broadcast_to(places[:, :, None], (n_img, GRID, GRID, width // 2))
    col_place = jnp.broadcast_to(places[:, None], (n_img, GRID, GRID, width // 2))
    place = jnp.concatenate([row_place, col_place], axis=-1).reshape(n_img, patches, width)
    place = jnp.pad(place, ((0, 0), (0, padded - patches), (0, 0)))
    x_zero = (seq.at(spread_tokens).astype(full) + place).reshape(-1, width)
    x_zero = seq.land(x_zero, qkv, near_b, out)
    qkv_far = seq.at(qkv.got)
    far_b, far_c = Sent(core_swap(qkv_far)), Sent(x_swap(qkv_far))
    out.join()
    out.launch()
    vectors, bias_fc1, bias_qkv = unpack_vectors(seq.at(order), (qkv_near, qkv_far), n, rows, ffq)
    _, _, full_bout, gain_one_f, shift_one_f, full_bfc2, gain_two_f, shift_two_f = vectors
    normed_one = layer_norm(x_zero, gain_one_f, shift_one_f).astype(half)
    normed_one = seq.land(normed_one, far_b)

    first = attention_forward(
        seq.at(order), normed_one, bias_qkv[:2], ((qkv_near, qkv_far), (near_b.value, far_b.value)),
        n_img, patches, factor,
    )
    first = (seq.land(first[0], near_c, far_c, out), *first[1:])
    near_c, far_c = seq.at((near_c.value, far_c.value))
    near_d, far_d = Sent(core_swap(near_c)), Sent(core_swap(far_c))
    out.join()
    out.launch()
    cot = seq.land(spread_rows(cotangent).reshape(-1, width), near_d, far_d)
    second = attention_forward(
        seq.at(order), normed_one, bias_qkv[2:], ((near_c, far_c), (near_d.value, far_d.value)),
        n_img, patches, factor,
    )
    second = (seq.land(second[0], out, rest), *second[1:])
    out_a = seq.at(out.join())
    out_b = Sent(core_swap(out_a))
    seq.land((), out_b)
    rest_a = seq.at(rest.value)
    rest_b = Sent(core_swap(rest_a))
    up_c = Sent(x_swap(seq.at(rest_a[:, :, :hidden])))
    outs = (out_a, out_b.value)
    qkv_parts = (
        (qkv_near, qkv_far), (near_b.value, far_b.value), (near_c, far_c), (near_d.value, far_d.value)
    )
    qkvs = (*first[:2], *second[:2])
    mixed = (*first[2:4], *second[2:4])
    lses = (*first[4:], *second[4:])
    after_attn, normed_two = attention_out(
        seq.at(order), x_zero, mixed, outs, full_bout, gain_two_f, shift_two_f
    )
    normed_two = seq.land(normed_two, rest_b)

    up_g1, down_g1, g_bias_1, back_sum, out_sum = mlp(
        seq.at(order), normed_two, cot, bias_fc1[1], rest_b.value, rest_b.value, hidden
    )
    up_g0, down_g0, g_bias_0, back_sum, out_sum = mlp(
        order, normed_two, cot, bias_fc1[0], rest_a, rest_a, hidden, (out_sum, back_sum)
    )
    up_g0 = seq.land(up_g0, up_c, two)
    up_g1 = seq.at(up_g1)
    up_got = Sent(core_swap(up_g1))
    down_g1 = seq.at(down_g1)
    down_got = Sent(core_swap(down_g1))
    seq.land((), up_got)
    red_up = Reduce(seq, (up_g0, up_got.value), n)
    red_up.launch()
    seq.land((), down_got)
    red_down = Reduce(seq, (down_g0, down_got.value), n)
    red_down.launch(near)
    up_c, two = seq.at((up_c.value, two.value))
    up_d, two_d = Sent(core_swap(up_c)), Sent(core_swap(two))
    up_g2, down_g2, g_bias_2, back_sum, out_sum = mlp(
        seq.at(order), normed_two, cot, bias_fc1[2], up_c, two, 0, (out_sum, back_sum)
    )
    up_g2 = seq.land(up_g2, up_d, two_d, red_up, red_down)
    red_up.launch()
    red_down.launch()
    up_g3, down_g3, g_bias_3, grad_two_in, block = mlp(
        seq.at(order), normed_two, cot, bias_fc1[3], up_d.value, two_d.value, 0,
        (out_sum, back_sum), (after_attn, full_bfc2),
    )
    up_g3 = seq.land(up_g3, red_up, red_down)
    up_got = Sent(core_swap(up_g3))
    down_g3 = seq.at(down_g3)
    down_got = Sent(core_swap(down_g3))
    red_up.launch()
    red_down.launch()
    seq.land((), up_got)
    two_up = Reduce(seq, (up_g2, up_got.value), n)
    two_up.launch()
    seq.land((), down_got)
    two_down = Reduce(seq, (down_g2, down_got.value), n)
    two_down.launch(near)

    after_grad, mg0, mg1, mg2, mg3, g_out, sums_two = attention_out_back(
        seq.at(order), grad_two_in, after_attn, cot, gain_two_f, mixed, outs
    )
    mg2 = seq.at(mg2)
    g_w2, g_w3, proj2, proj3, sums_b = attention_back(
        seq.at(order), normed_one, qkvs[2:], lses[2:], (mg2, mg3), g_out, (2, 3), n_img, patches, factor, n
    )
    g_w3 = seq.land(g_w3, red_up, red_down, two_up, two_down)
    w_3 = Sent(core_swap(g_w3))
    two_up.launch()
    two_down.launch()
    seq.land((), w_3)
    middle = n // 2
    half_shape = (2,) * (len(bits) - 1)
    w_high = Sent(x_swap(seq.at(rounded_sum([g_w2[middle:], w_3.value[middle:]]))))
    g_w0, g_w1, proj0, proj1, sums_a = attention_back(
        seq.at(order), normed_one, qkvs[:2], lses[:2], (mg0, mg1), g_out, (0, 1), n_img, patches, factor, n
    )
    g_w1 = seq.land(g_w1, two_up, two_down, w_high)
    w_1 = Sent(core_swap(g_w1))
    two_up.launch()
    two_down.launch()
    seq.land((), w_1)
    red_w = Reduce(seq, (g_w0, w_1.value), n)
    red_w.launch(0, [w_high.value.reshape(half_shape + w_high.value.shape[1:])])
    w_low = Sent(x_swap(seq.at(rounded_sum([g_w2[:middle], w_3.value[:middle]]))))
    tokens_grad, sums_one = input_back(
        seq.at(order), x_zero, after_grad, gain_one_f, (proj0, proj1, proj2, proj3), qkv_parts
    )
    sums_one = seq.land(sums_one, two_up, two_down, red_w, w_low)
    red_w.terms = [*red_w.terms, w_low.value.reshape(half_shape + w_low.value.shape[1:])]
    while len(red_w.axes) > 2:
        red_w.launch()
        seq.land((), red_w)
    red_w.launch()
    packed = pack_sums(
        seq.at(order),
        n,
        rows,
        ffq,
        (sums_a, sums_b),
        (jnp.stack([g_bias_0, g_bias_1]), jnp.stack([g_bias_2, g_bias_3])),
        (sums_two, sums_one),
    )
    sums = Reduce(seq, (packed,), n, full)
    while len(sums.axes) > 3:
        sums.launch()
        seq.land((), sums)
    sums.launch()
    own_part = jnp.stack([red_up.rest().piece(), red_down.rest().piece()])
    across_part = jnp.stack([two_up.rest().piece(), two_down.rest().piece()])
    pair = seq.at(jnp.stack([own_part, across_part]))
    cross = Sent(x_swap(pair))
    seq.land((), red_w, sums)
    red_w.launch()
    sums.launch()
    seq.land((), sums, red_w)
    w_spread = Spread(seq, red_w.piece())
    sums.launch()
    seq.land((), cross)
    totals = jnp.stack([rounded_sum([pair[0], cross.value[1]]), rounded_sum([pair[1], cross.value[0]])])
    totals = seq.at(totals)
    beside = Sent(core_swap(totals))
    block, tokens_grad = seq.at((block, tokens_grad))
    block_out, grad_tokens = seq.land((compact(block), compact(tokens_grad)), sums, beside)
    mlp_pieces = seq.at((totals[0], beside.value[0], totals[1], beside.value[1]))
    out_fc1, out_fc2 = finish_mlp(q, mlp_pieces, n)
    packed = sums.piece()
    out_fc2, packed = seq.land((out_fc2, packed), w_spread)
    w_spread.cross()
    peers = Sent([xor_swap(packed, "dp", 4, m) for m in (1, 2, 3)])
    seq.land((), w_spread, peers)
    beside, across, opposite_sum = peers.value
    small_sums = (packed + beside) + (across + opposite_sum)
    out_qkv, out_out = finish_attention(seq.value, w_spread.pieces)
    small_out = [small_sums[k, :rows] for k in range(8)]
    out_bfc1 = small_sums[8:12, :ffq].reshape(-1)
    o_bq, o_bv, o_bout, o_gone, o_sone, o_bfc2, o_gtwo, o_stwo = small_out
    return (
        block_out,
        grad_tokens,
        out_qkv,
        o_bq,
        o_bv,
        out_out,
        o_bout,
        o_gone,
        o_sone,
        out_fc1,
        out_bfc1,
        out_fc2,
        o_bfc2,
        o_gtwo,
        o_stwo,
    )


def solution(mesh):
    rows_split = P(("dp", "fsdp"), None)
    matrix = P("fsdp", None)
    vector = P("fsdp")
    return jax.shard_map(
        local,
        mesh=mesh,
        in_specs=(
            rows_split, P(("dp", "fsdp")), matrix, vector, vector, matrix, vector, vector, vector,
            matrix, vector, matrix, vector, vector, vector, rows_split,
        ),
        out_specs=(
            rows_split, rows_split, matrix, vector, vector, matrix, vector, vector, vector,
            matrix, vector, matrix, vector, vector, vector,
        ),
        check_vma=False,
    )
```

```python
import math

import jax
import jax.numpy as jnp
from jax import lax
from jax.experimental import pallas as pl
from jax.experimental.pallas import tpu as pltpu
from jax.sharding import PartitionSpec as P

HEADS = 16
GRID = 14
NSCALE = 16
norm_eps = 1e-06
half = jnp.bfloat16
full = jnp.float32


def xor_swap(value, axis, size, mask):
    return lax.ppermute(value, axis, [(i, i ^ mask) for i in range(size)])


def core_swap(value):
    return xor_swap(value, "dp", 4, 1)


def x_swap(value):
    return xor_swap(value, "dp", 4, 2)


def masks(bits):
    found = [0]
    for bit in bits:
        found = found + [m | (1 << bit) for m in found]
    return found


class Order:
    def __init__(self, value):
        self.value = value

    def at(self, value):
        value, self.value = lax.optimization_barrier((value, self.value))
        return value

    def land(self, value, *sent):
        value, flights = self.at((value, [s.flight for s in sent]))
        for s, flight in zip(sent, flights, strict=True):
            s.accept(flight)
        return value


class Sent:
    def __init__(self, flight):
        self.flight = flight

    def accept(self, value):
        self.value = value


class Gather:
    def __init__(self, seq, piece, n, bits):
        self.seq, self.held, self.n, self.bits = seq, piece[None], n, list(bits)

    def launch(self):
        self.held = self.seq.at(self.held)
        self.flight = xor_swap(self.held, "fsdp", self.n, 1 << self.bits.pop(0))

    def accept(self, value):
        self.got = value

    def join(self):
        self.held = jnp.concatenate([self.held, self.got])
        return self.held


def rounded_sum(terms, kind=half):
    return sum(t.astype(full) for t in terms).astype(kind)


class Reduce:
    def __init__(self, seq, terms, n, kind=half):
        self.kind = kind
        self.seq, self.n, self.axes = seq, n, list(range(n.bit_length() - 1))
        self.terms = [t.reshape((2,) * len(self.axes) + t.shape[1:]) for t in terms]

    def launch(self, bit=None, more=()):
        bit = self.axes[0] if bit is None else bit
        axis = self.axes.index(bit)
        self.axes.pop(axis)
        low, high = [
            [lax.index_in_dim(t, side, axis, keepdims=False) for t in self.terms] for side in (0, 1)
        ]
        self.terms = low
        self.flight = xor_swap(self.seq.at(rounded_sum([*high, *more], self.kind)), "fsdp", self.n, 1 << bit)

    def accept(self, value):
        self.terms = [*self.terms, value]

    def rest(self):
        while self.axes:
            self.launch()
            self.seq.land((), self)
        return self

    def piece(self):
        return rounded_sum(self.terms, self.kind)


class Spread:
    def __init__(self, seq, piece):
        self.seq, self.pieces = seq, [seq.at(piece)]
        self.flight = [core_swap(self.pieces[0]), x_swap(self.pieces[0])]

    def cross(self):
        self.flight = [core_swap(self.seq.at(self.pieces[2]))]

    def accept(self, value):
        self.pieces += value


ANYWHERE = pl.BlockSpec(memory_space=pl.ANY)
ON_CHIP = pl.BlockSpec(memory_space=pltpu.VMEM)
SCALARS = pl.BlockSpec(memory_space=pltpu.SMEM)


def dot(left, right, dim_left, dim_right):
    return lax.dot_general(
        left, right, (((dim_left,), (dim_right,)), ((), ())), preferred_element_type=full
    )


def call(kernel, name, operands, in_specs, outs, out_specs, scratch):
    return pl.pallas_call(
        kernel,
        out_shape=[jax.ShapeDtypeStruct(shape, kind) for shape, kind in outs],
        in_specs=in_specs,
        out_specs=out_specs,
        scratch_shapes=scratch,
        compiler_params=pltpu.CompilerParams(vmem_limit_bytes=58 * 2**20),
        name=name,
    )(*operands)


def loop(count, body, unroll=1):
    def step(i, carry):
        body(i)
        return carry

    lax.fori_loop(0, count, step, 0, unroll=unroll)


def tile(i, size):
    return pl.ds(pl.multiple_of(i * size, size), size)


def bring(src, dst, sem):
    pltpu.make_async_copy(src, dst, sem).start()


def arrived(dst, sem):
    pltpu.make_async_copy(dst, dst, sem).wait()


def fetch(parts, order_ref, place, sem):
    base = 0
    for part in parts:

        def start(r, part=part, base=base):
            shard = r if order_ref is None else order_ref[base + r]
            pltpu.make_async_copy(part.at[r], place(shard), sem).start()

        loop(part.shape[0], start)
        base += part.shape[0]


def head_rows(s, q, n, rows, quarter):
    per = n // 4
    return pl.multiple_of(((s // per) ^ q) * quarter + (s % per) * rows, rows)


def pair_scores(q2, k2):
    first = lax.broadcasted_iota(jnp.int32, q2.shape, 1) < q2.shape[1] // 2
    both = apart(q2, first)
    return both, dot(k2, both, 1, 1), first


def apart(value, first):
    zero = jnp.zeros_like(value)
    return jnp.concatenate([jnp.where(first, value, zero), jnp.where(first, zero, value)])


def attention_forward(order, normed, bias, weights, n_img, patches, factor):
    groups, n_parts = len(weights), len(weights[0])
    wide = weights[0][0].shape[2]
    count, width = normed.shape
    rows = width // sum(part.shape[0] for part in weights[0])
    padded = count // n_img
    quarter = wide // 3

    def kernel(order_ref, normed_ref, bias_ref, *refs):
        w_refs, refs = refs[: groups * n_parts], refs[groups * n_parts :]
        qkv_refs, mixed_refs, refs = refs[:groups], refs[groups : 2 * groups], refs[2 * groups :]
        lse_refs, (w_held, sems) = refs[:groups], refs[groups:]
        for g in range(groups):
            fetch(
                [w.at[:, pl.ds(0, rows)] for w in w_refs[g * n_parts : (g + 1) * n_parts]],
                order_ref,
                lambda s, g=g: w_held.at[g, pl.ds(pl.multiple_of(s * rows, rows), rows)],
                sems.at[g],
            )
        for g in range(groups):
            pltpu.make_async_copy(w_held.at[g], w_held.at[g], sems.at[g]).wait()

            def project(t, g=g):
                at = tile(t, quarter)
                product = dot(normed_ref[...], w_held[g, :, at], 1, 0)
                qkv_refs[g][:, at] = (product + bias_ref[g, :, at]).astype(half)

            loop(3, project)

            def attend(i, g=g):
                at = tile(i // 2, padded)
                lanes = [pl.ds(pl.multiple_of(t * quarter + (i % 2) * 128, 128), 128) for t in range(3)]
                q2 = qkv_refs[g][at, lanes[0]] * factor
                k2 = qkv_refs[g][at, lanes[1]]
                v2 = qkv_refs[g][at, lanes[2]]
                _, scores, first = pair_scores(q2, k2)
                key = lax.broadcasted_iota(jnp.int32, scores.shape, 0)
                scores = jnp.where(key < patches, scores, -1e30)
                top = jnp.max(scores, axis=0, keepdims=True)
                raised = jnp.exp(scores - top)
                total = jnp.sum(raised, axis=0, keepdims=True)
                lse_refs[g][i] = top + jnp.log(total)
                out = dot((raised * (1.0 / total)).astype(half), v2, 0, 0)
                mixed_refs[g][at, lanes[0]] = jnp.where(first, out[:padded], out[padded:]).astype(half)

            loop(2 * n_img, attend, 2 * n_img)

    return call(
        kernel,
        "attention_forward",
        (order, normed, bias, *(part for w in weights for part in w)),
        [SCALARS, ON_CHIP, ON_CHIP] + [ANYWHERE] * (groups * n_parts),
        [((count, wide), half)] * groups
        + [((count, quarter), half)] * groups
        + [((2 * n_img, 1, 2 * padded), full)] * groups,
        [ON_CHIP] * (3 * groups),
        [pltpu.VMEM((groups, width, wide), half), pltpu.SemaphoreType.DMA((groups,))],
    )


def layer_norm(value, gain, shift):
    center = jnp.mean(value, axis=-1, keepdims=True)
    offset = value - center
    spread = jnp.mean(offset * offset, axis=-1, keepdims=True)
    return offset * lax.rsqrt(spread + norm_eps) * gain + shift


def layer_norm_back(value, grad, gain):
    center = jnp.mean(value, axis=-1, keepdims=True)
    offset = value - center
    scale = lax.rsqrt(jnp.mean(offset * offset, axis=-1, keepdims=True) + norm_eps)
    unit = offset * scale
    scaled = grad * gain
    inner = jnp.mean(scaled * unit, axis=-1, keepdims=True)
    return scale * (scaled - jnp.mean(scaled, axis=-1, keepdims=True) - unit * inner), grad * unit


def load_out(order_ref, out_refs, held, sem, n, rows, quarter):
    q = order_ref[n]
    for j in range(4):
        column = pl.multiple_of((q ^ j) * quarter, quarter)
        fetch(
            [out_refs[j % 2].at[:, :, pl.ds(j // 2 * quarter, quarter)]],
            order_ref,
            lambda s, column=column: held.at[
                pl.ds(head_rows(s, q, n, rows, quarter), rows), pl.ds(column, quarter)
            ],
            sem,
        )


CHUNK = 16
ROWS = 64


def attention_out(order, x_zero, mixed, outs, bias, gain, shift):
    count, width = x_zero.shape
    n, rows, _ = outs[0].shape
    quarter = mixed[0].shape[1]

    def kernel(order_ref, x_ref, bias_ref, gain_ref, shift_ref, *refs):
        mixed_refs, out_refs = refs[:4], refs[4:6]
        after_ref, normed_ref, held, x_held, sems = refs[6:]
        bring(x_ref, x_held, sems.at[1])
        load_out(order_ref, out_refs, held, sems.at[0], n, rows, quarter)
        together = jnp.concatenate([m[...] for m in mixed_refs], axis=1)
        pltpu.make_async_copy(held, held, sems.at[0]).wait()
        after_ref[...] = dot(together, held[...], 1, 0)
        arrived(x_held, sems.at[1])

        def finish(i):
            at = tile(i, CHUNK)
            after = x_held[at] + (after_ref[at] + bias_ref[...])
            after_ref[at] = after
            normed_ref[at] = layer_norm(after, gain_ref[...], shift_ref[...]).astype(half)

        loop(count // CHUNK, finish, 13)

    return call(
        kernel,
        "attention_out",
        (order, x_zero, bias, gain, shift, *mixed, *outs),
        [SCALARS, ANYWHERE] + [ON_CHIP] * 7 + [ANYWHERE] * 2,
        [((count, width), full), ((count, width), half)],
        [ON_CHIP] * 2,
        [
            pltpu.VMEM((width, width), half),
            pltpu.VMEM((count, width), full),
            pltpu.SemaphoreType.DMA((2,)),
        ],
    )


def mlp(order, normed, cot, bias, up_all, down_all, down_start, carried=None, ending=None):
    count, width = normed.shape
    n, rows, _ = up_all.shape
    hidden = bias.shape[1]
    share = hidden // n
    step = min(512, hidden)
    steps = hidden // step
    more = [*(carried or []), *(ending[:1] if ending else [])]
    last = list(ending[1:]) if ending else []

    def kernel(order_ref, bias_ref, *refs):
        last_refs, refs = refs[: len(last)], refs[len(last) :]
        normed_ref, cot_ref, up_ref, down_ref, refs = *refs[:4], refs[4:]
        more_refs, refs = refs[: len(more)], refs[len(more) :]
        g_up_ref, g_down_ref, g_bias_ref, back_ref, end_ref, refs = *refs[:5], refs[5:]
        held, refs = refs[: len(more)], refs[len(more) :]
        rows_in, cots, out, back, up, down, pre, act, act_half, pre_half, g_up, g_down, sems = refs
        bring(normed_ref, rows_in, sems.at[3])
        fetch(
            [up_ref.at[:, :, pl.ds(0, hidden)]],
            None,
            lambda s: up.at[pl.ds(pl.multiple_of(s * rows, rows), rows)],
            sems.at[0],
        )
        bring(cot_ref, cots, sems.at[4])
        fetch(
            [down_ref.at[:, :, pl.ds(down_start, width)]],
            None,
            lambda s: down.at[pl.ds(pl.multiple_of(s * share, share), share)],
            sems.at[1],
        )
        for k in range(len(more)):
            bring(more_refs[k], held[k], sems.at[5 + k])
        arrived(rows_in, sems.at[3])
        arrived(up, sems.at[0])
        for t in range(steps):
            at = pl.ds(t * step, step)
            pre[...] = dot(rows_in[...], up[:, at], 1, 0)
            if not t:
                arrived(cots, sems.at[4])
                arrived(down, sems.at[1])
            act[...] = dot(cots[...], down[at, :], 1, 1)

            def gelu(i, at=at):
                some = tile(i, 2 * CHUNK)
                x = pre[some] + bias_ref[:, at]
                below = 0.5 * (1.0 + lax.erf(x * math.sqrt(0.5)))
                density = jnp.exp(-0.5 * x * x) * (1.0 / math.sqrt(2.0 * math.pi))
                act_half[some] = (x * below).astype(half)
                pre_half[some] = (act[some] * (below + x * density)).astype(half)

            loop(count // CHUNK // 2, gelu)
            p = pre_half[...]
            h = act_half[...]
            more_back = dot(p, up[:, at], 1, 1)
            more_out = dot(h, down[at, :], 1, 0)
            if t:
                back[...] += more_back
                out[...] += more_out
            elif carried:
                arrived(held[0], sems.at[5])
                arrived(held[1], sems.at[6])
                out[...] = held[0][...] + more_out
                back[...] = held[1][...] + more_back
            else:
                out[...] = more_out
                back[...] = more_back
            if t == steps - 1:
                bring(back, back_ref, sems.at[3])
                if not ending:
                    bring(out, end_ref, sems.at[4])
            g_down[at, :] = dot(h, cots[...], 0, 0).astype(half)
            if t == steps - 1:

                def send_down(r):
                    at = pl.multiple_of(order_ref[r] * share, share)
                    bring(g_down.at[pl.ds(at, share)], g_down_ref.at[r], sems.at[2])

                loop(n, send_down)
            g_up[:, at] = dot(rows_in[...], p, 0, 0).astype(half)
            g_bias_ref[:, at] = jnp.sum(p.astype(full), axis=0, keepdims=True)

        def send_up(r):
            at = pl.multiple_of(order_ref[r] * rows, rows)
            bring(g_up.at[pl.ds(at, rows)], g_up_ref.at[r], sems.at[0])

        loop(n, send_up)
        if ending:
            arrived(held[2], sems.at[7])

            def finish(i):
                at = tile(i, 2 * CHUNK)
                end_ref[at] = (held[2][at] + (out[at] + last_refs[0][...])).astype(half)

            loop(count // CHUNK // 2, finish)
        else:
            arrived(end_ref, sems.at[4])
        arrived(back_ref, sems.at[3])
        arrived(g_down_ref, sems.at[2])
        arrived(g_up_ref, sems.at[0])

    sums = pltpu.VMEM((count, width), full)
    wide = pltpu.VMEM((count, width), half)
    square = pltpu.VMEM((width, hidden), half)
    return call(
        kernel,
        "mlp",
        (order, bias, *last, normed, cot, up_all, down_all, *more),
        [SCALARS] + [ON_CHIP] * (1 + len(last)) + [ANYWHERE] * (4 + len(more)),
        [
            ((n, rows, hidden), half),
            ((n, share, width), half),
            ((1, hidden), full),
            ((count, width), full),
            ((count, width), half if ending else full),
        ],
        [ANYWHERE, ANYWHERE, ON_CHIP, ANYWHERE, ON_CHIP if ending else ANYWHERE],
        [
            *([sums] * len(more)),
            wide,
            wide,
            sums,
            sums,
            square,
            pltpu.VMEM((hidden, width), half),
            pltpu.VMEM((count, step), full),
            pltpu.VMEM((count, step), full),
            pltpu.VMEM((count, step), half),
            pltpu.VMEM((count, step), half),
            square,
            pltpu.VMEM((hidden, width), half),
            pltpu.SemaphoreType.DMA((5 + len(more),)),
        ],
    )


def attention_out_back(order, grad, after, cot, gain, mixed, outs):
    count, width = after.shape
    n, rows, _ = outs[0].shape
    quarter = mixed[0].shape[1]

    def kernel(order_ref, grad_ref, after_ref, cot_ref, gain_ref, *refs):
        mixed_refs, out_refs, refs = refs[:4], refs[4:6], refs[6:]
        after_grad_ref, mixed_grad_refs, g_out_ref, sums_ref = refs[0], refs[1:5], refs[5], refs[6]
        held, branch, terms, grad, after, cot, mixes, sems = refs[7:]
        block = count // 4
        for k in range(4):
            some = pl.ds(k * block, block)
            bring(grad_ref.at[some], grad.at[some], sems.at[1 + k])
            bring(after_ref.at[some], after.at[some], sems.at[5 + k])
            bring(cot_ref.at[some], cot.at[some], sems.at[9 + k])
        load_out(order_ref, out_refs, held, sems.at[0], n, rows, quarter)
        for j in range(4):
            bring(mixed_refs[j], mixes.at[j], sems.at[13])
        terms[...] = jnp.zeros_like(terms)

        def fold(value):
            return jnp.sum(value.reshape(CHUNK // 8, 8, width), axis=0)

        def back(i, k):
            at = pl.ds(pl.multiple_of(k * block + i * CHUNK, CHUNK), CHUNK)
            incoming = grad[at]
            part, gain_terms = layer_norm_back(after[at], incoming, gain_ref[...])
            own = cot[at].astype(full)
            total = own + part
            after_grad_ref[at] = total
            rounded = total.astype(half)
            branch[at] = rounded
            terms[0] += fold(rounded.astype(full))
            terms[1] += fold(gain_terms)
            terms[2] += fold(incoming)
            terms[3] += fold(own)

        for k in range(4):
            some = pl.ds(k * block, block)
            arrived(grad.at[some], sems.at[1 + k])
            arrived(after.at[some], sems.at[5 + k])
            arrived(cot.at[some], sems.at[9 + k])
            loop(block // CHUNK, lambda i, k=k: back(i, k), 13)
        for k in range(4):
            sums_ref[k] = jnp.sum(terms[k], axis=0, keepdims=True)
        arrived(held, sems.at[0])
        arrived(mixes, sems.at[13])
        for j in range(4):
            mixed_grad_refs[j][...] = dot(branch[...], held[j * quarter : (j + 1) * quarter], 1, 1).astype(half)
            g_out_ref[j * quarter : (j + 1) * quarter] = dot(mixes[j], branch[...], 0, 0).astype(half)

    return call(
        kernel,
        "attention_out_back",
        (order, grad, after, cot, gain, *mixed, *outs),
        [SCALARS] + [ANYWHERE] * 3 + [ON_CHIP] + [ANYWHERE] * 6,
        [((count, width), full)]
        + [((count, quarter), half)] * 4
        + [((width, width), half), ((4, 1, width), full)],
        [ON_CHIP] * 7,
        [
            pltpu.VMEM((width, width), half),
            pltpu.VMEM((count, width), half),
            pltpu.VMEM((4, 8, width), full),
            pltpu.VMEM((count, width), full),
            pltpu.VMEM((count, width), full),
            pltpu.VMEM((count, width), half),
            pltpu.VMEM((4, count, quarter), half),
            pltpu.SemaphoreType.DMA((14,)),
        ],
    )


def attention_back(order, normed, qkvs, lses, mixed_grads, g_out, which, n_img, patches, factor, n):
    groups = len(qkvs)
    count, width = normed.shape
    wide = qkvs[0].shape[1]
    quarter = wide // 3
    padded = count // n_img
    rows = width // n

    def kernel(order_ref, normed_ref, g_out_ref, *refs):
        qkv_refs, mg_refs, refs = refs[:groups], refs[groups : 2 * groups], refs[2 * groups :]
        lse_refs, refs = refs[:groups], refs[groups:]
        g_w_refs, proj_refs, sums_ref = refs[:groups], refs[groups : 2 * groups], refs[2 * groups]
        g_w, normed_held, g_out_held, sems = refs[2 * groups + 1 :]
        q = order_ref[n]
        bring(g_out_ref, g_out_held, sems.at[groups])
        bring(normed_ref, normed_held, sems.at[groups + 1])
        for g in range(groups):

            def attend(i, g=g):
                at = tile(i // 2, padded)
                lanes = [pl.ds(pl.multiple_of(t * quarter + (i % 2) * 128, 128), 128) for t in range(3)]
                q2 = qkv_refs[g][at, lanes[0]] * factor
                k2 = qkv_refs[g][at, lanes[1]]
                v2 = qkv_refs[g][at, lanes[2]]
                both, scores, first = pair_scores(q2, k2)
                key = lax.broadcasted_iota(jnp.int32, scores.shape, 0)
                probs = jnp.where(key < patches, jnp.exp(scores - lse_refs[g][i]), 0.0)
                o_both = apart(mg_refs[g][at, lanes[0]], first)
                g_probs = dot(v2, o_both, 1, 1)
                weighted = jnp.sum(probs * g_probs, axis=0, keepdims=True)
                g_scores = (probs * (g_probs - weighted)).astype(half)
                g_query = dot(g_scores, k2, 0, 0)
                g_query = jnp.where(first, g_query[:padded], g_query[padded:]) * factor
                proj_refs[g][at, lanes[0]] = g_query.astype(half)
                proj_refs[g][at, lanes[1]] = dot(g_scores, both, 1, 0).astype(half)
                proj_refs[g][at, lanes[2]] = dot(probs.astype(half), o_both, 1, 0).astype(half)

            loop(2 * n_img, attend, 4)
            if not g:
                arrived(g_out_held, sems.at[groups])
                arrived(normed_held, sems.at[groups + 1])

            def send_out(r, g=g):
                at = head_rows(order_ref[r], q, n, rows, quarter)
                column = pl.multiple_of((q ^ which[g]) * quarter, quarter)
                pltpu.make_async_copy(
                    g_out_held.at[pl.ds(at, rows), pl.ds(column, quarter)],
                    g_w_refs[g].at[r, :, pl.ds(wide, quarter)],
                    sems.at[g],
                ).start()

            loop(n, send_out)

            def weigh(t, g=g):
                at = tile(t, quarter)
                some = proj_refs[g][:, at]
                g_w[g, :, at] = dot(normed_held[...], some, 0, 0).astype(half)
                sums_ref[g, :, at] = jnp.sum(some.astype(full), axis=0, keepdims=True)

            loop(3, weigh)

            def send(r, g=g):
                at = pl.multiple_of(order_ref[r] * rows, rows)
                pltpu.make_async_copy(
                    g_w.at[g, pl.ds(at, rows)], g_w_refs[g].at[r, :, pl.ds(0, wide)], sems.at[g]
                ).start()

            loop(n, send)
        for g in range(groups):
            pltpu.make_async_copy(g_w_refs[g], g_w_refs[g], sems.at[g]).wait()

    return call(
        kernel,
        "attention_back",
        (order, normed, g_out, *qkvs, *mixed_grads, *lses),
        [SCALARS] + [ANYWHERE] * 2 + [ON_CHIP] * (3 * groups),
        [((n, rows, wide + quarter), half)] * groups
        + [((count, wide), half)] * groups
        + [((groups, 1, wide), full)],
        [ANYWHERE] * groups + [ON_CHIP] * (groups + 1),
        [
            pltpu.VMEM((groups, width, wide), half),
            pltpu.VMEM((count, width), half),
            pltpu.VMEM((width, width), half),
            pltpu.SemaphoreType.DMA((groups + 2,)),
        ],
    )


def input_back(order, x_zero, after_grad, gain, projs, weights):
    count, width = x_zero.shape
    wide = weights[0][0].shape[2]
    rows = width // sum(part.shape[0] for part in weights[0])
    parts = [part for w in weights for part in w]
    n_parts = len(weights[0])

    def kernel(order_ref, x_ref, after_ref, gain_ref, *refs):
        proj_refs, w_refs = refs[:4], refs[4 : 4 + len(parts)]
        token_ref, sums_ref, held, terms, x_held, after_held, sems = refs[4 + len(parts) :]
        for j in range(4):
            fetch(
                [w.at[:, pl.ds(0, rows)] for w in w_refs[j * n_parts : (j + 1) * n_parts]],
                order_ref,
                lambda s, j=j: held.at[j, pl.ds(pl.multiple_of(s * rows, rows), rows)],
                sems.at[j],
            )
        bring(x_ref, x_held, sems.at[4])
        bring(after_ref, after_held, sems.at[5])
        for j in range(4):
            arrived(held.at[j], sems.at[j])
            product = dot(proj_refs[j][...], held[j], 1, 1)
            if j == 0:
                token_ref[...] = product
            else:
                token_ref[...] += product
        arrived(x_held, sems.at[4])
        arrived(after_held, sems.at[5])
        terms[...] = jnp.zeros_like(terms)

        def fold(value):
            return jnp.sum(value.reshape(ROWS // 8, 8, width), axis=0)

        def back(i):
            at = tile(i, ROWS)
            incoming = token_ref[at]
            part, gain_terms = layer_norm_back(x_held[at], incoming, gain_ref[...])
            token_ref[at] = after_held[at] + part
            terms[0] += fold(gain_terms)
            terms[1] += fold(incoming)

        loop(count // ROWS, back)
        for k in range(2):
            sums_ref[k] = jnp.sum(terms[k], axis=0, keepdims=True)

    return call(
        kernel,
        "input_back",
        (order, x_zero, after_grad, gain, *projs, *parts),
        [SCALARS] + [ANYWHERE] * 2 + [ON_CHIP] * 5 + [ANYWHERE] * len(parts),
        [((count, width), full), ((2, 1, width), full)],
        [ON_CHIP] * 2,
        [
            pltpu.VMEM((4, width, wide), half),
            pltpu.VMEM((2, 8, width), full),
            pltpu.VMEM((count, width), full),
            pltpu.VMEM((count, width), full),
            pltpu.SemaphoreType.DMA((6,)),
        ],
    )


def payloads(which, w_fc1, w_fc2):
    rows, ff = w_fc1.shape
    full_share, width = w_fc2.shape
    share = full_share // 4
    n = ff // full_share
    hidden = n * share
    own, across = which
    if share % 128:
        fc1 = [lax.dynamic_slice(w_fc1, (0, (4 * s + own) * share), (rows, share)) for s in range(n)]
        fc2 = [lax.dynamic_slice(w_fc2, (g * share, 0), (share, width)).astype(half) for g in which]
        rest = jnp.concatenate([*fc1, fc2[0].reshape(rows, -1).astype(full)], axis=1)
        return rest.astype(half), fc2[1]

    def kernel(which_ref, fc1_ref, fc2_ref, rest_ref, two_ref):
        for s in range(n):
            at = pl.ds(pl.multiple_of((4 * s + which_ref[0]) * share, share), share)
            rest_ref[:, s * share : (s + 1) * share] = fc1_ref[:, at].astype(half)
        rest_ref[:, hidden : hidden + width] = fc2_ref[tile(which_ref[0], share), :].astype(half)
        two_ref[...] = fc2_ref[tile(which_ref[1], share), :].astype(half)

    return call(
        kernel,
        "payloads",
        (jnp.stack(which), w_fc1, w_fc2),
        [SCALARS] + [ON_CHIP] * 2,
        [((rows, hidden + width), half), ((share, width), half)],
        [ON_CHIP] * 2,
        [],
    )


def natural_quarters(q, pieces):
    once = [jnp.where((q & 1) == 1, pieces[i ^ 1], pieces[i]) for i in range(4)]
    return [jnp.where(q >= 2, once[i ^ 2], once[i]) for i in range(4)]


def finish_mlp(q, totals, swapped, n):
    _, _, rows, width = totals.shape
    share = width // n
    if share % 128:
        pieces = natural_quarters(q, [totals[0], swapped[0], totals[1], swapped[1]])
        fc1 = jnp.stack([p[0].reshape(rows, n, share) for p in pieces], axis=2).reshape(rows, 4 * width)
        return fc1.astype(full), jnp.concatenate([p[1] for p in pieces]).astype(full)

    def kernel(q_ref, *refs):
        fc1_ref, fc2_ref = refs[2:]
        for j in range(4):
            g = q_ref[0] ^ j
            held = refs[j % 2].at[j // 2]
            for s in range(n):
                at = pl.ds(pl.multiple_of((4 * s + g) * share, share), share)
                fc1_ref[:, at] = held[0, :, s * share : (s + 1) * share].astype(full)
            fc2_ref[tile(g, rows), :] = held[1].astype(full)

    return call(
        kernel,
        "finish_mlp",
        (q[None], totals, swapped),
        [SCALARS] + [ON_CHIP] * 2,
        [((rows, 4 * width), full), ((4 * rows, width), full)],
        [ON_CHIP] * 2,
        [],
    )


def finish_attention(q, pieces):
    rows, width = pieces[0].shape
    quarter = width // 4

    def kernel(q_ref, *refs):
        qkv_ref, out_ref = refs[4:]
        for j in range(4):
            g = q_ref[0] ^ j
            for t in range(3):
                at = pl.ds(pl.multiple_of(t * width + g * quarter, quarter), quarter)
                qkv_ref[:, at] = refs[j][:, t * quarter : (t + 1) * quarter].astype(full)
            out_ref[:, tile(g, quarter)] = refs[j][:, 3 * quarter :].astype(full)

    return call(
        kernel,
        "finish_attention",
        (q[None], *pieces),
        [SCALARS] + [ON_CHIP] * 4,
        [((rows, 3 * width), full), ((rows, width), full)],
        [ON_CHIP] * 2,
        [],
    )


BELOW = 16


def first_payload(q, w_qkv, vectors):
    rows, columns = w_qkv.shape
    width = columns // 3
    quarter = width // 4
    wide = 3 * quarter

    def kernel(q_ref, w_ref, *refs):
        out_ref, held, low, sem = refs[len(vectors) :]
        for t in range(3):
            at = pl.multiple_of(t * width + q_ref[0] * quarter, quarter)
            pltpu.make_async_copy(
                w_ref.at[:, pl.ds(at, quarter)], held.at[:, pl.ds(t * quarter, quarter)], sem.at[0]
            ).start()
        low[...] = jnp.zeros_like(low)
        for k, vector in enumerate(refs[: len(vectors)]):
            low[k : k + 1, : vector.shape[1]] = vector[...]
        out_ref[rows:] = low[...].astype(half)
        pltpu.make_async_copy(held, held, sem.at[0]).wait()
        out_ref[:rows] = held[...].astype(half)

    return call(
        kernel,
        "first_payload",
        (q[None], w_qkv, *(v[None] for v in vectors)),
        [SCALARS, ANYWHERE] + [ON_CHIP] * len(vectors),
        [((rows + BELOW, wide), half)],
        [ON_CHIP],
        [pltpu.VMEM((rows, wide), full), pltpu.VMEM((BELOW, wide), full), pltpu.SemaphoreType.DMA((1,))],
    )[0]


def unpack_vectors(order, parts, n, rows, share):
    width = n * rows
    quarter = width // 4
    if rows % 128 or share % 128:
        q = order[n]
        held = jnp.concatenate([p[:, rows:] for p in parts]).astype(full)
        held = held[jnp.zeros((n,), jnp.int32).at[order[:n]].set(jnp.arange(n, dtype=jnp.int32))]
        groups = jnp.arange(4, dtype=jnp.int32) ^ q
        vectors = jnp.stack([held[:, k, :rows].reshape(1, width) for k in range(8)])
        units = held[:, 8, : 4 * share].reshape(n, 4, share).transpose(1, 0, 2)[groups]
        ends = [vectors[k].reshape(4, 1, quarter)[groups] for k in range(2)]
        return vectors, units.reshape(4, 1, width), jnp.concatenate([ends[0], 0 * ends[0], ends[1]], axis=2)

    def kernel(order_ref, *refs):
        part_refs, (vector_ref, fc1_ref, qkv_ref, held, wider, sem) = refs[: len(parts)], refs[len(parts) :]
        base = 0
        for part in part_refs:
            size = part.shape[0]
            pltpu.make_async_copy(part.at[:, pl.ds(rows, BELOW)], held.at[pl.ds(base, size)], sem.at[0]).start()
            base += size
        pltpu.make_async_copy(held, held, sem.at[0]).wait()
        wider[...] = held[...].astype(full)
        q = order_ref[n]
        for r in range(n):
            at = tile(order_ref[r], rows)
            for k in range(8):
                vector_ref[k, :, at] = wider[r, k : k + 1, :rows]
            for j in range(4):
                fc1_ref[j, :, tile(order_ref[r], share)] = wider[r, 8:9, tile(q ^ j, share)]
        for j in range(4):
            at = tile(q ^ j, quarter)
            qkv_ref[j, :, :quarter] = vector_ref[0, :, at]
            qkv_ref[j, :, quarter : 2 * quarter] = jnp.zeros((1, quarter), full)
            qkv_ref[j, :, 2 * quarter :] = vector_ref[1, :, at]

    return call(
        kernel,
        "unpack_vectors",
        (order, *parts),
        [SCALARS] + [ANYWHERE] * len(parts),
        [((8, 1, width), full), ((4, 1, width), full), ((4, 1, 3 * quarter), full)],
        [ON_CHIP] * 3,
        [
            pltpu.VMEM((n, BELOW, 3 * quarter), half),
            pltpu.VMEM((n, BELOW, 3 * quarter), full),
            pltpu.SemaphoreType.DMA((1,)),
        ],
    )


def pack_sums(order, n, rows, share, proj_sums, unit_sums, wide_sums):
    width = n * rows
    quarter = width // 4
    if rows % 128 or share % 128:
        groups = jnp.arange(4, dtype=jnp.int32) ^ order[n]
        proj = jnp.concatenate(proj_sums)[groups]
        units = jnp.concatenate(unit_sums)[groups].reshape(4, n, share)
        flat = [proj[:, :, :quarter].reshape(width), proj[:, :, 2 * quarter :].reshape(width)]
        two, one = wide_sums
        flat += [two[0], one[0], one[1], two[3], two[1], two[2]]
        flat = [v.reshape(n, 1, rows) for v in flat]
        stacked = [jnp.pad(v, ((0, 0), (0, 0), (0, 128 - rows))) for v in flat]
        stacked.append(jnp.pad(units.transpose(1, 0, 2), ((0, 0), (0, 4), (0, 128 - share))))
        return jnp.concatenate(stacked, axis=1)[order[:n]]

    def kernel(order_ref, proj_a, proj_b, unit_a, unit_b, two_ref, one_ref, out_ref, proj, units):
        proj[:2], proj[2:] = proj_a[...], proj_b[...]
        units[:2], units[2:] = unit_a[...], unit_b[...]
        q = order_ref[n]
        per = n // 4
        for r in range(n):
            s = order_ref[r]
            j = (s // per) ^ q
            at = tile(s, rows)
            inside = pl.multiple_of((s % per) * rows, rows)
            out_ref[r, 0:1] = proj[j, :, pl.ds(inside, rows)]
            out_ref[r, 1:2] = proj[j, :, pl.ds(2 * quarter + inside, rows)]
            for k, (ref, row) in enumerate(
                ((two_ref, 0), (one_ref, 0), (one_ref, 1), (two_ref, 3), (two_ref, 1), (two_ref, 2))
            ):
                out_ref[r, 2 + k : 3 + k] = ref[row, :, at]
            for g in range(4):
                out_ref[r, 8 + g : 9 + g] = units[q ^ g, :, tile(s, share)]
            out_ref[r, 12:] = jnp.zeros((4, rows), full)

    sums_two, sums_one = wide_sums
    return call(
        kernel,
        "pack_sums",
        (order, *proj_sums, *unit_sums, sums_two, sums_one),
        [SCALARS] + [ON_CHIP] * 6,
        [((n, 16, rows), full)],
        [ON_CHIP],
        [pltpu.VMEM((4, 1, 3 * quarter), full), pltpu.VMEM((4, 1, width), full)],
    )[0]


def table(codes, width):
    ratio = 0.3 * jnp.exp(codes.astype(full) * (math.log(10.0 / 0.3) / (NSCALE - 1)))
    quarter = width // 4
    omega = jnp.exp(jnp.arange(quarter).astype(full) * (-math.log(10000.0) / quarter))
    steps = jnp.arange(GRID, dtype=jnp.int32).astype(full)
    angle = ratio[:, None, None] * steps[None, :, None] * omega[None, None, :]
    return jnp.concatenate([jnp.sin(angle), jnp.cos(angle)], axis=-1)


def local(
    tokens,
    scale_codes,
    w_qkv,
    b_q,
    b_v,
    w_out,
    b_out,
    gain_one,
    shift_one,
    w_fc1,
    b_fc1,
    w_fc2,
    b_fc2,
    gain_two,
    shift_two,
    cotangent,
):
    n = lax.axis_size("fsdp")
    q = lax.axis_index("dp")
    f = lax.axis_index("fsdp")
    row_count, width = tokens.shape
    rows = width // n
    ff = b_fc1.shape[0] * n
    ffq = ff // n // 4
    hidden = n * ffq
    quarter = width // 4
    n_img = scale_codes.shape[0]
    patches = row_count // n_img
    padded = -(-patches // 16) * 16
    factor = 1.0 / math.sqrt(width // HEADS)
    seq = Order(q)
    bits = list(reversed(range(n.bit_length() - 1)))
    near = min(1, len(bits) - 1)
    shard_order = jnp.asarray(masks(bits), jnp.int32) ^ f
    group_order = jnp.arange(4, dtype=jnp.int32) ^ q
    order = jnp.concatenate([shard_order, q[None]])

    def last_three(chain):
        while len(chain.bits) > 3:
            chain.launch()
            seq.land((), chain)
            chain.join()
        return chain

    small = [b_q, b_v, b_out, gain_one, shift_one, b_fc2, gain_two, shift_two, b_fc1]
    qkv = last_three(Gather(seq, first_payload(q, w_qkv, small), n, bits))
    qkv.launch()
    rest_own, two_own = payloads([seq.at(q), q ^ 2], w_fc1, w_fc2)
    rest_own, two_own = seq.land((rest_own, two_own), qkv)
    rest = Sent(lax.all_gather(rest_own, "fsdp", axis=0, tiled=False))
    two = Sent(lax.all_gather(two_own, "fsdp", axis=0, tiled=False))
    out_own = [lax.dynamic_slice(w_out, (0, g * quarter), (rows, quarter)) for g in (q, q ^ 2)]
    out = last_three(Gather(seq, jnp.concatenate(out_own, axis=1).astype(half), n, bits))

    def spread_rows(value):
        split = value.reshape(n_img, patches, width)
        return jnp.pad(split, ((0, 0), (0, padded - patches), (0, 0)))

    def compact(value):
        return value.reshape(n_img, padded, width)[:, :patches].reshape(row_count, width)

    qkv.join()
    qkv.launch()
    spread_tokens = seq.land(spread_rows(seq.at(tokens)), qkv)
    qkv_near = qkv.join()
    qkv.launch()
    near_b, near_c = Sent(core_swap(qkv.held)), Sent(x_swap(qkv.held))
    out.launch()
    places = table(scale_codes, width)
    row_place = jnp.broadcast_to(places[:, :, None], (n_img, GRID, GRID, width // 2))
    col_place = jnp.broadcast_to(places[:, None], (n_img, GRID, GRID, width // 2))
    place = jnp.concatenate([row_place, col_place], axis=-1).reshape(n_img, patches, width)
    place = jnp.pad(place, ((0, 0), (0, padded - patches), (0, 0)))
    x_zero = (seq.at(spread_tokens).astype(full) + place).reshape(-1, width)
    x_zero = seq.land(x_zero, qkv, near_b, out)
    qkv_far = seq.at(qkv.got)
    far_b, far_c = Sent(core_swap(qkv_far)), Sent(x_swap(qkv_far))
    out.join()
    out.launch()
    vectors, bias_fc1, bias_qkv = unpack_vectors(seq.at(order), (qkv_near, qkv_far), n, rows, ffq)
    _, _, full_bout, gain_one_f, shift_one_f, full_bfc2, gain_two_f, shift_two_f = vectors
    normed_one = layer_norm(x_zero, gain_one_f, shift_one_f).astype(half)
    normed_one = seq.land(normed_one, far_b)

    first = attention_forward(
        seq.at(order), normed_one, bias_qkv[:2], ((qkv_near, qkv_far), (near_b.value, far_b.value)),
        n_img, patches, factor,
    )
    first = (seq.land(first[0], near_c, far_c, out), *first[1:])
    near_c, far_c = seq.at((near_c.value, far_c.value))
    near_d, far_d = Sent(core_swap(near_c)), Sent(core_swap(far_c))
    out.join()
    out.launch()
    cot = seq.land(spread_rows(cotangent).reshape(-1, width), near_d, far_d)
    second = attention_forward(
        seq.at(order), normed_one, bias_qkv[2:], ((near_c, far_c), (near_d.value, far_d.value)),
        n_img, patches, factor,
    )
    second = (seq.land(second[0], out, rest), *second[1:])
    out_a = seq.at(out.join())
    out_b = Sent(core_swap(out_a))
    seq.land((), out_b)
    rest_a = seq.at(rest.value)
    rest_b = Sent(core_swap(rest_a))
    up_c = Sent(x_swap(seq.at(rest_a[:, :, :hidden])))
    outs = (out_a, out_b.value)
    qkv_parts = (
        (qkv_near, qkv_far), (near_b.value, far_b.value), (near_c, far_c), (near_d.value, far_d.value)
    )
    qkvs = (*first[:2], *second[:2])
    mixed = (*first[2:4], *second[2:4])
    lses = (*first[4:], *second[4:])
    after_attn, normed_two = attention_out(
        seq.at(order), x_zero, mixed, outs, full_bout, gain_two_f, shift_two_f
    )
    normed_two = seq.land(normed_two, rest_b)

    up_g1, down_g1, g_bias_1, back_sum, out_sum = mlp(
        seq.at(order), normed_two, cot, bias_fc1[1], rest_b.value, rest_b.value, hidden
    )
    up_g0, down_g0, g_bias_0, back_sum, out_sum = mlp(
        order, normed_two, cot, bias_fc1[0], rest_a, rest_a, hidden, (out_sum, back_sum)
    )
    up_g0 = seq.land(up_g0, up_c, two)
    up_g1 = seq.at(up_g1)
    up_got = Sent(core_swap(up_g1))
    down_g1 = seq.at(down_g1)
    down_got = Sent(core_swap(down_g1))
    seq.land((), up_got)
    red_up = Reduce(seq, (up_g0, up_got.value), n)
    red_up.launch()
    seq.land((), down_got)
    red_down = Reduce(seq, (down_g0, down_got.value), n)
    red_down.launch(near)
    up_c, two = seq.at((up_c.value, two.value))
    up_d, two_d = Sent(core_swap(up_c)), Sent(core_swap(two))
    up_g2, down_g2, g_bias_2, back_sum, out_sum = mlp(
        seq.at(order), normed_two, cot, bias_fc1[2], up_c, two, 0, (out_sum, back_sum)
    )
    up_g2 = seq.land(up_g2, up_d, two_d, red_up, red_down)
    red_up.launch()
    red_down.launch()
    up_g3, down_g3, g_bias_3, grad_two_in, block = mlp(
        seq.at(order), normed_two, cot, bias_fc1[3], up_d.value, two_d.value, 0,
        (out_sum, back_sum), (after_attn, full_bfc2),
    )
    up_g3 = seq.land(up_g3, red_up, red_down)
    up_got = Sent(core_swap(up_g3))
    down_g3 = seq.at(down_g3)
    down_got = Sent(core_swap(down_g3))
    red_up.launch()
    red_down.launch()
    seq.land((), up_got)
    two_up = Reduce(seq, (up_g2, up_got.value), n)
    two_up.launch()
    seq.land((), down_got)
    two_down = Reduce(seq, (down_g2, down_got.value), n)
    two_down.launch(near)

    after_grad, mg0, mg1, mg2, mg3, g_out, sums_two = attention_out_back(
        seq.at(order), grad_two_in, after_attn, cot, gain_two_f, mixed, outs
    )
    mg2 = seq.at(mg2)
    g_w2, g_w3, proj2, proj3, sums_b = attention_back(
        seq.at(order), normed_one, qkvs[2:], lses[2:], (mg2, mg3), g_out, (2, 3), n_img, patches, factor, n
    )
    g_w3 = seq.land(g_w3, red_up, red_down, two_up, two_down)
    w_3 = Sent(core_swap(g_w3))
    two_up.launch()
    two_down.launch()
    seq.land((), w_3)
    middle = n // 2
    half_shape = (2,) * (len(bits) - 1)
    w_high = Sent(x_swap(seq.at(rounded_sum([g_w2[middle:], w_3.value[middle:]]))))
    g_w0, g_w1, proj0, proj1, sums_a = attention_back(
        seq.at(order), normed_one, qkvs[:2], lses[:2], (mg0, mg1), g_out, (0, 1), n_img, patches, factor, n
    )
    g_w1 = seq.land(g_w1, two_up, two_down, w_high)
    w_1 = Sent(core_swap(g_w1))
    two_up.launch()
    two_down.launch()
    seq.land((), w_1)
    red_w = Reduce(seq, (g_w0, w_1.value), n)
    red_w.launch(0, [w_high.value.reshape(half_shape + w_high.value.shape[1:])])
    w_low = Sent(x_swap(seq.at(rounded_sum([g_w2[:middle], w_3.value[:middle]]))))
    tokens_grad, sums_one = input_back(
        seq.at(order), x_zero, after_grad, gain_one_f, (proj0, proj1, proj2, proj3), qkv_parts
    )
    sums_one = seq.land(sums_one, two_up, two_down, red_w, w_low)
    red_w.terms = [*red_w.terms, w_low.value.reshape(half_shape + w_low.value.shape[1:])]
    while len(red_w.axes) > 2:
        red_w.launch()
        seq.land((), red_w)
    red_w.launch()
    packed = pack_sums(
        seq.at(order),
        n,
        rows,
        ffq,
        (sums_a, sums_b),
        (jnp.stack([g_bias_0, g_bias_1]), jnp.stack([g_bias_2, g_bias_3])),
        (sums_two, sums_one),
    )
    sums = Reduce(seq, (packed,), n, full)
    while len(sums.axes) > 3:
        sums.launch()
        seq.land((), sums)
    sums.launch()
    own_part = jnp.stack([red_up.rest().piece(), red_down.rest().piece()])
    across_part = jnp.stack([two_up.rest().piece(), two_down.rest().piece()])
    pair = seq.at(jnp.stack([own_part, across_part]))
    cross = Sent(x_swap(pair))
    grad_tokens = seq.land(compact(seq.at(tokens_grad)), red_w, sums)
    red_w.launch()
    sums.launch()
    block_out = seq.land(compact(seq.at(block)), sums, red_w)
    w_spread = Spread(seq, red_w.piece())
    sums.launch()
    seq.land((), cross)
    totals = jnp.stack([rounded_sum([pair[0], cross.value[1]]), rounded_sum([pair[1], cross.value[0]])])
    totals = seq.at(totals)
    swapped = Sent(core_swap(totals))
    seq.land((), sums, swapped)
    packed = seq.at(sums.piece())
    peers = Sent([xor_swap(packed, "dp", 4, m) for m in (1, 2, 3)])
    out_fc1, out_fc2 = finish_mlp(q, totals, seq.at(swapped.value), n)
    out_fc2 = seq.land(out_fc2, w_spread, peers)
    w_spread.cross()
    seq.land((), w_spread)
    beside, across, opposite_sum = peers.value
    small_sums = (packed + beside) + (across + opposite_sum)
    out_qkv, out_out = finish_attention(seq.value, w_spread.pieces)
    small_out = [small_sums[k, :rows] for k in range(8)]
    out_bfc1 = small_sums[8:12, :ffq].reshape(-1)
    o_bq, o_bv, o_bout, o_gone, o_sone, o_bfc2, o_gtwo, o_stwo = small_out
    return (
        block_out,
        grad_tokens,
        out_qkv,
        o_bq,
        o_bv,
        out_out,
        o_bout,
        o_gone,
        o_sone,
        out_fc1,
        out_bfc1,
        out_fc2,
        o_bfc2,
        o_gtwo,
        o_stwo,
    )


def solution(mesh):
    rows_split = P(("dp", "fsdp"), None)
    matrix = P("fsdp", None)
    vector = P("fsdp")
    return jax.shard_map(
        local,
        mesh=mesh,
        in_specs=(
            rows_split, P(("dp", "fsdp")), matrix, vector, vector, matrix, vector, vector, vector,
            matrix, vector, matrix, vector, vector, vector, rows_split,
        ),
        out_specs=(
            rows_split, rows_split, matrix, vector, vector, matrix, vector, vector, vector,
            matrix, vector, matrix, vector, vector, vector,
        ),
        check_vma=False,
    )
```

```python
import math

import jax
import jax.numpy as jnp
from jax import lax
from jax.experimental import pallas as pl
from jax.experimental.pallas import tpu as pltpu
from jax.sharding import PartitionSpec as P

HEADS = 16
GRID = 14
NSCALE = 16
norm_eps = 1e-06
half = jnp.bfloat16
full = jnp.float32


def xor_swap(value, axis, size, mask):
    return lax.ppermute(value, axis, [(i, i ^ mask) for i in range(size)])


def core_swap(value):
    return xor_swap(value, "dp", 4, 1)


def x_swap(value):
    return xor_swap(value, "dp", 4, 2)


def masks(bits):
    found = [0]
    for bit in bits:
        found = found + [m | (1 << bit) for m in found]
    return found


class Order:
    def __init__(self, value):
        self.value = value

    def at(self, value):
        value, self.value = lax.optimization_barrier((value, self.value))
        return value

    def land(self, value, *sent):
        value, flights = self.at((value, [s.flight for s in sent]))
        for s, flight in zip(sent, flights, strict=True):
            s.accept(flight)
        return value


class Sent:
    def __init__(self, flight):
        self.flight = flight

    def accept(self, value):
        self.value = value


class Gather:
    def __init__(self, seq, piece, n, bits):
        self.seq, self.held, self.n, self.bits = seq, piece[None], n, list(bits)

    def launch(self):
        self.held = self.seq.at(self.held)
        self.flight = xor_swap(self.held, "fsdp", self.n, 1 << self.bits.pop(0))

    def accept(self, value):
        self.got = value

    def join(self):
        self.held = jnp.concatenate([self.held, self.got])
        return self.held


def rounded_sum(terms, kind=half):
    return sum(t.astype(full) for t in terms).astype(kind)


class Reduce:
    def __init__(self, seq, terms, n, kind=half):
        self.kind = kind
        self.seq, self.n, self.axes = seq, n, list(range(n.bit_length() - 1))
        self.terms = [t.reshape((2,) * len(self.axes) + t.shape[1:]) for t in terms]

    def launch(self, bit=None, more=()):
        bit = self.axes[0] if bit is None else bit
        axis = self.axes.index(bit)
        self.axes.pop(axis)
        low, high = [
            [lax.index_in_dim(t, side, axis, keepdims=False) for t in self.terms] for side in (0, 1)
        ]
        self.terms = low
        self.flight = xor_swap(self.seq.at(rounded_sum([*high, *more], self.kind)), "fsdp", self.n, 1 << bit)

    def accept(self, value):
        self.terms = [*self.terms, value]

    def rest(self):
        while self.axes:
            self.launch()
            self.seq.land((), self)
        return self

    def piece(self):
        return rounded_sum(self.terms, self.kind)


class Spread:
    def __init__(self, seq, piece):
        self.seq, self.pieces = seq, [seq.at(piece)]
        self.flight = [core_swap(self.pieces[0]), x_swap(self.pieces[0])]

    def cross(self):
        self.flight = [core_swap(self.seq.at(self.pieces[2]))]

    def accept(self, value):
        self.pieces += value


ANYWHERE = pl.BlockSpec(memory_space=pl.ANY)
ON_CHIP = pl.BlockSpec(memory_space=pltpu.VMEM)
SCALARS = pl.BlockSpec(memory_space=pltpu.SMEM)


def dot(left, right, dim_left, dim_right):
    return lax.dot_general(
        left, right, (((dim_left,), (dim_right,)), ((), ())), preferred_element_type=full
    )


def call(kernel, name, operands, in_specs, outs, out_specs, scratch):
    return pl.pallas_call(
        kernel,
        out_shape=[jax.ShapeDtypeStruct(shape, kind) for shape, kind in outs],
        in_specs=in_specs,
        out_specs=out_specs,
        scratch_shapes=scratch,
        compiler_params=pltpu.CompilerParams(vmem_limit_bytes=58 * 2**20),
        name=name,
    )(*operands)


def loop(count, body, unroll=1):
    def step(i, carry):
        body(i)
        return carry

    lax.fori_loop(0, count, step, 0, unroll=unroll)


def tile(i, size):
    return pl.ds(pl.multiple_of(i * size, size), size)


def bring(src, dst, sem):
    pltpu.make_async_copy(src, dst, sem).start()


def arrived(dst, sem):
    pltpu.make_async_copy(dst, dst, sem).wait()


def fetch(parts, order_ref, place, sem):
    base = 0
    for part in parts:

        def start(r, part=part, base=base):
            shard = r if order_ref is None else order_ref[base + r]
            pltpu.make_async_copy(part.at[r], place(shard), sem).start()

        loop(part.shape[0], start)
        base += part.shape[0]


def head_rows(s, q, n, rows, quarter):
    per = n // 4
    return pl.multiple_of(((s // per) ^ q) * quarter + (s % per) * rows, rows)


def pair_scores(q2, k2):
    first = lax.broadcasted_iota(jnp.int32, q2.shape, 1) < q2.shape[1] // 2
    both = apart(q2, first)
    return both, dot(k2, both, 1, 1), first


def apart(value, first):
    zero = jnp.zeros_like(value)
    return jnp.concatenate([jnp.where(first, value, zero), jnp.where(first, zero, value)])


def attention_forward(order, normed, bias, weights, n_img, patches, factor):
    groups, n_parts = len(weights), len(weights[0])
    wide = weights[0][0].shape[2]
    count, width = normed.shape
    rows = width // sum(part.shape[0] for part in weights[0])
    padded = count // n_img
    quarter = wide // 3

    def kernel(order_ref, normed_ref, bias_ref, *refs):
        w_refs, refs = refs[: groups * n_parts], refs[groups * n_parts :]
        qkv_refs, mixed_refs, refs = refs[:groups], refs[groups : 2 * groups], refs[2 * groups :]
        lse_refs, (w_held, sems) = refs[:groups], refs[groups:]
        for g in range(groups):
            fetch(
                [w.at[:, pl.ds(0, rows)] for w in w_refs[g * n_parts : (g + 1) * n_parts]],
                order_ref,
                lambda s, g=g: w_held.at[g, pl.ds(pl.multiple_of(s * rows, rows), rows)],
                sems.at[g],
            )
        for g in range(groups):
            pltpu.make_async_copy(w_held.at[g], w_held.at[g], sems.at[g]).wait()

            def project(t, g=g):
                at = tile(t, quarter)
                product = dot(normed_ref[...], w_held[g, :, at], 1, 0)
                qkv_refs[g][:, at] = (product + bias_ref[g, :, at]).astype(half)

            loop(3, project)

            def attend(i, g=g):
                at = tile(i // 2, padded)
                lanes = [pl.ds(pl.multiple_of(t * quarter + (i % 2) * 128, 128), 128) for t in range(3)]
                q2 = qkv_refs[g][at, lanes[0]] * factor
                k2 = qkv_refs[g][at, lanes[1]]
                v2 = qkv_refs[g][at, lanes[2]]
                _, scores, first = pair_scores(q2, k2)
                key = lax.broadcasted_iota(jnp.int32, scores.shape, 0)
                scores = jnp.where(key < patches, scores, -1e30)
                top = jnp.max(scores, axis=0, keepdims=True)
                raised = jnp.exp(scores - top)
                total = jnp.sum(raised, axis=0, keepdims=True)
                lse_refs[g][i] = top + jnp.log(total)
                out = dot((raised * (1.0 / total)).astype(half), v2, 0, 0)
                mixed_refs[g][at, lanes[0]] = jnp.where(first, out[:padded], out[padded:]).astype(half)

            loop(2 * n_img, attend, 2 * n_img)

    return call(
        kernel,
        "attention_forward",
        (order, normed, bias, *(part for w in weights for part in w)),
        [SCALARS, ON_CHIP, ON_CHIP] + [ANYWHERE] * (groups * n_parts),
        [((count, wide), half)] * groups
        + [((count, quarter), half)] * groups
        + [((2 * n_img, 1, 2 * padded), full)] * groups,
        [ON_CHIP] * (3 * groups),
        [pltpu.VMEM((groups, width, wide), half), pltpu.SemaphoreType.DMA((groups,))],
    )


def layer_norm(value, gain, shift):
    center = jnp.mean(value, axis=-1, keepdims=True)
    offset = value - center
    spread = jnp.mean(offset * offset, axis=-1, keepdims=True)
    return offset * lax.rsqrt(spread + norm_eps) * gain + shift


def layer_norm_back(value, grad, gain):
    center = jnp.mean(value, axis=-1, keepdims=True)
    offset = value - center
    scale = lax.rsqrt(jnp.mean(offset * offset, axis=-1, keepdims=True) + norm_eps)
    unit = offset * scale
    scaled = grad * gain
    inner = jnp.mean(scaled * unit, axis=-1, keepdims=True)
    return scale * (scaled - jnp.mean(scaled, axis=-1, keepdims=True) - unit * inner), grad * unit


def load_out(order_ref, out_refs, held, sem, n, rows, quarter):
    q = order_ref[n]
    for j in range(4):
        column = pl.multiple_of((q ^ j) * quarter, quarter)
        fetch(
            [out_refs[j % 2].at[:, :, pl.ds(j // 2 * quarter, quarter)]],
            order_ref,
            lambda s, column=column: held.at[
                pl.ds(head_rows(s, q, n, rows, quarter), rows), pl.ds(column, quarter)
            ],
            sem,
        )


CHUNK = 16
ROWS = 64


def attention_out(order, x_zero, mixed, outs, bias, gain, shift):
    count, width = x_zero.shape
    n, rows, _ = outs[0].shape
    quarter = mixed[0].shape[1]

    def kernel(order_ref, x_ref, bias_ref, gain_ref, shift_ref, *refs):
        mixed_refs, out_refs = refs[:4], refs[4:6]
        after_ref, normed_ref, held, x_held, sems = refs[6:]
        bring(x_ref, x_held, sems.at[1])
        load_out(order_ref, out_refs, held, sems.at[0], n, rows, quarter)
        together = jnp.concatenate([m[...] for m in mixed_refs], axis=1)
        pltpu.make_async_copy(held, held, sems.at[0]).wait()
        after_ref[...] = dot(together, held[...], 1, 0)
        arrived(x_held, sems.at[1])

        def finish(i):
            at = tile(i, CHUNK)
            after = x_held[at] + (after_ref[at] + bias_ref[...])
            after_ref[at] = after
            normed_ref[at] = layer_norm(after, gain_ref[...], shift_ref[...]).astype(half)

        loop(count // CHUNK, finish, 13)

    return call(
        kernel,
        "attention_out",
        (order, x_zero, bias, gain, shift, *mixed, *outs),
        [SCALARS, ANYWHERE] + [ON_CHIP] * 7 + [ANYWHERE] * 2,
        [((count, width), full), ((count, width), half)],
        [ON_CHIP] * 2,
        [
            pltpu.VMEM((width, width), half),
            pltpu.VMEM((count, width), full),
            pltpu.SemaphoreType.DMA((2,)),
        ],
    )


def mlp(order, normed, cot, bias, up_all, down_all, down_start, carried=None, ending=None):
    count, width = normed.shape
    n, rows, _ = up_all.shape
    hidden = bias.shape[1]
    share = hidden // n
    step = min(512, hidden)
    steps = hidden // step
    more = [*(carried or []), *(ending[:1] if ending else [])]
    last = list(ending[1:]) if ending else []

    def kernel(order_ref, bias_ref, *refs):
        last_refs, refs = refs[: len(last)], refs[len(last) :]
        normed_ref, cot_ref, up_ref, down_ref, refs = *refs[:4], refs[4:]
        more_refs, refs = refs[: len(more)], refs[len(more) :]
        g_up_ref, g_down_ref, g_bias_ref, back_ref, end_ref, refs = *refs[:5], refs[5:]
        held, refs = refs[: len(more)], refs[len(more) :]
        rows_in, cots, out, back, up, down, pre, act, act_half, pre_half, g_up, g_down, sems = refs
        bring(normed_ref, rows_in, sems.at[3])
        fetch(
            [up_ref.at[:, :, pl.ds(0, hidden)]],
            None,
            lambda s: up.at[pl.ds(pl.multiple_of(s * rows, rows), rows)],
            sems.at[0],
        )
        bring(cot_ref, cots, sems.at[4])
        fetch(
            [down_ref.at[:, :, pl.ds(down_start, width)]],
            None,
            lambda s: down.at[pl.ds(pl.multiple_of(s * share, share), share)],
            sems.at[1],
        )
        for k in range(len(more)):
            bring(more_refs[k], held[k], sems.at[5 + k])
        arrived(rows_in, sems.at[3])
        arrived(up, sems.at[0])
        for t in range(steps):
            at = pl.ds(t * step, step)
            pre[...] = dot(rows_in[...], up[:, at], 1, 0)
            if not t:
                arrived(cots, sems.at[4])
                arrived(down, sems.at[1])
            act[...] = dot(cots[...], down[at, :], 1, 1)

            def gelu(i, at=at):
                some = tile(i, 2 * CHUNK)
                x = pre[some] + bias_ref[:, at]
                below = 0.5 * (1.0 + lax.erf(x * math.sqrt(0.5)))
                density = jnp.exp(-0.5 * x * x) * (1.0 / math.sqrt(2.0 * math.pi))
                act_half[some] = (x * below).astype(half)
                pre_half[some] = (act[some] * (below + x * density)).astype(half)

            loop(count // CHUNK // 2, gelu)
            p = pre_half[...]
            h = act_half[...]
            more_back = dot(p, up[:, at], 1, 1)
            more_out = dot(h, down[at, :], 1, 0)
            if t:
                back[...] += more_back
                out[...] += more_out
            elif carried:
                arrived(held[0], sems.at[5])
                arrived(held[1], sems.at[6])
                out[...] = held[0][...] + more_out
                back[...] = held[1][...] + more_back
            else:
                out[...] = more_out
                back[...] = more_back
            if t == steps - 1:
                bring(back, back_ref, sems.at[3])
                if not ending:
                    bring(out, end_ref, sems.at[4])
            g_down[at, :] = dot(h, cots[...], 0, 0).astype(half)
            if t == steps - 1:

                def send_down(r):
                    at = pl.multiple_of(order_ref[r] * share, share)
                    bring(g_down.at[pl.ds(at, share)], g_down_ref.at[r], sems.at[2])

                loop(n, send_down)
            g_up[:, at] = dot(rows_in[...], p, 0, 0).astype(half)
            g_bias_ref[:, at] = jnp.sum(p.astype(full), axis=0, keepdims=True)

        def send_up(r):
            at = pl.multiple_of(order_ref[r] * rows, rows)
            bring(g_up.at[pl.ds(at, rows)], g_up_ref.at[r], sems.at[0])

        loop(n, send_up)
        if ending:
            arrived(held[2], sems.at[7])

            def finish(i):
                at = tile(i, 2 * CHUNK)
                end_ref[at] = (held[2][at] + (out[at] + last_refs[0][...])).astype(half)

            loop(count // CHUNK // 2, finish)
        else:
            arrived(end_ref, sems.at[4])
        arrived(back_ref, sems.at[3])
        arrived(g_down_ref, sems.at[2])
        arrived(g_up_ref, sems.at[0])

    sums = pltpu.VMEM((count, width), full)
    wide = pltpu.VMEM((count, width), half)
    square = pltpu.VMEM((width, hidden), half)
    return call(
        kernel,
        "mlp",
        (order, bias, *last, normed, cot, up_all, down_all, *more),
        [SCALARS] + [ON_CHIP] * (1 + len(last)) + [ANYWHERE] * (4 + len(more)),
        [
            ((n, rows, hidden), half),
            ((n, share, width), half),
            ((1, hidden), full),
            ((count, width), full),
            ((count, width), half if ending else full),
        ],
        [ANYWHERE, ANYWHERE, ON_CHIP, ANYWHERE, ON_CHIP if ending else ANYWHERE],
        [
            *([sums] * len(more)),
            wide,
            wide,
            sums,
            sums,
            square,
            pltpu.VMEM((hidden, width), half),
            pltpu.VMEM((count, step), full),
            pltpu.VMEM((count, step), full),
            pltpu.VMEM((count, step), half),
            pltpu.VMEM((count, step), half),
            square,
            pltpu.VMEM((hidden, width), half),
            pltpu.SemaphoreType.DMA((5 + len(more),)),
        ],
    )


def attention_out_back(order, grad, after, cot, gain, mixed, outs):
    count, width = after.shape
    n, rows, _ = outs[0].shape
    quarter = mixed[0].shape[1]

    def kernel(order_ref, grad_ref, after_ref, cot_ref, gain_ref, *refs):
        mixed_refs, out_refs, refs = refs[:4], refs[4:6], refs[6:]
        after_grad_ref, mixed_grad_refs, g_out_ref, sums_ref = refs[0], refs[1:5], refs[5], refs[6]
        held, branch, terms, grad, after, cot, mixes, sems = refs[7:]
        block = count // 4
        for k in range(4):
            some = pl.ds(k * block, block)
            bring(grad_ref.at[some], grad.at[some], sems.at[1 + k])
            bring(after_ref.at[some], after.at[some], sems.at[5 + k])
            bring(cot_ref.at[some], cot.at[some], sems.at[9 + k])
        load_out(order_ref, out_refs, held, sems.at[0], n, rows, quarter)
        for j in range(4):
            bring(mixed_refs[j], mixes.at[j], sems.at[13])
        terms[...] = jnp.zeros_like(terms)

        def fold(value):
            return jnp.sum(value.reshape(CHUNK // 8, 8, width), axis=0)

        def back(i, k):
            at = pl.ds(pl.multiple_of(k * block + i * CHUNK, CHUNK), CHUNK)
            incoming = grad[at]
            part, gain_terms = layer_norm_back(after[at], incoming, gain_ref[...])
            own = cot[at].astype(full)
            total = own + part
            after_grad_ref[at] = total
            rounded = total.astype(half)
            branch[at] = rounded
            terms[0] += fold(rounded.astype(full))
            terms[1] += fold(gain_terms)
            terms[2] += fold(incoming)
            terms[3] += fold(own)

        for k in range(4):
            some = pl.ds(k * block, block)
            arrived(grad.at[some], sems.at[1 + k])
            arrived(after.at[some], sems.at[5 + k])
            arrived(cot.at[some], sems.at[9 + k])
            loop(block // CHUNK, lambda i, k=k: back(i, k), 13)
        for k in range(4):
            sums_ref[k] = jnp.sum(terms[k], axis=0, keepdims=True)
        arrived(held, sems.at[0])
        arrived(mixes, sems.at[13])
        for j in range(4):
            mixed_grad_refs[j][...] = dot(branch[...], held[j * quarter : (j + 1) * quarter], 1, 1).astype(half)
            g_out_ref[j * quarter : (j + 1) * quarter] = dot(mixes[j], branch[...], 0, 0).astype(half)

    return call(
        kernel,
        "attention_out_back",
        (order, grad, after, cot, gain, *mixed, *outs),
        [SCALARS] + [ANYWHERE] * 3 + [ON_CHIP] + [ANYWHERE] * 6,
        [((count, width), full)]
        + [((count, quarter), half)] * 4
        + [((width, width), half), ((4, 1, width), full)],
        [ON_CHIP] * 7,
        [
            pltpu.VMEM((width, width), half),
            pltpu.VMEM((count, width), half),
            pltpu.VMEM((4, 8, width), full),
            pltpu.VMEM((count, width), full),
            pltpu.VMEM((count, width), full),
            pltpu.VMEM((count, width), half),
            pltpu.VMEM((4, count, quarter), half),
            pltpu.SemaphoreType.DMA((14,)),
        ],
    )


def attention_back(order, normed, qkvs, lses, mixed_grads, g_out, which, n_img, patches, factor, n):
    groups = len(qkvs)
    count, width = normed.shape
    wide = qkvs[0].shape[1]
    quarter = wide // 3
    padded = count // n_img
    rows = width // n

    def kernel(order_ref, normed_ref, g_out_ref, *refs):
        qkv_refs, mg_refs, refs = refs[:groups], refs[groups : 2 * groups], refs[2 * groups :]
        lse_refs, refs = refs[:groups], refs[groups:]
        g_w_refs, proj_refs, sums_ref = refs[:groups], refs[groups : 2 * groups], refs[2 * groups]
        g_w, normed_held, g_out_held, sems = refs[2 * groups + 1 :]
        q = order_ref[n]
        bring(g_out_ref, g_out_held, sems.at[groups])
        bring(normed_ref, normed_held, sems.at[groups + 1])
        for g in range(groups):

            def attend(i, g=g):
                at = tile(i // 2, padded)
                lanes = [pl.ds(pl.multiple_of(t * quarter + (i % 2) * 128, 128), 128) for t in range(3)]
                q2 = qkv_refs[g][at, lanes[0]] * factor
                k2 = qkv_refs[g][at, lanes[1]]
                v2 = qkv_refs[g][at, lanes[2]]
                both, scores, first = pair_scores(q2, k2)
                key = lax.broadcasted_iota(jnp.int32, scores.shape, 0)
                probs = jnp.where(key < patches, jnp.exp(scores - lse_refs[g][i]), 0.0)
                o_both = apart(mg_refs[g][at, lanes[0]], first)
                g_probs = dot(v2, o_both, 1, 1)
                weighted = jnp.sum(probs * g_probs, axis=0, keepdims=True)
                g_scores = (probs * (g_probs - weighted)).astype(half)
                g_query = dot(g_scores, k2, 0, 0)
                g_query = jnp.where(first, g_query[:padded], g_query[padded:]) * factor
                proj_refs[g][at, lanes[0]] = g_query.astype(half)
                proj_refs[g][at, lanes[1]] = dot(g_scores, both, 1, 0).astype(half)
                proj_refs[g][at, lanes[2]] = dot(probs.astype(half), o_both, 1, 0).astype(half)

            loop(2 * n_img, attend, 4)
            if not g:
                arrived(g_out_held, sems.at[groups])
                arrived(normed_held, sems.at[groups + 1])

            def send_out(r, g=g):
                at = head_rows(order_ref[r], q, n, rows, quarter)
                column = pl.multiple_of((q ^ which[g]) * quarter, quarter)
                pltpu.make_async_copy(
                    g_out_held.at[pl.ds(at, rows), pl.ds(column, quarter)],
                    g_w_refs[g].at[r, :, pl.ds(wide, quarter)],
                    sems.at[g],
                ).start()

            loop(n, send_out)

            def weigh(t, g=g):
                at = tile(t, quarter)
                some = proj_refs[g][:, at]
                g_w[g, :, at] = dot(normed_held[...], some, 0, 0).astype(half)
                sums_ref[g, :, at] = jnp.sum(some.astype(full), axis=0, keepdims=True)

            loop(3, weigh)

            def send(r, g=g):
                at = pl.multiple_of(order_ref[r] * rows, rows)
                pltpu.make_async_copy(
                    g_w.at[g, pl.ds(at, rows)], g_w_refs[g].at[r, :, pl.ds(0, wide)], sems.at[g]
                ).start()

            loop(n, send)
        for g in range(groups):
            pltpu.make_async_copy(g_w_refs[g], g_w_refs[g], sems.at[g]).wait()

    return call(
        kernel,
        "attention_back",
        (order, normed, g_out, *qkvs, *mixed_grads, *lses),
        [SCALARS] + [ANYWHERE] * 2 + [ON_CHIP] * (3 * groups),
        [((n, rows, wide + quarter), half)] * groups
        + [((count, wide), half)] * groups
        + [((groups, 1, wide), full)],
        [ANYWHERE] * groups + [ON_CHIP] * (groups + 1),
        [
            pltpu.VMEM((groups, width, wide), half),
            pltpu.VMEM((count, width), half),
            pltpu.VMEM((width, width), half),
            pltpu.SemaphoreType.DMA((groups + 2,)),
        ],
    )


def input_back(order, x_zero, after_grad, gain, projs, weights):
    count, width = x_zero.shape
    wide = weights[0][0].shape[2]
    rows = width // sum(part.shape[0] for part in weights[0])
    parts = [part for w in weights for part in w]
    n_parts = len(weights[0])

    def kernel(order_ref, x_ref, after_ref, gain_ref, *refs):
        proj_refs, w_refs = refs[:4], refs[4 : 4 + len(parts)]
        token_ref, sums_ref, held, terms, x_held, after_held, sems = refs[4 + len(parts) :]
        for j in range(4):
            fetch(
                [w.at[:, pl.ds(0, rows)] for w in w_refs[j * n_parts : (j + 1) * n_parts]],
                order_ref,
                lambda s, j=j: held.at[j, pl.ds(pl.multiple_of(s * rows, rows), rows)],
                sems.at[j],
            )
        bring(x_ref, x_held, sems.at[4])
        bring(after_ref, after_held, sems.at[5])
        for j in range(4):
            arrived(held.at[j], sems.at[j])
            product = dot(proj_refs[j][...], held[j], 1, 1)
            if j == 0:
                token_ref[...] = product
            else:
                token_ref[...] += product
        arrived(x_held, sems.at[4])
        arrived(after_held, sems.at[5])
        terms[...] = jnp.zeros_like(terms)

        def fold(value):
            return jnp.sum(value.reshape(ROWS // 8, 8, width), axis=0)

        def back(i):
            at = tile(i, ROWS)
            incoming = token_ref[at]
            part, gain_terms = layer_norm_back(x_held[at], incoming, gain_ref[...])
            token_ref[at] = after_held[at] + part
            terms[0] += fold(gain_terms)
            terms[1] += fold(incoming)

        loop(count // ROWS, back)
        for k in range(2):
            sums_ref[k] = jnp.sum(terms[k], axis=0, keepdims=True)

    return call(
        kernel,
        "input_back",
        (order, x_zero, after_grad, gain, *projs, *parts),
        [SCALARS] + [ANYWHERE] * 2 + [ON_CHIP] * 5 + [ANYWHERE] * len(parts),
        [((count, width), full), ((2, 1, width), full)],
        [ON_CHIP] * 2,
        [
            pltpu.VMEM((4, width, wide), half),
            pltpu.VMEM((2, 8, width), full),
            pltpu.VMEM((count, width), full),
            pltpu.VMEM((count, width), full),
            pltpu.SemaphoreType.DMA((6,)),
        ],
    )


def payloads(which, w_fc1, w_fc2):
    rows, ff = w_fc1.shape
    full_share, width = w_fc2.shape
    share = full_share // 4
    n = ff // full_share
    hidden = n * share
    own, across = which
    if share % 128:
        fc1 = [lax.dynamic_slice(w_fc1, (0, (4 * s + own) * share), (rows, share)) for s in range(n)]
        fc2 = [lax.dynamic_slice(w_fc2, (g * share, 0), (share, width)).astype(half) for g in which]
        rest = jnp.concatenate([*fc1, fc2[0].reshape(rows, -1).astype(full)], axis=1)
        return rest.astype(half), fc2[1]

    def kernel(which_ref, fc1_ref, fc2_ref, rest_ref, two_ref):
        for s in range(n):
            at = pl.ds(pl.multiple_of((4 * s + which_ref[0]) * share, share), share)
            rest_ref[:, s * share : (s + 1) * share] = fc1_ref[:, at].astype(half)
        rest_ref[:, hidden : hidden + width] = fc2_ref[tile(which_ref[0], share), :].astype(half)
        two_ref[...] = fc2_ref[tile(which_ref[1], share), :].astype(half)

    return call(
        kernel,
        "payloads",
        (jnp.stack(which), w_fc1, w_fc2),
        [SCALARS] + [ON_CHIP] * 2,
        [((rows, hidden + width), half), ((share, width), half)],
        [ON_CHIP] * 2,
        [],
    )


def natural_quarters(q, pieces):
    once = [jnp.where((q & 1) == 1, pieces[i ^ 1], pieces[i]) for i in range(4)]
    return [jnp.where(q >= 2, once[i ^ 2], once[i]) for i in range(4)]


def finish_mlp(q, totals, swapped, n):
    _, _, rows, width = totals.shape
    share = width // n
    if share % 128:
        pieces = natural_quarters(q, [totals[0], swapped[0], totals[1], swapped[1]])
        fc1 = jnp.stack([p[0].reshape(rows, n, share) for p in pieces], axis=2).reshape(rows, 4 * width)
        return fc1.astype(full), jnp.concatenate([p[1] for p in pieces]).astype(full)

    def kernel(q_ref, *refs):
        fc1_ref, fc2_ref = refs[2:]
        for j in range(4):
            g = q_ref[0] ^ j
            held = refs[j % 2].at[j // 2]
            for s in range(n):
                at = pl.ds(pl.multiple_of((4 * s + g) * share, share), share)
                fc1_ref[:, at] = held[0, :, s * share : (s + 1) * share].astype(full)
            fc2_ref[tile(g, rows), :] = held[1].astype(full)

    return call(
        kernel,
        "finish_mlp",
        (q[None], totals, swapped),
        [SCALARS] + [ON_CHIP] * 2,
        [((rows, 4 * width), full), ((4 * rows, width), full)],
        [ON_CHIP] * 2,
        [],
    )


def finish_attention(q, pieces):
    rows, width = pieces[0].shape
    quarter = width // 4

    def kernel(q_ref, *refs):
        qkv_ref, out_ref = refs[4:]
        for j in range(4):
            g = q_ref[0] ^ j
            for t in range(3):
                at = pl.ds(pl.multiple_of(t * width + g * quarter, quarter), quarter)
                qkv_ref[:, at] = refs[j][:, t * quarter : (t + 1) * quarter].astype(full)
            out_ref[:, tile(g, quarter)] = refs[j][:, 3 * quarter :].astype(full)

    return call(
        kernel,
        "finish_attention",
        (q[None], *pieces),
        [SCALARS] + [ON_CHIP] * 4,
        [((rows, 3 * width), full), ((rows, width), full)],
        [ON_CHIP] * 2,
        [],
    )


BELOW = 16


def first_payload(q, w_qkv, vectors):
    rows, columns = w_qkv.shape
    width = columns // 3
    quarter = width // 4
    wide = 3 * quarter

    def kernel(q_ref, w_ref, *refs):
        out_ref, held, low, sem = refs[len(vectors) :]
        for t in range(3):
            at = pl.multiple_of(t * width + q_ref[0] * quarter, quarter)
            pltpu.make_async_copy(
                w_ref.at[:, pl.ds(at, quarter)], held.at[:, pl.ds(t * quarter, quarter)], sem.at[0]
            ).start()
        low[...] = jnp.zeros_like(low)
        for k, vector in enumerate(refs[: len(vectors)]):
            low[k : k + 1, : vector.shape[1]] = vector[...]
        out_ref[rows:] = low[...].astype(half)
        pltpu.make_async_copy(held, held, sem.at[0]).wait()
        out_ref[:rows] = held[...].astype(half)

    return call(
        kernel,
        "first_payload",
        (q[None], w_qkv, *(v[None] for v in vectors)),
        [SCALARS, ANYWHERE] + [ON_CHIP] * len(vectors),
        [((rows + BELOW, wide), half)],
        [ON_CHIP],
        [pltpu.VMEM((rows, wide), full), pltpu.VMEM((BELOW, wide), full), pltpu.SemaphoreType.DMA((1,))],
    )[0]


def unpack_vectors(order, parts, n, rows, share):
    width = n * rows
    quarter = width // 4
    if rows % 128 or share % 128:
        q = order[n]
        held = jnp.concatenate([p[:, rows:] for p in parts]).astype(full)
        held = held[jnp.zeros((n,), jnp.int32).at[order[:n]].set(jnp.arange(n, dtype=jnp.int32))]
        groups = jnp.arange(4, dtype=jnp.int32) ^ q
        vectors = jnp.stack([held[:, k, :rows].reshape(1, width) for k in range(8)])
        units = held[:, 8, : 4 * share].reshape(n, 4, share).transpose(1, 0, 2)[groups]
        ends = [vectors[k].reshape(4, 1, quarter)[groups] for k in range(2)]
        return vectors, units.reshape(4, 1, width), jnp.concatenate([ends[0], 0 * ends[0], ends[1]], axis=2)

    def kernel(order_ref, *refs):
        part_refs, (vector_ref, fc1_ref, qkv_ref, held, wider, sem) = refs[: len(parts)], refs[len(parts) :]
        base = 0
        for part in part_refs:
            size = part.shape[0]
            pltpu.make_async_copy(part.at[:, pl.ds(rows, BELOW)], held.at[pl.ds(base, size)], sem.at[0]).start()
            base += size
        pltpu.make_async_copy(held, held, sem.at[0]).wait()
        wider[...] = held[...].astype(full)
        q = order_ref[n]
        for r in range(n):
            at = tile(order_ref[r], rows)
            for k in range(8):
                vector_ref[k, :, at] = wider[r, k : k + 1, :rows]
            for j in range(4):
                fc1_ref[j, :, tile(order_ref[r], share)] = wider[r, 8:9, tile(q ^ j, share)]
        for j in range(4):
            at = tile(q ^ j, quarter)
            qkv_ref[j, :, :quarter] = vector_ref[0, :, at]
            qkv_ref[j, :, quarter : 2 * quarter] = jnp.zeros((1, quarter), full)
            qkv_ref[j, :, 2 * quarter :] = vector_ref[1, :, at]

    return call(
        kernel,
        "unpack_vectors",
        (order, *parts),
        [SCALARS] + [ANYWHERE] * len(parts),
        [((8, 1, width), full), ((4, 1, width), full), ((4, 1, 3 * quarter), full)],
        [ON_CHIP] * 3,
        [
            pltpu.VMEM((n, BELOW, 3 * quarter), half),
            pltpu.VMEM((n, BELOW, 3 * quarter), full),
            pltpu.SemaphoreType.DMA((1,)),
        ],
    )


def pack_sums(order, n, rows, share, proj_sums, unit_sums, wide_sums):
    width = n * rows
    quarter = width // 4
    if rows % 128 or share % 128:
        groups = jnp.arange(4, dtype=jnp.int32) ^ order[n]
        proj = jnp.concatenate(proj_sums)[groups]
        units = jnp.concatenate(unit_sums)[groups].reshape(4, n, share)
        flat = [proj[:, :, :quarter].reshape(width), proj[:, :, 2 * quarter :].reshape(width)]
        two, one = wide_sums
        flat += [two[0], one[0], one[1], two[3], two[1], two[2]]
        flat = [v.reshape(n, 1, rows) for v in flat]
        stacked = [jnp.pad(v, ((0, 0), (0, 0), (0, 128 - rows))) for v in flat]
        stacked.append(jnp.pad(units.transpose(1, 0, 2), ((0, 0), (0, 4), (0, 128 - share))))
        return jnp.concatenate(stacked, axis=1)[order[:n]]

    def kernel(order_ref, proj_a, proj_b, unit_a, unit_b, two_ref, one_ref, out_ref, proj, units):
        proj[:2], proj[2:] = proj_a[...], proj_b[...]
        units[:2], units[2:] = unit_a[...], unit_b[...]
        q = order_ref[n]
        per = n // 4
        for r in range(n):
            s = order_ref[r]
            j = (s // per) ^ q
            at = tile(s, rows)
            inside = pl.multiple_of((s % per) * rows, rows)
            out_ref[r, 0:1] = proj[j, :, pl.ds(inside, rows)]
            out_ref[r, 1:2] = proj[j, :, pl.ds(2 * quarter + inside, rows)]
            for k, (ref, row) in enumerate(
                ((two_ref, 0), (one_ref, 0), (one_ref, 1), (two_ref, 3), (two_ref, 1), (two_ref, 2))
            ):
                out_ref[r, 2 + k : 3 + k] = ref[row, :, at]
            for g in range(4):
                out_ref[r, 8 + g : 9 + g] = units[q ^ g, :, tile(s, share)]
            out_ref[r, 12:] = jnp.zeros((4, rows), full)

    sums_two, sums_one = wide_sums
    return call(
        kernel,
        "pack_sums",
        (order, *proj_sums, *unit_sums, sums_two, sums_one),
        [SCALARS] + [ON_CHIP] * 6,
        [((n, 16, rows), full)],
        [ON_CHIP],
        [pltpu.VMEM((4, 1, 3 * quarter), full), pltpu.VMEM((4, 1, width), full)],
    )[0]


def table(codes, width):
    ratio = 0.3 * jnp.exp(codes.astype(full) * (math.log(10.0 / 0.3) / (NSCALE - 1)))
    quarter = width // 4
    omega = jnp.exp(jnp.arange(quarter).astype(full) * (-math.log(10000.0) / quarter))
    steps = jnp.arange(GRID, dtype=jnp.int32).astype(full)
    angle = ratio[:, None, None] * steps[None, :, None] * omega[None, None, :]
    return jnp.concatenate([jnp.sin(angle), jnp.cos(angle)], axis=-1)


def local(
    tokens,
    scale_codes,
    w_qkv,
    b_q,
    b_v,
    w_out,
    b_out,
    gain_one,
    shift_one,
    w_fc1,
    b_fc1,
    w_fc2,
    b_fc2,
    gain_two,
    shift_two,
    cotangent,
):
    n = lax.axis_size("fsdp")
    q = lax.axis_index("dp")
    f = lax.axis_index("fsdp")
    row_count, width = tokens.shape
    rows = width // n
    ff = b_fc1.shape[0] * n
    ffq = ff // n // 4
    hidden = n * ffq
    quarter = width // 4
    n_img = scale_codes.shape[0]
    patches = row_count // n_img
    padded = -(-patches // 16) * 16
    factor = 1.0 / math.sqrt(width // HEADS)
    seq = Order(q)
    bits = list(reversed(range(n.bit_length() - 1)))
    near = min(1, len(bits) - 1)
    shard_order = jnp.asarray(masks(bits), jnp.int32) ^ f
    group_order = jnp.arange(4, dtype=jnp.int32) ^ q
    order = jnp.concatenate([shard_order, q[None]])

    def last_three(chain):
        while len(chain.bits) > 3:
            chain.launch()
            seq.land((), chain)
            chain.join()
        return chain

    small = [b_q, b_v, b_out, gain_one, shift_one, b_fc2, gain_two, shift_two, b_fc1]
    qkv = last_three(Gather(seq, first_payload(q, w_qkv, small), n, bits))
    qkv.launch()
    rest_own, two_own = payloads([seq.at(q), q ^ 2], w_fc1, w_fc2)
    rest_own, two_own = seq.land((rest_own, two_own), qkv)
    rest = Sent(lax.all_gather(rest_own, "fsdp", axis=0, tiled=False))
    two = Sent(lax.all_gather(two_own, "fsdp", axis=0, tiled=False))
    out_own = [lax.dynamic_slice(w_out, (0, g * quarter), (rows, quarter)) for g in (q, q ^ 2)]
    out = last_three(Gather(seq, jnp.concatenate(out_own, axis=1).astype(half), n, bits))

    def spread_rows(value):
        split = value.reshape(n_img, patches, width)
        return jnp.pad(split, ((0, 0), (0, padded - patches), (0, 0)))

    def compact(value):
        return value.reshape(n_img, padded, width)[:, :patches].reshape(row_count, width)

    qkv.join()
    qkv.launch()
    spread_tokens = seq.land(spread_rows(seq.at(tokens)), qkv)
    qkv_near = qkv.join()
    qkv.launch()
    near_b, near_c = Sent(core_swap(qkv.held)), Sent(x_swap(qkv.held))
    out.launch()
    places = table(scale_codes, width)
    row_place = jnp.broadcast_to(places[:, :, None], (n_img, GRID, GRID, width // 2))
    col_place = jnp.broadcast_to(places[:, None], (n_img, GRID, GRID, width // 2))
    place = jnp.concatenate([row_place, col_place], axis=-1).reshape(n_img, patches, width)
    place = jnp.pad(place, ((0, 0), (0, padded - patches), (0, 0)))
    x_zero = (seq.at(spread_tokens).astype(full) + place).reshape(-1, width)
    x_zero = seq.land(x_zero, qkv, near_b, out)
    qkv_far = seq.at(qkv.got)
    far_b, far_c = Sent(core_swap(qkv_far)), Sent(x_swap(qkv_far))
    out.join()
    out.launch()
    vectors, bias_fc1, bias_qkv = unpack_vectors(seq.at(order), (qkv_near, qkv_far), n, rows, ffq)
    _, _, full_bout, gain_one_f, shift_one_f, full_bfc2, gain_two_f, shift_two_f = vectors
    normed_one = layer_norm(x_zero, gain_one_f, shift_one_f).astype(half)
    normed_one = seq.land(normed_one, far_b)

    first = attention_forward(
        seq.at(order), normed_one, bias_qkv[:2], ((qkv_near, qkv_far), (near_b.value, far_b.value)),
        n_img, patches, factor,
    )
    first = (seq.land(first[0], near_c, far_c, out), *first[1:])
    near_c, far_c = seq.at((near_c.value, far_c.value))
    near_d, far_d = Sent(core_swap(near_c)), Sent(core_swap(far_c))
    out.join()
    out.launch()
    cot = seq.land(spread_rows(cotangent).reshape(-1, width), near_d, far_d)
    second = attention_forward(
        seq.at(order), normed_one, bias_qkv[2:], ((near_c, far_c), (near_d.value, far_d.value)),
        n_img, patches, factor,
    )
    second = (seq.land(second[0], out, rest), *second[1:])
    out_a = seq.at(out.join())
    out_b = Sent(core_swap(out_a))
    seq.land((), out_b)
    rest_a = seq.at(rest.value)
    rest_b = Sent(core_swap(rest_a))
    up_c = Sent(x_swap(seq.at(rest_a[:, :, :hidden])))
    outs = (out_a, out_b.value)
    qkv_parts = (
        (qkv_near, qkv_far), (near_b.value, far_b.value), (near_c, far_c), (near_d.value, far_d.value)
    )
    qkvs = (*first[:2], *second[:2])
    mixed = (*first[2:4], *second[2:4])
    lses = (*first[4:], *second[4:])
    after_attn, normed_two = attention_out(
        seq.at(order), x_zero, mixed, outs, full_bout, gain_two_f, shift_two_f
    )
    normed_two = seq.land(normed_two, rest_b)

    up_g1, down_g1, g_bias_1, back_sum, out_sum = mlp(
        seq.at(order), normed_two, cot, bias_fc1[1], rest_b.value, rest_b.value, hidden
    )
    up_g0, down_g0, g_bias_0, back_sum, out_sum = mlp(
        order, normed_two, cot, bias_fc1[0], rest_a, rest_a, hidden, (out_sum, back_sum)
    )
    up_g0 = seq.land(up_g0, up_c, two)
    up_g1 = seq.at(up_g1)
    up_got = Sent(core_swap(up_g1))
    down_g1 = seq.at(down_g1)
    down_got = Sent(core_swap(down_g1))
    seq.land((), up_got)
    red_up = Reduce(seq, (up_g0, up_got.value), n)
    red_up.launch()
    seq.land((), down_got)
    red_down = Reduce(seq, (down_g0, down_got.value), n)
    red_down.launch(near)
    up_c, two = seq.at((up_c.value, two.value))
    up_d, two_d = Sent(core_swap(up_c)), Sent(core_swap(two))
    up_g2, down_g2, g_bias_2, back_sum, out_sum = mlp(
        seq.at(order), normed_two, cot, bias_fc1[2], up_c, two, 0, (out_sum, back_sum)
    )
    up_g2 = seq.land(up_g2, up_d, two_d, red_up, red_down)
    red_up.launch()
    red_down.launch()
    up_g3, down_g3, g_bias_3, grad_two_in, block = mlp(
        seq.at(order), normed_two, cot, bias_fc1[3], up_d.value, two_d.value, 0,
        (out_sum, back_sum), (after_attn, full_bfc2),
    )
    up_g3 = seq.land(up_g3, red_up, red_down)
    up_got = Sent(core_swap(up_g3))
    down_g3 = seq.at(down_g3)
    down_got = Sent(core_swap(down_g3))
    red_up.launch()
    red_down.launch()
    seq.land((), up_got)
    two_up = Reduce(seq, (up_g2, up_got.value), n)
    two_up.launch()
    seq.land((), down_got)
    two_down = Reduce(seq, (down_g2, down_got.value), n)
    two_down.launch(near)

    after_grad, mg0, mg1, mg2, mg3, g_out, sums_two = attention_out_back(
        seq.at(order), grad_two_in, after_attn, cot, gain_two_f, mixed, outs
    )
    mg2 = seq.at(mg2)
    g_w2, g_w3, proj2, proj3, sums_b = attention_back(
        seq.at(order), normed_one, qkvs[2:], lses[2:], (mg2, mg3), g_out, (2, 3), n_img, patches, factor, n
    )
    g_w3 = seq.land(g_w3, red_up, red_down, two_up, two_down)
    w_3 = Sent(core_swap(g_w3))
    two_up.launch()
    two_down.launch()
    seq.land((), w_3)
    middle = n // 2
    half_shape = (2,) * (len(bits) - 1)
    w_high = Sent(x_swap(seq.at(rounded_sum([g_w2[middle:], w_3.value[middle:]]))))
    g_w0, g_w1, proj0, proj1, sums_a = attention_back(
        seq.at(order), normed_one, qkvs[:2], lses[:2], (mg0, mg1), g_out, (0, 1), n_img, patches, factor, n
    )
    g_w1 = seq.land(g_w1, two_up, two_down, w_high)
    w_1 = Sent(core_swap(g_w1))
    two_up.launch()
    two_down.launch()
    seq.land((), w_1)
    red_w = Reduce(seq, (g_w0, w_1.value), n)
    red_w.launch(0, [w_high.value.reshape(half_shape + w_high.value.shape[1:])])
    w_low = Sent(x_swap(seq.at(rounded_sum([g_w2[:middle], w_3.value[:middle]]))))
    tokens_grad, sums_one = input_back(
        seq.at(order), x_zero, after_grad, gain_one_f, (proj0, proj1, proj2, proj3), qkv_parts
    )
    sums_one = seq.land(sums_one, two_up, two_down, red_w, w_low)
    red_w.terms = [*red_w.terms, w_low.value.reshape(half_shape + w_low.value.shape[1:])]
    while len(red_w.axes) > 2:
        red_w.launch()
        seq.land((), red_w)
    red_w.launch()
    packed = pack_sums(
        seq.at(order),
        n,
        rows,
        ffq,
        (sums_a, sums_b),
        (jnp.stack([g_bias_0, g_bias_1]), jnp.stack([g_bias_2, g_bias_3])),
        (sums_two, sums_one),
    )
    sums = Reduce(seq, (packed,), n, full)
    while len(sums.axes) > 3:
        sums.launch()
        seq.land((), sums)
    sums.launch()
    own_part = jnp.stack([red_up.rest().piece(), red_down.rest().piece()])
    across_part = jnp.stack([two_up.rest().piece(), two_down.rest().piece()])
    pair = seq.at(jnp.stack([own_part, across_part]))
    cross = Sent(x_swap(pair))
    seq.land((), red_w, sums)
    red_w.launch()
    sums.launch()
    block, tokens_grad = seq.at((block, tokens_grad))
    block_out, grad_tokens = seq.land((compact(block), compact(tokens_grad)), sums, red_w)
    w_spread = Spread(seq, red_w.piece())
    sums.launch()
    seq.land((), cross)
    totals = jnp.stack([rounded_sum([pair[0], cross.value[1]]), rounded_sum([pair[1], cross.value[0]])])
    totals = seq.at(totals)
    swapped = Sent(core_swap(totals))
    seq.land((), sums, swapped)
    packed = seq.at(sums.piece())
    peers = Sent([xor_swap(packed, "dp", 4, m) for m in (1, 2, 3)])
    out_fc1, out_fc2 = finish_mlp(q, totals, seq.at(swapped.value), n)
    out_fc2 = seq.land(out_fc2, w_spread, peers)
    w_spread.cross()
    seq.land((), w_spread)
    beside, across, opposite_sum = peers.value
    small_sums = (packed + beside) + (across + opposite_sum)
    out_qkv, out_out = finish_attention(seq.value, w_spread.pieces)
    small_out = [small_sums[k, :rows] for k in range(8)]
    out_bfc1 = small_sums[8:12, :ffq].reshape(-1)
    o_bq, o_bv, o_bout, o_gone, o_sone, o_bfc2, o_gtwo, o_stwo = small_out
    return (
        block_out,
        grad_tokens,
        out_qkv,
        o_bq,
        o_bv,
        out_out,
        o_bout,
        o_gone,
        o_sone,
        out_fc1,
        out_bfc1,
        out_fc2,
        o_bfc2,
        o_gtwo,
        o_stwo,
    )


def solution(mesh):
    rows_split = P(("dp", "fsdp"), None)
    matrix = P("fsdp", None)
    vector = P("fsdp")
    return jax.shard_map(
        local,
        mesh=mesh,
        in_specs=(
            rows_split, P(("dp", "fsdp")), matrix, vector, vector, matrix, vector, vector, vector,
            matrix, vector, matrix, vector, vector, vector, rows_split,
        ),
        out_specs=(
            rows_split, rows_split, matrix, vector, vector, matrix, vector, vector, vector,
            matrix, vector, matrix, vector, vector, vector,
        ),
        check_vma=False,
    )
```
